256 devices in a mesh: rep: 2 (over y), ep: 128 (over x, z, core).
Axes of the slice: x: 4, y: 2, z: 16, core: 2. Of those that a mesh axis runs over, the one named last changes fastest.
The devices are a block of a 4x16x16 slice.
Arguments:
- cache_kv: bfloat16 [512, 2048, 576], P(('rep', 'ep')), parts along dimension 0, may hold values from -6 to 6
- new_kv: bfloat16 [512, 2, 576], P(('rep', 'ep')), parts along dimension 0, may hold values from -6 to 6
- queries: bfloat16 [512, 2, 64, 576], P(('rep', 'ep')), parts along dimension 0, may hold values from -256 to 256
- lengths: int32 [512], P(('rep', 'ep')), parts along dimension 0, may hold values from 256 to 2048
- resid: bfloat16 [512, 2, 7168], P(('rep', 'ep')), parts along dimension 0, may hold values from -18 to 18
- value_up: bfloat16 [512, 8192], P(None, 'ep'), may hold values from -1.5 to 1.5
- out_proj: bfloat16 [8192, 7168], P('ep'), may hold values from -0.09375 to 0.09375
- norm_gain: bfloat16 [7168], replicated, may hold values from 0.25 to 1.75
- router: bfloat16 [7168, 16], replicated, may hold values from -0.0625 to 0.0625
- expert_ids: int32 [512, 2, 8], P(('rep', 'ep')), parts along dimension 0, may hold values from 0 to 15, as said below
- slots: int32 [512, 2, 8], P(('rep', 'ep')), parts along dimension 0, may hold values from 0 to 3, as said below
- w_gate: bfloat16 [7168, 16384], P(None, 'ep'), may hold values from -0.0625 to 0.0625
- w_up: bfloat16 [7168, 16384], P(None, 'ep'), may hold values from -0.0625 to 0.0625
- w_down: bfloat16 [16384, 7168], P('ep'), may hold values from -0.1875 to 0.1875
Outputs:
- mixed: bfloat16 [512, 2, 7168], P(('rep', 'ep')), parts along dimension 0
The draws below stay inside these ranges and needn't reach their ends.
There are 2 independent parts, one for each index of `rep`. The reference program is written for one: setup_inputs(seed, part) draws one part's arguments, and reference() takes and returns one part's arrays. A program takes and returns all parts, laid end to end along the dimension named above; an argument that names none is the same for every part. Nothing has to cross between parts.
Inputs may be any that keep to these rules, and one draw needn't show every extreme that they name: `expert_ids`: each row names 8 different experts. In each aligned block of 4 rows (the rows of one device), the rows that name the same expert carry the distinct slots 0 up to their number minus one for it; in every block some expert is named by all 4 rows.
All inputs are finite; a program needn't handle non-finite values.
Results may differ from the reference program's by a relative error of at most 0.0065.
Values may be sent and summed in bfloat16 or wider, within the bound.
No kernel may reach another device: no remote copies, remote signals or barrier semaphores. Data moves between devices by JAX's collectives and lax.ppermute only.
A program may use at most 128 MiB of HBM per device.

```python
import jax
import jax.numpy as jnp
from jax import lax

D = 7168
H = 64
LAT = 512
VH = 128
FFW = 1024
EXPERTS = 16
TOP = 8
CAP = 2
STEPS = 2
CACHE = 2048
KV = 576
QK = 192
TOK_DEV = 4
BATCH = 256
N_EP = 128


def attention_pair(key):
    cache_part = jax.random.truncated_normal(jax.random.fold_in(key, 21), -6.0, 6.0, (BATCH, CACHE, KV), jnp.float32)
    query_part = jax.random.truncated_normal(jax.random.fold_in(key, 22), -6.0, 6.0, (BATCH, STEPS, H, KV), jnp.float32)
    return (cache_part, query_part)


def draw_cache_kv(key, part):
    return attention_pair(key)[0].astype(jnp.bfloat16)


def draw_queries(key, part):
    return attention_pair(key)[1].astype(jnp.bfloat16)


def draw_resid(key, part):
    columns = jnp.exp(jax.random.uniform(jax.random.fold_in(key, 31), (D,), jnp.float32, jnp.log(0.3), jnp.log(3.0)))
    base = jax.random.truncated_normal(jax.random.fold_in(key, 34), -6.0, 6.0, (BATCH, STEPS, D), jnp.float32)
    return (base * columns).astype(jnp.bfloat16)


def routing_pair(key):
    rows_all = BATCH * STEPS
    blocks = rows_all // TOK_DEV
    expert_range = jnp.arange(EXPERTS, dtype=jnp.int32)
    base = jax.random.randint(jax.random.fold_in(key, 41), (rows_all, EXPERTS), 0, 1 << 20)
    order = jax.random.permutation(jax.random.fold_in(key, 42), EXPERTS).astype(jnp.int32)
    forced = jax.random.randint(jax.random.fold_in(key, 43), (blocks,), 0, EXPERTS)
    forced_rows = jnp.repeat(forced, TOK_DEV)
    boost = jnp.where(expert_range[None, :] == forced_rows[:, None], 1 << 24, 0)
    scores = (base + order[None, :] * (1 << 16) + boost) * EXPERTS + expert_range[None, :]
    _, chosen = lax.top_k(scores, TOP)
    chosen = chosen.astype(jnp.int32)
    row_in_block = jnp.arange(rows_all, dtype=jnp.int32) % TOK_DEV
    priority = jax.random.randint(jax.random.fold_in(key, 44), (rows_all, EXPERTS), 0, 1 << 20) * TOK_DEV + row_in_block[:, None]
    named = jnp.any(chosen[:, :, None] == expert_range[None, None, :], axis=1)
    named_block = named.reshape(blocks, TOK_DEV, EXPERTS)
    priority_block = priority.reshape(blocks, TOK_DEV, EXPERTS)
    earlier = named_block[:, None, :, :] & (priority_block[:, None, :, :] < priority_block[:, :, None, :])
    rank = jnp.sum(earlier.astype(jnp.int32), axis=2).reshape(rows_all, EXPERTS)
    slot_values = jnp.take_along_axis(rank, chosen, axis=1)
    return (chosen.reshape(BATCH, STEPS, TOP), slot_values.reshape(BATCH, STEPS, TOP))


def draw_expert_ids(key, part):
    return routing_pair(key)[0]


def draw_slots(key, part):
    return routing_pair(key)[1]


def set_ends(drawn, rng, least, high):
    longest = drawn.shape.index(max(drawn.shape))
    spots = []
    for shift in (0, 1):
        where = [jax.random.randint(jax.random.fold_in(rng, axis), (), 0, length) for axis, length in enumerate(drawn.shape)]
        where[longest] = (where[longest] + shift) % drawn.shape[longest]
        spots.append(tuple(where))
    return drawn.at[spots[0]].set(least).at[spots[1]].set(high)


def steps_of(rng, extent, cuts, smallest, top_value):
    factor_of, own = 1.0, jax.random.fold_in(rng, 6)
    for position, blocks in cuts:
        steps = jnp.exp(jax.random.uniform(jax.random.fold_in(own, position), (blocks,), jnp.float32, smallest / len(cuts), top_value / len(cuts)))
        factor_of = factor_of * jnp.repeat(steps, extent[position] // blocks).reshape([-1 if axis == position else 1 for axis in range(len(extent))])
    return factor_of


def normal_values(own_key, dims, deviation, bound, pieces=(), held_as=jnp.bfloat16):
    loudness = steps_of(own_key, dims, pieces, -0.22, 0.18) if pieces else 1.0
    values = jax.random.normal(own_key, dims, jnp.float32) * deviation * loudness
    return jnp.minimum(jnp.maximum(values, -bound), bound).astype(held_as)


def setup_inputs(seed: int = 0, part: int = 0) -> dict:
    key_list = jax.random.split(jax.random.key(seed), 15)
    part_splits = jax.random.split(jax.random.fold_in(key_list[14], part), 15)
    cache_kv = draw_cache_kv(jax.random.fold_in(jax.random.fold_in(key_list[14], part), 71), part)
    new_kv = normal_values(part_splits[1], (BATCH, STEPS, KV), 1.0, 6.0, ((0, 128),))
    queries = draw_queries(jax.random.fold_in(jax.random.fold_in(key_list[14], part), 71), part)
    lengths = set_ends(jax.random.randint(part_splits[3], (BATCH,), CACHE // 8, CACHE + 1), jax.random.fold_in(part_splits[3], 1), CACHE // 8, CACHE).astype(jnp.int32)
    resid = draw_resid(jax.random.fold_in(jax.random.fold_in(key_list[14], part), 71), part)
    value_up = normal_values(key_list[5], (LAT, H * VH), (max(1, LAT // 32)) ** -0.5, 1.5, ((1, 128),))
    out_proj = normal_values(key_list[6], (H * VH, D), (H * VH // 2) ** -0.5, 0.09375, ((0, 128),))
    norm_gain = jnp.clip(1.0 + 0.15 * jax.random.normal(key_list[7], (D,), jnp.float32), 0.25, 1.75).astype(jnp.bfloat16)
    router = normal_values(key_list[8], (D, EXPERTS), D ** -0.5, 0.0625)
    expert_ids = draw_expert_ids(jax.random.fold_in(jax.random.fold_in(key_list[14], part), 71), part)
    slots = draw_slots(jax.random.fold_in(jax.random.fold_in(key_list[14], part), 71), part)
    w_gate = normal_values(key_list[11], (D, EXPERTS * FFW), D ** -0.5, 0.0625, ((1, 128),))
    w_up = normal_values(key_list[12], (D, EXPERTS * FFW), D ** -0.5, 0.0625, ((1, 128),))
    w_down = normal_values(key_list[13], (EXPERTS * FFW, D), FFW ** -0.5, 0.1875, ((0, 128),))
    return dict(cache_kv=cache_kv, new_kv=new_kv, queries=queries, lengths=lengths, resid=resid, value_up=value_up, out_proj=out_proj, norm_gain=norm_gain, router=router, expert_ids=expert_ids, slots=slots, w_gate=w_gate, w_up=w_up, w_down=w_down)


route_scale = 2.827
norm_eps = 1e-06

def attend_one(packed):
    cache_rows, new_rows, query_rows, length = packed
    score_scale = 1.0 / QK ** 0.5
    query_full = query_rows.astype(jnp.float32)
    cache_full = cache_rows.astype(jnp.float32)
    new_full = new_rows.astype(jnp.float32)
    score_cache = jnp.einsum('shk,pk->shp', query_full, cache_full) * score_scale
    is_live = jnp.arange(CACHE, dtype=jnp.int32) < length
    score_cache = jnp.where(is_live[None, None, :], score_cache, -jnp.inf)
    score_new = jnp.einsum('shk,tk->sht', query_full, new_full) * score_scale
    step_ids = jnp.arange(STEPS, dtype=jnp.int32)
    causal = step_ids[None, :] <= step_ids[:, None]
    score_new = jnp.where(causal[:, None, :], score_new, -jnp.inf)
    row_peak = jnp.maximum(lax.optimization_barrier(jnp.max(score_cache, axis=-1)), lax.optimization_barrier(jnp.max(score_new, axis=-1)))
    exp_cache = jnp.exp(score_cache - row_peak[..., None])
    exp_new = jnp.exp(score_new - row_peak[..., None])
    exp_total = lax.optimization_barrier(jnp.sum(exp_cache, axis=-1)) + lax.optimization_barrier(jnp.sum(exp_new, axis=-1))
    prob_cache = (exp_cache / exp_total[..., None]).astype(jnp.bfloat16)
    prob_new = (exp_new / exp_total[..., None]).astype(jnp.bfloat16)
    context = jnp.einsum('shp,pc->shc', prob_cache.astype(jnp.float32), cache_full[:, :LAT])
    context = context + jnp.einsum('sht,tc->shc', prob_new.astype(jnp.float32), new_full[:, :LAT])
    return context.astype(jnp.bfloat16)

def reference(cache_kv, new_kv, queries, lengths, resid, value_up, out_proj, norm_gain, router, expert_ids, slots, w_gate, w_up, w_down):
    contexts = lax.map(attend_one, (cache_kv, new_kv, queries, lengths))
    values = jnp.einsum('bshc,chv->bshv', contexts.astype(jnp.float32), value_up.reshape(LAT, H, VH).astype(jnp.float32)).astype(jnp.bfloat16)
    rows_all = BATCH * STEPS
    attended = jnp.dot(values.reshape(rows_all, H * VH), out_proj, preferred_element_type=jnp.float32)
    hidden = resid.reshape(rows_all, D).astype(jnp.float32) + attended
    mean_square = lax.optimization_barrier(jnp.mean(hidden * hidden, axis=-1, keepdims=True))
    normed = (hidden * lax.rsqrt(mean_square + norm_eps) * norm_gain.astype(jnp.float32)).astype(jnp.bfloat16)
    logits = jnp.dot(normed, router, preferred_element_type=jnp.float32)
    route_ids = expert_ids.reshape(rows_all, TOP).astype(jnp.int32)
    route_slots = slots.reshape(rows_all, TOP).astype(jnp.int32)
    picked = jnp.take_along_axis(logits, route_ids, axis=1)
    gates = jax.nn.sigmoid(picked)
    weights = route_scale * gates / lax.optimization_barrier(jnp.sum(gates, axis=1, keepdims=True))
    is_kept = route_slots < CAP
    token_index = jnp.broadcast_to(jnp.arange(rows_all, dtype=jnp.int32)[:, None], (rows_all, TOP))
    source = token_index // TOK_DEV
    slot_total = EXPERTS * N_EP * CAP
    flat_slot = route_ids * (N_EP * CAP) + source * CAP + route_slots
    flat_slot = jnp.where(is_kept, flat_slot, slot_total).astype(jnp.int32)
    owner_row = jnp.full((slot_total + 1,), rows_all, dtype=jnp.int32).at[flat_slot.reshape(-1)].set(token_index.reshape(-1))
    share_row = jnp.zeros((slot_total + 1,), jnp.float32).at[flat_slot.reshape(-1)].set(weights.reshape(-1))
    owner_row = owner_row[:slot_total].reshape(EXPERTS, N_EP * CAP)
    share_row = share_row[:slot_total].reshape(EXPERTS, N_EP * CAP)
    padded = jnp.concatenate([normed, jnp.zeros((1, D), jnp.bfloat16)], axis=0)

    def expert_step(expert_mix, packed):
        expert_index, owners, shares = packed
        token_rows = padded[owners]
        gate_cols = lax.dynamic_slice_in_dim(w_gate, expert_index * FFW, FFW, 1)
        up_cols = lax.dynamic_slice_in_dim(w_up, expert_index * FFW, FFW, 1)
        down_rows = lax.dynamic_slice_in_dim(w_down, expert_index * FFW, FFW, 0)
        gate = jnp.dot(token_rows, gate_cols, preferred_element_type=jnp.float32)
        upward = jnp.dot(token_rows, up_cols, preferred_element_type=jnp.float32)
        act = (jax.nn.silu(gate) * upward).astype(jnp.bfloat16)
        produced = jnp.dot(act, down_rows, preferred_element_type=jnp.float32) * shares[:, None]
        return (expert_mix.at[owners].add(produced), None)
    start_mix = jnp.zeros((rows_all + 1, D), jnp.float32)
    expert_mix, _ = lax.scan(expert_step, start_mix, (jnp.arange(EXPERTS, dtype=jnp.int32), owner_row, share_row))
    mixed = (hidden + expert_mix[:rows_all]).astype(jnp.bfloat16)
    return mixed.reshape(BATCH, STEPS, D)
```

```python
import math

import jax
import jax.numpy as jnp
from jax import lax
from jax.sharding import Mesh
from jax.sharding import PartitionSpec as P

D = 7168
H = 64
LAT = 512
VH = 128
EXPERTS = 16
TOP = 8
CAP = 2
QK = 192

CORES = 2
NEAR = 4
FAR = 4
RING = NEAR * FAR
EXTRA = 128

route_scale = 2.827
norm_eps = 1e-06


ZAX = ("zb", "j")
NEAR_GROUPS = (0, 1, RING - 1, 2)
OFFSETS = tuple((g + NEAR * k) % RING for g in NEAR_GROUPS for k in range(FAR))


def shift_x(a, step):
    n = lax.axis_size("x")
    return lax.ppermute(a, "x", [(i, (i + step) % n) for i in range(n)])


def shift_z(a, step):
    return lax.ppermute(a, ZAX, [(i, (i + step) % RING) for i in range(RING)])


def swap_core(a):
    return lax.ppermute(a, "c", [(i, (i + 1) % CORES) for i in range(CORES)])


def roll_left(a, amount, axis=0):
    n = a.shape[axis]
    return lax.dynamic_slice_in_dim(jnp.concatenate([a, a], axis=axis), amount, n, axis)


def softmax_parts(score_cache, score_new):
    row_peak = jnp.maximum(jnp.max(score_cache, axis=-1), jnp.max(score_new, axis=-1))
    exp_cache = jnp.exp(score_cache - row_peak[..., None])
    exp_new = jnp.exp(score_new - row_peak[..., None])
    exp_total = jnp.sum(exp_cache, axis=-1) + jnp.sum(exp_new, axis=-1)
    prob_cache = (exp_cache / exp_total[..., None]).astype(jnp.bfloat16)
    prob_new = (exp_new / exp_total[..., None]).astype(jnp.bfloat16)
    return (prob_cache, prob_new)


def attention(cache_kv, new_kv, queries, lengths):
    score_scale = 1.0 / math.sqrt(QK)
    cache_len = cache_kv.shape[1]
    step_count = new_kv.shape[1]
    score_new = (
        jnp.einsum("bshk,btk->bsht", queries, new_kv, preferred_element_type=jnp.float32)
        * score_scale
    )
    step_ids = jnp.arange(step_count, dtype=jnp.int32)
    causal = step_ids[None, :] <= step_ids[:, None]
    score_new = jnp.where(causal[None, :, None, :], score_new, -jnp.inf)
    score_cache = (
        jnp.einsum("bshk,bpk->bshp", queries, cache_kv, preferred_element_type=jnp.float32)
        * score_scale
    )
    position = jnp.arange(cache_len, dtype=jnp.int32)
    is_live = position[None, :] < lengths[:, None]
    score_cache = jnp.where(is_live[:, None, None, :], score_cache, -jnp.inf)
    prob_cache, prob_new = softmax_parts(score_cache, score_new)
    context = jnp.einsum(
        "bshp,bpc->bshc", prob_cache, cache_kv[:, :, :LAT], preferred_element_type=jnp.float32
    )
    context = context + jnp.einsum(
        "bsht,btc->bshc", prob_new, new_kv[:, :, :LAT], preferred_element_type=jnp.float32
    )
    return context.astype(jnp.bfloat16)


def reduce_z(rows, tok):
    size = FAR * tok
    half = rows.shape[1] // 2
    sent = rows.astype(jnp.bfloat16)
    right = shift_z(sent[size : 2 * size], 1)
    left = shift_z(sent[2 * size : 3 * size], -1)
    ahead = shift_z(sent[3 * size :, :half], 2)
    behind = shift_z(sent[3 * size :, half:], -2)
    behind = jnp.concatenate([behind[size - tok :], behind[: size - tok]], axis=0)
    total = rows[:size] + right.astype(jnp.float32) + left.astype(jnp.float32)
    total = total + jnp.concatenate([ahead, behind], axis=1).astype(jnp.float32)
    sent = total.astype(jnp.bfloat16)
    out = total[:tok]
    for k in range(1, FAR):
        step = NEAR * k if NEAR * k <= RING // 2 else NEAR * k - RING
        out = out + shift_z(sent[k * tok : (k + 1) * tok], step).astype(jnp.float32)
    return out


def body(
    cache_kv,
    new_kv,
    queries,
    lengths,
    resid,
    value_up,
    out_proj,
    norm_gain,
    router,
    expert_ids,
    slots,
    w_gate,
    w_up,
    w_down,
):
    bf16, f32 = jnp.bfloat16, jnp.float32
    nx = lax.axis_size("x")
    x = lax.axis_index("x")
    z = lax.axis_index(ZAX)
    seqs, steps = queries.shape[:2]
    tok = seqs * steps

    mine = jnp.concatenate([value_up.T, out_proj], axis=1)
    rows = mine.shape[0]
    from_left = shift_x(mine, 1)
    from_right = shift_x(mine, -1)
    far_a = shift_x(from_left[: rows // 2], 1)
    far_b = shift_x(from_right[rows // 2 :], -1)
    opposite = jnp.concatenate([far_a, far_b], axis=0)
    pieces = []
    for piece in (mine, from_left, from_right, opposite):
        pieces += [piece, swap_core(piece)]
    head_w = jnp.concatenate(pieces, axis=0)
    head_up = head_w[:, :LAT].reshape(nx, VH, LAT)
    head_out = head_w[:, LAT:]

    gate_w = jnp.concatenate([w_gate, swap_core(w_gate)], axis=1)
    up_w = jnp.concatenate([w_up, swap_core(w_up)], axis=1)
    down_w = jnp.concatenate([w_down, swap_core(w_down)], axis=0)

    context = attention(cache_kv, new_kv, queries, lengths)
    context = context.reshape(tok, nx, RING, LAT)
    order = jnp.stack([x, (x + nx - 1) % nx, (x + 1) % nx, (x + 2) % nx])
    pick = (order[:, None] == jnp.arange(nx)[None, :]).astype(bf16)
    outgoing = jnp.einsum("thzc,rh->zrtc", context, pick, preferred_element_type=f32).astype(bf16)
    arrived = lax.all_to_all(
        outgoing.reshape(RING, nx * tok, LAT), ZAX, split_axis=0, concat_axis=0, tiled=True
    )
    arrived = arrived.reshape(RING, nx, tok, LAT)
    values = jnp.einsum("zrtc,rvc->ztrv", arrived, head_up, preferred_element_type=f32)
    values = values.astype(bf16).reshape(RING, tok * nx * VH)
    values = roll_left(values, z)
    values = jnp.stack([values[o] for o in OFFSETS]).reshape(RING * tok, nx * VH)
    partial = jnp.dot(values, head_out, preferred_element_type=f32)
    attended = reduce_z(partial, tok)

    hidden = resid.reshape(tok, D).astype(f32) + attended
    mean_square = jnp.mean(hidden * hidden, axis=-1, keepdims=True)
    normed = (hidden * lax.rsqrt(mean_square + norm_eps) * norm_gain.astype(f32)).astype(bf16)

    route_ids = expert_ids.reshape(tok, TOP)
    route_slots = slots.reshape(tok, TOP)
    logits = jnp.dot(normed, router, preferred_element_type=f32)
    is_pick = route_ids[:, :, None] == jnp.arange(EXPERTS, dtype=jnp.int32)[None, None, :]
    picked = jnp.sum(jnp.where(is_pick, logits[:, None, :], 0.0), axis=-1)
    gates = jax.nn.sigmoid(picked)
    weights = route_scale * gates / jnp.sum(gates, axis=1, keepdims=True)
    share = jnp.sum(jnp.where(is_pick, weights[:, :, None], 0.0), axis=1)
    slot = jnp.sum(jnp.where(is_pick, route_slots[:, :, None] + 1, 0), axis=1)
    places = [(slot == s + 1).astype(bf16) for s in range(CAP)]
    high = share.astype(bf16)
    rest = share - high.astype(f32)
    middle = rest.astype(bf16)
    low = (rest - middle.astype(f32)).astype(bf16)
    extra = jnp.concatenate(places + [high, middle, low], axis=1)
    extra = jnp.pad(extra, ((0, 0), (0, EXTRA - extra.shape[1])))
    payload = jnp.concatenate([normed, extra], axis=1)

    own = lax.all_gather(payload, ZAX, axis=0, tiled=True)
    count = own.shape[0]
    group_left = shift_x(own, 1)
    group_right = shift_x(own, -1)
    group_a = shift_x(group_left[: count // 2], 1)
    group_b = shift_x(group_right[count // 2 :], -1)
    group_far = jnp.concatenate([group_a, group_b], axis=0)

    e_own = FAR * x + z // NEAR
    e_range = jnp.arange(EXPERTS)
    same = jnp.repeat(jnp.repeat(jnp.eye(RING, dtype=bf16), tok, axis=0), CAP, axis=1)

    def routing_of(group, expert):
        table = group[:, D:]
        hot = (e_range == expert).astype(bf16)
        cols = jnp.stack([jnp.pad(hot, (n * EXPERTS, EXTRA - (n + 1) * EXPERTS)) for n in range(CAP + 3)], axis=1)
        got = jnp.dot(table, cols, preferred_element_type=f32)
        sel = jnp.tile(got[:, :CAP].astype(bf16), (1, RING)) * same
        return sel, got[:, CAP : CAP + 1] + got[:, CAP + 1 : CAP + 2] + got[:, CAP + 2 : CAP + 3]

    def expert(group):
        tokens = group[:, :D]
        gate = jnp.dot(tokens, gate_w, preferred_element_type=f32)
        upward = jnp.dot(tokens, up_w, preferred_element_type=f32)
        act = (jax.nn.silu(gate) * upward).astype(bf16)
        sel, part = routing_of(group, e_own)
        act = lax.dot_general(sel, act, (((0,), (0,)), ((), ())), preferred_element_type=f32).astype(bf16)
        part = jnp.sum(sel.astype(f32) * part, axis=0)[:, None]
        out = jnp.dot(act, down_w, preferred_element_type=f32)
        return (out * part).astype(bf16)

    back_left = shift_x(expert(group_left), -1)
    back_right = shift_x(expert(group_right), 1)
    back_far = shift_x(expert(group_far), 2)
    back_own = expert(own)
    parts = jnp.concatenate([back_own, back_right, back_left, back_far], axis=0)
    spread = []
    for r in range(nx):
        sel, _ = routing_of(own, FAR * order[r] + z // NEAR)
        spread.append(sel)
    spread = jnp.concatenate(spread, axis=1).reshape(RING, tok * nx * RING * CAP)
    spread = roll_left(spread, z)
    spread = jnp.stack([spread[o] for o in OFFSETS]).reshape(RING * tok, nx * RING * CAP)
    mixed_rows = jnp.dot(spread, parts, preferred_element_type=f32)
    expert_mix = reduce_z(mixed_rows, tok)
    mixed = (hidden + expert_mix).astype(bf16)
    return mixed.reshape(resid.shape)


def solution(mesh):
    chips = mesh.shape["ep"] // (RING * CORES)
    grid = mesh.devices.reshape(mesh.shape["rep"], chips, FAR, NEAR, CORES)
    fine = Mesh(grid, ("rep", "x", "zb", "j", "c"))
    ep = ("x", "zb", "j", "c")
    both = ("rep",) + ep
    return jax.shard_map(
        body,
        mesh=fine,
        in_specs=(
            P(both, None, None),
            P(both, None, None),
            P(both, None, None, None),
            P(both),
            P(both, None, None),
            P(None, ep),
            P(ep, None),
            P(),
            P(),
            P(both, None, None),
            P(both, None, None),
            P(None, ep),
            P(None, ep),
            P(ep, None),
        ),
        out_specs=P(both, None, None),
        check_vma=False,
    )
```

```python
import functools
import math

import jax
import jax.numpy as jnp
from jax import lax
from jax.experimental import pallas as pl
from jax.experimental.pallas import tpu as pltpu
from jax.sharding import Mesh
from jax.sharding import PartitionSpec as P


D = 7168
LAT = 512
EXPERTS = 16
TOP = 8
CAP = 2
QK = 192

CORES = 2
NEAR = 4
FAR = 4
RING = NEAR * FAR
EXTRA = 128

route_scale = 2.827
norm_eps = 1e-06


ZAX = ("zb", "j")
NEAR_GROUPS = (0, 1, RING - 1, 2)
OFFSETS = tuple((g + NEAR * k) % RING for g in NEAR_GROUPS for k in range(FAR))


def shift_x(a, step):
    n = lax.axis_size("x")
    return lax.ppermute(a, "x", [(i, (i + step) % n) for i in range(n)])


def shift_z(a, step):
    return lax.ppermute(a, ZAX, [(i, (i + step) % RING) for i in range(RING)])


def swap_core(a):
    return lax.ppermute(a, "c", [(i, (i + 1) % CORES) for i in range(CORES)])


def roll_left(a, amount, axis=0):
    n = a.shape[axis]
    return lax.dynamic_slice_in_dim(jnp.concatenate([a, a], axis=axis), amount, n, axis)


def softmax_parts(score_cache, score_new):
    row_peak = jnp.maximum(jnp.max(score_cache, axis=-1), jnp.max(score_new, axis=-1))
    exp_cache = jnp.exp(score_cache - row_peak[..., None])
    exp_new = jnp.exp(score_new - row_peak[..., None])
    exp_total = jnp.sum(exp_cache, axis=-1) + jnp.sum(exp_new, axis=-1)
    prob_cache = (exp_cache / exp_total[..., None]).astype(jnp.bfloat16)
    prob_new = (exp_new / exp_total[..., None]).astype(jnp.bfloat16)
    return (prob_cache, prob_new)


def attention(cache_kv, new_kv, queries, lengths):
    score_scale = 1.0 / math.sqrt(QK)
    cache_len = cache_kv.shape[1]
    step_count = new_kv.shape[1]
    score_new = (
        jnp.einsum("bshk,btk->bsht", queries, new_kv, preferred_element_type=jnp.float32)
        * score_scale
    )
    step_ids = jnp.arange(step_count, dtype=jnp.int32)
    causal = step_ids[None, :] <= step_ids[:, None]
    score_new = jnp.where(causal[None, :, None, :], score_new, -jnp.inf)
    score_cache = (
        jnp.einsum("bshk,bpk->bshp", queries, cache_kv, preferred_element_type=jnp.float32)
        * score_scale
    )
    position = jnp.arange(cache_len, dtype=jnp.int32)
    is_live = position[None, :] < lengths[:, None]
    score_cache = jnp.where(is_live[:, None, None, :], score_cache, -jnp.inf)
    prob_cache, prob_new = softmax_parts(score_cache, score_new)
    context = jnp.einsum(
        "bshp,bpc->bshc", prob_cache, cache_kv[:, :, :LAT], preferred_element_type=jnp.float32
    )
    context = context + jnp.einsum(
        "bsht,btc->bshc", prob_new, new_kv[:, :, :LAT], preferred_element_type=jnp.float32
    )
    return context.astype(jnp.bfloat16)


def reduce_z(own, right, left, ahead, behind):
    size = own.shape[0]
    tok = size // FAR
    right = shift_z(right, 1)
    left = shift_z(left, -1)
    ahead = shift_z(ahead, 2)
    behind = shift_z(behind, -2)
    behind = jnp.concatenate([behind[size - tok :], behind[: size - tok]], axis=0)
    total = own + right.astype(jnp.float32) + left.astype(jnp.float32)
    total = total + jnp.concatenate([ahead, behind], axis=1).astype(jnp.float32)
    sent = total.astype(jnp.bfloat16)
    out = total[:tok]
    for k in range(1, FAR):
        step = NEAR * k if NEAR * k <= RING // 2 else NEAR * k - RING
        out = out + shift_z(sent[k * tok : (k + 1) * tok], step).astype(jnp.float32)
    return out


def ring_place(index):
    group, k = index // FAR, lax.rem(index, FAR)
    first = jnp.where(group == 2, RING - 1, jnp.where(group == 3, 2, group))
    return lax.rem(first + NEAR * k, RING)


PIECES = 8
OUT_TILE = 512


def attend_kernel(tok, z_ref, arrived, *refs):
    pieces = refs[:PIECES]
    own, right, left, ahead, behind, up, rows, up_sem, row_sem = refs[PIECES:]
    f32, bf16 = jnp.float32, jnp.bfloat16
    part = pieces[0].shape[0]
    dim = rows.shape[1]
    half = dim // 2
    for i, piece in enumerate(pieces):
        pltpu.make_async_copy(
            piece.at[:, pl.ds(0, LAT)], up.at[pl.ds(i * part, part)], up_sem.at[i]
        ).start()
    for c in range(2):
        for i, piece in enumerate(pieces):
            pltpu.make_async_copy(
                piece.at[:, pl.ds(LAT + c * half, half)],
                rows.at[pl.ds(i * part, part), pl.ds(c * half, half)],
                row_sem.at[c, i],
            ).start()
    for i, piece in enumerate(pieces):
        pltpu.make_async_copy(
            piece.at[:, pl.ds(0, LAT)], up.at[pl.ds(i * part, part)], up_sem.at[i]
        ).wait()
    count = arrived.shape[0] * arrived.shape[1]
    heads = arrived.shape[1] // tok
    context = arrived[...].reshape(count, LAT)
    values = lax.dot_general(context, up[...], (((1,), (1,)), ((), ())), preferred_element_type=f32)
    row = lax.broadcasted_iota(jnp.int32, values.shape, 0)
    col = lax.broadcasted_iota(jnp.int32, values.shape, 1)
    same_head = lax.rem(row // tok, heads) == col // (part * PIECES // heads)
    values = jnp.where(same_head, values, 0.0).astype(bf16)
    shape = (RING * tok, count)
    place = lax.broadcasted_iota(jnp.int32, shape, 0)
    source = lax.broadcasted_iota(jnp.int32, shape, 1)
    chip = lax.rem(ring_place(place // tok) + z_ref[0], RING)
    take = (source // (tok * heads) == chip) & (lax.rem(source, tok) == lax.rem(place, tok))
    values = jnp.dot(jnp.where(take, 1.0, 0.0).astype(bf16), values, preferred_element_type=f32)
    values = values.astype(bf16)
    size = FAR * tok
    for c in range(2):
        for i, piece in enumerate(pieces):
            pltpu.make_async_copy(
                piece.at[:, pl.ds(LAT + c * half, half)],
                rows.at[pl.ds(i * part, part), pl.ds(c * half, half)],
                row_sem.at[c, i],
            ).wait()
        for n in range(half // OUT_TILE):
            cols = pl.ds(c * half + n * OUT_TILE, OUT_TILE)
            got = jnp.dot(values, rows[:, cols], preferred_element_type=f32)
            own[:, cols] = got[:size]
            right[:, cols] = got[size : 2 * size].astype(bf16)
            left[:, cols] = got[2 * size : 3 * size].astype(bf16)
            last = ahead if c == 0 else behind
            last[:, pl.ds(n * OUT_TILE, OUT_TILE)] = got[3 * size :].astype(bf16)


def attend_out(z, arrived, pieces, tok):
    part, width = pieces[0].shape
    dim = width - LAT
    size = FAR * tok
    f32, bf16 = jnp.float32, jnp.bfloat16
    vmem = pl.BlockSpec(memory_space=pltpu.VMEM)
    return pl.pallas_call(
        functools.partial(attend_kernel, tok),
        out_shape=(
            jax.ShapeDtypeStruct((size, dim), f32),
            jax.ShapeDtypeStruct((size, dim), bf16),
            jax.ShapeDtypeStruct((size, dim), bf16),
            jax.ShapeDtypeStruct((size, dim // 2), bf16),
            jax.ShapeDtypeStruct((size, dim // 2), bf16),
        ),
        in_specs=[pl.BlockSpec(memory_space=pltpu.SMEM), vmem]
        + [pl.BlockSpec(memory_space=pltpu.HBM)] * PIECES,
        out_specs=[vmem] * 5,
        scratch_shapes=[
            pltpu.VMEM((PIECES * part, LAT), bf16),
            pltpu.VMEM((PIECES * part, dim), bf16),
            pltpu.SemaphoreType.DMA((PIECES,)),
            pltpu.SemaphoreType.DMA((2, PIECES)),
        ],
        compiler_params=pltpu.CompilerParams(vmem_limit_bytes=16 << 20),
        cost_estimate=pl.CostEstimate(
            flops=2 * RING * tok * PIECES * part * dim * 4,
            bytes_accessed=PIECES * part * width * 2,
            transcendentals=0,
        ),
        name="attend_out",
    )(z.reshape(1).astype(jnp.int32), arrived, *pieces)


CHUNKS = 7


def expert_kernel(tok, inputs, groups, e_ref, *refs):
    tokens = refs[:inputs]
    gate_a, gate_b, up_a, up_b, down_a, down_b = refs[inputs : inputs + 6]
    outs = refs[inputs + 6 : inputs + 6 + groups]
    wide, deep, held, first_sem, second_sem = refs[inputs + 6 + groups :]
    f32, bf16 = jnp.float32, jnp.bfloat16
    dim, part = gate_a.shape
    chunk = dim // CHUNKS

    def first(k, i):
        return pltpu.make_async_copy(
            (gate_a, gate_b, up_a, up_b)[i].at[pl.ds(k * chunk, chunk)],
            wide.at[pl.ds(k * chunk, chunk), pl.ds(i * part, part)],
            first_sem.at[k, i],
        )

    def second(i):
        return pltpu.make_async_copy(
            (down_a, down_b)[i], deep.at[pl.ds(i * part, part)], second_sem.at[i]
        )

    for k in range(CHUNKS):
        for i in range(4):
            first(k, i).start()
    for i in range(2):
        second(i).start()
    at = 0
    for ref in tokens:
        held[pl.ds(at, ref.shape[0])] = ref[...]
        at += ref.shape[0]
    total = jnp.zeros((at, 4 * part), f32)
    for k in range(CHUNKS):
        for i in range(4):
            first(k, i).wait()
        rows = pl.ds(k * chunk, chunk)
        total = total + jnp.dot(held[:, rows], wide[rows, :], preferred_element_type=f32)
    gate, upward = total[:, : 2 * part], total[:, 2 * part :]
    act = (gate / (1.0 + jnp.exp(-gate)) * upward).astype(bf16)

    count = at // groups
    kinds = CAP + 3
    shape = (8, EXTRA)
    kind = lax.broadcasted_iota(jnp.int32, shape, 0)
    place = lax.broadcasted_iota(jnp.int32, shape, 1)
    hot = (place == kind * EXPERTS + e_ref[0]) & (kind < kinds)
    hot = jnp.where(hot, 1.0, 0.0).astype(bf16)
    small, shares = [], []
    for g in range(groups):
        table = held[pl.ds(g * count, count), pl.ds(dim, EXTRA)]
        got = lax.dot_general(hot, table, (((1,), (1,)), ((), ())), preferred_element_type=f32)
        shape = (RING * CAP, count)
        slot = lax.broadcasted_iota(jnp.int32, shape, 0)
        token = lax.broadcasted_iota(jnp.int32, shape, 1)
        sel = jnp.where(lax.rem(slot, CAP) == 0, got[0:1], got[1:2])
        sel = jnp.where(slot // CAP == token // tok, sel, 0.0)
        share = got[CAP : CAP + 1] + got[CAP + 1 : CAP + 2] + got[CAP + 2 : CAP + 3]
        shares.append(jnp.sum(sel * share, axis=1, keepdims=True))
        picked = jnp.dot(sel.astype(bf16), act[g * count : (g + 1) * count], preferred_element_type=f32)
        small.append(picked.astype(bf16))
    small = jnp.concatenate(small, axis=0) if groups > 1 else small[0]
    share = jnp.concatenate(shares, axis=0) if groups > 1 else shares[0]
    for i in range(2):
        second(i).wait()
    slots = RING * CAP
    for k in range(CHUNKS):
        cols = pl.ds(k * chunk, chunk)
        got = jnp.dot(small, deep[:, cols], preferred_element_type=f32) * share
        for g in range(groups):
            outs[g][:, cols] = got[g * slots : (g + 1) * slots].astype(bf16)


def expert_part(e, tokens, weights, tok, groups):
    bf16 = jnp.bfloat16
    dim, part = weights[0].shape
    rows = sum(t.shape[0] for t in tokens)
    vmem = pl.BlockSpec(memory_space=pltpu.VMEM)
    hbm = pl.BlockSpec(memory_space=pltpu.HBM)
    return pl.pallas_call(
        functools.partial(expert_kernel, tok, len(tokens), groups),
        out_shape=(jax.ShapeDtypeStruct((RING * CAP, dim), bf16),) * groups,
        in_specs=[pl.BlockSpec(memory_space=pltpu.SMEM)] + [vmem] * len(tokens) + [hbm] * 6,
        out_specs=[vmem] * groups,
        scratch_shapes=[
            pltpu.VMEM((dim, 4 * part), bf16),
            pltpu.VMEM((2 * part, dim), bf16),
            pltpu.VMEM((rows, dim + EXTRA), bf16),
            pltpu.SemaphoreType.DMA((CHUNKS, 4)),
            pltpu.SemaphoreType.DMA((2,)),
        ],
        compiler_params=pltpu.CompilerParams(vmem_limit_bytes=20 << 20),
        cost_estimate=pl.CostEstimate(
            flops=2 * rows * dim * part * 6, bytes_accessed=12 * dim * part, transcendentals=0
        ),
        name="expert_part",
    )(e.reshape(1).astype(jnp.int32), *tokens, *weights)


def layer(
    cache_kv,
    new_kv,
    queries,
    lengths,
    resid,
    value_up,
    out_proj,
    norm_gain,
    router,
    expert_ids,
    slots,
    w_gate,
    w_up,
    w_down,
):
    bf16, f32 = jnp.bfloat16, jnp.float32
    nx = lax.axis_size("x")
    x = lax.axis_index("x")
    z = lax.axis_index(ZAX)
    seqs, steps = queries.shape[:2]
    tok = seqs * steps

    mine = jnp.concatenate([value_up.T, out_proj], axis=1)
    rows = mine.shape[0]
    from_left = shift_x(mine, 1)
    from_right = shift_x(mine, -1)
    ffn = (w_gate, swap_core(w_gate), w_up, swap_core(w_up), w_down, swap_core(w_down))

    context = attention(cache_kv, new_kv, queries, lengths)
    context = context.reshape(tok, nx, RING, LAT)
    order = jnp.stack([x, (x + nx - 1) % nx, (x + 1) % nx, (x + 2) % nx])
    pick = (order[:, None] == jnp.arange(nx)[None, :]).astype(bf16)
    outgoing = jnp.einsum("thzc,rh->zrtc", context, pick, preferred_element_type=f32).astype(bf16)
    outgoing = outgoing.reshape(RING, nx * tok, LAT)
    from_left, from_right, _ = lax.optimization_barrier((from_left, from_right, outgoing))
    far_a = shift_x(from_left[: rows // 2], 1)
    far_b = shift_x(from_right[rows // 2 :], -1)
    opposite = jnp.concatenate([far_a, far_b], axis=0)
    pieces = []
    for piece in (mine, from_left, from_right, opposite):
        pieces += [piece, swap_core(piece)]
    arrived = lax.all_to_all(outgoing, ZAX, split_axis=0, concat_axis=0, tiled=True)
    attended = reduce_z(*attend_out(z, arrived, pieces, tok))

    hidden = resid.reshape(tok, D).astype(f32) + attended
    mean_square = jnp.mean(hidden * hidden, axis=-1, keepdims=True)
    normed = (hidden * lax.rsqrt(mean_square + norm_eps) * norm_gain.astype(f32)).astype(bf16)

    route_ids = expert_ids.reshape(tok, TOP)
    route_slots = slots.reshape(tok, TOP)
    logits = jnp.dot(normed, router, preferred_element_type=f32)
    is_pick = route_ids[:, :, None] == jnp.arange(EXPERTS, dtype=jnp.int32)[None, None, :]
    picked = jnp.sum(jnp.where(is_pick, logits[:, None, :], 0.0), axis=-1)
    gates = jax.nn.sigmoid(picked)
    weights = route_scale * gates / jnp.sum(gates, axis=1, keepdims=True)
    share = jnp.sum(jnp.where(is_pick, weights[:, :, None], 0.0), axis=1)
    slot = jnp.sum(jnp.where(is_pick, route_slots[:, :, None] + 1, 0), axis=1)
    places = [(slot == s + 1).astype(bf16) for s in range(CAP)]
    high = share.astype(bf16)
    rest = share - high.astype(f32)
    middle = rest.astype(bf16)
    low = (rest - middle.astype(f32)).astype(bf16)
    extra = jnp.concatenate(places + [high, middle, low], axis=1)
    extra = jnp.pad(extra, ((0, 0), (0, EXTRA - extra.shape[1])))
    payload = jnp.concatenate([normed, extra], axis=1)

    own = lax.all_gather(payload, ZAX, axis=0, tiled=True)
    count = own.shape[0]
    group_left = shift_x(own, 1)
    group_right = shift_x(own, -1)
    group_a = shift_x(group_left[: count // 2], 1)
    group_b = shift_x(group_right[count // 2 :], -1)
    e_own = FAR * x + z // NEAR
    e_range = jnp.arange(EXPERTS)
    same = jnp.repeat(jnp.repeat(jnp.eye(RING, dtype=bf16), tok, axis=0), CAP, axis=1)

    def routing_of(group, expert):
        hot = (e_range == expert).astype(bf16)
        cols = jnp.stack([jnp.pad(hot, (n * EXPERTS, EXTRA - (n + 1) * EXPERTS)) for n in range(CAP)], axis=1)
        got = jnp.dot(group[:, D:], cols, preferred_element_type=f32).astype(bf16)
        return jnp.tile(got, (1, RING)) * same

    (back_own,) = expert_part(e_own, (own,), ffn, tok, 1)
    sent_left, sent_right = expert_part(e_own, (group_left, group_right), ffn, tok, 2)
    back_left = shift_x(sent_left, -1)
    back_right = shift_x(sent_right, 1)
    (sent_far,) = expert_part(e_own, (group_a, group_b), ffn, tok, 1)
    back_far = shift_x(sent_far, 2)
    parts = jnp.concatenate([back_own, back_right, back_left, back_far], axis=0)
    spread = []
    for r in range(nx):
        spread.append(routing_of(own, FAR * order[r] + z // NEAR))
    spread = jnp.concatenate(spread, axis=1).reshape(RING, tok * nx * RING * CAP)
    spread = roll_left(spread, z)
    spread = jnp.stack([spread[o] for o in OFFSETS]).reshape(RING * tok, nx * RING * CAP)
    mixed_rows = jnp.dot(spread, parts, preferred_element_type=f32)
    size = FAR * tok
    rounded = mixed_rows.astype(bf16)
    expert_mix = reduce_z(
        mixed_rows[:size],
        rounded[size : 2 * size],
        rounded[2 * size : 3 * size],
        rounded[3 * size :, : D // 2],
        rounded[3 * size :, D // 2 :],
    )
    mixed = (hidden + expert_mix).astype(bf16)
    return mixed.reshape(resid.shape)


def solution(mesh):
    chips = mesh.shape["ep"] // (RING * CORES)
    grid = mesh.devices.reshape(mesh.shape["rep"], chips, FAR, NEAR, CORES)
    fine = Mesh(grid, ("rep", "x", "zb", "j", "c"))
    ep = ("x", "zb", "j", "c")
    both = ("rep",) + ep
    return jax.shard_map(
        layer,
        mesh=fine,
        in_specs=(
            P(both, None, None),
            P(both, None, None),
            P(both, None, None, None),
            P(both),
            P(both, None, None),
            P(None, ep),
            P(ep, None),
            P(),
            P(),
            P(both, None, None),
            P(both, None, None),
            P(None, ep),
            P(None, ep),
            P(ep, None),
        ),
        out_specs=P(both, None, None),
        check_vma=False,
    )
```

```python
import functools
import math

import jax
import jax.numpy as jnp
from jax import lax
from jax.experimental import pallas as pl
from jax.experimental.pallas import tpu as pltpu
from jax.sharding import Mesh
from jax.sharding import PartitionSpec as P


D = 7168
LAT = 512
VH = 128
EXPERTS = 16
TOP = 8
CAP = 2
QK = 192

CORES = 2
NEAR = 4
FAR = 4
RING = NEAR * FAR
SLOTS = RING * CAP
EXTRA = 128

route_scale = 2.827
norm_eps = 1e-06


ZAX = ("zb", "j")
f32, bf16 = jnp.float32, jnp.bfloat16
NT = (((1,), (1,)), ((), ()))


def shift_x(a, step):
    n = lax.axis_size("x")
    return lax.ppermute(a, "x", [(i, (i + step) % n) for i in range(n)])


def shift_z(a, step):
    return lax.ppermute(a, ZAX, [(i, (i + step) % RING) for i in range(RING)])


def swap_core(a):
    return lax.ppermute(a, "c", [(i, (i + 1) % CORES) for i in range(CORES)])


def iota(shape, axis):
    return lax.broadcasted_iota(jnp.int32, shape, axis)


def one_hot(mask):
    return jnp.where(mask, 1.0, 0.0).astype(bf16)


def column(hop, x, nx):
    step = jnp.where(hop == 1, nx - 1, jnp.where(hop == 2, 1, jnp.where(hop == 3, 2, 0)))
    return lax.rem(x + step, nx)


def chip_at(place, j):
    group, block = place // FAR, lax.rem(place, FAR)
    step = jnp.where(group == 2, NEAR - 1, jnp.where(group == 3, 2, group))
    return NEAR * block + lax.rem(j + step, NEAR)


def smem():
    return pl.BlockSpec(memory_space=pltpu.SMEM)


def vmem():
    return pl.BlockSpec(memory_space=pltpu.VMEM)


def hbm():
    return pl.BlockSpec(memory_space=pltpu.HBM)


def params(mib):
    return pltpu.CompilerParams(vmem_limit_bytes=mib << 20)


def cost(flops, nbytes):
    return pl.CostEstimate(flops=flops, bytes_accessed=nbytes, transcendentals=0)


def context_kernel(nx, where_ref, lengths, keys, queries, new, out, held):
    seq = pl.program_id(0)
    seqs = pl.num_programs(0)
    steps, heads = queries.shape[1], queries.shape[2]
    count = steps * heads
    scale = 1.0 / math.sqrt(QK)
    query = queries[0].reshape(count, queries.shape[3])
    score = jnp.dot(query, keys[0], preferred_element_type=f32) * scale
    score = jnp.where(iota(score.shape, 1) < lengths[seq], score, -jnp.inf)
    wide = query.astype(f32)
    step_of = iota((count, 1), 0) // heads
    latest = []
    peak = jnp.max(score, axis=1, keepdims=True)
    for t in range(steps):
        key = new[0, t : t + 1, :].astype(f32)
        got = jnp.sum(wide * key, axis=1, keepdims=True) * scale
        got = jnp.where(step_of >= t, got, -jnp.inf)
        latest.append(got)
        peak = jnp.maximum(peak, got)
    probs = jnp.exp(score - peak)
    total = jnp.sum(probs, axis=1, keepdims=True)
    latest = [jnp.exp(got - peak) for got in latest]
    for got in latest:
        total = total + got
    share = 1.0 / total
    probs = (probs * share).astype(bf16)
    context = lax.dot_general(probs, keys[0, :LAT, :], NT, preferred_element_type=f32)
    for t, got in enumerate(latest):
        part = (got * share).astype(bf16).astype(f32)
        context = context + part * new[0, t : t + 1, :LAT].astype(f32)
    held[pl.ds(pl.multiple_of(seq * count, count), count), :] = context.astype(bf16)

    @pl.when(seq == seqs - 1)
    def _():
        rows = held.shape[0]
        tok = rows // heads
        shape = (rows, rows)
        to, source = iota(shape, 0), iota(shape, 1)
        hop = lax.rem(to // tok, nx)
        head = column(hop, where_ref[0], nx) * RING + to // (tok * nx)
        take = (lax.rem(to, tok) == source // heads) & (head == lax.rem(source, heads))
        out[...] = jnp.dot(one_hot(take), held[...], preferred_element_type=f32).astype(bf16)


def context_rows(where, nx, cache_kv, new_kv, queries, lengths):
    seqs, length, width = cache_kv.shape
    steps, heads = queries.shape[1:3]
    rows = seqs * steps * heads
    keys = jnp.swapaxes(cache_kv, 1, 2)
    return pl.pallas_call(
        functools.partial(context_kernel, nx),
        grid=(seqs,),
        out_shape=jax.ShapeDtypeStruct((rows, LAT), bf16),
        in_specs=[
            smem(),
            smem(),
            pl.BlockSpec((1, width, length), lambda b: (b, 0, 0)),
            pl.BlockSpec((1, steps, heads, width), lambda b: (b, 0, 0, 0)),
            pl.BlockSpec((1, steps, width), lambda b: (b, 0, 0)),
        ],
        out_specs=pl.BlockSpec((rows, LAT), lambda b: (0, 0)),
        scratch_shapes=[pltpu.VMEM((rows, LAT), bf16)],
        compiler_params=params(24),
        cost_estimate=cost(2 * rows * length * (width + LAT), 2 * cache_kv.size),
        name="context_rows",
    )(where, lengths, keys, queries, new_kv)


OUT_TILE = 512


def put_rows(got, outs, c, n, half):
    own, right, left, ahead, behind = outs
    size = own.shape[0]
    cols = pl.ds(c * half + n * OUT_TILE, OUT_TILE)
    own[:, cols] = got[:size]
    right[:, cols] = got[size : 2 * size].astype(bf16)
    left[:, cols] = got[2 * size : 3 * size].astype(bf16)
    last = ahead if c == 0 else behind
    last[:, pl.ds(n * OUT_TILE, OUT_TILE)] = got[3 * size :].astype(bf16)


def row_shapes(size, dim):
    return (
        jax.ShapeDtypeStruct((size, dim), f32),
        jax.ShapeDtypeStruct((size, dim), bf16),
        jax.ShapeDtypeStruct((size, dim), bf16),
        jax.ShapeDtypeStruct((size, dim // 2), bf16),
        jax.ShapeDtypeStruct((size, dim // 2), bf16),
    )


def attend_kernel(tok, nx, count, where_ref, arrived, *refs):
    pieces = refs[:count]
    outs = refs[count : count + 5]
    up, rows, up_sem, row_sem = refs[count + 5 :]
    half = rows.shape[1] // 2
    starts = [0]
    for piece in pieces:
        starts.append(starts[-1] + piece.shape[0])

    def up_copy(i):
        return pltpu.make_async_copy(
            pieces[i].at[:, pl.ds(0, LAT)],
            up.at[pl.ds(starts[i], pieces[i].shape[0])],
            up_sem.at[i],
        )

    def row_copy(c, i):
        return pltpu.make_async_copy(
            pieces[i].at[:, pl.ds(LAT + c * half, half)],
            rows.at[pl.ds(starts[i], pieces[i].shape[0]), pl.ds(c * half, half)],
            row_sem.at[c, i],
        )

    for i in range(count):
        up_copy(i).start()
    for c in range(2):
        for i in range(count):
            row_copy(c, i).start()
    for i in range(count):
        up_copy(i).wait()
    values = lax.dot_general(arrived[...], up[...], NT, preferred_element_type=f32)
    hop = lax.rem(iota(values.shape, 0) // tok, nx)
    values = jnp.where(hop == iota(values.shape, 1) // VH, values, 0.0).astype(bf16)
    shape = (RING * tok, arrived.shape[0])
    place, source = iota(shape, 0), iota(shape, 1)
    take = (source // (tok * nx) == chip_at(place // tok, where_ref[2])) & (
        lax.rem(source, tok) == lax.rem(place, tok)
    )
    values = jnp.dot(one_hot(take), values, preferred_element_type=f32).astype(bf16)
    for c in range(2):
        for i in range(count):
            row_copy(c, i).wait()
        for n in range(half // OUT_TILE):
            cols = pl.ds(c * half + n * OUT_TILE, OUT_TILE)
            put_rows(jnp.dot(values, rows[:, cols], preferred_element_type=f32), outs, c, n, half)


def attend_out(where, nx, arrived, pieces, tok):
    depth = sum(p.shape[0] for p in pieces)
    dim = pieces[0].shape[1] - LAT
    count = len(pieces)
    return pl.pallas_call(
        functools.partial(attend_kernel, tok, nx, count),
        out_shape=row_shapes(FAR * tok, dim),
        in_specs=[smem(), vmem()] + [hbm()] * count,
        out_specs=[vmem()] * 5,
        scratch_shapes=[
            pltpu.VMEM((depth, LAT), bf16),
            pltpu.VMEM((depth, dim), bf16),
            pltpu.SemaphoreType.DMA((count,)),
            pltpu.SemaphoreType.DMA((2, count)),
        ],
        compiler_params=params(16),
        cost_estimate=cost(8 * RING * tok * depth * dim, 2 * depth * dim),
        name="attend_out",
    )(where, arrived, *pieces)


def dispatch_kernel(tok, nx, where_ref, tokens, *refs):
    outs, spread = refs[:nx], refs[nx]
    count, width = tokens.shape
    dim = width - EXTRA
    table = tokens[:, pl.ds(dim, EXTRA)]
    shape = (nx * CAP, EXTRA)
    row, place = iota(shape, 0), iota(shape, 1)
    expert = FAR * column(row // CAP, where_ref[0], nx) + where_ref[1]
    hot = one_hot(place == lax.rem(row, CAP) * EXPERTS + expert)
    got = lax.dot_general(hot, table, NT, preferred_element_type=f32)
    shape = (SLOTS, count)
    slot, token = iota(shape, 0), iota(shape, 1)
    parts = []
    for r in range(nx):
        sel = jnp.where(lax.rem(slot, CAP) == 0, got[CAP * r : CAP * r + 1], got[CAP * r + 1 : CAP * r + 2])
        parts.append(jnp.where(slot // CAP == token // tok, sel, 0.0))
    sel = jnp.concatenate(parts, axis=0).astype(bf16)
    for n in range(pl.cdiv(width, OUT_TILE)):
        cols = pl.ds(n * OUT_TILE, min(OUT_TILE, width - n * OUT_TILE))
        rows = jnp.dot(sel, tokens[:, cols], preferred_element_type=f32).astype(bf16)
        for r in range(nx):
            outs[r][:, cols] = rows[r * SLOTS : (r + 1) * SLOTS]
    shape = (count, count)
    place, token = iota(shape, 0), iota(shape, 1)
    take = (token // tok == chip_at(place // tok, where_ref[2])) & (
        lax.rem(token, tok) == lax.rem(place, tok)
    )
    spread[...] = lax.dot_general(one_hot(take), sel, NT, preferred_element_type=f32).astype(bf16)


def dispatch(where, nx, tokens, tok):
    count, width = tokens.shape
    return pl.pallas_call(
        functools.partial(dispatch_kernel, tok, nx),
        out_shape=(jax.ShapeDtypeStruct((SLOTS, width), bf16),) * nx
        + (jax.ShapeDtypeStruct((count, nx * SLOTS), bf16),),
        in_specs=[smem(), vmem()],
        out_specs=[vmem()] * (nx + 1),
        compiler_params=params(12),
        cost_estimate=cost(2 * nx * SLOTS * count * width, 4 * count * width),
        name="dispatch",
    )(where, tokens)


CHUNKS = 7


def expert_kernel(groups, where_ref, *refs):
    tokens = refs[:groups]
    gate_a, gate_b, up_a, up_b, down_a, down_b = refs[groups : groups + 6]
    outs = refs[groups + 6 : 2 * groups + 6]
    wide, deep, held, first_sem, second_sem = refs[2 * groups + 6 :]
    dim, part = gate_a.shape
    chunk = dim // CHUNKS

    def first(k, i):
        return pltpu.make_async_copy(
            (gate_a, gate_b, up_a, up_b)[i].at[pl.ds(k * chunk, chunk)],
            wide.at[pl.ds(k * chunk, chunk), pl.ds(i * part, part)],
            first_sem.at[k, i],
        )

    def second(i):
        return pltpu.make_async_copy(
            (down_a, down_b)[i], deep.at[pl.ds(i * part, part)], second_sem.at[i]
        )

    for k in range(CHUNKS):
        for i in range(4):
            first(k, i).start()
    for i in range(2):
        second(i).start()
    rows = groups * SLOTS
    if groups > 1:
        for g, ref in enumerate(tokens):
            held[pl.ds(g * SLOTS, SLOTS)] = ref[...]
    else:
        held = tokens[0]
    total = jnp.zeros((rows, 4 * part), f32)
    for k in range(CHUNKS):
        for i in range(4):
            first(k, i).wait()
        cols = pl.ds(k * chunk, chunk)
        total = total + jnp.dot(held[:, cols], wide[cols, :], preferred_element_type=f32)
    gate, upward = total[:, : 2 * part], total[:, 2 * part :]
    act = (gate / (1.0 + jnp.exp(-gate)) * upward).astype(bf16)
    shape = (EXTRA, EXTRA)
    expert = FAR * where_ref[0] + where_ref[1]
    from_share = iota(shape, 0) - CAP * EXPERTS
    hot = (from_share >= 0) & (from_share < 3 * EXPERTS) & (lax.rem(from_share + EXTRA, EXPERTS) == expert)
    share = jnp.dot(held[:, pl.ds(dim, EXTRA)], one_hot(hot), preferred_element_type=f32)[:, :1]
    for i in range(2):
        second(i).wait()
    for k in range(CHUNKS):
        cols = pl.ds(k * chunk, chunk)
        got = jnp.dot(act, deep[:, cols], preferred_element_type=f32) * share
        for g in range(groups):
            outs[g][:, cols] = got[g * SLOTS : (g + 1) * SLOTS].astype(bf16)


def expert_part(where, tokens, weights):
    dim, part = weights[0].shape
    groups = len(tokens)
    rows = groups * SLOTS
    return pl.pallas_call(
        functools.partial(expert_kernel, groups),
        out_shape=(jax.ShapeDtypeStruct((SLOTS, dim), bf16),) * groups,
        in_specs=[smem()] + [vmem()] * groups + [hbm()] * 6,
        out_specs=[vmem()] * groups,
        scratch_shapes=[
            pltpu.VMEM((dim, 4 * part), bf16),
            pltpu.VMEM((2 * part, dim), bf16),
            pltpu.VMEM((rows if groups > 1 else 16, dim + EXTRA), bf16),
            pltpu.SemaphoreType.DMA((CHUNKS, 4)),
            pltpu.SemaphoreType.DMA((2,)),
        ],
        compiler_params=params(20),
        cost_estimate=cost(12 * rows * dim * part, 12 * dim * part),
        name="expert_part",
    )(where, *tokens, *weights)


def collect_kernel(count, spread, *refs):
    parts, outs = refs[:count], refs[count:]
    half = parts[0].shape[1] // 2
    for c in range(2):
        for n in range(half // OUT_TILE):
            cols = pl.ds(c * half + n * OUT_TILE, OUT_TILE)
            rows = jnp.concatenate([part[:, cols] for part in parts], axis=0)
            put_rows(jnp.dot(spread[...], rows, preferred_element_type=f32), outs, c, n, half)


def collect(spread, parts, tok):
    dim = parts[0].shape[1]
    count = len(parts)
    return pl.pallas_call(
        functools.partial(collect_kernel, count),
        out_shape=row_shapes(FAR * tok, dim),
        in_specs=[vmem()] * (count + 1),
        out_specs=[vmem()] * 5,
        compiler_params=params(12),
        cost_estimate=cost(2 * spread.size * dim, 8 * FAR * tok * dim),
        name="collect",
    )(spread, *parts)


def reduce_z(own, right, left, ahead, behind):
    size, dim = own.shape
    right = shift_z(right, 1)
    left = shift_z(left, -1)
    ahead = shift_z(ahead, 2)
    behind = shift_z(behind, -2)
    total = own + right.astype(f32) + left.astype(f32)
    total = total + jnp.concatenate([ahead, behind], axis=1).astype(f32)
    sent = total.astype(bf16).reshape(FAR, size // FAR, dim)
    got = lax.all_to_all(sent, "zb", split_axis=0, concat_axis=0, tiled=True)
    return jnp.sum(got.astype(f32), axis=0)


def layer(
    cache_kv,
    new_kv,
    queries,
    lengths,
    resid,
    value_up,
    out_proj,
    norm_gain,
    router,
    expert_ids,
    slots,
    w_gate,
    w_up,
    w_down,
):
    nx = lax.axis_size("x")
    seqs, steps = queries.shape[:2]
    tok = seqs * steps
    where = jnp.stack([lax.axis_index(a) for a in ("x", "zb", "j")]).astype(jnp.int32)

    mine = jnp.concatenate([value_up.T, out_proj], axis=1)
    rows = mine.shape[0]
    from_left = shift_x(mine, 1)
    from_right = shift_x(mine, -1)

    outgoing = context_rows(where, nx, cache_kv, new_kv, queries, lengths)
    from_left, from_right, _ = lax.optimization_barrier((from_left, from_right, outgoing))
    far_a = shift_x(from_left[: rows // 2], 1)
    far_b = shift_x(from_right[rows // 2 :], -1)
    pieces = [mine, swap_core(mine), from_left, swap_core(from_left), from_right, swap_core(from_right)]
    pieces += [far_a, far_b, swap_core(far_a), swap_core(far_b)]
    ffn = (w_gate, swap_core(w_gate), w_up, swap_core(w_up), w_down, swap_core(w_down))
    arrived = lax.all_to_all(
        outgoing.reshape(RING, nx * tok, LAT), ZAX, split_axis=0, concat_axis=0, tiled=True
    )
    arrived = arrived.reshape(RING * nx * tok, LAT)
    attended = reduce_z(*attend_out(where, nx, arrived, pieces, tok))

    hidden = resid.reshape(tok, D).astype(f32) + attended
    mean_square = jnp.mean(hidden * hidden, axis=-1, keepdims=True)
    normed = (hidden * lax.rsqrt(mean_square + norm_eps) * norm_gain.astype(f32)).astype(bf16)

    route_ids = expert_ids.reshape(tok, TOP)
    route_slots = slots.reshape(tok, TOP)
    logits = jnp.dot(normed, router, preferred_element_type=f32)
    is_pick = route_ids[:, :, None] == jnp.arange(EXPERTS, dtype=jnp.int32)[None, None, :]
    picked = jnp.sum(jnp.where(is_pick, logits[:, None, :], 0.0), axis=-1)
    gates = jax.nn.sigmoid(picked)
    weights = route_scale * gates / jnp.sum(gates, axis=1, keepdims=True)
    share = jnp.sum(jnp.where(is_pick, weights[:, :, None], 0.0), axis=1)
    slot = jnp.sum(jnp.where(is_pick, route_slots[:, :, None] + 1, 0), axis=1)
    places = [(slot == s + 1).astype(bf16) for s in range(CAP)]
    high = share.astype(bf16)
    rest = share - high.astype(f32)
    middle = rest.astype(bf16)
    low = (rest - middle.astype(f32)).astype(bf16)
    extra = jnp.concatenate(places + [high, middle, low], axis=1)
    extra = jnp.pad(extra, ((0, 0), (0, EXTRA - extra.shape[1])))
    payload = jnp.concatenate([normed, extra], axis=1)

    ring = lax.all_gather(payload, ZAX, axis=0, tiled=True)
    *sent, spread = dispatch(where, nx, ring, tok)
    from_right = shift_x(sent[1], -1)
    from_left = shift_x(sent[2], 1)
    from_far = shift_x(sent[3], 2)
    done = expert_part(where, (sent[0], from_right, from_left), ffn)
    back_left = shift_x(done[1], 1)
    back_right = shift_x(done[2], -1)
    (far_done,) = expert_part(where, (from_far,), ffn)
    back_far = shift_x(far_done, 2)
    expert_mix = reduce_z(*collect(spread, (done[0], back_left, back_right, back_far), tok))
    mixed = (hidden + expert_mix).astype(bf16)
    return mixed.reshape(resid.shape)


def solution(mesh):
    chips = mesh.shape["ep"] // (RING * CORES)
    grid = mesh.devices.reshape(mesh.shape["rep"], chips, FAR, NEAR, CORES)
    fine = Mesh(grid, ("rep", "x", "zb", "j", "c"))
    ep = ("x", "zb", "j", "c")
    both = ("rep",) + ep
    return jax.shard_map(
        layer,
        mesh=fine,
        in_specs=(
            P(both, None, None),
            P(both, None, None),
            P(both, None, None, None),
            P(both),
            P(both, None, None),
            P(None, ep),
            P(ep, None),
            P(),
            P(),
            P(both, None, None),
            P(both, None, None),
            P(None, ep),
            P(None, ep),
            P(ep, None),
        ),
        out_specs=P(both, None, None),
        check_vma=False,
    )
```

```python
import functools
import math

import jax
import jax.numpy as jnp
from jax import lax
from jax.experimental import pallas as pl
from jax.experimental.pallas import tpu as pltpu
from jax.sharding import Mesh
from jax.sharding import PartitionSpec as P


D = 7168
LAT = 512
VH = 128
EXPERTS = 16
TOP = 8
CAP = 2
QK = 192

CORES = 2
NEAR = 4
FAR = 4
RING = NEAR * FAR
SLOTS = RING * CAP
EXTRA = 128

route_scale = 2.827
norm_eps = 1e-06


ZAX = ("zb", "j")
f32, bf16 = jnp.float32, jnp.bfloat16
NT = (((1,), (1,)), ((), ()))


def shift_x(a, step):
    n = lax.axis_size("x")
    return lax.ppermute(a, "x", [(i, (i + step) % n) for i in range(n)])


def shift_z(a, step):
    return lax.ppermute(a, ZAX, [(i, (i + step) % RING) for i in range(RING)])


def swap_core(a):
    return lax.ppermute(a, "c", [(i, (i + 1) % CORES) for i in range(CORES)])


def iota(shape, axis):
    return lax.broadcasted_iota(jnp.int32, shape, axis)


def one_hot(mask):
    return jnp.where(mask, 1.0, 0.0).astype(bf16)


def column(hop, x, nx):
    step = jnp.where(hop == 1, nx - 1, jnp.where(hop == 2, 1, jnp.where(hop == 3, 2, 0)))
    return lax.rem(x + step, nx)


def chip_at(place, j):
    group, block = place // FAR, lax.rem(place, FAR)
    step = jnp.where(group == 2, NEAR - 1, jnp.where(group == 3, 2, group))
    return NEAR * block + lax.rem(j + step, NEAR)


def smem():
    return pl.BlockSpec(memory_space=pltpu.SMEM)


def vmem():
    return pl.BlockSpec(memory_space=pltpu.VMEM)


def hbm():
    return pl.BlockSpec(memory_space=pltpu.HBM)


def params(mib):
    return pltpu.CompilerParams(vmem_limit_bytes=mib << 20)


def cost(flops, nbytes):
    return pl.CostEstimate(flops=flops, bytes_accessed=nbytes, transcendentals=0)


def context_kernel(nx, where_ref, lengths, keys, queries, new, out, held):
    seq = pl.program_id(0)
    seqs = pl.num_programs(0)
    steps, heads = queries.shape[1], queries.shape[2]
    count = steps * heads
    scale = 1.0 / math.sqrt(QK)
    query = queries[0].reshape(count, queries.shape[3])
    score = jnp.dot(query, keys[0], preferred_element_type=f32) * scale
    score = jnp.where(iota(score.shape, 1) < lengths[seq], score, -jnp.inf)
    wide = query.astype(f32)
    step_of = iota((count, 1), 0) // heads
    latest = []
    peak = jnp.max(score, axis=1, keepdims=True)
    for t in range(steps):
        key = new[0, t : t + 1, :].astype(f32)
        got = jnp.sum(wide * key, axis=1, keepdims=True) * scale
        got = jnp.where(step_of >= t, got, -jnp.inf)
        latest.append(got)
        peak = jnp.maximum(peak, got)
    probs = jnp.exp(score - peak)
    total = jnp.sum(probs, axis=1, keepdims=True)
    latest = [jnp.exp(got - peak) for got in latest]
    for got in latest:
        total = total + got
    share = 1.0 / total
    probs = (probs * share).astype(bf16)
    context = lax.dot_general(probs, keys[0, :LAT, :], NT, preferred_element_type=f32)
    for t, got in enumerate(latest):
        part = (got * share).astype(bf16).astype(f32)
        context = context + part * new[0, t : t + 1, :LAT].astype(f32)
    held[pl.ds(pl.multiple_of(seq * count, count), count), :] = context.astype(bf16)

    @pl.when(seq == seqs - 1)
    def _():
        rows = held.shape[0]
        tok = rows // heads
        shape = (rows, rows)
        to, source = iota(shape, 0), iota(shape, 1)
        hop = lax.rem(to // tok, nx)
        head = column(hop, where_ref[0], nx) * RING + to // (tok * nx)
        take = (lax.rem(to, tok) == source // heads) & (head == lax.rem(source, heads))
        out[...] = jnp.dot(one_hot(take), held[...], preferred_element_type=f32).astype(bf16)


def context_rows(where, nx, cache_kv, new_kv, queries, lengths):
    seqs, length, width = cache_kv.shape
    steps, heads = queries.shape[1:3]
    rows = seqs * steps * heads
    keys = jnp.swapaxes(cache_kv, 1, 2)
    return pl.pallas_call(
        functools.partial(context_kernel, nx),
        grid=(seqs,),
        out_shape=jax.ShapeDtypeStruct((rows, LAT), bf16),
        in_specs=[
            smem(),
            smem(),
            pl.BlockSpec((1, width, length), lambda b: (b, 0, 0)),
            pl.BlockSpec((1, steps, heads, width), lambda b: (b, 0, 0, 0)),
            pl.BlockSpec((1, steps, width), lambda b: (b, 0, 0)),
        ],
        out_specs=pl.BlockSpec((rows, LAT), lambda b: (0, 0)),
        scratch_shapes=[pltpu.VMEM((rows, LAT), bf16)],
        compiler_params=params(60),
        cost_estimate=cost(2 * rows * length * (width + LAT), 2 * cache_kv.size),
        name="context_rows",
    )(where, lengths, keys, queries, new_kv)


def pack_kernel(up, rows, tops, lows, sem):
    half, at = tops.shape[0], up.shape[1]
    copies = []
    for i, out in enumerate((tops, lows)):
        part = pl.ds(i * half, half)
        copies.append(pltpu.make_async_copy(rows.at[part], out.at[:, pl.ds(at, rows.shape[1])], sem.at[i, 0]))
        copies.append(pltpu.make_async_copy(up.at[part], out.at[:, pl.ds(0, at)], sem.at[i, 1]))
    for copy in copies:
        copy.start()
    for copy in copies:
        copy.wait()


def pack(up, rows):
    shape = (rows.shape[0] // 2, up.shape[1] + rows.shape[1])
    return pl.pallas_call(
        pack_kernel,
        out_shape=(jax.ShapeDtypeStruct(shape, bf16),) * 2,
        in_specs=[hbm()] * 2,
        out_specs=[vmem()] * 2,
        scratch_shapes=[pltpu.SemaphoreType.DMA((2, 2))],
        compiler_params=params(4),
        cost_estimate=cost(1, 4 * rows.size),
        name="pack",
    )(up, rows)


OUT_TILE = 512


def put_rows(got, outs, c, n, half):
    own, right, left, ahead, behind = outs
    size = own.shape[0]
    cols = pl.ds(c * half + n * OUT_TILE, OUT_TILE)
    own[:, cols] = got[:size]
    right[:, cols] = got[size : 2 * size].astype(bf16)
    left[:, cols] = got[2 * size : 3 * size].astype(bf16)
    last = ahead if c == 0 else behind
    last[:, pl.ds(n * OUT_TILE, OUT_TILE)] = got[3 * size :].astype(bf16)


def row_shapes(size, dim):
    return (
        jax.ShapeDtypeStruct((size, dim), f32),
        jax.ShapeDtypeStruct((size, dim), bf16),
        jax.ShapeDtypeStruct((size, dim), bf16),
        jax.ShapeDtypeStruct((size, dim // 2), bf16),
        jax.ShapeDtypeStruct((size, dim // 2), bf16),
    )


def attend_kernel(tok, nx, count, first, last, where_ref, arrived, *refs):
    pieces = refs[:count]
    outs, (up, rows, up_sem, row_sem) = refs[count:-4], refs[-4:]
    if last:
        before, outs = outs[0], outs[1:]
    half = rows.shape[1] // 2
    starts = [0]
    for piece in pieces:
        starts.append(starts[-1] + piece.shape[0])

    def up_copy(i):
        return pltpu.make_async_copy(
            pieces[i].at[:, pl.ds(0, LAT)],
            up.at[pl.ds(starts[i], pieces[i].shape[0])],
            up_sem.at[i],
        )

    def row_copy(c, i):
        return pltpu.make_async_copy(
            pieces[i].at[:, pl.ds(LAT + c * half, half)],
            rows.at[pl.ds(starts[i], pieces[i].shape[0]), pl.ds(c * half, half)],
            row_sem.at[c, i],
        )

    for i in range(count):
        up_copy(i).start()
    for c in range(2):
        for i in range(count):
            row_copy(c, i).start()
    for i in range(count):
        up_copy(i).wait()
    values = lax.dot_general(arrived[...], up[...], NT, preferred_element_type=f32)
    hop = lax.rem(iota(values.shape, 0) // tok, nx)
    values = jnp.where(hop == first + iota(values.shape, 1) // VH, values, 0.0).astype(bf16)
    shape = (RING * tok, arrived.shape[0])
    place, source = iota(shape, 0), iota(shape, 1)
    take = (source // (tok * nx) == chip_at(place // tok, where_ref[2])) & (
        lax.rem(source, tok) == lax.rem(place, tok)
    )
    values = jnp.dot(one_hot(take), values, preferred_element_type=f32).astype(bf16)
    for c in range(2):
        for i in range(count):
            row_copy(c, i).wait()
        for n in range(half // OUT_TILE):
            cols = pl.ds(c * half + n * OUT_TILE, OUT_TILE)
            got = jnp.dot(values, rows[:, cols], preferred_element_type=f32)
            if last:
                put_rows(before[:, cols] + got, outs, c, n, half)
            else:
                outs[0][:, cols] = got


def attend_part(where, nx, arrived, pieces, tok, first, before):
    depth = sum(p.shape[0] for p in pieces)
    dim = pieces[0].shape[1] - LAT
    count = len(pieces)
    last = before is not None
    part = jax.ShapeDtypeStruct((RING * tok, dim), f32)
    return pl.pallas_call(
        functools.partial(attend_kernel, tok, nx, count, first, last),
        out_shape=row_shapes(FAR * tok, dim) if last else part,
        in_specs=[smem(), vmem()] + [hbm()] * count + [vmem()] * last,
        out_specs=[vmem()] * 5 if last else vmem(),
        scratch_shapes=[
            pltpu.VMEM((depth, LAT), bf16),
            pltpu.VMEM((depth, dim), bf16),
            pltpu.SemaphoreType.DMA((count,)),
            pltpu.SemaphoreType.DMA((2, count)),
        ],
        compiler_params=params(12),
        cost_estimate=cost(8 * RING * tok * depth * dim, 2 * depth * dim),
        name="attend_part",
    )(where, arrived, *pieces, *([before] if last else []))


def dispatch_kernel(tok, nx, where_ref, tokens, *refs):
    outs, spread = refs[:nx], refs[nx]
    count, width = tokens.shape
    dim = width - EXTRA
    table = tokens[:, pl.ds(dim, EXTRA)]
    shape = (nx * CAP, EXTRA)
    row, place = iota(shape, 0), iota(shape, 1)
    expert = FAR * column(row // CAP, where_ref[0], nx) + where_ref[1]
    hot = one_hot(place == lax.rem(row, CAP) * EXPERTS + expert)
    got = lax.dot_general(hot, table, NT, preferred_element_type=f32)
    shape = (SLOTS, count)
    slot, token = iota(shape, 0), iota(shape, 1)
    parts = []
    for r in range(nx):
        sel = jnp.where(lax.rem(slot, CAP) == 0, got[CAP * r : CAP * r + 1], got[CAP * r + 1 : CAP * r + 2])
        parts.append(jnp.where(slot // CAP == token // tok, sel, 0.0))
    sel = jnp.concatenate(parts, axis=0).astype(bf16)
    for n in range(pl.cdiv(width, OUT_TILE)):
        cols = pl.ds(n * OUT_TILE, min(OUT_TILE, width - n * OUT_TILE))
        rows = jnp.dot(sel, tokens[:, cols], preferred_element_type=f32).astype(bf16)
        for r in range(nx):
            outs[r][:, cols] = rows[r * SLOTS : (r + 1) * SLOTS]
    shape = (count, count)
    place, token = iota(shape, 0), iota(shape, 1)
    take = (token // tok == chip_at(place // tok, where_ref[2])) & (
        lax.rem(token, tok) == lax.rem(place, tok)
    )
    spread[...] = lax.dot_general(one_hot(take), sel, NT, preferred_element_type=f32).astype(bf16)


def dispatch(where, nx, tokens, tok):
    count, width = tokens.shape
    return pl.pallas_call(
        functools.partial(dispatch_kernel, tok, nx),
        out_shape=(jax.ShapeDtypeStruct((SLOTS, width), bf16),) * nx
        + (jax.ShapeDtypeStruct((count, nx * SLOTS), bf16),),
        in_specs=[smem(), vmem()],
        out_specs=[vmem()] * (nx + 1),
        compiler_params=params(12),
        cost_estimate=cost(2 * nx * SLOTS * count * width, 4 * count * width),
        name="dispatch",
    )(where, tokens)


CHUNKS = 7


def stage_kernel(gate_a, gate_b, up_a, up_b, down_a, down_b, wide, deep, sem):
    part = gate_a.shape[1]
    copies = [
        pltpu.make_async_copy(ref, wide.at[:, pl.ds(i * part, part)], sem.at[i])
        for i, ref in enumerate((gate_a, gate_b, up_a, up_b))
    ]
    copies += [
        pltpu.make_async_copy(ref, deep.at[pl.ds(i * part, part)], sem.at[4 + i])
        for i, ref in enumerate((down_a, down_b))
    ]
    for copy in copies:
        copy.start()
    for copy in copies:
        copy.wait()


def stage(weights):
    dim, part = weights[0].shape
    return pl.pallas_call(
        stage_kernel,
        out_shape=(
            jax.ShapeDtypeStruct((dim, 4 * part), bf16),
            jax.ShapeDtypeStruct((2 * part, dim), bf16),
        ),
        in_specs=[hbm()] * 6,
        out_specs=[vmem()] * 2,
        scratch_shapes=[pltpu.SemaphoreType.DMA((6,))],
        compiler_params=params(40),
        cost_estimate=cost(4 * 1000 * dim * part, 12 * dim * part),
        name="stage",
    )(*weights)


def expert_kernel(groups, where_ref, *refs):
    tokens = refs[:groups]
    wide, deep = refs[groups : groups + 2]
    outs = refs[groups + 2 : 2 * groups + 2]
    held = refs[2 * groups + 2] if groups > 1 else tokens[0]
    dim = wide.shape[0]
    part = wide.shape[1] // 2
    chunk = dim // CHUNKS
    if groups > 1:
        for g, ref in enumerate(tokens):
            held[pl.ds(g * SLOTS, SLOTS)] = ref[...]
    total = jnp.dot(held[:, pl.ds(0, dim)], wide[...], preferred_element_type=f32)
    gate, upward = total[:, :part], total[:, part:]
    act = (gate / (1.0 + jnp.exp(-gate)) * upward).astype(bf16)
    shape = (EXTRA, EXTRA)
    expert = FAR * where_ref[0] + where_ref[1]
    from_share = iota(shape, 0) - CAP * EXPERTS
    hot = (from_share >= 0) & (from_share < 3 * EXPERTS) & (lax.rem(from_share + EXTRA, EXPERTS) == expert)
    share = jnp.dot(held[:, pl.ds(dim, EXTRA)], one_hot(hot), preferred_element_type=f32)[:, :1]
    for k in range(CHUNKS):
        cols = pl.ds(k * chunk, chunk)
        got = jnp.dot(act, deep[:, cols], preferred_element_type=f32) * share
        for g in range(groups):
            outs[g][:, cols] = got[g * SLOTS : (g + 1) * SLOTS].astype(bf16)


def expert_part(where, tokens, weights):
    wide, deep = weights
    dim = wide.shape[0]
    groups = len(tokens)
    rows = groups * SLOTS
    held = [pltpu.VMEM((rows, dim + EXTRA), bf16)] if groups > 1 else []
    return pl.pallas_call(
        functools.partial(expert_kernel, groups),
        out_shape=(jax.ShapeDtypeStruct((SLOTS, dim), bf16),) * groups,
        in_specs=[smem()] + [vmem()] * (groups + 2),
        out_specs=[vmem()] * groups,
        scratch_shapes=held,
        compiler_params=params(8),
        cost_estimate=cost(6 * rows * wide.size, 2 * rows * dim),
        name="expert_part",
    )(where, *tokens, wide, deep)


def collect_kernel(count, spread, *refs):
    parts, outs = refs[:count], refs[count:]
    half = parts[0].shape[1] // 2
    for c in range(2):
        for n in range(half // OUT_TILE):
            cols = pl.ds(c * half + n * OUT_TILE, OUT_TILE)
            rows = jnp.concatenate([part[:, cols] for part in parts], axis=0)
            put_rows(jnp.dot(spread[...], rows, preferred_element_type=f32), outs, c, n, half)


def collect(spread, parts, tok):
    dim = parts[0].shape[1]
    count = len(parts)
    return pl.pallas_call(
        functools.partial(collect_kernel, count),
        out_shape=row_shapes(FAR * tok, dim),
        in_specs=[vmem()] * (count + 1),
        out_specs=[vmem()] * 5,
        compiler_params=params(12),
        cost_estimate=cost(2 * spread.size * dim, 8 * FAR * tok * dim),
        name="collect",
    )(spread, *parts)


def reduce_z(own, right, left, ahead, behind):
    size, dim = own.shape
    right = shift_z(right, 1)
    left = shift_z(left, -1)
    ahead = shift_z(ahead, 2)
    behind = shift_z(behind, -2)
    total = own + right.astype(f32) + left.astype(f32)
    total = total + jnp.concatenate([ahead, behind], axis=1).astype(f32)
    sent = total.astype(bf16).reshape(FAR, size // FAR, dim)
    got = lax.all_to_all(sent, "zb", split_axis=0, concat_axis=0, tiled=True)
    return jnp.sum(got.astype(f32), axis=0)


def layer(
    cache_kv,
    new_kv,
    queries,
    lengths,
    resid,
    value_up,
    out_proj,
    norm_gain,
    router,
    expert_ids,
    slots,
    w_gate,
    w_up,
    w_down,
):
    nx = lax.axis_size("x")
    seqs, steps = queries.shape[:2]
    tok = seqs * steps
    where = jnp.stack([lax.axis_index(a) for a in ("x", "zb", "j")]).astype(jnp.int32)

    tops, lows = pack(value_up.T, out_proj)
    top_left = shift_x(tops, 1)
    low_right = shift_x(lows, -1)
    low_left = shift_x(lows, 1)
    top_right = shift_x(tops, -1)

    outgoing = context_rows(where, nx, cache_kv, new_kv, queries, lengths)
    arrived = lax.all_to_all(
        outgoing.reshape(RING, nx * tok, LAT), ZAX, split_axis=0, concat_axis=0, tiled=True
    )
    top_far = shift_x(top_left, 1)
    low_far = shift_x(low_right, -1)
    near = (tops, lows, top_left, low_left, top_right, low_right)
    near = sum(([near[i], near[i + 1], swap_core(near[i]), swap_core(near[i + 1])] for i in (0, 2, 4)), [])
    beyond = [top_far, low_far, swap_core(top_far), swap_core(low_far)]
    weights = stage((w_gate, swap_core(w_gate), w_up, swap_core(w_up), w_down, swap_core(w_down)))
    arrived = arrived.reshape(RING * nx * tok, LAT)
    most = attend_part(where, nx, arrived, near, tok, 0, None)
    attended = reduce_z(*attend_part(where, nx, arrived, beyond, tok, nx - 1, most))

    hidden = resid.reshape(tok, D).astype(f32) + attended
    mean_square = jnp.mean(hidden * hidden, axis=-1, keepdims=True)
    normed = (hidden * lax.rsqrt(mean_square + norm_eps) * norm_gain.astype(f32)).astype(bf16)

    route_ids = expert_ids.reshape(tok, TOP)
    route_slots = slots.reshape(tok, TOP)
    logits = jnp.dot(normed, router, preferred_element_type=f32)
    is_pick = route_ids[:, :, None] == jnp.arange(EXPERTS, dtype=jnp.int32)[None, None, :]
    picked = jnp.sum(jnp.where(is_pick, logits[:, None, :], 0.0), axis=-1)
    gates = jax.nn.sigmoid(picked)
    gates = route_scale * gates / jnp.sum(gates, axis=1, keepdims=True)
    share = jnp.sum(jnp.where(is_pick, gates[:, :, None], 0.0), axis=1)
    slot = jnp.sum(jnp.where(is_pick, route_slots[:, :, None] + 1, 0), axis=1)
    places = [(slot == s + 1).astype(bf16) for s in range(CAP)]
    high = share.astype(bf16)
    rest = share - high.astype(f32)
    middle = rest.astype(bf16)
    low = (rest - middle.astype(f32)).astype(bf16)
    extra = jnp.concatenate(places + [high, middle, low], axis=1)
    extra = jnp.pad(extra, ((0, 0), (0, EXTRA - extra.shape[1])))
    payload = jnp.concatenate([normed, extra], axis=1)

    ring = lax.all_gather(payload, ZAX, axis=0, tiled=True)
    *sent, spread = dispatch(where, nx, ring, tok)
    from_right = shift_x(sent[1], -1)
    from_left = shift_x(sent[2], 1)
    from_far = shift_x(sent[3], 2)
    done = expert_part(where, (sent[0], from_right, from_left), weights)
    back_left = shift_x(done[1], 1)
    back_right = shift_x(done[2], -1)
    (far_done,) = expert_part(where, (from_far,), weights)
    back_far = shift_x(far_done, 2)
    expert_mix = reduce_z(*collect(spread, (done[0], back_left, back_right, back_far), tok))
    mixed = (hidden + expert_mix).astype(bf16)
    return mixed.reshape(resid.shape)


def solution(mesh):
    chips = mesh.shape["ep"] // (RING * CORES)
    grid = mesh.devices.reshape(mesh.shape["rep"], chips, FAR, NEAR, CORES)
    fine = Mesh(grid, ("rep", "x", "zb", "j", "c"))
    ep = ("x", "zb", "j", "c")
    both = ("rep",) + ep
    return jax.shard_map(
        layer,
        mesh=fine,
        in_specs=(
            P(both, None, None),
            P(both, None, None),
            P(both, None, None, None),
            P(both),
            P(both, None, None),
            P(None, ep),
            P(ep, None),
            P(),
            P(),
            P(both, None, None),
            P(both, None, None),
            P(None, ep),
            P(None, ep),
            P(ep, None),
        ),
        out_specs=P(both, None, None),
        check_vma=False,
    )
```

```python
import functools
import math

import jax
import jax.numpy as jnp
from jax import lax
from jax.experimental import pallas as pl
from jax.experimental.pallas import tpu as pltpu
from jax.sharding import Mesh
from jax.sharding import PartitionSpec as P


D = 7168
LAT = 512
VH = 128
EXPERTS = 16
TOP = 8
CAP = 2
QK = 192

CORES = 2
NEAR = 4
FAR = 4
RING = NEAR * FAR
SLOTS = RING * CAP
EXTRA = 128

route_scale = 2.827
norm_eps = 1e-06


ZAX = ("zb", "j")
f32, bf16 = jnp.float32, jnp.bfloat16
NT = (((1,), (1,)), ((), ()))


def shift_x(a, step):
    n = lax.axis_size("x")
    return lax.ppermute(a, "x", [(i, (i + step) % n) for i in range(n)])


def shift_z(a, step):
    return lax.ppermute(a, ZAX, [(i, (i + step) % RING) for i in range(RING)])


def swap_core(a):
    return lax.ppermute(a, "c", [(i, (i + 1) % CORES) for i in range(CORES)])


def iota(shape, axis):
    return lax.broadcasted_iota(jnp.int32, shape, axis)


def one_hot(mask):
    return jnp.where(mask, 1.0, 0.0).astype(bf16)


def column(hop, x, nx):
    step = jnp.where(hop == 1, nx - 1, jnp.where(hop == 2, 1, jnp.where(hop == 3, 2, 0)))
    return lax.rem(x + step, nx)


def chip_at(place, j):
    group, block = place // FAR, lax.rem(place, FAR)
    step = jnp.where(group == 2, NEAR - 1, jnp.where(group == 3, 2, group))
    return NEAR * block + lax.rem(j + step, NEAR)


def smem():
    return pl.BlockSpec(memory_space=pltpu.SMEM)


def vmem():
    return pl.BlockSpec(memory_space=pltpu.VMEM)


def hbm():
    return pl.BlockSpec(memory_space=pltpu.HBM)


def held_in_hbm(a):
    return pltpu.with_memory_space_constraint(a, pltpu.HBM)


def held_in_vmem(a):
    return pltpu.with_memory_space_constraint(a, pltpu.VMEM)


def params(mib):
    return pltpu.CompilerParams(vmem_limit_bytes=mib << 20)


def cost(flops, nbytes):
    return pl.CostEstimate(flops=flops, bytes_accessed=nbytes, transcendentals=0)


def context_kernel(nx, where_ref, lengths, keys, queries, new, out, held):
    seq = pl.program_id(0)
    seqs = pl.num_programs(0)
    steps, heads = queries.shape[1], queries.shape[2]
    count = steps * heads
    scale = 1.0 / math.sqrt(QK)
    query = queries[0].reshape(count, queries.shape[3])
    score = jnp.dot(query, keys[0], preferred_element_type=f32) * scale
    score = jnp.where(iota(score.shape, 1) < lengths[seq], score, -jnp.inf)
    wide = query.astype(f32)
    step_of = iota((count, 1), 0) // heads
    latest = []
    peak = jnp.max(score, axis=1, keepdims=True)
    for t in range(steps):
        key = new[0, t : t + 1, :].astype(f32)
        got = jnp.sum(wide * key, axis=1, keepdims=True) * scale
        got = jnp.where(step_of >= t, got, -jnp.inf)
        latest.append(got)
        peak = jnp.maximum(peak, got)
    probs = jnp.exp(score - peak)
    total = jnp.sum(probs, axis=1, keepdims=True)
    latest = [jnp.exp(got - peak) for got in latest]
    for got in latest:
        total = total + got
    share = 1.0 / total
    probs = (probs * share).astype(bf16)
    context = lax.dot_general(probs, keys[0, :LAT, :], NT, preferred_element_type=f32)
    for t, got in enumerate(latest):
        part = (got * share).astype(bf16).astype(f32)
        context = context + part * new[0, t : t + 1, :LAT].astype(f32)
    held[pl.ds(pl.multiple_of(seq * count, count), count), :] = context.astype(bf16)

    @pl.when(seq == seqs - 1)
    def _():
        rows = held.shape[0]
        tok = rows // heads
        shape = (rows, rows)
        to, source = iota(shape, 0), iota(shape, 1)
        hop = lax.rem(to // tok, nx)
        head = column(hop, where_ref[0], nx) * RING + to // (tok * nx)
        take = (lax.rem(to, tok) == source // heads) & (head == lax.rem(source, heads))
        out[...] = jnp.dot(one_hot(take), held[...], preferred_element_type=f32).astype(bf16)


def context_rows(where, nx, cache_kv, new_kv, queries, lengths):
    seqs, length, width = cache_kv.shape
    steps, heads = queries.shape[1:3]
    rows = seqs * steps * heads
    keys = jnp.swapaxes(cache_kv, 1, 2)
    return pl.pallas_call(
        functools.partial(context_kernel, nx),
        grid=(seqs,),
        out_shape=jax.ShapeDtypeStruct((rows, LAT), bf16),
        in_specs=[
            smem(),
            smem(),
            pl.BlockSpec((1, width, length), lambda b: (b, 0, 0)),
            pl.BlockSpec((1, steps, heads, width), lambda b: (b, 0, 0, 0)),
            pl.BlockSpec((1, steps, width), lambda b: (b, 0, 0)),
        ],
        out_specs=pl.BlockSpec((rows, LAT), lambda b: (0, 0)),
        scratch_shapes=[pltpu.VMEM((rows, LAT), bf16)],
        compiler_params=params(24),
        cost_estimate=cost(2 * rows * length * (width + LAT), 2 * cache_kv.size),
        name="context_rows",
    )(where, lengths, held_in_hbm(keys), held_in_hbm(queries), new_kv)


def pack_kernel(up, rows, tops, lows, sem):
    half, at = tops.shape[0], up.shape[1]
    copies = []
    for i, out in enumerate((tops, lows)):
        part = pl.ds(i * half, half)
        copies.append(pltpu.make_async_copy(rows.at[part], out.at[:, pl.ds(at, rows.shape[1])], sem.at[i, 0]))
        copies.append(pltpu.make_async_copy(up.at[part], out.at[:, pl.ds(0, at)], sem.at[i, 1]))
    for copy in copies:
        copy.start()
    for copy in copies:
        copy.wait()


def pack(up, rows):
    shape = (rows.shape[0] // 2, up.shape[1] + rows.shape[1])
    return pl.pallas_call(
        pack_kernel,
        out_shape=(jax.ShapeDtypeStruct(shape, bf16),) * 2,
        in_specs=[hbm()] * 2,
        out_specs=[vmem()] * 2,
        scratch_shapes=[pltpu.SemaphoreType.DMA((2, 2))],
        compiler_params=params(12),
        cost_estimate=cost(1, 4 * rows.size),
        name="pack",
    )(held_in_hbm(up), held_in_hbm(rows))


OUT_TILE = 512


def put_rows(got, outs, c, n, half):
    own, right, left, ahead, behind = outs
    size = own.shape[0]
    cols = pl.ds(c * half + n * OUT_TILE, OUT_TILE)
    own[:, cols] = got[:size]
    right[:, cols] = got[size : 2 * size].astype(bf16)
    left[:, cols] = got[2 * size : 3 * size].astype(bf16)
    last = ahead if c == 0 else behind
    last[:, pl.ds(n * OUT_TILE, OUT_TILE)] = got[3 * size :].astype(bf16)


def row_shapes(size, dim):
    return (
        jax.ShapeDtypeStruct((size, dim), f32),
        jax.ShapeDtypeStruct((size, dim), bf16),
        jax.ShapeDtypeStruct((size, dim), bf16),
        jax.ShapeDtypeStruct((size, dim // 2), bf16),
        jax.ShapeDtypeStruct((size, dim // 2), bf16),
    )


def attend_kernel(tok, nx, count, first, last, where_ref, arrived, *refs):
    pieces = refs[:count]
    outs, (up, rows, up_sem, row_sem) = refs[count:-4], refs[-4:]
    if last:
        before, outs = outs[0], outs[1:]
    half = rows.shape[1] // 2
    starts = [0]
    for piece in pieces:
        starts.append(starts[-1] + piece.shape[0])

    def up_copy(i):
        return pltpu.make_async_copy(
            pieces[i].at[:, pl.ds(0, LAT)],
            up.at[pl.ds(starts[i], pieces[i].shape[0])],
            up_sem.at[i],
        )

    def row_copy(c, i):
        return pltpu.make_async_copy(
            pieces[i].at[:, pl.ds(LAT + c * half, half)],
            rows.at[pl.ds(starts[i], pieces[i].shape[0]), pl.ds(c * half, half)],
            row_sem.at[c, i],
        )

    for i in range(count):
        up_copy(i).start()
    for c in range(2):
        for i in range(count):
            row_copy(c, i).start()
    for i in range(count):
        up_copy(i).wait()
    values = lax.dot_general(arrived[...], up[...], NT, preferred_element_type=f32)
    hop = lax.rem(iota(values.shape, 0) // tok, nx)
    values = jnp.where(hop == first + iota(values.shape, 1) // VH, values, 0.0).astype(bf16)
    shape = (RING * tok, arrived.shape[0])
    place, source = iota(shape, 0), iota(shape, 1)
    take = (source // (tok * nx) == chip_at(place // tok, where_ref[2])) & (
        lax.rem(source, tok) == lax.rem(place, tok)
    )
    values = jnp.dot(one_hot(take), values, preferred_element_type=f32).astype(bf16)
    for c in range(2):
        for i in range(count):
            row_copy(c, i).wait()
        for n in range(half // OUT_TILE):
            cols = pl.ds(c * half + n * OUT_TILE, OUT_TILE)
            got = jnp.dot(values, rows[:, cols], preferred_element_type=f32)
            if last:
                put_rows(before[:, cols] + got, outs, c, n, half)
            else:
                outs[0][:, cols] = got


def attend_part(where, nx, arrived, pieces, tok, first, before):
    depth = sum(p.shape[0] for p in pieces)
    dim = pieces[0].shape[1] - LAT
    count = len(pieces)
    last = before is not None
    part = jax.ShapeDtypeStruct((RING * tok, dim), f32)
    return pl.pallas_call(
        functools.partial(attend_kernel, tok, nx, count, first, last),
        out_shape=row_shapes(FAR * tok, dim) if last else part,
        in_specs=[smem(), vmem()] + [hbm()] * count + [vmem()] * last,
        out_specs=[vmem()] * 5 if last else vmem(),
        scratch_shapes=[
            pltpu.VMEM((depth, LAT), bf16),
            pltpu.VMEM((depth, dim), bf16),
            pltpu.SemaphoreType.DMA((count,)),
            pltpu.SemaphoreType.DMA((2, count)),
        ],
        compiler_params=params(12),
        cost_estimate=cost(8 * RING * tok * depth * dim, 2 * depth * dim),
        name="attend_part",
    )(where, arrived, *[held_in_hbm(p) for p in pieces], *([before] if last else []))


def dispatch_kernel(tok, nx, where_ref, tokens, *refs):
    outs, spread = refs[:nx], refs[nx]
    count, width = tokens.shape
    dim = width - EXTRA
    table = tokens[:, pl.ds(dim, EXTRA)]
    shape = (nx * CAP, EXTRA)
    row, place = iota(shape, 0), iota(shape, 1)
    expert = FAR * column(row // CAP, where_ref[0], nx) + where_ref[1]
    hot = one_hot(place == lax.rem(row, CAP) * EXPERTS + expert)
    got = lax.dot_general(hot, table, NT, preferred_element_type=f32)
    shape = (SLOTS, count)
    slot, token = iota(shape, 0), iota(shape, 1)
    parts = []
    for r in range(nx):
        sel = jnp.where(lax.rem(slot, CAP) == 0, got[CAP * r : CAP * r + 1], got[CAP * r + 1 : CAP * r + 2])
        parts.append(jnp.where(slot // CAP == token // tok, sel, 0.0))
    sel = jnp.concatenate(parts, axis=0).astype(bf16)
    for n in range(pl.cdiv(width, OUT_TILE)):
        cols = pl.ds(n * OUT_TILE, min(OUT_TILE, width - n * OUT_TILE))
        rows = jnp.dot(sel, tokens[:, cols], preferred_element_type=f32).astype(bf16)
        for r in range(nx):
            outs[r][:, cols] = rows[r * SLOTS : (r + 1) * SLOTS]
    shape = (count, count)
    place, token = iota(shape, 0), iota(shape, 1)
    take = (token // tok == chip_at(place // tok, where_ref[2])) & (
        lax.rem(token, tok) == lax.rem(place, tok)
    )
    spread[...] = lax.dot_general(one_hot(take), sel, NT, preferred_element_type=f32).astype(bf16)


def dispatch(where, nx, tokens, tok):
    count, width = tokens.shape
    return pl.pallas_call(
        functools.partial(dispatch_kernel, tok, nx),
        out_shape=(jax.ShapeDtypeStruct((SLOTS, width), bf16),) * nx
        + (jax.ShapeDtypeStruct((count, nx * SLOTS), bf16),),
        in_specs=[smem(), vmem()],
        out_specs=[vmem()] * (nx + 1),
        compiler_params=params(12),
        cost_estimate=cost(2 * nx * SLOTS * count * width, 4 * count * width),
        name="dispatch",
    )(where, tokens)


CHUNKS = 7


def stage_kernel(gate_a, gate_b, up_a, up_b, down_a, down_b, wide, deep, sem):
    part = gate_a.shape[1]
    copies = [
        pltpu.make_async_copy(ref, wide.at[:, pl.ds(i * part, part)], sem.at[i])
        for i, ref in enumerate((gate_a, gate_b, up_a, up_b))
    ]
    copies += [
        pltpu.make_async_copy(ref, deep.at[pl.ds(i * part, part)], sem.at[4 + i])
        for i, ref in enumerate((down_a, down_b))
    ]
    for copy in copies:
        copy.start()
    for copy in copies:
        copy.wait()


def stage(weights):
    dim, part = weights[0].shape
    return pl.pallas_call(
        stage_kernel,
        out_shape=(
            jax.ShapeDtypeStruct((dim, 4 * part), bf16),
            jax.ShapeDtypeStruct((2 * part, dim), bf16),
        ),
        in_specs=[hbm()] * 6,
        out_specs=[vmem()] * 2,
        scratch_shapes=[pltpu.SemaphoreType.DMA((6,))],
        compiler_params=params(4),
        cost_estimate=cost(4 * 1000 * dim * part, 12 * dim * part),
        name="stage",
    )(*[held_in_hbm(w) for w in weights])


def expert_kernel(groups, where_ref, *refs):
    tokens = refs[:groups]
    wide, deep = refs[groups : groups + 2]
    outs = refs[groups + 2 : 2 * groups + 2]
    held = refs[2 * groups + 2] if groups > 1 else tokens[0]
    dim = wide.shape[0]
    part = wide.shape[1] // 2
    chunk = dim // CHUNKS
    if groups > 1:
        for g, ref in enumerate(tokens):
            held[pl.ds(g * SLOTS, SLOTS)] = ref[...]
    total = jnp.dot(held[:, pl.ds(0, dim)], wide[...], preferred_element_type=f32)
    gate, upward = total[:, :part], total[:, part:]
    act = (gate / (1.0 + jnp.exp(-gate)) * upward).astype(bf16)
    shape = (EXTRA, EXTRA)
    expert = FAR * where_ref[0] + where_ref[1]
    from_share = iota(shape, 0) - CAP * EXPERTS
    hot = (from_share >= 0) & (from_share < 3 * EXPERTS) & (lax.rem(from_share + EXTRA, EXPERTS) == expert)
    share = jnp.dot(held[:, pl.ds(dim, EXTRA)], one_hot(hot), preferred_element_type=f32)[:, :1]
    for k in range(CHUNKS):
        cols = pl.ds(k * chunk, chunk)
        got = jnp.dot(act, deep[:, cols], preferred_element_type=f32) * share
        for g in range(groups):
            outs[g][:, cols] = got[g * SLOTS : (g + 1) * SLOTS].astype(bf16)


def expert_part(where, tokens, weights):
    wide, deep = weights
    dim = wide.shape[0]
    groups = len(tokens)
    rows = groups * SLOTS
    held = [pltpu.VMEM((rows, dim + EXTRA), bf16)] if groups > 1 else []
    return pl.pallas_call(
        functools.partial(expert_kernel, groups),
        out_shape=(jax.ShapeDtypeStruct((SLOTS, dim), bf16),) * groups,
        in_specs=[smem()] + [vmem()] * (groups + 2),
        out_specs=[vmem()] * groups,
        scratch_shapes=held,
        compiler_params=params(8),
        cost_estimate=cost(6 * rows * wide.size, 2 * rows * dim),
        name="expert_part",
    )(where, *tokens, held_in_vmem(wide), held_in_vmem(deep))


def collect_kernel(count, spread, *refs):
    parts, outs = refs[:count], refs[count:]
    half = parts[0].shape[1] // 2
    for c in range(2):
        for n in range(half // OUT_TILE):
            cols = pl.ds(c * half + n * OUT_TILE, OUT_TILE)
            rows = jnp.concatenate([part[:, cols] for part in parts], axis=0)
            put_rows(jnp.dot(spread[...], rows, preferred_element_type=f32), outs, c, n, half)


def collect(spread, parts, tok):
    dim = parts[0].shape[1]
    count = len(parts)
    return pl.pallas_call(
        functools.partial(collect_kernel, count),
        out_shape=row_shapes(FAR * tok, dim),
        in_specs=[vmem()] * (count + 1),
        out_specs=[vmem()] * 5,
        compiler_params=params(12),
        cost_estimate=cost(2 * spread.size * dim, 8 * FAR * tok * dim),
        name="collect",
    )(spread, *parts)


def reduce_z(own, right, left, ahead, behind):
    size, dim = own.shape
    right = shift_z(right, 1)
    left = shift_z(left, -1)
    ahead = shift_z(ahead, 2)
    behind = shift_z(behind, -2)
    total = own + right.astype(f32) + left.astype(f32)
    total = total + jnp.concatenate([ahead, behind], axis=1).astype(f32)
    sent = total.astype(bf16).reshape(FAR, size // FAR, dim)
    got = lax.all_to_all(sent, "zb", split_axis=0, concat_axis=0, tiled=True)
    return jnp.sum(got.astype(f32), axis=0)


def layer(
    cache_kv,
    new_kv,
    queries,
    lengths,
    resid,
    value_up,
    out_proj,
    norm_gain,
    router,
    expert_ids,
    slots,
    w_gate,
    w_up,
    w_down,
):
    nx = lax.axis_size("x")
    seqs, steps = queries.shape[:2]
    tok = seqs * steps
    where = jnp.stack([lax.axis_index(a) for a in ("x", "zb", "j")]).astype(jnp.int32)

    tops, lows = pack(value_up.T, out_proj)
    top_left = shift_x(tops, 1)
    low_right = shift_x(lows, -1)
    low_left = shift_x(lows, 1)
    top_right = shift_x(tops, -1)

    outgoing = context_rows(where, nx, cache_kv, new_kv, queries, lengths)
    arrived = lax.all_to_all(
        outgoing.reshape(RING, nx * tok, LAT), ZAX, split_axis=0, concat_axis=0, tiled=True
    )
    top_far = shift_x(top_left, 1)
    low_far = shift_x(low_right, -1)
    near = (tops, lows, top_left, low_left, top_right, low_right)
    near = sum(([near[i], near[i + 1], swap_core(near[i]), swap_core(near[i + 1])] for i in (0, 2, 4)), [])
    beyond = [top_far, low_far, swap_core(top_far), swap_core(low_far)]
    weights = stage((w_gate, swap_core(w_gate), w_up, swap_core(w_up), w_down, swap_core(w_down)))
    arrived = arrived.reshape(RING * nx * tok, LAT)
    most = attend_part(where, nx, arrived, near, tok, 0, None)
    attended = reduce_z(*attend_part(where, nx, arrived, beyond, tok, nx - 1, most))

    hidden = resid.reshape(tok, D).astype(f32) + attended
    mean_square = jnp.mean(hidden * hidden, axis=-1, keepdims=True)
    normed = (hidden * lax.rsqrt(mean_square + norm_eps) * norm_gain.astype(f32)).astype(bf16)

    route_ids = expert_ids.reshape(tok, TOP)
    route_slots = slots.reshape(tok, TOP)
    logits = jnp.dot(normed, router, preferred_element_type=f32)
    is_pick = route_ids[:, :, None] == jnp.arange(EXPERTS, dtype=jnp.int32)[None, None, :]
    picked = jnp.sum(jnp.where(is_pick, logits[:, None, :], 0.0), axis=-1)
    gates = jax.nn.sigmoid(picked)
    gates = route_scale * gates / jnp.sum(gates, axis=1, keepdims=True)
    share = jnp.sum(jnp.where(is_pick, gates[:, :, None], 0.0), axis=1)
    slot = jnp.sum(jnp.where(is_pick, route_slots[:, :, None] + 1, 0), axis=1)
    places = [(slot == s + 1).astype(bf16) for s in range(CAP)]
    high = share.astype(bf16)
    rest = share - high.astype(f32)
    middle = rest.astype(bf16)
    low = (rest - middle.astype(f32)).astype(bf16)
    extra = jnp.concatenate(places + [high, middle, low], axis=1)
    extra = jnp.pad(extra, ((0, 0), (0, EXTRA - extra.shape[1])))
    payload = jnp.concatenate([normed, extra], axis=1)

    ring = lax.all_gather(payload, ZAX, axis=0, tiled=True)
    *sent, spread = dispatch(where, nx, ring, tok)
    from_right = shift_x(sent[1], -1)
    from_left = shift_x(sent[2], 1)
    from_far = shift_x(sent[3], 2)
    done = expert_part(where, (sent[0], from_right, from_left), weights)
    back_left = shift_x(done[1], 1)
    back_right = shift_x(done[2], -1)
    (far_done,) = expert_part(where, (from_far,), weights)
    back_far = shift_x(far_done, 2)
    expert_mix = reduce_z(*collect(spread, (done[0], back_left, back_right, back_far), tok))
    mixed = (hidden + expert_mix).astype(bf16)
    return mixed.reshape(resid.shape)


def solution(mesh):
    chips = mesh.shape["ep"] // (RING * CORES)
    grid = mesh.devices.reshape(mesh.shape["rep"], chips, FAR, NEAR, CORES)
    fine = Mesh(grid, ("rep", "x", "zb", "j", "c"))
    ep = ("x", "zb", "j", "c")
    both = ("rep",) + ep
    return jax.shard_map(
        layer,
        mesh=fine,
        in_specs=(
            P(both, None, None),
            P(both, None, None),
            P(both, None, None, None),
            P(both),
            P(both, None, None),
            P(None, ep),
            P(ep, None),
            P(),
            P(),
            P(both, None, None),
            P(both, None, None),
            P(None, ep),
            P(None, ep),
            P(ep, None),
        ),
        out_specs=P(both, None, None),
        check_vma=False,
    )
```

```python
import functools
import math

import jax
import jax.numpy as jnp
from jax import lax
from jax.experimental import pallas as pl
from jax.experimental.pallas import tpu as pltpu
from jax.sharding import Mesh
from jax.sharding import PartitionSpec as P


D = 7168
LAT = 512
VH = 128
EXPERTS = 16
TOP = 8
CAP = 2
QK = 192

CORES = 2
NEAR = 4
FAR = 4
RING = NEAR * FAR
SLOTS = RING * CAP
EXTRA = 128

route_scale = 2.827
norm_eps = 1e-06


ZAX = ("zb", "j")
f32, bf16 = jnp.float32, jnp.bfloat16
NT = (((1,), (1,)), ((), ()))


def shift_x(a, step):
    n = lax.axis_size("x")
    return lax.ppermute(a, "x", [(i, (i + step) % n) for i in range(n)])


def shift_z(a, step):
    return lax.ppermute(a, ZAX, [(i, (i + step) % RING) for i in range(RING)])


def swap_core(a):
    return lax.ppermute(a, "c", [(i, (i + 1) % CORES) for i in range(CORES)])


def iota(shape, axis):
    return lax.broadcasted_iota(jnp.int32, shape, axis)


def one_hot(mask):
    return jnp.where(mask, 1.0, 0.0).astype(bf16)


def column(hop, x, nx):
    step = jnp.where(hop == 1, nx - 1, jnp.where(hop == 2, 1, jnp.where(hop == 3, 2, 0)))
    return lax.rem(x + step, nx)


def chip_at(place, j):
    group, block = place // FAR, lax.rem(place, FAR)
    step = jnp.where(group == 2, NEAR - 1, jnp.where(group == 3, 2, group))
    return NEAR * block + lax.rem(j + step, NEAR)


def smem():
    return pl.BlockSpec(memory_space=pltpu.SMEM)


def vmem():
    return pl.BlockSpec(memory_space=pltpu.VMEM)


def hbm():
    return pl.BlockSpec(memory_space=pltpu.HBM)


def held_in_hbm(a):
    return pltpu.with_memory_space_constraint(a, pltpu.HBM)


def held_in_vmem(a):
    return pltpu.with_memory_space_constraint(a, pltpu.VMEM)


def params(mib):
    return pltpu.CompilerParams(vmem_limit_bytes=mib << 20)


def cost(flops, nbytes):
    return pl.CostEstimate(flops=flops, bytes_accessed=nbytes, transcendentals=0)


def context_kernel(nx, where_ref, lengths, keys, queries, new, out, held):
    seq = pl.program_id(0)
    seqs = pl.num_programs(0)
    steps, heads = queries.shape[1], queries.shape[2]
    count = steps * heads
    scale = 1.0 / math.sqrt(QK)
    query = queries[0].reshape(count, queries.shape[3])
    score = jnp.dot(query, keys[0], preferred_element_type=f32) * scale
    score = jnp.where(iota(score.shape, 1) < lengths[seq], score, -jnp.inf)
    wide = query.astype(f32)
    step_of = iota((count, 1), 0) // heads
    latest = []
    peak = jnp.max(score, axis=1, keepdims=True)
    for t in range(steps):
        key = new[0, t : t + 1, :].astype(f32)
        got = jnp.sum(wide * key, axis=1, keepdims=True) * scale
        got = jnp.where(step_of >= t, got, -jnp.inf)
        latest.append(got)
        peak = jnp.maximum(peak, got)
    probs = jnp.exp(score - peak)
    total = jnp.sum(probs, axis=1, keepdims=True)
    latest = [jnp.exp(got - peak) for got in latest]
    for got in latest:
        total = total + got
    share = 1.0 / total
    probs = (probs * share).astype(bf16)
    context = lax.dot_general(probs, keys[0, :LAT, :], NT, preferred_element_type=f32)
    for t, got in enumerate(latest):
        part = (got * share).astype(bf16).astype(f32)
        context = context + part * new[0, t : t + 1, :LAT].astype(f32)
    held[pl.ds(pl.multiple_of(seq * count, count), count), :] = context.astype(bf16)

    @pl.when(seq == seqs - 1)
    def _():
        rows = held.shape[0]
        tok = rows // heads
        shape = (rows, rows)
        to, source = iota(shape, 0), iota(shape, 1)
        hop = lax.rem(to // tok, nx)
        head = column(hop, where_ref[0], nx) * RING + to // (tok * nx)
        take = (lax.rem(to, tok) == source // heads) & (head == lax.rem(source, heads))
        out[...] = jnp.dot(one_hot(take), held[...], preferred_element_type=f32).astype(bf16)


def context_rows(where, nx, cache_kv, new_kv, queries, lengths):
    seqs, length, width = cache_kv.shape
    steps, heads = queries.shape[1:3]
    rows = seqs * steps * heads
    keys = jnp.swapaxes(cache_kv, 1, 2)
    return pl.pallas_call(
        functools.partial(context_kernel, nx),
        grid=(seqs,),
        out_shape=jax.ShapeDtypeStruct((rows, LAT), bf16),
        in_specs=[
            smem(),
            smem(),
            pl.BlockSpec((1, width, length), lambda b: (b, 0, 0)),
            pl.BlockSpec((1, steps, heads, width), lambda b: (b, 0, 0, 0)),
            pl.BlockSpec((1, steps, width), lambda b: (b, 0, 0)),
        ],
        out_specs=pl.BlockSpec((rows, LAT), lambda b: (0, 0)),
        scratch_shapes=[pltpu.VMEM((rows, LAT), bf16)],
        compiler_params=params(24),
        cost_estimate=cost(2 * rows * length * (width + LAT), 2 * cache_kv.size),
        name="context_rows",
    )(where, lengths, held_in_hbm(keys), held_in_hbm(queries), new_kv)


def pack_kernel(up, rows, tops, lows, sem):
    half, at = tops.shape[0], up.shape[1]
    copies = []
    for i, out in enumerate((tops, lows)):
        part = pl.ds(i * half, half)
        copies.append(pltpu.make_async_copy(rows.at[part], out.at[:, pl.ds(at, rows.shape[1])], sem.at[i, 0]))
        copies.append(pltpu.make_async_copy(up.at[part], out.at[:, pl.ds(0, at)], sem.at[i, 1]))
    for copy in copies:
        copy.start()
    for copy in copies:
        copy.wait()


def pack(up, rows):
    shape = (rows.shape[0] // 2, up.shape[1] + rows.shape[1])
    return pl.pallas_call(
        pack_kernel,
        out_shape=(jax.ShapeDtypeStruct(shape, bf16),) * 2,
        in_specs=[hbm()] * 2,
        out_specs=[vmem()] * 2,
        scratch_shapes=[pltpu.SemaphoreType.DMA((2, 2))],
        compiler_params=params(12),
        cost_estimate=cost(1, 4 * rows.size),
        name="pack",
    )(held_in_hbm(up), held_in_hbm(rows))


HALVES = 2
TILE = 256


def put_rows(got, outs, n):
    own, right, left, ahead, behind = outs
    size, width = own.shape[0], ahead.shape[1]
    cols = pl.ds(n * TILE, TILE)
    own[:, cols] = got[:size]
    right[:, cols] = got[size : 2 * size].astype(bf16)
    left[:, cols] = got[2 * size : 3 * size].astype(bf16)
    last, at = (ahead, n * TILE) if n * TILE < width else (behind, n * TILE - width)
    last[:, pl.ds(at, TILE)] = got[3 * size :].astype(bf16)


def row_shapes(size, width):
    return (
        jax.ShapeDtypeStruct((size, width), f32),
        jax.ShapeDtypeStruct((size, width), bf16),
        jax.ShapeDtypeStruct((size, width), bf16),
        jax.ShapeDtypeStruct((size, width // 2), bf16),
        jax.ShapeDtypeStruct((size, width // 2), bf16),
    )


def tiles_of(parts, at, n):
    half = (parts[0].shape[1] - at) // HALVES
    got = [p[:, pl.ds(at + c * half + n * TILE, TILE)] for c in range(HALVES) for p in parts]
    return jnp.concatenate(got, axis=0)


def attend_kernel(tok, nx, count, first, last, where_ref, arrived, *refs):
    pieces, outs = refs[:count], refs[count:]
    if last:
        before, outs = outs[0], outs[1:]
    up = jnp.concatenate([piece[:, pl.ds(0, LAT)] for piece in pieces], axis=0)
    values = lax.dot_general(arrived[...], up, NT, preferred_element_type=f32)
    hop = lax.rem(iota(values.shape, 0) // tok, nx)
    values = jnp.where(hop == first + iota(values.shape, 1) // VH, values, 0.0).astype(bf16)
    shape = (RING * HALVES * tok, arrived.shape[0])
    row, source = iota(shape, 0), iota(shape, 1)
    chip = chip_at(row // (HALVES * tok), where_ref[2])
    take = (source // (tok * nx) == chip) & (lax.rem(source, tok) == lax.rem(row, tok))
    half = lax.rem(row // tok, HALVES)
    taken = [
        jnp.dot(one_hot(take & (half == c)), values, preferred_element_type=f32).astype(bf16)
        for c in range(HALVES)
    ]
    values = jnp.concatenate(taken, axis=1)
    for n in range(outs[0].shape[1] // TILE):
        got = jnp.dot(values, tiles_of(pieces, LAT, n), preferred_element_type=f32)
        cols = pl.ds(n * TILE, TILE)
        if last:
            put_rows(before[:, cols] + got, outs, n)
        else:
            outs[0][:, cols] = got


def attend_part(where, nx, arrived, pieces, tok, first, before):
    depth = sum(p.shape[0] for p in pieces)
    width = (pieces[0].shape[1] - LAT) // HALVES
    count = len(pieces)
    last = before is not None
    part = jax.ShapeDtypeStruct((RING * HALVES * tok, width), f32)
    return pl.pallas_call(
        functools.partial(attend_kernel, tok, nx, count, first, last),
        out_shape=row_shapes(FAR * HALVES * tok, width) if last else part,
        in_specs=[smem(), vmem()] + [vmem()] * count + [vmem()] * last,
        out_specs=[vmem()] * 5 if last else vmem(),
        compiler_params=params(6),
        cost_estimate=cost(8 * RING * tok * depth * width * HALVES, 4 * depth * width),
        name="attend_part",
    )(where, arrived, *[held_in_vmem(p) for p in pieces], *([before] if last else []))


SEND_TILE = 512


def dispatch_kernel(tok, nx, where_ref, tokens, *refs):
    outs, spread = refs[:nx], refs[nx]
    count, width = tokens.shape
    half = width - EXTRA
    table = tokens[:, pl.ds(half, EXTRA)]
    shape = (nx * CAP, EXTRA)
    row, place = iota(shape, 0), iota(shape, 1)
    expert = FAR * column(row // CAP, where_ref[0], nx) + where_ref[1]
    hot = one_hot(place == lax.rem(row, CAP) * EXPERTS + expert)
    got = lax.dot_general(hot, table, NT, preferred_element_type=f32)
    shape = (SLOTS, count)
    slot, token = iota(shape, 0), iota(shape, 1)
    parts = []
    for r in range(nx):
        sel = jnp.where(lax.rem(slot, CAP) == 0, got[CAP * r : CAP * r + 1], got[CAP * r + 1 : CAP * r + 2])
        parts.append(jnp.where(slot // CAP == token // (HALVES * tok), sel, 0.0))
    sel = jnp.concatenate(parts, axis=0)
    of_half = lax.rem(iota(sel.shape, 1) // tok, HALVES)
    sels = [jnp.where(of_half == c, sel, 0.0).astype(bf16) for c in range(HALVES)]
    both = jnp.concatenate(sels, axis=0)
    rows = nx * SLOTS
    for n in range(half // SEND_TILE):
        got = jnp.dot(both, tokens[:, pl.ds(n * SEND_TILE, SEND_TILE)], preferred_element_type=f32).astype(bf16)
        for c in range(HALVES):
            for r in range(nx):
                at = c * rows + r * SLOTS
                outs[r][:, pl.ds(c * half + n * SEND_TILE, SEND_TILE)] = got[at : at + SLOTS]
    got = jnp.dot(sels[0], table, preferred_element_type=f32).astype(bf16)
    for r in range(nx):
        outs[r][:, pl.ds(HALVES * half, EXTRA)] = got[r * SLOTS : (r + 1) * SLOTS]
    shape = (count, count)
    row, token = iota(shape, 0), iota(shape, 1)
    chip = chip_at(row // (HALVES * tok), where_ref[2])
    take = (token // (HALVES * tok) == chip) & (lax.rem(token, HALVES * tok) == lax.rem(row, HALVES * tok))
    for c in range(HALVES):
        got = lax.dot_general(one_hot(take), sels[c], NT, preferred_element_type=f32)
        spread[:, pl.ds(c * rows, rows)] = got.astype(bf16)


def dispatch(where, nx, tokens, tok):
    count, width = tokens.shape
    full = HALVES * (width - EXTRA) + EXTRA
    return pl.pallas_call(
        functools.partial(dispatch_kernel, tok, nx),
        out_shape=(jax.ShapeDtypeStruct((SLOTS, full), bf16),) * nx
        + (jax.ShapeDtypeStruct((count, HALVES * nx * SLOTS), bf16),),
        in_specs=[smem(), vmem()],
        out_specs=[vmem()] * (nx + 1),
        compiler_params=params(12),
        cost_estimate=cost(2 * nx * SLOTS * count * full, 4 * count * width),
        name="dispatch",
    )(where, tokens)


CHUNKS = 7


def stage_kernel(gate_a, gate_b, up_a, up_b, down_a, down_b, wide, deep, sem):
    part = gate_a.shape[1]
    copies = [
        pltpu.make_async_copy(ref, wide.at[:, pl.ds(i * part, part)], sem.at[i])
        for i, ref in enumerate((gate_a, gate_b, up_a, up_b))
    ]
    copies += [
        pltpu.make_async_copy(ref, deep.at[pl.ds(i * part, part)], sem.at[4 + i])
        for i, ref in enumerate((down_a, down_b))
    ]
    for copy in copies:
        copy.start()
    for copy in copies:
        copy.wait()


def stage(weights):
    dim, part = weights[0].shape
    return pl.pallas_call(
        stage_kernel,
        out_shape=(
            jax.ShapeDtypeStruct((dim, 4 * part), bf16),
            jax.ShapeDtypeStruct((2 * part, dim), bf16),
        ),
        in_specs=[hbm()] * 6,
        out_specs=[vmem()] * 2,
        scratch_shapes=[pltpu.SemaphoreType.DMA((6,))],
        compiler_params=params(4),
        cost_estimate=cost(4 * 1000 * dim * part, 12 * dim * part),
        name="stage",
    )(*[held_in_hbm(w) for w in weights])


def expert_kernel(groups, where_ref, *refs):
    tokens = refs[:groups]
    wide, deep = refs[groups : groups + 2]
    outs = refs[groups + 2 : 2 * groups + 2]
    held = refs[2 * groups + 2] if groups > 1 else tokens[0]
    dim = wide.shape[0]
    part = wide.shape[1] // 2
    chunk = dim // CHUNKS
    if groups > 1:
        for g, ref in enumerate(tokens):
            held[pl.ds(g * SLOTS, SLOTS)] = ref[...]
    total = jnp.dot(held[:, pl.ds(0, dim)], wide[...], preferred_element_type=f32)
    gate, upward = total[:, :part], total[:, part:]
    act = (gate / (1.0 + jnp.exp(-gate)) * upward).astype(bf16)
    shape = (EXTRA, EXTRA)
    expert = FAR * where_ref[0] + where_ref[1]
    from_share = iota(shape, 0) - CAP * EXPERTS
    hot = (from_share >= 0) & (from_share < 3 * EXPERTS) & (lax.rem(from_share + EXTRA, EXPERTS) == expert)
    share = jnp.dot(held[:, pl.ds(dim, EXTRA)], one_hot(hot), preferred_element_type=f32)[:, :1]
    for k in range(CHUNKS):
        cols = pl.ds(k * chunk, chunk)
        got = jnp.dot(act, deep[:, cols], preferred_element_type=f32) * share
        for g in range(groups):
            outs[g][:, cols] = got[g * SLOTS : (g + 1) * SLOTS].astype(bf16)


def expert_part(where, tokens, weights):
    wide, deep = weights
    dim = wide.shape[0]
    groups = len(tokens)
    rows = groups * SLOTS
    held = [pltpu.VMEM((rows, dim + EXTRA), bf16)] if groups > 1 else []
    return pl.pallas_call(
        functools.partial(expert_kernel, groups),
        out_shape=(jax.ShapeDtypeStruct((SLOTS, dim), bf16),) * groups,
        in_specs=[smem()] + [vmem()] * (groups + 2),
        out_specs=[vmem()] * groups,
        scratch_shapes=held,
        compiler_params=params(8),
        cost_estimate=cost(6 * rows * wide.size, 2 * rows * dim),
        name="expert_part",
    )(where, *tokens, held_in_vmem(wide), held_in_vmem(deep))


def collect_kernel(count, spread, *refs):
    parts, outs = refs[:count], refs[count:]
    for n in range(outs[0].shape[1] // TILE):
        put_rows(jnp.dot(spread[...], tiles_of(parts, 0, n), preferred_element_type=f32), outs, n)


def collect(spread, parts):
    width = parts[0].shape[1] // HALVES
    count = len(parts)
    return pl.pallas_call(
        functools.partial(collect_kernel, count),
        out_shape=row_shapes(spread.shape[0] // NEAR, width),
        in_specs=[vmem()] * (count + 1),
        out_specs=[vmem()] * 5,
        compiler_params=params(12),
        cost_estimate=cost(2 * spread.size * width, 4 * spread.shape[0] * width),
        name="collect",
    )(spread, *parts)


def reduce_z(own, right, left, ahead, behind):
    size, width = own.shape
    ahead = shift_z(ahead, 2)
    behind = shift_z(behind, -2)
    right = shift_z(right, 1)
    left = shift_z(left, -1)
    total = own + right.astype(f32) + left.astype(f32)
    total = total + jnp.concatenate([ahead, behind], axis=1).astype(f32)
    sent = total.astype(bf16).reshape(FAR, size // FAR, width)
    got = lax.all_to_all(sent, "zb", split_axis=0, concat_axis=0, tiled=True)
    return jnp.sum(got.astype(f32), axis=0)


def layer(
    cache_kv,
    new_kv,
    queries,
    lengths,
    resid,
    value_up,
    out_proj,
    norm_gain,
    router,
    expert_ids,
    slots,
    w_gate,
    w_up,
    w_down,
):
    nx = lax.axis_size("x")
    seqs, steps = queries.shape[:2]
    tok = seqs * steps
    where = jnp.stack([lax.axis_index(a) for a in ("x", "zb", "j")]).astype(jnp.int32)

    tops, lows = pack(value_up.T, out_proj)
    top_left = shift_x(tops, 1)
    low_right = shift_x(lows, -1)
    low_left = shift_x(lows, 1)
    top_right = shift_x(tops, -1)

    outgoing = context_rows(where, nx, cache_kv, new_kv, queries, lengths)
    arrived = lax.all_to_all(
        outgoing.reshape(RING, nx * tok, LAT), ZAX, split_axis=0, concat_axis=0, tiled=True
    )
    top_far = shift_x(top_left, 1)
    low_far = shift_x(low_right, -1)
    near = (tops, lows, top_left, low_left, top_right, low_right)
    near = sum(([near[i], near[i + 1], swap_core(near[i]), swap_core(near[i + 1])] for i in (0, 2, 4)), [])
    beyond = [top_far, low_far, swap_core(top_far), swap_core(low_far)]
    weights = stage((w_gate, swap_core(w_gate), w_up, swap_core(w_up), w_down, swap_core(w_down)))
    arrived = arrived.reshape(RING * nx * tok, LAT)
    most = attend_part(where, nx, arrived, near, tok, 0, None)
    attended = reduce_z(*attend_part(where, nx, arrived, beyond, tok, nx - 1, most))

    half = D // HALVES
    rows = resid.reshape(tok, HALVES, half).swapaxes(0, 1).reshape(HALVES * tok, half)
    hidden = rows.astype(f32) + attended
    square = jnp.sum(hidden * hidden, axis=-1).reshape(HALVES, tok)
    scale = lax.rsqrt(jnp.sum(square, axis=0) / D + norm_eps)
    gain = jnp.repeat(norm_gain.astype(f32).reshape(HALVES, half), tok, axis=0)
    normed = (hidden * jnp.tile(scale, HALVES)[:, None] * gain).astype(bf16)

    route_ids = expert_ids.reshape(tok, TOP)
    route_slots = slots.reshape(tok, TOP)
    wide_router = router.reshape(HALVES, half, EXPERTS).swapaxes(0, 1).reshape(half, HALVES * EXPERTS)
    logits = jnp.dot(normed, wide_router, preferred_element_type=f32).reshape(HALVES, tok, HALVES, EXPERTS)
    logits = sum(logits[c, :, c] for c in range(HALVES))
    is_pick = route_ids[:, :, None] == jnp.arange(EXPERTS, dtype=jnp.int32)[None, None, :]
    picked = jnp.sum(jnp.where(is_pick, logits[:, None, :], 0.0), axis=-1)
    gates = jax.nn.sigmoid(picked)
    gates = route_scale * gates / jnp.sum(gates, axis=1, keepdims=True)
    share = jnp.sum(jnp.where(is_pick, gates[:, :, None], 0.0), axis=1)
    slot = jnp.sum(jnp.where(is_pick, route_slots[:, :, None] + 1, 0), axis=1)
    places = [(slot == s + 1).astype(bf16) for s in range(CAP)]
    high = share.astype(bf16)
    rest = share - high.astype(f32)
    middle = rest.astype(bf16)
    low = (rest - middle.astype(f32)).astype(bf16)
    extra = jnp.concatenate(places + [high, middle, low], axis=1)
    extra = jnp.pad(extra, ((0, 0), (0, EXTRA - extra.shape[1])))
    payload = jnp.concatenate([normed, jnp.tile(extra, (HALVES, 1))], axis=1)

    ring = lax.all_gather(payload, ZAX, axis=0, tiled=True)
    *sent, spread = dispatch(where, nx, ring, tok)
    from_right = shift_x(sent[1], -1)
    from_left = shift_x(sent[2], 1)
    from_far = shift_x(sent[3], 2)
    done = expert_part(where, (sent[0], from_right, from_left), weights)
    back_left = shift_x(done[1], 1)
    back_right = shift_x(done[2], -1)
    (far_done,) = expert_part(where, (from_far,), weights)
    back_far = shift_x(far_done, 2)
    expert_mix = reduce_z(*collect(spread, (done[0], back_left, back_right, back_far)))
    mixed = (hidden + expert_mix).astype(bf16).reshape(HALVES, tok, half)
    return mixed.swapaxes(0, 1).reshape(resid.shape)


def solution(mesh):
    chips = mesh.shape["ep"] // (RING * CORES)
    grid = mesh.devices.reshape(mesh.shape["rep"], chips, FAR, NEAR, CORES)
    fine = Mesh(grid, ("rep", "x", "zb", "j", "c"))
    ep = ("x", "zb", "j", "c")
    both = ("rep",) + ep
    return jax.shard_map(
        layer,
        mesh=fine,
        in_specs=(
            P(both, None, None),
            P(both, None, None),
            P(both, None, None, None),
            P(both),
            P(both, None, None),
            P(None, ep),
            P(ep, None),
            P(),
            P(),
            P(both, None, None),
            P(both, None, None),
            P(None, ep),
            P(None, ep),
            P(ep, None),
        ),
        out_specs=P(both, None, None),
        check_vma=False,
    )
```

```python
import functools
import math

import jax
import jax.numpy as jnp
from jax import lax
from jax.experimental import pallas as pl
from jax.experimental.pallas import tpu as pltpu
from jax.sharding import Mesh
from jax.sharding import PartitionSpec as P


D = 7168
LAT = 512
VH = 128
EXPERTS = 16
TOP = 8
CAP = 2
QK = 192

CORES = 2
NEAR = 4
FAR = 4
RING = NEAR * FAR
SLOTS = RING * CAP
EXTRA = 128

route_scale = 2.827
norm_eps = 1e-06


ZAX = ("zb", "j")
f32, bf16 = jnp.float32, jnp.bfloat16
NT = (((1,), (1,)), ((), ()))


def shift_x(a, step):
    n = lax.axis_size("x")
    return lax.ppermute(a, "x", [(i, (i + step) % n) for i in range(n)])


def shift_z(a, step):
    return lax.ppermute(a, ZAX, [(i, (i + step) % RING) for i in range(RING)])


def swap_core(a):
    return lax.ppermute(a, "c", [(i, (i + 1) % CORES) for i in range(CORES)])


def iota(shape, axis):
    return lax.broadcasted_iota(jnp.int32, shape, axis)


def one_hot(mask):
    return jnp.where(mask, 1.0, 0.0).astype(bf16)


def column(hop, x, nx):
    step = jnp.where(hop == 1, nx - 1, jnp.where(hop == 2, 1, jnp.where(hop == 3, 2, 0)))
    return lax.rem(x + step, nx)


def chip_at(place, where_ref):
    group, block = place // FAR, lax.rem(place, FAR)
    step = jnp.where(group == 2, RING - 1, jnp.where(group == 3, 2, group))
    return lax.rem(NEAR * where_ref[1] + where_ref[2] + step + NEAR * block, RING)


def smem():
    return pl.BlockSpec(memory_space=pltpu.SMEM)


def vmem():
    return pl.BlockSpec(memory_space=pltpu.VMEM)


def hbm():
    return pl.BlockSpec(memory_space=pltpu.HBM)


def held_in_hbm(a):
    return pltpu.with_memory_space_constraint(a, pltpu.HBM)


def held_in_vmem(a):
    return pltpu.with_memory_space_constraint(a, pltpu.VMEM)


def params(mib):
    return pltpu.CompilerParams(vmem_limit_bytes=mib << 20)


def cost(flops, nbytes):
    return pl.CostEstimate(flops=flops, bytes_accessed=nbytes, transcendentals=0)


def context_kernel(nx, where_ref, keys, queries, new, out, held):
    seq = pl.program_id(0)
    seqs = pl.num_programs(0)
    steps, heads = queries.shape[1], queries.shape[2]
    count = steps * heads
    scale = 1.0 / math.sqrt(QK)
    query = queries[0].reshape(count, queries.shape[3])
    score = jnp.dot(query, keys[0], preferred_element_type=f32) * scale
    score = jnp.where(iota(score.shape, 1) < where_ref[3 + seq], score, -jnp.inf)
    wide = query.astype(f32)
    step_of = iota((count, 1), 0) // heads
    latest = []
    peak = jnp.max(score, axis=1, keepdims=True)
    for t in range(steps):
        key = new[0, t : t + 1, :].astype(f32)
        got = jnp.sum(wide * key, axis=1, keepdims=True) * scale
        got = jnp.where(step_of >= t, got, -jnp.inf)
        latest.append(got)
        peak = jnp.maximum(peak, got)
    probs = jnp.exp(score - peak)
    total = jnp.sum(probs, axis=1, keepdims=True)
    latest = [jnp.exp(got - peak) for got in latest]
    for got in latest:
        total = total + got
    share = 1.0 / total
    probs = (probs * share).astype(bf16)
    context = lax.dot_general(probs, keys[0, :LAT, :], NT, preferred_element_type=f32)
    for t, got in enumerate(latest):
        part = (got * share).astype(bf16).astype(f32)
        context = context + part * new[0, t : t + 1, :LAT].astype(f32)
    held[pl.ds(pl.multiple_of(seq * count, count), count), :] = context.astype(bf16)

    @pl.when(seq == seqs - 1)
    def _():
        rows = held.shape[0]
        tok = rows // heads
        shape = (rows, rows)
        to, source = iota(shape, 0), iota(shape, 1)
        hop = lax.rem(to // tok, nx)
        head = column(hop, where_ref[0], nx) * RING + to // (tok * nx)
        take = (lax.rem(to, tok) == source // heads) & (head == lax.rem(source, heads))
        out[...] = jnp.dot(one_hot(take), held[...], preferred_element_type=f32).astype(bf16)


def context_rows(where, nx, cache_kv, new_kv, queries):
    seqs, length, width = cache_kv.shape
    steps, heads = queries.shape[1:3]
    rows = seqs * steps * heads
    keys = jnp.swapaxes(cache_kv, 1, 2)
    return pl.pallas_call(
        functools.partial(context_kernel, nx),
        grid=(seqs,),
        out_shape=jax.ShapeDtypeStruct((rows, LAT), bf16),
        in_specs=[
            smem(),
            pl.BlockSpec((1, width, length), lambda b: (b, 0, 0)),
            pl.BlockSpec((1, steps, heads, width), lambda b: (b, 0, 0, 0)),
            pl.BlockSpec((1, steps, width), lambda b: (b, 0, 0)),
        ],
        out_specs=pl.BlockSpec((rows, LAT), lambda b: (0, 0)),
        scratch_shapes=[pltpu.VMEM((rows, LAT), bf16)],
        compiler_params=params(24),
        cost_estimate=cost(2 * rows * length * (width + LAT), 2 * cache_kv.size),
        name="context_rows",
    )(where, held_in_hbm(keys), held_in_hbm(queries), held_in_hbm(new_kv))


def pack_kernel(up, rows, tops, lows, sem):
    half, at = tops.shape[0], up.shape[1]
    copies = []
    for i, out in enumerate((tops, lows)):
        part = pl.ds(i * half, half)
        copies.append(pltpu.make_async_copy(rows.at[part], out.at[:, pl.ds(at, rows.shape[1])], sem.at[i, 0]))
        copies.append(pltpu.make_async_copy(up.at[part], out.at[:, pl.ds(0, at)], sem.at[i, 1]))
    for copy in copies:
        copy.start()
    for copy in copies:
        copy.wait()


def pack(up, rows):
    shape = (rows.shape[0] // 2, up.shape[1] + rows.shape[1])
    return pl.pallas_call(
        pack_kernel,
        out_shape=(jax.ShapeDtypeStruct(shape, bf16),) * 2,
        in_specs=[hbm()] * 2,
        out_specs=[vmem()] * 2,
        scratch_shapes=[pltpu.SemaphoreType.DMA((2, 2))],
        compiler_params=params(12),
        cost_estimate=cost(1, 4 * rows.size),
        name="pack",
    )(held_in_hbm(up), held_in_hbm(rows))


HALVES = 2
TILE = 256


def put_rows(got, outs, n):
    own, right, left, ahead, behind = outs
    size, width = own.shape[0], ahead.shape[1]
    cols = pl.ds(n * TILE, TILE)
    own[:, cols] = got[:size]
    right[:, cols] = got[size : 2 * size].astype(bf16)
    left[:, cols] = got[2 * size : 3 * size].astype(bf16)
    rows = got[3 * size :].astype(bf16)
    if n * TILE < width:
        ahead[:, cols] = rows
    else:
        block, cols = size // FAR, pl.ds(n * TILE - width, TILE)
        behind[pl.ds(block, size - block), cols] = rows[: size - block]
        behind[pl.ds(0, block), cols] = rows[size - block :]


def row_shapes(size, width):
    return (
        jax.ShapeDtypeStruct((size, width), f32),
        jax.ShapeDtypeStruct((size, width), bf16),
        jax.ShapeDtypeStruct((size, width), bf16),
        jax.ShapeDtypeStruct((size, width // 2), bf16),
        jax.ShapeDtypeStruct((size, width // 2), bf16),
    )


def tiles_of(parts, at, n):
    half = (parts[0].shape[1] - at) // HALVES
    got = [p[:, pl.ds(at + c * half + n * TILE, TILE)] for c in range(HALVES) for p in parts]
    return jnp.concatenate(got, axis=0)


def attend_kernel(tok, nx, count, first, last, where_ref, arrived, *refs):
    pieces, outs = refs[:count], refs[count:]
    if last:
        before, outs = outs[0], outs[1:]
    up = jnp.concatenate([piece[:, pl.ds(0, LAT)] for piece in pieces], axis=0)
    values = lax.dot_general(arrived[...], up, NT, preferred_element_type=f32)
    hop = lax.rem(iota(values.shape, 0) // tok, nx)
    values = jnp.where(hop == first + iota(values.shape, 1) // VH, values, 0.0).astype(bf16)
    shape = (RING * HALVES * tok, arrived.shape[0])
    row, source = iota(shape, 0), iota(shape, 1)
    chip = chip_at(row // (HALVES * tok), where_ref)
    take = (source // (tok * nx) == chip) & (lax.rem(source, tok) == lax.rem(row, tok))
    half = lax.rem(row // tok, HALVES)
    taken = [
        jnp.dot(one_hot(take & (half == c)), values, preferred_element_type=f32).astype(bf16)
        for c in range(HALVES)
    ]
    values = jnp.concatenate(taken, axis=1)
    for n in range(outs[0].shape[1] // TILE):
        got = jnp.dot(values, tiles_of(pieces, LAT, n), preferred_element_type=f32)
        cols = pl.ds(n * TILE, TILE)
        if last:
            put_rows(before[:, cols] + got, outs, n)
        else:
            outs[0][:, cols] = got


def attend_part(where, nx, arrived, pieces, tok, first, before):
    depth = sum(p.shape[0] for p in pieces)
    width = (pieces[0].shape[1] - LAT) // HALVES
    count = len(pieces)
    last = before is not None
    part = jax.ShapeDtypeStruct((RING * HALVES * tok, width), f32)
    return pl.pallas_call(
        functools.partial(attend_kernel, tok, nx, count, first, last),
        out_shape=row_shapes(FAR * HALVES * tok, width) if last else part,
        in_specs=[smem(), vmem()] + [vmem()] * count + [vmem()] * last,
        out_specs=[vmem()] * 5 if last else vmem(),
        compiler_params=params(6),
        cost_estimate=cost(8 * RING * tok * depth * width * HALVES, 4 * depth * width),
        name="attend_part",
    )(where, arrived, *pieces, *([before] if last else []))


SEND_TILE = 512


def dispatch_kernel(tok, nx, where_ref, tokens, *refs):
    outs, spread = refs[:nx], refs[nx]
    count, width = tokens.shape
    half = width - EXTRA
    table = tokens[:, pl.ds(half, EXTRA)]
    shape = (nx * CAP, EXTRA)
    row, place = iota(shape, 0), iota(shape, 1)
    expert = FAR * column(row // CAP, where_ref[0], nx) + where_ref[1]
    hot = one_hot(place == lax.rem(row, CAP) * EXPERTS + expert)
    got = lax.dot_general(hot, table, NT, preferred_element_type=f32)
    shape = (SLOTS, count)
    slot, token = iota(shape, 0), iota(shape, 1)
    parts = []
    for r in range(nx):
        sel = jnp.where(lax.rem(slot, CAP) == 0, got[CAP * r : CAP * r + 1], got[CAP * r + 1 : CAP * r + 2])
        parts.append(jnp.where(slot // CAP == token // (HALVES * tok), sel, 0.0))
    sel = jnp.concatenate(parts, axis=0)
    of_half = lax.rem(iota(sel.shape, 1) // tok, HALVES)
    sels = [jnp.where(of_half == c, sel, 0.0).astype(bf16) for c in range(HALVES)]
    both = jnp.concatenate(sels, axis=0)
    rows = nx * SLOTS
    for n in range(half // SEND_TILE):
        got = jnp.dot(both, tokens[:, pl.ds(n * SEND_TILE, SEND_TILE)], preferred_element_type=f32).astype(bf16)
        for c in range(HALVES):
            for r in range(nx):
                at = c * rows + r * SLOTS
                outs[r][:, pl.ds(c * half + n * SEND_TILE, SEND_TILE)] = got[at : at + SLOTS]
    got = jnp.dot(sels[0], table, preferred_element_type=f32).astype(bf16)
    for r in range(nx):
        outs[r][:, pl.ds(HALVES * half, EXTRA)] = got[r * SLOTS : (r + 1) * SLOTS]
    shape = (count, count)
    row, token = iota(shape, 0), iota(shape, 1)
    chip = chip_at(row // (HALVES * tok), where_ref)
    take = (token // (HALVES * tok) == chip) & (lax.rem(token, HALVES * tok) == lax.rem(row, HALVES * tok))
    for c in range(HALVES):
        got = lax.dot_general(one_hot(take), sels[c], NT, preferred_element_type=f32)
        spread[:, pl.ds(c * rows, rows)] = got.astype(bf16)


def dispatch(where, nx, tokens, tok):
    count, width = tokens.shape
    full = HALVES * (width - EXTRA) + EXTRA
    return pl.pallas_call(
        functools.partial(dispatch_kernel, tok, nx),
        out_shape=(jax.ShapeDtypeStruct((SLOTS, full), bf16),) * nx
        + (jax.ShapeDtypeStruct((count, HALVES * nx * SLOTS), bf16),),
        in_specs=[smem(), vmem()],
        out_specs=[vmem()] * (nx + 1),
        compiler_params=params(12),
        cost_estimate=cost(2 * nx * SLOTS * count * full, 4 * count * width),
        name="dispatch",
    )(where, tokens)


CHUNKS = 7


def stage_kernel(gate_a, gate_b, up_a, up_b, down_a, down_b, wide, deep, sem):
    part = gate_a.shape[1]
    copies = [
        pltpu.make_async_copy(ref, wide.at[:, pl.ds(i * part, part)], sem.at[i])
        for i, ref in enumerate((gate_a, gate_b, up_a, up_b))
    ]
    copies += [
        pltpu.make_async_copy(ref, deep.at[pl.ds(i * part, part)], sem.at[4 + i])
        for i, ref in enumerate((down_a, down_b))
    ]
    for copy in copies:
        copy.start()
    for copy in copies:
        copy.wait()


def stage(weights):
    dim, part = weights[0].shape
    return pl.pallas_call(
        stage_kernel,
        out_shape=(
            jax.ShapeDtypeStruct((dim, 4 * part), bf16),
            jax.ShapeDtypeStruct((2 * part, dim), bf16),
        ),
        in_specs=[hbm()] * 6,
        out_specs=[vmem()] * 2,
        scratch_shapes=[pltpu.SemaphoreType.DMA((6,))],
        compiler_params=params(4),
        cost_estimate=cost(4 * 1000 * dim * part, 12 * dim * part),
        name="stage",
    )(*[held_in_hbm(w) for w in weights])


def expert_kernel(groups, where_ref, *refs):
    tokens = refs[:groups]
    wide, deep = refs[groups : groups + 2]
    outs = refs[groups + 2 : 2 * groups + 2]
    held = refs[2 * groups + 2] if groups > 1 else tokens[0]
    dim = wide.shape[0]
    part = wide.shape[1] // 2
    chunk = dim // CHUNKS
    if groups > 1:
        for g, ref in enumerate(tokens):
            held[pl.ds(g * SLOTS, SLOTS)] = ref[...]
    total = jnp.dot(held[:, pl.ds(0, dim)], wide[...], preferred_element_type=f32)
    gate, upward = total[:, :part], total[:, part:]
    act = (gate / (1.0 + jnp.exp(-gate)) * upward).astype(bf16)
    shape = (EXTRA, EXTRA)
    expert = FAR * where_ref[0] + where_ref[1]
    from_share = iota(shape, 0) - CAP * EXPERTS
    hot = (from_share >= 0) & (from_share < 3 * EXPERTS) & (lax.rem(from_share + EXTRA, EXPERTS) == expert)
    share = jnp.dot(held[:, pl.ds(dim, EXTRA)], one_hot(hot), preferred_element_type=f32)[:, :1]
    for k in range(CHUNKS):
        cols = pl.ds(k * chunk, chunk)
        got = jnp.dot(act, deep[:, cols], preferred_element_type=f32) * share
        for g in range(groups):
            outs[g][:, cols] = got[g * SLOTS : (g + 1) * SLOTS].astype(bf16)


def expert_part(where, tokens, weights):
    wide, deep = weights
    dim = wide.shape[0]
    groups = len(tokens)
    rows = groups * SLOTS
    held = [pltpu.VMEM((rows, dim + EXTRA), bf16)] if groups > 1 else []
    return pl.pallas_call(
        functools.partial(expert_kernel, groups),
        out_shape=(jax.ShapeDtypeStruct((SLOTS, dim), bf16),) * groups,
        in_specs=[smem()] + [vmem()] * (groups + 2),
        out_specs=[vmem()] * groups,
        scratch_shapes=held,
        compiler_params=params(8),
        cost_estimate=cost(6 * rows * wide.size, 2 * rows * dim),
        name="expert_part",
    )(where, *tokens, held_in_vmem(wide), held_in_vmem(deep))


def collect_kernel(count, spread, *refs):
    parts, outs = refs[:count], refs[count:]
    for n in range(outs[0].shape[1] // TILE):
        put_rows(jnp.dot(spread[...], tiles_of(parts, 0, n), preferred_element_type=f32), outs, n)


def collect(spread, parts):
    width = parts[0].shape[1] // HALVES
    count = len(parts)
    return pl.pallas_call(
        functools.partial(collect_kernel, count),
        out_shape=row_shapes(spread.shape[0] // NEAR, width),
        in_specs=[vmem()] * (count + 1),
        out_specs=[vmem()] * 5,
        compiler_params=params(12),
        cost_estimate=cost(2 * spread.size * width, 4 * spread.shape[0] * width),
        name="collect",
    )(spread, *parts)


def merge_kernel(own, right, left, ahead, behind, first, *rest):
    block = first.shape[0]
    width = ahead.shape[1]
    for c, last in enumerate((ahead, behind)):
        cols = pl.ds(c * width, width)
        total = own[:, cols] + right[:, cols].astype(f32) + left[:, cols].astype(f32)
        total = total + last[...].astype(f32)
        first[:, cols] = total[:block]
        for k, out in enumerate(rest):
            out[:, cols] = total[(k + 1) * block : (k + 2) * block].astype(bf16)


def merge(own, *others):
    size, width = own.shape
    block = (size // FAR, width)
    return pl.pallas_call(
        merge_kernel,
        out_shape=(jax.ShapeDtypeStruct(block, f32),) + (jax.ShapeDtypeStruct(block, bf16),) * (FAR - 1),
        in_specs=[vmem()] * 5,
        out_specs=[vmem()] * FAR,
        compiler_params=params(4),
        cost_estimate=cost(4 * size * width, 12 * size * width),
        name="merge",
    )(own, *others)


def reduce_z(own, right, left, ahead, behind):
    right = shift_z(right, 1)
    left = shift_z(left, -1)
    ahead = shift_z(ahead, 2)
    behind = shift_z(behind, -2)
    out, *sent = merge(own, right, left, ahead, behind)
    for k, rows in enumerate(sent):
        step = NEAR * (k + 1)
        out = out + shift_z(rows, step if step <= RING // 2 else step - RING).astype(f32)
    return out


def layer(
    cache_kv,
    new_kv,
    queries,
    lengths,
    resid,
    value_up,
    out_proj,
    norm_gain,
    router,
    expert_ids,
    slots,
    w_gate,
    w_up,
    w_down,
):
    nx = lax.axis_size("x")
    seqs, steps = queries.shape[:2]
    tok = seqs * steps
    where = jnp.stack([lax.axis_index(a) for a in ("x", "zb", "j")]).astype(jnp.int32)
    where = jnp.concatenate([where, lengths.astype(jnp.int32)])

    tops, lows = pack(value_up.T, out_proj)
    top_left = shift_x(tops, 1)
    low_right = shift_x(lows, -1)
    low_left = shift_x(lows, 1)
    top_right = shift_x(tops, -1)

    outgoing = context_rows(where, nx, cache_kv, new_kv, queries)
    arrived = lax.all_to_all(
        outgoing.reshape(RING, nx * tok, LAT), ZAX, split_axis=0, concat_axis=0, tiled=True
    )
    top_far = shift_x(top_left, 1)
    low_far = shift_x(low_right, -1)
    near = [tops, lows, swap_core(tops), swap_core(lows)]
    for pair in ((top_left, low_left), (top_right, low_right)):
        near += [*pair, *map(swap_core, pair)]
    beyond = [top_far, low_far, swap_core(top_far), swap_core(low_far)]
    weights = stage((w_gate, swap_core(w_gate), w_up, swap_core(w_up), w_down, swap_core(w_down)))
    arrived = arrived.reshape(RING * nx * tok, LAT)
    most = attend_part(where, nx, arrived, near, tok, 0, None)
    attended = reduce_z(*attend_part(where, nx, arrived, beyond, tok, nx - 1, most))

    half = D // HALVES
    rows = resid.reshape(tok, HALVES, half).swapaxes(0, 1).reshape(HALVES * tok, half)
    hidden = rows.astype(f32) + attended
    square = jnp.sum(hidden * hidden, axis=-1).reshape(HALVES, tok)
    scale = lax.rsqrt(jnp.sum(square, axis=0) / D + norm_eps)
    gain = jnp.repeat(norm_gain.astype(f32).reshape(HALVES, half), tok, axis=0)
    normed = (hidden * jnp.tile(scale, HALVES)[:, None] * gain).astype(bf16)

    route_ids = expert_ids.reshape(tok, TOP)
    route_slots = slots.reshape(tok, TOP)
    wide_router = router.reshape(HALVES, half, EXPERTS).swapaxes(0, 1).reshape(half, HALVES * EXPERTS)
    logits = jnp.dot(normed, wide_router, preferred_element_type=f32).reshape(HALVES, tok, HALVES, EXPERTS)
    logits = sum(logits[c, :, c] for c in range(HALVES))
    is_pick = route_ids[:, :, None] == jnp.arange(EXPERTS, dtype=jnp.int32)[None, None, :]
    picked = jnp.sum(jnp.where(is_pick, logits[:, None, :], 0.0), axis=-1)
    gates = jax.nn.sigmoid(picked)
    gates = route_scale * gates / jnp.sum(gates, axis=1, keepdims=True)
    share = jnp.sum(jnp.where(is_pick, gates[:, :, None], 0.0), axis=1)
    slot = jnp.sum(jnp.where(is_pick, route_slots[:, :, None] + 1, 0), axis=1)
    places = [(slot == s + 1).astype(bf16) for s in range(CAP)]
    high = share.astype(bf16)
    rest = share - high.astype(f32)
    middle = rest.astype(bf16)
    low = (rest - middle.astype(f32)).astype(bf16)
    extra = jnp.concatenate(places + [high, middle, low], axis=1)
    extra = jnp.pad(extra, ((0, 0), (0, EXTRA - extra.shape[1])))
    payload = jnp.concatenate([normed, jnp.tile(extra, (HALVES, 1))], axis=1)

    ring = lax.all_gather(payload, ZAX, axis=0, tiled=True)
    *sent, spread = dispatch(where, nx, ring, tok)
    from_right = shift_x(sent[1], -1)
    from_left = shift_x(sent[2], 1)
    from_far = shift_x(sent[3], 2)
    done = expert_part(where, (sent[0], from_right, from_left), weights)
    back_left = shift_x(done[1], 1)
    back_right = shift_x(done[2], -1)
    (far_done,) = expert_part(where, (from_far,), weights)
    back_far = shift_x(far_done, 2)
    expert_mix = reduce_z(*collect(spread, (done[0], back_left, back_right, back_far)))
    mixed = (hidden + expert_mix).astype(bf16).reshape(HALVES, tok, half)
    return mixed.swapaxes(0, 1).reshape(resid.shape)


def solution(mesh):
    chips = mesh.shape["ep"] // (RING * CORES)
    grid = mesh.devices.reshape(mesh.shape["rep"], chips, FAR, NEAR, CORES)
    fine = Mesh(grid, ("rep", "x", "zb", "j", "c"))
    ep = ("x", "zb", "j", "c")
    both = ("rep",) + ep
    return jax.shard_map(
        layer,
        mesh=fine,
        in_specs=(
            P(both, None, None),
            P(both, None, None),
            P(both, None, None, None),
            P(both),
            P(both, None, None),
            P(None, ep),
            P(ep, None),
            P(),
            P(),
            P(both, None, None),
            P(both, None, None),
            P(None, ep),
            P(None, ep),
            P(ep, None),
        ),
        out_specs=P(both, None, None),
        check_vma=False,
    )
```

```python
import functools
import math

import jax
import jax.numpy as jnp
from jax import lax
from jax.experimental import pallas as pl
from jax.experimental.pallas import tpu as pltpu
from jax.sharding import Mesh
from jax.sharding import PartitionSpec as P


D = 7168
LAT = 512
VH = 128
EXPERTS = 16
TOP = 8
CAP = 2
QK = 192

CORES = 2
NEAR = 4
FAR = 4
RING = NEAR * FAR
SLOTS = RING * CAP
EXTRA = 128

route_scale = 2.827
norm_eps = 1e-06


ZAX = ("zb", "j")
f32, bf16 = jnp.float32, jnp.bfloat16
NT = (((1,), (1,)), ((), ()))


def shift_x(a, step):
    n = lax.axis_size("x")
    return lax.ppermute(a, "x", [(i, (i + step) % n) for i in range(n)])


def shift_z(a, step):
    return lax.ppermute(a, ZAX, [(i, (i + step) % RING) for i in range(RING)])


def swap_core(a):
    return lax.ppermute(a, "c", [(i, (i + 1) % CORES) for i in range(CORES)])


def iota(shape, axis):
    return lax.broadcasted_iota(jnp.int32, shape, axis)


def one_hot(mask):
    return jnp.where(mask, 1.0, 0.0).astype(bf16)


def column(hop, x, nx):
    step = jnp.where(hop == 1, nx - 1, jnp.where(hop == 2, 1, jnp.where(hop == 3, 2, 0)))
    return lax.rem(x + step, nx)


def chip_at(place, where_ref):
    group, block = place // FAR, lax.rem(place, FAR)
    step = jnp.where(group == 2, RING - 1, jnp.where(group == 3, 2, group))
    return lax.rem(NEAR * where_ref[1] + where_ref[2] + step + NEAR * block, RING)


def smem():
    return pl.BlockSpec(memory_space=pltpu.SMEM)


def vmem():
    return pl.BlockSpec(memory_space=pltpu.VMEM)


def hbm():
    return pl.BlockSpec(memory_space=pltpu.HBM)


def held_in_hbm(a):
    return pltpu.with_memory_space_constraint(a, pltpu.HBM)


def held_in_vmem(a):
    return pltpu.with_memory_space_constraint(a, pltpu.VMEM)


def params(mib):
    return pltpu.CompilerParams(vmem_limit_bytes=mib << 20)


def cost(flops, nbytes):
    return pl.CostEstimate(flops=flops, bytes_accessed=nbytes, transcendentals=0)


def context_kernel(nx, where_ref, keys, queries, new, out, held):
    seq = pl.program_id(0)
    seqs = pl.num_programs(0)
    steps, heads = queries.shape[1], queries.shape[2]
    count = steps * heads
    scale = 1.0 / math.sqrt(QK)
    query = queries[0].reshape(count, queries.shape[3])
    score = jnp.dot(query, keys[0], preferred_element_type=f32) * scale
    score = jnp.where(iota(score.shape, 1) < where_ref[3 + seq], score, -jnp.inf)
    wide = query.astype(f32)
    step_of = iota((count, 1), 0) // heads
    latest = []
    peak = jnp.max(score, axis=1, keepdims=True)
    for t in range(steps):
        key = new[0, t : t + 1, :].astype(f32)
        got = jnp.sum(wide * key, axis=1, keepdims=True) * scale
        got = jnp.where(step_of >= t, got, -jnp.inf)
        latest.append(got)
        peak = jnp.maximum(peak, got)
    probs = jnp.exp(score - peak)
    total = jnp.sum(probs, axis=1, keepdims=True)
    latest = [jnp.exp(got - peak) for got in latest]
    for got in latest:
        total = total + got
    share = 1.0 / total
    probs = (probs * share).astype(bf16)
    context = lax.dot_general(probs, keys[0, :LAT, :], NT, preferred_element_type=f32)
    for t, got in enumerate(latest):
        part = (got * share).astype(bf16).astype(f32)
        context = context + part * new[0, t : t + 1, :LAT].astype(f32)
    held[pl.ds(pl.multiple_of(seq * count, count), count), :] = context.astype(bf16)

    @pl.when(seq == seqs - 1)
    def _():
        rows = held.shape[0]
        tok = rows // heads
        shape = (rows, rows)
        to, source = iota(shape, 0), iota(shape, 1)
        hop = lax.rem(to // tok, nx)
        head = column(hop, where_ref[0], nx) * RING + to // (tok * nx)
        take = (lax.rem(to, tok) == source // heads) & (head == lax.rem(source, heads))
        out[...] = jnp.dot(one_hot(take), held[...], preferred_element_type=f32).astype(bf16)


def context_rows(where, nx, cache_kv, new_kv, queries):
    seqs, length, width = cache_kv.shape
    steps, heads = queries.shape[1:3]
    rows = seqs * steps * heads
    keys = jnp.swapaxes(cache_kv, 1, 2)
    return pl.pallas_call(
        functools.partial(context_kernel, nx),
        grid=(seqs,),
        out_shape=jax.ShapeDtypeStruct((rows, LAT), bf16),
        in_specs=[
            smem(),
            pl.BlockSpec((1, width, length), lambda b: (b, 0, 0)),
            pl.BlockSpec((1, steps, heads, width), lambda b: (b, 0, 0, 0)),
            pl.BlockSpec((1, steps, width), lambda b: (b, 0, 0)),
        ],
        out_specs=pl.BlockSpec((rows, LAT), lambda b: (0, 0)),
        scratch_shapes=[pltpu.VMEM((rows, LAT), bf16)],
        compiler_params=params(24),
        cost_estimate=cost(2 * rows * length * (width + LAT), 2 * cache_kv.size),
        name="context_rows",
    )(where, held_in_hbm(keys), held_in_hbm(queries), held_in_hbm(new_kv))


def pack_kernel(up, rows, tops, lows, sem):
    half, at = tops.shape[0], up.shape[1]
    copies = []
    for i, out in enumerate((tops, lows)):
        part = pl.ds(i * half, half)
        copies.append(pltpu.make_async_copy(rows.at[part], out.at[:, pl.ds(at, rows.shape[1])], sem.at[i, 0]))
        copies.append(pltpu.make_async_copy(up.at[part], out.at[:, pl.ds(0, at)], sem.at[i, 1]))
    for copy in copies:
        copy.start()
    for copy in copies:
        copy.wait()


def pack(up, rows):
    shape = (rows.shape[0] // 2, up.shape[1] + rows.shape[1])
    return pl.pallas_call(
        pack_kernel,
        out_shape=(jax.ShapeDtypeStruct(shape, bf16),) * 2,
        in_specs=[hbm()] * 2,
        out_specs=[vmem()] * 2,
        scratch_shapes=[pltpu.SemaphoreType.DMA((2, 2))],
        compiler_params=params(12),
        cost_estimate=cost(1, 4 * rows.size),
        name="pack",
    )(held_in_hbm(up), held_in_hbm(rows))


HALVES = 2
TILE = 256


def put_rows(got, outs, n):
    own, right, left, ahead, behind = outs
    size, width = own.shape[0], ahead.shape[1]
    cols = pl.ds(n * TILE, TILE)
    own[:, cols] = got[:size]
    right[:, cols] = got[size : 2 * size].astype(bf16)
    left[:, cols] = got[2 * size : 3 * size].astype(bf16)
    rows = got[3 * size :].astype(bf16)
    if n * TILE < width:
        ahead[:, cols] = rows
    else:
        block, cols = size // FAR, pl.ds(n * TILE - width, TILE)
        behind[pl.ds(block, size - block), cols] = rows[: size - block]
        behind[pl.ds(0, block), cols] = rows[size - block :]


def row_shapes(size, width):
    return (
        jax.ShapeDtypeStruct((size, width), f32),
        jax.ShapeDtypeStruct((size, width), bf16),
        jax.ShapeDtypeStruct((size, width), bf16),
        jax.ShapeDtypeStruct((size, width // 2), bf16),
        jax.ShapeDtypeStruct((size, width // 2), bf16),
    )


def tiles_of(parts, at, n):
    half = (parts[0].shape[1] - at) // HALVES
    got = [p[:, pl.ds(at + c * half + n * TILE, TILE)] for c in range(HALVES) for p in parts]
    return jnp.concatenate(got, axis=0)


def attend_kernel(tok, nx, count, first, last, where_ref, arrived, *refs):
    pieces, outs = refs[:count], refs[count:]
    if last:
        before, outs = outs[0], outs[1:]
    up = jnp.concatenate([piece[:, pl.ds(0, LAT)] for piece in pieces], axis=0)
    values = lax.dot_general(arrived[...], up, NT, preferred_element_type=f32)
    hop = lax.rem(iota(values.shape, 0) // tok, nx)
    values = jnp.where(hop == first + iota(values.shape, 1) // VH, values, 0.0).astype(bf16)
    shape = (RING * HALVES * tok, arrived.shape[0])
    row, source = iota(shape, 0), iota(shape, 1)
    chip = chip_at(row // (HALVES * tok), where_ref)
    take = (source // (tok * nx) == chip) & (lax.rem(source, tok) == lax.rem(row, tok))
    half = lax.rem(row // tok, HALVES)
    taken = [
        jnp.dot(one_hot(take & (half == c)), values, preferred_element_type=f32).astype(bf16)
        for c in range(HALVES)
    ]
    values = jnp.concatenate(taken, axis=1)
    for n in range(outs[0].shape[1] // TILE):
        got = jnp.dot(values, tiles_of(pieces, LAT, n), preferred_element_type=f32)
        cols = pl.ds(n * TILE, TILE)
        if last:
            put_rows(before[:, cols] + got, outs, n)
        else:
            outs[0][:, cols] = got


def attend_part(where, nx, arrived, pieces, tok, first, before):
    depth = sum(p.shape[0] for p in pieces)
    width = (pieces[0].shape[1] - LAT) // HALVES
    count = len(pieces)
    last = before is not None
    part = jax.ShapeDtypeStruct((RING * HALVES * tok, width), f32)
    return pl.pallas_call(
        functools.partial(attend_kernel, tok, nx, count, first, last),
        out_shape=row_shapes(FAR * HALVES * tok, width) if last else part,
        in_specs=[smem(), vmem()] + [vmem()] * count + [vmem()] * last,
        out_specs=[vmem()] * 5 if last else vmem(),
        compiler_params=params(6),
        cost_estimate=cost(8 * RING * tok * depth * width * HALVES, 4 * depth * width),
        name="attend_part",
    )(where, arrived, *pieces, *([before] if last else []))


SEND_TILE = 512


def dispatch_kernel(tok, nx, where_ref, tokens, *refs):
    outs, spread = refs[:nx], refs[nx]
    count, width = tokens.shape
    half = width - EXTRA
    table = tokens[:, pl.ds(half, EXTRA)]
    shape = (nx * CAP, EXTRA)
    row, place = iota(shape, 0), iota(shape, 1)
    expert = FAR * column(row // CAP, where_ref[0], nx) + where_ref[1]
    hot = one_hot(place == lax.rem(row, CAP) * EXPERTS + expert)
    got = lax.dot_general(hot, table, NT, preferred_element_type=f32)
    shape = (SLOTS, count)
    slot, token = iota(shape, 0), iota(shape, 1)
    parts = []
    for r in range(nx):
        sel = jnp.where(lax.rem(slot, CAP) == 0, got[CAP * r : CAP * r + 1], got[CAP * r + 1 : CAP * r + 2])
        parts.append(jnp.where(slot // CAP == token // (HALVES * tok), sel, 0.0))
    sel = jnp.concatenate(parts, axis=0)
    of_half = lax.rem(iota(sel.shape, 1) // tok, HALVES)
    sels = [jnp.where(of_half == c, sel, 0.0).astype(bf16) for c in range(HALVES)]
    both = jnp.concatenate(sels, axis=0)
    rows = nx * SLOTS
    for n in range(half // SEND_TILE):
        got = jnp.dot(both, tokens[:, pl.ds(n * SEND_TILE, SEND_TILE)], preferred_element_type=f32).astype(bf16)
        for c in range(HALVES):
            for r in range(nx):
                at = c * rows + r * SLOTS
                outs[r][:, pl.ds(c * half + n * SEND_TILE, SEND_TILE)] = got[at : at + SLOTS]
    got = jnp.dot(sels[0], table, preferred_element_type=f32).astype(bf16)
    for r in range(nx):
        outs[r][:, pl.ds(HALVES * half, EXTRA)] = got[r * SLOTS : (r + 1) * SLOTS]
    shape = (count, count)
    row, token = iota(shape, 0), iota(shape, 1)
    chip = chip_at(row // (HALVES * tok), where_ref)
    take = (token // (HALVES * tok) == chip) & (lax.rem(token, HALVES * tok) == lax.rem(row, HALVES * tok))
    for c in range(HALVES):
        got = lax.dot_general(one_hot(take), sels[c], NT, preferred_element_type=f32)
        spread[:, pl.ds(c * rows, rows)] = got.astype(bf16)


def dispatch(where, nx, tokens, tok):
    count, width = tokens.shape
    full = HALVES * (width - EXTRA) + EXTRA
    return pl.pallas_call(
        functools.partial(dispatch_kernel, tok, nx),
        out_shape=(jax.ShapeDtypeStruct((SLOTS, full), bf16),) * nx
        + (jax.ShapeDtypeStruct((count, HALVES * nx * SLOTS), bf16),),
        in_specs=[smem(), vmem()],
        out_specs=[vmem()] * (nx + 1),
        compiler_params=params(12),
        cost_estimate=cost(2 * nx * SLOTS * count * full, 4 * count * width),
        name="dispatch",
    )(where, tokens)


CHUNKS = 7


def stage_kernel(gate_a, gate_b, up_a, up_b, down_a, down_b, wide, deep, sem):
    part = gate_a.shape[1]
    copies = [
        pltpu.make_async_copy(ref, wide.at[:, pl.ds(i * part, part)], sem.at[i])
        for i, ref in enumerate((gate_a, gate_b, up_a, up_b))
    ]
    copies += [
        pltpu.make_async_copy(ref, deep.at[pl.ds(i * part, part)], sem.at[4 + i])
        for i, ref in enumerate((down_a, down_b))
    ]
    for copy in copies:
        copy.start()
    for copy in copies:
        copy.wait()


def stage(weights):
    dim, part = weights[0].shape
    return pl.pallas_call(
        stage_kernel,
        out_shape=(
            jax.ShapeDtypeStruct((dim, 4 * part), bf16),
            jax.ShapeDtypeStruct((2 * part, dim), bf16),
        ),
        in_specs=[hbm()] * 6,
        out_specs=[vmem()] * 2,
        scratch_shapes=[pltpu.SemaphoreType.DMA((6,))],
        compiler_params=params(4),
        cost_estimate=cost(4 * 1000 * dim * part, 12 * dim * part),
        name="stage",
    )(*[held_in_hbm(w) for w in weights])


def expert_kernel(groups, where_ref, *refs):
    tokens = refs[:groups]
    wide, deep = refs[groups : groups + 2]
    outs = refs[groups + 2 : 2 * groups + 2]
    held = refs[2 * groups + 2] if groups > 1 else tokens[0]
    dim = wide.shape[0]
    part = wide.shape[1] // 2
    chunk = dim // CHUNKS
    if groups > 1:
        for g, ref in enumerate(tokens):
            held[pl.ds(g * SLOTS, SLOTS)] = ref[...]
    total = jnp.dot(held[:, pl.ds(0, dim)], wide[...], preferred_element_type=f32)
    gate, upward = total[:, :part], total[:, part:]
    act = (gate / (1.0 + jnp.exp(-gate)) * upward).astype(bf16)
    shape = (EXTRA, EXTRA)
    expert = FAR * where_ref[0] + where_ref[1]
    from_share = iota(shape, 0) - CAP * EXPERTS
    hot = (from_share >= 0) & (from_share < 3 * EXPERTS) & (lax.rem(from_share + EXTRA, EXPERTS) == expert)
    share = jnp.dot(held[:, pl.ds(dim, EXTRA)], one_hot(hot), preferred_element_type=f32)[:, :1]
    for k in range(CHUNKS):
        cols = pl.ds(k * chunk, chunk)
        got = jnp.dot(act, deep[:, cols], preferred_element_type=f32) * share
        for g in range(groups):
            outs[g][:, cols] = got[g * SLOTS : (g + 1) * SLOTS].astype(bf16)


def expert_part(where, tokens, weights):
    wide, deep = weights
    dim = wide.shape[0]
    groups = len(tokens)
    rows = groups * SLOTS
    held = [pltpu.VMEM((rows, dim + EXTRA), bf16)] if groups > 1 else []
    return pl.pallas_call(
        functools.partial(expert_kernel, groups),
        out_shape=(jax.ShapeDtypeStruct((SLOTS, dim), bf16),) * groups,
        in_specs=[smem()] + [vmem()] * (groups + 2),
        out_specs=[vmem()] * groups,
        scratch_shapes=held,
        compiler_params=params(8),
        cost_estimate=cost(6 * rows * wide.size, 2 * rows * dim),
        name="expert_part",
    )(where, *tokens, held_in_vmem(wide), held_in_vmem(deep))


def collect_kernel(count, spread, *refs):
    parts, outs = refs[:count], refs[count:]
    for n in range(outs[0].shape[1] // TILE):
        put_rows(jnp.dot(spread[...], tiles_of(parts, 0, n), preferred_element_type=f32), outs, n)


def collect(spread, parts):
    width = parts[0].shape[1] // HALVES
    count = len(parts)
    return pl.pallas_call(
        functools.partial(collect_kernel, count),
        out_shape=row_shapes(spread.shape[0] // NEAR, width),
        in_specs=[vmem()] * (count + 1),
        out_specs=[vmem()] * 5,
        compiler_params=params(12),
        cost_estimate=cost(2 * spread.size * width, 4 * spread.shape[0] * width),
        name="collect",
    )(spread, *parts)


def merge_kernel(own, right, left, ahead, behind, first, *rest):
    block = first.shape[0]
    width = ahead.shape[1]
    for c, last in enumerate((ahead, behind)):
        cols = pl.ds(c * width, width)
        total = own[:, cols] + right[:, cols].astype(f32) + left[:, cols].astype(f32)
        total = total + last[...].astype(f32)
        first[:, cols] = total[:block]
        for k, out in enumerate(rest):
            out[:, cols] = total[(k + 1) * block : (k + 2) * block].astype(bf16)


def merge(own, *others):
    size, width = own.shape
    block = (size // FAR, width)
    return pl.pallas_call(
        merge_kernel,
        out_shape=(jax.ShapeDtypeStruct(block, f32),) + (jax.ShapeDtypeStruct(block, bf16),) * (FAR - 1),
        in_specs=[vmem()] * 5,
        out_specs=[vmem()] * FAR,
        compiler_params=params(4),
        cost_estimate=cost(4 * size * width, 12 * size * width),
        name="merge",
    )(own, *others)


def reduce_z(own, right, left, ahead, behind):
    ahead = shift_z(ahead, 2)
    behind = shift_z(behind, -2)
    right = shift_z(right, 1)
    left = shift_z(left, -1)
    first, *sent = merge(own, right, left, ahead, behind)
    middle = shift_z(sent[1], 2 * NEAR)
    others = [middle, shift_z(sent[0], NEAR), shift_z(sent[2], -NEAR)]
    return first + sum(rows.astype(f32) for rows in others)


def layer(
    cache_kv,
    new_kv,
    queries,
    lengths,
    resid,
    value_up,
    out_proj,
    norm_gain,
    router,
    expert_ids,
    slots,
    w_gate,
    w_up,
    w_down,
):
    nx = lax.axis_size("x")
    seqs, steps = queries.shape[:2]
    tok = seqs * steps
    where = jnp.stack([lax.axis_index(a) for a in ("x", "zb", "j")]).astype(jnp.int32)
    where = jnp.concatenate([where, lengths.astype(jnp.int32)])

    tops, lows = pack(value_up.T, out_proj)
    top_left = shift_x(tops, 1)
    low_right = shift_x(lows, -1)
    low_left = shift_x(lows, 1)
    top_right = shift_x(tops, -1)

    outgoing = context_rows(where, nx, cache_kv, new_kv, queries)
    arrived = lax.all_to_all(
        outgoing.reshape(RING, nx * tok, LAT), ZAX, split_axis=0, concat_axis=0, tiled=True
    )
    top_far = shift_x(top_left, 1)
    low_far = shift_x(low_right, -1)
    near = []
    for pair in ((tops, lows), (top_left, low_left), (top_right, low_right)):
        near += [*pair, *map(swap_core, pair)]
    beyond = [top_far, low_far, swap_core(top_far), swap_core(low_far)]
    others = [swap_core(w) for w in (w_gate, w_up, w_down)]
    weights = stage((w_gate, others[0], w_up, others[1], w_down, others[2]))
    arrived = arrived.reshape(RING * nx * tok, LAT)
    most = attend_part(where, nx, arrived, near, tok, 0, None)
    attended = reduce_z(*attend_part(where, nx, arrived, beyond, tok, nx - 1, most))

    half = D // HALVES
    rows = resid.reshape(tok, HALVES, half).swapaxes(0, 1).reshape(HALVES * tok, half)
    hidden = rows.astype(f32) + attended
    square = jnp.sum(hidden * hidden, axis=-1).reshape(HALVES, tok)
    scale = lax.rsqrt(jnp.sum(square, axis=0) / D + norm_eps)
    gain = jnp.repeat(norm_gain.astype(f32).reshape(HALVES, half), tok, axis=0)
    normed = (hidden * jnp.tile(scale, HALVES)[:, None] * gain).astype(bf16)

    route_ids = expert_ids.reshape(tok, TOP)
    route_slots = slots.reshape(tok, TOP)
    wide_router = router.reshape(HALVES, half, EXPERTS).swapaxes(0, 1).reshape(half, HALVES * EXPERTS)
    logits = jnp.dot(normed, wide_router, preferred_element_type=f32).reshape(HALVES, tok, HALVES, EXPERTS)
    logits = sum(logits[c, :, c] for c in range(HALVES))
    is_pick = route_ids[:, :, None] == jnp.arange(EXPERTS, dtype=jnp.int32)[None, None, :]
    picked = jnp.sum(jnp.where(is_pick, logits[:, None, :], 0.0), axis=-1)
    gates = jax.nn.sigmoid(picked)
    gates = route_scale * gates / jnp.sum(gates, axis=1, keepdims=True)
    share = jnp.sum(jnp.where(is_pick, gates[:, :, None], 0.0), axis=1)
    slot = jnp.sum(jnp.where(is_pick, route_slots[:, :, None] + 1, 0), axis=1)
    places = [(slot == s + 1).astype(bf16) for s in range(CAP)]
    high = share.astype(bf16)
    rest = share - high.astype(f32)
    middle = rest.astype(bf16)
    low = (rest - middle.astype(f32)).astype(bf16)
    extra = jnp.concatenate(places + [high, middle, low], axis=1)
    extra = jnp.pad(extra, ((0, 0), (0, EXTRA - extra.shape[1])))
    payload = jnp.concatenate([normed, jnp.tile(extra, (HALVES, 1))], axis=1)

    ring = lax.all_gather(payload, ZAX, axis=0, tiled=True)
    *sent, spread = dispatch(where, nx, ring, tok)
    from_right = shift_x(sent[1], -1)
    from_left = shift_x(sent[2], 1)
    from_far = shift_x(sent[3], 2)
    done = expert_part(where, (sent[0], from_right, from_left), weights)
    back_left = shift_x(done[1], 1)
    back_right = shift_x(done[2], -1)
    (far_done,) = expert_part(where, (from_far,), weights)
    back_far = shift_x(far_done, 2)
    expert_mix = reduce_z(*collect(spread, (done[0], back_left, back_right, back_far)))
    mixed = (hidden + expert_mix).astype(bf16).reshape(HALVES, tok, half)
    return mixed.swapaxes(0, 1).reshape(resid.shape)


def solution(mesh):
    chips = mesh.shape["ep"] // (RING * CORES)
    grid = mesh.devices.reshape(mesh.shape["rep"], chips, FAR, NEAR, CORES)
    fine = Mesh(grid, ("rep", "x", "zb", "j", "c"))
    ep = ("x", "zb", "j", "c")
    both = ("rep",) + ep
    return jax.shard_map(
        layer,
        mesh=fine,
        in_specs=(
            P(both, None, None),
            P(both, None, None),
            P(both, None, None, None),
            P(both),
            P(both, None, None),
            P(None, ep),
            P(ep, None),
            P(),
            P(),
            P(both, None, None),
            P(both, None, None),
            P(None, ep),
            P(None, ep),
            P(ep, None),
        ),
        out_specs=P(both, None, None),
        check_vma=False,
    )
```

```python
import functools
import math

import jax
import jax.numpy as jnp
from jax import lax
from jax.experimental import pallas as pl
from jax.experimental.pallas import tpu as pltpu
from jax.sharding import Mesh
from jax.sharding import PartitionSpec as P


D = 7168
LAT = 512
VH = 128
EXPERTS = 16
TOP = 8
CAP = 2
QK = 192

CORES = 2
NEAR = 4
FAR = 4
RING = NEAR * FAR
SLOTS = RING * CAP
EXTRA = 128

route_scale = 2.827
norm_eps = 1e-06


ZAX = ("zb", "j")
f32, bf16 = jnp.float32, jnp.bfloat16
NT = (((1,), (1,)), ((), ()))


def shift_x(a, step):
    n = lax.axis_size("x")
    return lax.ppermute(a, "x", [(i, (i + step) % n) for i in range(n)])


def shift_z(a, step):
    return lax.ppermute(a, ZAX, [(i, (i + step) % RING) for i in range(RING)])


def swap_core(a):
    return lax.ppermute(a, "c", [(i, (i + 1) % CORES) for i in range(CORES)])


def iota(shape, axis):
    return lax.broadcasted_iota(jnp.int32, shape, axis)


def one_hot(mask):
    return jnp.where(mask, 1.0, 0.0).astype(bf16)


def column(hop, x, nx):
    step = jnp.where(hop == 1, nx - 1, jnp.where(hop == 2, 1, jnp.where(hop == 3, 2, 0)))
    return lax.rem(x + step, nx)


def chip_at(place, where_ref):
    group, block = place // FAR, lax.rem(place, FAR)
    step = jnp.where(group == 2, RING - 1, jnp.where(group == 3, 2, group))
    return lax.rem(NEAR * where_ref[1] + where_ref[2] + step + NEAR * block, RING)


def smem():
    return pl.BlockSpec(memory_space=pltpu.SMEM)


def vmem():
    return pl.BlockSpec(memory_space=pltpu.VMEM)


def hbm():
    return pl.BlockSpec(memory_space=pltpu.HBM)


def held_in_hbm(a):
    return pltpu.with_memory_space_constraint(a, pltpu.HBM)


def held_in_vmem(a):
    return pltpu.with_memory_space_constraint(a, pltpu.VMEM)


def params(mib):
    return pltpu.CompilerParams(vmem_limit_bytes=mib << 20)


def cost(flops, nbytes):
    return pl.CostEstimate(flops=flops, bytes_accessed=nbytes, transcendentals=0)


def context_kernel(nx, where_ref, keys, queries, new, out, held):
    seq = pl.program_id(0)
    seqs = pl.num_programs(0)
    steps, heads = queries.shape[1], queries.shape[2]
    count = steps * heads
    scale = 1.0 / math.sqrt(QK)
    query = queries[0].reshape(count, queries.shape[3])
    score = jnp.dot(query, keys[0], preferred_element_type=f32) * scale
    score = jnp.where(iota(score.shape, 1) < where_ref[3 + seq], score, -jnp.inf)
    wide = query.astype(f32)
    step_of = iota((count, 1), 0) // heads
    latest = []
    peak = jnp.max(score, axis=1, keepdims=True)
    for t in range(steps):
        key = new[0, t : t + 1, :].astype(f32)
        got = jnp.sum(wide * key, axis=1, keepdims=True) * scale
        got = jnp.where(step_of >= t, got, -jnp.inf)
        latest.append(got)
        peak = jnp.maximum(peak, got)
    probs = jnp.exp(score - peak)
    total = jnp.sum(probs, axis=1, keepdims=True)
    latest = [jnp.exp(got - peak) for got in latest]
    for got in latest:
        total = total + got
    share = 1.0 / total
    probs = (probs * share).astype(bf16)
    context = lax.dot_general(probs, keys[0, :LAT, :], NT, preferred_element_type=f32)
    for t, got in enumerate(latest):
        part = (got * share).astype(bf16).astype(f32)
        context = context + part * new[0, t : t + 1, :LAT].astype(f32)
    held[pl.ds(pl.multiple_of(seq * count, count), count), :] = context.astype(bf16)

    @pl.when(seq == seqs - 1)
    def _():
        rows = held.shape[0]
        tok = rows // heads
        shape = (rows, rows)
        to, source = iota(shape, 0), iota(shape, 1)
        hop = lax.rem(to // tok, nx)
        head = column(hop, where_ref[0], nx) * RING + to // (tok * nx)
        take = (lax.rem(to, tok) == source // heads) & (head == lax.rem(source, heads))
        out[...] = jnp.dot(one_hot(take), held[...], preferred_element_type=f32).astype(bf16)


def context_rows(where, nx, cache_kv, new_kv, queries):
    seqs, length, width = cache_kv.shape
    steps, heads = queries.shape[1:3]
    rows = seqs * steps * heads
    keys = jnp.swapaxes(cache_kv, 1, 2)
    return pl.pallas_call(
        functools.partial(context_kernel, nx),
        grid=(seqs,),
        out_shape=jax.ShapeDtypeStruct((rows, LAT), bf16),
        in_specs=[
            smem(),
            pl.BlockSpec((1, width, length), lambda b: (b, 0, 0)),
            pl.BlockSpec((1, steps, heads, width), lambda b: (b, 0, 0, 0)),
            pl.BlockSpec((1, steps, width), lambda b: (b, 0, 0)),
        ],
        out_specs=pl.BlockSpec((rows, LAT), lambda b: (0, 0)),
        scratch_shapes=[pltpu.VMEM((rows, LAT), bf16)],
        compiler_params=params(24),
        cost_estimate=cost(2 * rows * length * (width + LAT), 2 * cache_kv.size),
        name="context_rows",
    )(where, held_in_hbm(keys), held_in_hbm(queries), held_in_hbm(new_kv))


def pack_kernel(up, rows, tops, lows, sem):
    half, at = tops.shape[0], up.shape[1]
    copies = []
    for i, out in enumerate((tops, lows)):
        part = pl.ds(i * half, half)
        copies.append(pltpu.make_async_copy(rows.at[part], out.at[:, pl.ds(at, rows.shape[1])], sem.at[i, 0]))
        copies.append(pltpu.make_async_copy(up.at[part], out.at[:, pl.ds(0, at)], sem.at[i, 1]))
    for copy in copies:
        copy.start()
    for copy in copies:
        copy.wait()


def pack(up, rows):
    shape = (rows.shape[0] // 2, up.shape[1] + rows.shape[1])
    return pl.pallas_call(
        pack_kernel,
        out_shape=(jax.ShapeDtypeStruct(shape, bf16),) * 2,
        in_specs=[hbm()] * 2,
        out_specs=[vmem()] * 2,
        scratch_shapes=[pltpu.SemaphoreType.DMA((2, 2))],
        compiler_params=params(12),
        cost_estimate=cost(1, 4 * rows.size),
        name="pack",
    )(held_in_hbm(up), held_in_hbm(rows))


HALVES = 2
TILE = 256


def put_rows(got, outs, n):
    own, right, left, ahead, behind = outs
    size, width = own.shape[0], ahead.shape[1]
    cols = pl.ds(n * TILE, TILE)
    own[:, cols] = got[:size]
    right[:, cols] = got[size : 2 * size].astype(bf16)
    left[:, cols] = got[2 * size : 3 * size].astype(bf16)
    rows = got[3 * size :].astype(bf16)
    if n * TILE < width:
        ahead[:, cols] = rows
    else:
        block, cols = size // FAR, pl.ds(n * TILE - width, TILE)
        behind[pl.ds(block, size - block), cols] = rows[: size - block]
        behind[pl.ds(0, block), cols] = rows[size - block :]


def row_shapes(size, width):
    return (
        jax.ShapeDtypeStruct((size, width), f32),
        jax.ShapeDtypeStruct((size, width), bf16),
        jax.ShapeDtypeStruct((size, width), bf16),
        jax.ShapeDtypeStruct((size, width // 2), bf16),
        jax.ShapeDtypeStruct((size, width // 2), bf16),
    )


def tiles_of(parts, at, n):
    half = (parts[0].shape[1] - at) // HALVES
    got = [p[:, pl.ds(at + c * half + n * TILE, TILE)] for c in range(HALVES) for p in parts]
    return jnp.concatenate(got, axis=0)


def attend_kernel(tok, nx, count, first, last, where_ref, arrived, *refs):
    pieces, outs = refs[:count], refs[count:]
    if last:
        before, outs = outs[0], outs[1:]
    up = jnp.concatenate([piece[:, pl.ds(0, LAT)] for piece in pieces], axis=0)
    values = lax.dot_general(arrived[...], up, NT, preferred_element_type=f32)
    hop = lax.rem(iota(values.shape, 0) // tok, nx)
    values = jnp.where(hop == first + iota(values.shape, 1) // VH, values, 0.0).astype(bf16)
    shape = (RING * HALVES * tok, arrived.shape[0])
    row, source = iota(shape, 0), iota(shape, 1)
    chip = chip_at(row // (HALVES * tok), where_ref)
    take = (source // (tok * nx) == chip) & (lax.rem(source, tok) == lax.rem(row, tok))
    half = lax.rem(row // tok, HALVES)
    taken = [
        jnp.dot(one_hot(take & (half == c)), values, preferred_element_type=f32).astype(bf16)
        for c in range(HALVES)
    ]
    values = jnp.concatenate(taken, axis=1)
    for n in range(outs[0].shape[1] // TILE):
        got = jnp.dot(values, tiles_of(pieces, LAT, n), preferred_element_type=f32)
        cols = pl.ds(n * TILE, TILE)
        if last:
            put_rows(before[:, cols] + got, outs, n)
        else:
            outs[0][:, cols] = got


def attend_part(where, nx, arrived, pieces, tok, first, before):
    depth = sum(p.shape[0] for p in pieces)
    width = (pieces[0].shape[1] - LAT) // HALVES
    count = len(pieces)
    last = before is not None
    part = jax.ShapeDtypeStruct((RING * HALVES * tok, width), f32)
    return pl.pallas_call(
        functools.partial(attend_kernel, tok, nx, count, first, last),
        out_shape=row_shapes(FAR * HALVES * tok, width) if last else part,
        in_specs=[smem(), vmem()] + [vmem()] * count + [vmem()] * last,
        out_specs=[vmem()] * 5 if last else vmem(),
        compiler_params=params(6),
        cost_estimate=cost(8 * RING * tok * depth * width * HALVES, 4 * depth * width),
        name="attend_part",
    )(where, arrived, *pieces, *([before] if last else []))


SEND_TILE = 512


def dispatch_kernel(tok, nx, where_ref, tokens, *refs):
    outs, spread = refs[:nx], refs[nx]
    count, width = tokens.shape
    half = width - EXTRA
    table = tokens[:, pl.ds(half, EXTRA)]
    shape = (nx * CAP, EXTRA)
    row, place = iota(shape, 0), iota(shape, 1)
    expert = FAR * column(row // CAP, where_ref[0], nx) + where_ref[1]
    hot = one_hot(place == lax.rem(row, CAP) * EXPERTS + expert)
    got = lax.dot_general(hot, table, NT, preferred_element_type=f32)
    shape = (SLOTS, count)
    slot, token = iota(shape, 0), iota(shape, 1)
    parts = []
    for r in range(nx):
        sel = jnp.where(lax.rem(slot, CAP) == 0, got[CAP * r : CAP * r + 1], got[CAP * r + 1 : CAP * r + 2])
        parts.append(jnp.where(slot // CAP == token // (HALVES * tok), sel, 0.0))
    sel = jnp.concatenate(parts, axis=0)
    of_half = lax.rem(iota(sel.shape, 1) // tok, HALVES)
    sels = [jnp.where(of_half == c, sel, 0.0).astype(bf16) for c in range(HALVES)]
    both = jnp.concatenate(sels, axis=0)
    rows = nx * SLOTS
    for n in range(half // SEND_TILE):
        got = jnp.dot(both, tokens[:, pl.ds(n * SEND_TILE, SEND_TILE)], preferred_element_type=f32).astype(bf16)
        for c in range(HALVES):
            for r in range(nx):
                at = c * rows + r * SLOTS
                outs[r][:, pl.ds(c * half + n * SEND_TILE, SEND_TILE)] = got[at : at + SLOTS]
    got = jnp.dot(sels[0], table, preferred_element_type=f32).astype(bf16)
    for r in range(nx):
        outs[r][:, pl.ds(HALVES * half, EXTRA)] = got[r * SLOTS : (r + 1) * SLOTS]
    shape = (count, count)
    row, token = iota(shape, 0), iota(shape, 1)
    chip = chip_at(row // (HALVES * tok), where_ref)
    take = (token // (HALVES * tok) == chip) & (lax.rem(token, HALVES * tok) == lax.rem(row, HALVES * tok))
    for c in range(HALVES):
        got = lax.dot_general(one_hot(take), sels[c], NT, preferred_element_type=f32)
        spread[:, pl.ds(c * rows, rows)] = got.astype(bf16)


def dispatch(where, nx, tokens, tok):
    count, width = tokens.shape
    full = HALVES * (width - EXTRA) + EXTRA
    return pl.pallas_call(
        functools.partial(dispatch_kernel, tok, nx),
        out_shape=(jax.ShapeDtypeStruct((SLOTS, full), bf16),) * nx
        + (jax.ShapeDtypeStruct((count, HALVES * nx * SLOTS), bf16),),
        in_specs=[smem(), vmem()],
        out_specs=[vmem()] * (nx + 1),
        compiler_params=params(12),
        cost_estimate=cost(2 * nx * SLOTS * count * full, 4 * count * width),
        name="dispatch",
    )(where, tokens)


CHUNKS = 7


def stage_kernel(gate_a, gate_b, up_a, up_b, down_a, down_b, wide, deep, sem):
    part = gate_a.shape[1]
    copies = [
        pltpu.make_async_copy(ref, wide.at[:, pl.ds(i * part, part)], sem.at[i])
        for i, ref in enumerate((gate_a, gate_b, up_a, up_b))
    ]
    copies += [
        pltpu.make_async_copy(ref, deep.at[pl.ds(i * part, part)], sem.at[4 + i])
        for i, ref in enumerate((down_a, down_b))
    ]
    for copy in copies:
        copy.start()
    for copy in copies:
        copy.wait()


def stage(weights):
    dim, part = weights[0].shape
    return pl.pallas_call(
        stage_kernel,
        out_shape=(
            jax.ShapeDtypeStruct((dim, 4 * part), bf16),
            jax.ShapeDtypeStruct((2 * part, dim), bf16),
        ),
        in_specs=[hbm()] * 6,
        out_specs=[vmem()] * 2,
        scratch_shapes=[pltpu.SemaphoreType.DMA((6,))],
        compiler_params=params(4),
        cost_estimate=cost(4 * 1000 * dim * part, 12 * dim * part),
        name="stage",
    )(*[held_in_hbm(w) for w in weights])


def expert_kernel(groups, where_ref, *refs):
    tokens = refs[:groups]
    wide, deep = refs[groups : groups + 2]
    outs = refs[groups + 2 : 2 * groups + 2]
    held = refs[2 * groups + 2] if groups > 1 else tokens[0]
    dim = wide.shape[0]
    part = wide.shape[1] // 2
    chunk = dim // CHUNKS
    if groups > 1:
        for g, ref in enumerate(tokens):
            held[pl.ds(g * SLOTS, SLOTS)] = ref[...]
    total = jnp.dot(held[:, pl.ds(0, dim)], wide[...], preferred_element_type=f32)
    gate, upward = total[:, :part], total[:, part:]
    act = (gate / (1.0 + jnp.exp(-gate)) * upward).astype(bf16)
    shape = (EXTRA, EXTRA)
    expert = FAR * where_ref[0] + where_ref[1]
    from_share = iota(shape, 0) - CAP * EXPERTS
    hot = (from_share >= 0) & (from_share < 3 * EXPERTS) & (lax.rem(from_share + EXTRA, EXPERTS) == expert)
    share = jnp.dot(held[:, pl.ds(dim, EXTRA)], one_hot(hot), preferred_element_type=f32)[:, :1]
    for k in range(CHUNKS):
        cols = pl.ds(k * chunk, chunk)
        got = jnp.dot(act, deep[:, cols], preferred_element_type=f32) * share
        for g in range(groups):
            outs[g][:, cols] = got[g * SLOTS : (g + 1) * SLOTS].astype(bf16)


def expert_part(where, tokens, weights):
    wide, deep = weights
    dim = wide.shape[0]
    groups = len(tokens)
    rows = groups * SLOTS
    held = [pltpu.VMEM((rows, dim + EXTRA), bf16)] if groups > 1 else []
    return pl.pallas_call(
        functools.partial(expert_kernel, groups),
        out_shape=(jax.ShapeDtypeStruct((SLOTS, dim), bf16),) * groups,
        in_specs=[smem()] + [vmem()] * (groups + 2),
        out_specs=[vmem()] * groups,
        scratch_shapes=held,
        compiler_params=params(8),
        cost_estimate=cost(6 * rows * wide.size, 2 * rows * dim),
        name="expert_part",
    )(where, *tokens, held_in_vmem(wide), held_in_vmem(deep))


def collect_kernel(count, spread, *refs):
    parts, outs = refs[:count], refs[count:]
    for n in range(outs[0].shape[1] // TILE):
        put_rows(jnp.dot(spread[...], tiles_of(parts, 0, n), preferred_element_type=f32), outs, n)


def collect(spread, parts):
    width = parts[0].shape[1] // HALVES
    count = len(parts)
    return pl.pallas_call(
        functools.partial(collect_kernel, count),
        out_shape=row_shapes(spread.shape[0] // NEAR, width),
        in_specs=[vmem()] * (count + 1),
        out_specs=[vmem()] * 5,
        compiler_params=params(12),
        cost_estimate=cost(2 * spread.size * width, 4 * spread.shape[0] * width),
        name="collect",
    )(spread, *parts)


def merge_kernel(own, right, left, ahead, behind, first, *rest):
    block = first.shape[0]
    width = ahead.shape[1]
    for c, last in enumerate((ahead, behind)):
        cols = pl.ds(c * width, width)
        total = own[:, cols] + right[:, cols].astype(f32) + left[:, cols].astype(f32)
        total = total + last[...].astype(f32)
        first[:, cols] = total[:block]
        for k, out in enumerate(rest):
            out[:, cols] = total[(k + 1) * block : (k + 2) * block].astype(bf16)


def merge(own, *others):
    size, width = own.shape
    block = (size // FAR, width)
    return pl.pallas_call(
        merge_kernel,
        out_shape=(jax.ShapeDtypeStruct(block, f32),) + (jax.ShapeDtypeStruct(block, bf16),) * (FAR - 1),
        in_specs=[vmem()] * 5,
        out_specs=[vmem()] * FAR,
        compiler_params=params(4),
        cost_estimate=cost(4 * size * width, 12 * size * width),
        name="merge",
    )(own, *others)


def half_swap(a):
    middle = a.shape[0] // 2
    return jnp.concatenate([a[middle:], a[:middle]], axis=0)


def route_kernel(first, one, two, three, rows, gain, router, ids, slots, hidden, payload):
    count, half = rows.shape
    total = first[...] + one[...].astype(f32) + two[...].astype(f32) + three[...].astype(f32)
    total = rows[...].astype(f32) + total
    hidden[...] = total
    square = jnp.sum(total * total, axis=1, keepdims=True)
    scale = lax.rsqrt((square + half_swap(square)) / D + norm_eps)
    normed = (total * scale * gain[...]).astype(bf16)
    payload[:, pl.ds(0, half)] = normed
    parts = [
        lax.dot_general(normed, router[:, pl.ds(c * half, half)], NT, preferred_element_type=f32)
        for c in range(HALVES)
    ]
    logits = jnp.where(iota(parts[0].shape, 0) < count // 2, parts[0], parts[1])
    logits = logits + half_swap(logits)
    logits = jnp.concatenate([logits] * (EXTRA // EXPERTS), axis=1)
    lane = iota(logits.shape, 1)
    place = jnp.zeros(logits.shape, jnp.int32)
    for k in range(TOP):
        place = jnp.where(lax.rem(lane, EXPERTS) == ids[:, k : k + 1], slots[:, k : k + 1] + 1, place)
    gates = jnp.where(place > 0, 1.0 / (1.0 + jnp.exp(-logits)), 0.0)
    share = route_scale * gates / jnp.sum(jnp.where(lane < EXPERTS, gates, 0.0), axis=1, keepdims=True)
    kind = lane // EXPERTS
    table = jnp.zeros(logits.shape, f32)
    for n in range(CAP):
        table = jnp.where((kind == n) & (place == n + 1), 1.0, table)
    rest = share
    for n in range(3):
        piece = rest.astype(bf16).astype(f32)
        table = jnp.where(kind == CAP + n, piece, table)
        rest = rest - piece
    payload[:, pl.ds(half, EXTRA)] = table.astype(bf16)


def route(added, rows, gain, router, ids, slots):
    count, half = rows.shape
    return pl.pallas_call(
        route_kernel,
        out_shape=(
            jax.ShapeDtypeStruct((count, half), f32),
            jax.ShapeDtypeStruct((count, half + EXTRA), bf16),
        ),
        in_specs=[vmem()] * 9,
        out_specs=[vmem()] * 2,
        compiler_params=params(4),
        cost_estimate=cost(4 * count * half * EXPERTS, 20 * count * half),
        name="route",
    )(*added, rows, gain, router, ids, slots)


def finish_kernel(hidden, first, one, two, three, out):
    seqs, steps, _ = out.shape
    half = hidden.shape[1]
    total = first[...] + one[...].astype(f32) + two[...].astype(f32) + three[...].astype(f32)
    total = (hidden[...] + total).astype(bf16)
    for c in range(HALVES):
        for b in range(seqs):
            at = (c * seqs + b) * steps
            out[b, :, pl.ds(c * half, half)] = total[at : at + steps]


def finish(hidden, added, shape):
    return pl.pallas_call(
        finish_kernel,
        out_shape=jax.ShapeDtypeStruct(shape, bf16),
        in_specs=[vmem()] * 5,
        out_specs=vmem(),
        compiler_params=params(4),
        cost_estimate=cost(5 * hidden.size, 14 * hidden.size),
        name="finish",
    )(hidden, *added)


def reduce_z(own, right, left, ahead, behind):
    right = shift_z(right, 1)
    left = shift_z(left, -1)
    ahead = shift_z(ahead, 2)
    behind = shift_z(behind, -2)
    first, *sent = merge(own, right, left, ahead, behind)
    others = [shift_z(sent[0], NEAR), shift_z(sent[1], 2 * NEAR), shift_z(sent[2], -NEAR)]
    return first, *others


def layer(
    cache_kv,
    new_kv,
    queries,
    lengths,
    resid,
    value_up,
    out_proj,
    norm_gain,
    router,
    expert_ids,
    slots,
    w_gate,
    w_up,
    w_down,
):
    nx = lax.axis_size("x")
    seqs, steps = queries.shape[:2]
    tok = seqs * steps
    where = jnp.stack([lax.axis_index(a) for a in ("x", "zb", "j")]).astype(jnp.int32)
    where = jnp.concatenate([where, lengths.astype(jnp.int32)])

    tops, lows = pack(value_up.T, out_proj)
    top_left = shift_x(tops, 1)
    low_right = shift_x(lows, -1)
    low_left = shift_x(lows, 1)
    top_right = shift_x(tops, -1)

    outgoing = context_rows(where, nx, cache_kv, new_kv, queries)
    arrived = lax.all_to_all(
        outgoing.reshape(RING, nx * tok, LAT), ZAX, split_axis=0, concat_axis=0, tiled=True
    )
    top_far = shift_x(top_left, 1)
    low_far = shift_x(low_right, -1)
    near = [tops, lows, swap_core(tops), swap_core(lows)]
    for pair in ((top_left, low_left), (top_right, low_right)):
        near += [*pair, *map(swap_core, pair)]
    beyond = [top_far, low_far, swap_core(top_far), swap_core(low_far)]
    others = [swap_core(w) for w in (w_gate, w_up, w_down)]
    weights = stage((w_gate, others[0], w_up, others[1], w_down, others[2]))
    arrived = arrived.reshape(RING * nx * tok, LAT)
    most = attend_part(where, nx, arrived, near, tok, 0, None)
    added = reduce_z(*attend_part(where, nx, arrived, beyond, tok, nx - 1, most))

    half = D // HALVES
    rows = resid.reshape(tok, HALVES, half).swapaxes(0, 1).reshape(HALVES * tok, half)
    gain = jnp.repeat(norm_gain.astype(f32).reshape(HALVES, half), tok, axis=0)
    ids, places = [
        jnp.tile(a.reshape(tok, TOP).astype(jnp.int32), (HALVES, 1)) for a in (expert_ids, slots)
    ]
    hidden, payload = route(added, rows, gain, router.T, ids, places)

    ring = lax.all_gather(payload, ZAX, axis=0, tiled=True)
    *sent, spread = dispatch(where, nx, ring, tok)
    from_right = shift_x(sent[1], -1)
    from_left = shift_x(sent[2], 1)
    from_far = shift_x(sent[3], 2)
    done = expert_part(where, (sent[0], from_right, from_left), weights)
    back_left = shift_x(done[1], 1)
    back_right = shift_x(done[2], -1)
    (far_done,) = expert_part(where, (from_far,), weights)
    back_far = shift_x(far_done, 2)
    added = reduce_z(*collect(spread, (done[0], back_left, back_right, back_far)))
    return finish(hidden, added, resid.shape)


def solution(mesh):
    chips = mesh.shape["ep"] // (RING * CORES)
    grid = mesh.devices.reshape(mesh.shape["rep"], chips, FAR, NEAR, CORES)
    fine = Mesh(grid, ("rep", "x", "zb", "j", "c"))
    ep = ("x", "zb", "j", "c")
    both = ("rep",) + ep
    return jax.shard_map(
        layer,
        mesh=fine,
        in_specs=(
            P(both, None, None),
            P(both, None, None),
            P(both, None, None, None),
            P(both),
            P(both, None, None),
            P(None, ep),
            P(ep, None),
            P(),
            P(),
            P(both, None, None),
            P(both, None, None),
            P(None, ep),
            P(None, ep),
            P(ep, None),
        ),
        out_specs=P(both, None, None),
        check_vma=False,
    )
```

```python
import functools
import math

import jax
import jax.numpy as jnp
from jax import lax
from jax.experimental import pallas as pl
from jax.experimental.pallas import tpu as pltpu
from jax.sharding import Mesh
from jax.sharding import PartitionSpec as P


D = 7168
LAT = 512
VH = 128
EXPERTS = 16
TOP = 8
CAP = 2
QK = 192

CORES = 2
NEAR = 4
FAR = 4
RING = NEAR * FAR
SLOTS = RING * CAP
EXTRA = 128

route_scale = 2.827
norm_eps = 1e-06


ZAX = ("zb", "j")
f32, bf16 = jnp.float32, jnp.bfloat16
NT = (((1,), (1,)), ((), ()))


def swap_x(a, bits):
    return lax.ppermute(a, "x", [(i, i ^ bits) for i in range(lax.axis_size("x"))])


def shift_z(a, step):
    return lax.ppermute(a, ZAX, [(i, (i + step) % RING) for i in range(RING)])


def swap_far(a, bits):
    return lax.ppermute(a, "zb", [(i, i ^ bits) for i in range(FAR)])


def swap_core(a):
    return lax.ppermute(a, "c", [(i, i ^ 1) for i in range(CORES)])


def iota(shape, axis):
    return lax.broadcasted_iota(jnp.int32, shape, axis)


def one_hot(mask):
    return jnp.where(mask, 1.0, 0.0).astype(bf16)


COLUMNS = (0, 1, 3, 2)


def column(index, x):
    return x ^ jnp.where(index == 2, 3, jnp.where(index == 3, 2, index))


STEPS = (0, 1, RING - 1, 2, RING - 2)


def chip_at(place, where_ref):
    group, bits = place // FAR, lax.rem(place, FAR)
    step = 0
    for i, value in enumerate(STEPS):
        step = jnp.where(group == i, value, step)
    chip = lax.rem(NEAR * where_ref[1] + where_ref[2] + step, RING)
    return NEAR * ((chip // NEAR) ^ bits) + lax.rem(chip, NEAR)


def of_tile(rows, n, tiles):
    size = rows.shape[0] // len(STEPS)
    if n < tiles // 2:
        return rows[: 4 * size]
    return jnp.concatenate([rows[: 3 * size], rows[4 * size :]], axis=0)


def smem():
    return pl.BlockSpec(memory_space=pltpu.SMEM)


def vmem():
    return pl.BlockSpec(memory_space=pltpu.VMEM)


def hbm():
    return pl.BlockSpec(memory_space=pltpu.HBM)


def held_in_hbm(a):
    return pltpu.with_memory_space_constraint(a, pltpu.HBM)


def held_in_vmem(a):
    return pltpu.with_memory_space_constraint(a, pltpu.VMEM)


def params(mib):
    return pltpu.CompilerParams(vmem_limit_bytes=mib << 20)


def cost(flops, nbytes):
    return pl.CostEstimate(flops=flops, bytes_accessed=nbytes, transcendentals=0)


def context_kernel(nx, where_ref, keys, queries, new, out, held):
    seq = pl.program_id(0)
    seqs = pl.num_programs(0)
    steps, heads = queries.shape[1], queries.shape[2]
    count = steps * heads
    scale = 1.0 / math.sqrt(QK)
    query = queries[0].reshape(count, queries.shape[3])
    score = jnp.dot(query, keys[0], preferred_element_type=f32) * scale
    score = jnp.where(iota(score.shape, 1) < where_ref[3 + seq], score, -jnp.inf)
    wide = query.astype(f32)
    step_of = iota((count, 1), 0) // heads
    latest = []
    peak = jnp.max(score, axis=1, keepdims=True)
    for t in range(steps):
        key = new[0, t : t + 1, :].astype(f32)
        got = jnp.sum(wide * key, axis=1, keepdims=True) * scale
        got = jnp.where(step_of >= t, got, -jnp.inf)
        latest.append(got)
        peak = jnp.maximum(peak, got)
    probs = jnp.exp(score - peak)
    total = jnp.sum(probs, axis=1, keepdims=True)
    latest = [jnp.exp(got - peak) for got in latest]
    for got in latest:
        total = total + got
    share = 1.0 / total
    probs = (probs * share).astype(bf16)
    context = lax.dot_general(probs, keys[0, :LAT, :], NT, preferred_element_type=f32)
    for t, got in enumerate(latest):
        part = (got * share).astype(bf16).astype(f32)
        context = context + part * new[0, t : t + 1, :LAT].astype(f32)
    held[pl.ds(pl.multiple_of(seq * count, count), count), :] = context.astype(bf16)

    @pl.when(seq == seqs - 1)
    def _():
        rows = held.shape[0]
        tok = rows // heads
        shape = (rows, rows)
        to, source = iota(shape, 0), iota(shape, 1)
        hop = lax.rem(to // tok, nx)
        head = column(hop, where_ref[0]) * RING + to // (tok * nx)
        take = (lax.rem(to, tok) == source // heads) & (head == lax.rem(source, heads))
        out[...] = jnp.dot(one_hot(take), held[...], preferred_element_type=f32).astype(bf16)


def context_rows(where, nx, cache_kv, new_kv, queries):
    seqs, length, width = cache_kv.shape
    steps, heads = queries.shape[1:3]
    rows = seqs * steps * heads
    keys = jnp.swapaxes(cache_kv, 1, 2)
    return pl.pallas_call(
        functools.partial(context_kernel, nx),
        grid=(seqs,),
        out_shape=jax.ShapeDtypeStruct((rows, LAT), bf16),
        in_specs=[
            smem(),
            pl.BlockSpec((1, width, length), lambda b: (b, 0, 0)),
            pl.BlockSpec((1, steps, heads, width), lambda b: (b, 0, 0, 0)),
            pl.BlockSpec((1, steps, width), lambda b: (b, 0, 0)),
        ],
        out_specs=pl.BlockSpec((rows, LAT), lambda b: (0, 0)),
        scratch_shapes=[pltpu.VMEM((rows, LAT), bf16)],
        compiler_params=params(24),
        cost_estimate=cost(2 * rows * length * (width + LAT), 2 * cache_kv.size),
        name="context_rows",
    )(where, held_in_hbm(keys), held_in_hbm(queries), held_in_hbm(new_kv))


def pack_kernel(up, rows, tops, lows, sem):
    half, at = tops.shape[0], up.shape[1]
    copies = []
    for i, out in enumerate((tops, lows)):
        part = pl.ds(i * half, half)
        copies.append(pltpu.make_async_copy(rows.at[part], out.at[:, pl.ds(at, rows.shape[1])], sem.at[i, 0]))
        copies.append(pltpu.make_async_copy(up.at[part], out.at[:, pl.ds(0, at)], sem.at[i, 1]))
    for copy in copies:
        copy.start()
    for copy in copies:
        copy.wait()


def pack(up, rows):
    shape = (rows.shape[0] // 2, up.shape[1] + rows.shape[1])
    return pl.pallas_call(
        pack_kernel,
        out_shape=(jax.ShapeDtypeStruct(shape, bf16),) * 2,
        in_specs=[hbm()] * 2,
        out_specs=[vmem()] * 2,
        scratch_shapes=[pltpu.SemaphoreType.DMA((2, 2))],
        compiler_params=params(12),
        cost_estimate=cost(1, 4 * rows.size),
        name="pack",
    )(held_in_hbm(up), held_in_hbm(rows))


HALVES = 2
TILE = 256


def put_rows(got, outs, n):
    own, right, left, ahead, behind = outs
    size, width = own.shape[0], ahead.shape[1]
    cols = pl.ds(n * TILE, TILE)
    own[:, cols] = got[:size]
    right[:, cols] = got[size : 2 * size].astype(bf16)
    left[:, cols] = got[2 * size : 3 * size].astype(bf16)
    last, at = (ahead, n * TILE) if n * TILE < width else (behind, n * TILE - width)
    last[:, pl.ds(at, TILE)] = got[3 * size :].astype(bf16)


def row_shapes(size, width):
    return (
        jax.ShapeDtypeStruct((size, width), f32),
        jax.ShapeDtypeStruct((size, width), bf16),
        jax.ShapeDtypeStruct((size, width), bf16),
        jax.ShapeDtypeStruct((size, width // 2), bf16),
        jax.ShapeDtypeStruct((size, width // 2), bf16),
    )


def tiles_of(parts, at, n):
    half = (parts[0].shape[1] - at) // HALVES
    got = [p[:, pl.ds(at + c * half + n * TILE, TILE)] for c in range(HALVES) for p in parts]
    return jnp.concatenate(got, axis=0)


def attend_kernel(tok, nx, count, first, last, where_ref, arrived, *refs):
    pieces, outs = refs[:count], refs[count:]
    if last:
        before, outs = outs[0], outs[1:]
    up = jnp.concatenate([piece[:, pl.ds(0, LAT)] for piece in pieces], axis=0)
    values = lax.dot_general(arrived[...], up, NT, preferred_element_type=f32)
    hop = lax.rem(iota(values.shape, 0) // tok, nx)
    values = jnp.where(hop == first + iota(values.shape, 1) // VH, values, 0.0).astype(bf16)
    shape = (len(STEPS) * FAR * HALVES * tok, arrived.shape[0])
    row, source = iota(shape, 0), iota(shape, 1)
    chip = chip_at(row // (HALVES * tok), where_ref)
    take = (source // (tok * nx) == chip) & (lax.rem(source, tok) == lax.rem(row, tok))
    half = lax.rem(row // tok, HALVES)
    taken = [
        jnp.dot(one_hot(take & (half == c)), values, preferred_element_type=f32).astype(bf16)
        for c in range(HALVES)
    ]
    values = jnp.concatenate(taken, axis=1)
    tiles = outs[0].shape[1] // TILE
    for n in range(tiles):
        got = jnp.dot(of_tile(values, n, tiles), tiles_of(pieces, LAT, n), preferred_element_type=f32)
        cols = pl.ds(n * TILE, TILE)
        if last:
            put_rows(before[:, cols] + got, outs, n)
        else:
            outs[0][:, cols] = got


def attend_part(where, nx, arrived, pieces, tok, first, before):
    depth = sum(p.shape[0] for p in pieces)
    width = (pieces[0].shape[1] - LAT) // HALVES
    count = len(pieces)
    last = before is not None
    part = jax.ShapeDtypeStruct((RING * HALVES * tok, width), f32)
    return pl.pallas_call(
        functools.partial(attend_kernel, tok, nx, count, first, last),
        out_shape=row_shapes(FAR * HALVES * tok, width) if last else part,
        in_specs=[smem(), vmem()] + [vmem()] * count + [vmem()] * last,
        out_specs=[vmem()] * 5 if last else vmem(),
        compiler_params=params(6),
        cost_estimate=cost(8 * RING * tok * depth * width * HALVES, 4 * depth * width),
        name="attend_part",
    )(where, arrived, *pieces, *([before] if last else []))


SEND_TILE = 512


def dispatch_kernel(tok, nx, where_ref, tokens, *refs):
    outs, spread = refs[:nx], refs[nx]
    count, width = tokens.shape
    half = width - EXTRA
    table = tokens[:, pl.ds(half, EXTRA)]
    shape = (nx * CAP, EXTRA)
    row, place = iota(shape, 0), iota(shape, 1)
    expert = FAR * column(row // CAP, where_ref[0]) + where_ref[1]
    hot = one_hot(place == lax.rem(row, CAP) * EXPERTS + expert)
    got = lax.dot_general(hot, table, NT, preferred_element_type=f32)
    shape = (SLOTS, count)
    slot, token = iota(shape, 0), iota(shape, 1)
    parts = []
    for r in range(nx):
        sel = jnp.where(lax.rem(slot, CAP) == 0, got[CAP * r : CAP * r + 1], got[CAP * r + 1 : CAP * r + 2])
        parts.append(jnp.where(slot // CAP == token // (HALVES * tok), sel, 0.0))
    sel = jnp.concatenate(parts, axis=0)
    of_half = lax.rem(iota(sel.shape, 1) // tok, HALVES)
    sels = [jnp.where(of_half == c, sel, 0.0).astype(bf16) for c in range(HALVES)]
    both = jnp.concatenate(sels, axis=0)
    rows = nx * SLOTS
    for n in range(half // SEND_TILE):
        got = jnp.dot(both, tokens[:, pl.ds(n * SEND_TILE, SEND_TILE)], preferred_element_type=f32).astype(bf16)
        for c in range(HALVES):
            for r in range(nx):
                at = c * rows + r * SLOTS
                outs[r][:, pl.ds(c * half + n * SEND_TILE, SEND_TILE)] = got[at : at + SLOTS]
    got = jnp.dot(sels[0], table, preferred_element_type=f32).astype(bf16)
    for r in range(nx):
        outs[r][:, pl.ds(HALVES * half, EXTRA)] = got[r * SLOTS : (r + 1) * SLOTS]
    shape = (spread.shape[0], count)
    row, token = iota(shape, 0), iota(shape, 1)
    chip = chip_at(row // (HALVES * tok), where_ref)
    take = (token // (HALVES * tok) == chip) & (lax.rem(token, HALVES * tok) == lax.rem(row, HALVES * tok))
    for c in range(HALVES):
        got = lax.dot_general(one_hot(take), sels[c], NT, preferred_element_type=f32)
        spread[:, pl.ds(c * rows, rows)] = got.astype(bf16)


def dispatch(where, nx, tokens, tok):
    count, width = tokens.shape
    full = HALVES * (width - EXTRA) + EXTRA
    return pl.pallas_call(
        functools.partial(dispatch_kernel, tok, nx),
        out_shape=(jax.ShapeDtypeStruct((SLOTS, full), bf16),) * nx
        + (jax.ShapeDtypeStruct((count // NEAR * len(STEPS), HALVES * nx * SLOTS), bf16),),
        in_specs=[smem(), vmem()],
        out_specs=[vmem()] * (nx + 1),
        compiler_params=params(12),
        cost_estimate=cost(2 * nx * SLOTS * count * full, 4 * count * width),
        name="dispatch",
    )(where, tokens)


CHUNKS = 7


def stage_kernel(gate_a, gate_b, up_a, up_b, down_a, down_b, wide, deep, sem):
    part = gate_a.shape[1]
    copies = [
        pltpu.make_async_copy(ref, wide.at[:, pl.ds(i * part, part)], sem.at[i])
        for i, ref in enumerate((gate_a, gate_b, up_a, up_b))
    ]
    copies += [
        pltpu.make_async_copy(ref, deep.at[pl.ds(i * part, part)], sem.at[4 + i])
        for i, ref in enumerate((down_a, down_b))
    ]
    for copy in copies:
        copy.start()
    for copy in copies:
        copy.wait()


def stage(weights):
    dim, part = weights[0].shape
    return pl.pallas_call(
        stage_kernel,
        out_shape=(
            jax.ShapeDtypeStruct((dim, 4 * part), bf16),
            jax.ShapeDtypeStruct((2 * part, dim), bf16),
        ),
        in_specs=[hbm()] * 6,
        out_specs=[vmem()] * 2,
        scratch_shapes=[pltpu.SemaphoreType.DMA((6,))],
        compiler_params=params(4),
        cost_estimate=cost(4 * 1000 * dim * part, 12 * dim * part),
        name="stage",
    )(*[held_in_hbm(w) for w in weights])


def expert_kernel(groups, where_ref, *refs):
    tokens = refs[:groups]
    wide, deep = refs[groups : groups + 2]
    outs = refs[groups + 2 : 2 * groups + 2]
    held = refs[2 * groups + 2] if groups > 1 else tokens[0]
    dim = wide.shape[0]
    part = wide.shape[1] // 2
    chunk = dim // CHUNKS
    if groups > 1:
        for g, ref in enumerate(tokens):
            held[pl.ds(g * SLOTS, SLOTS)] = ref[...]
    total = jnp.dot(held[:, pl.ds(0, dim)], wide[...], preferred_element_type=f32)
    gate, upward = total[:, :part], total[:, part:]
    act = (gate / (1.0 + jnp.exp(-gate)) * upward).astype(bf16)
    shape = (EXTRA, EXTRA)
    expert = FAR * where_ref[0] + where_ref[1]
    from_share = iota(shape, 0) - CAP * EXPERTS
    hot = (from_share >= 0) & (from_share < 3 * EXPERTS) & (lax.rem(from_share + EXTRA, EXPERTS) == expert)
    share = jnp.dot(held[:, pl.ds(dim, EXTRA)], one_hot(hot), preferred_element_type=f32)[:, :1]
    for k in range(CHUNKS):
        cols = pl.ds(k * chunk, chunk)
        got = jnp.dot(act, deep[:, cols], preferred_element_type=f32) * share
        for g in range(groups):
            outs[g][:, cols] = got[g * SLOTS : (g + 1) * SLOTS].astype(bf16)


def expert_part(where, tokens, weights):
    wide, deep = weights
    dim = wide.shape[0]
    groups = len(tokens)
    rows = groups * SLOTS
    held = [pltpu.VMEM((rows, dim + EXTRA), bf16)] if groups > 1 else []
    return pl.pallas_call(
        functools.partial(expert_kernel, groups),
        out_shape=(jax.ShapeDtypeStruct((SLOTS, dim), bf16),) * groups,
        in_specs=[smem()] + [vmem()] * (groups + 2),
        out_specs=[vmem()] * groups,
        scratch_shapes=held,
        compiler_params=params(8),
        cost_estimate=cost(6 * rows * wide.size, 2 * rows * dim),
        name="expert_part",
    )(where, *tokens, held_in_vmem(wide), held_in_vmem(deep))


def collect_kernel(count, spread, *refs):
    parts, outs = refs[:count], refs[count:]
    tiles = outs[0].shape[1] // TILE
    for n in range(tiles):
        got = jnp.dot(of_tile(spread[...], n, tiles), tiles_of(parts, 0, n), preferred_element_type=f32)
        put_rows(got, outs, n)


def collect(spread, parts):
    width = parts[0].shape[1] // HALVES
    count = len(parts)
    return pl.pallas_call(
        functools.partial(collect_kernel, count),
        out_shape=row_shapes(spread.shape[0] // len(STEPS), width),
        in_specs=[vmem()] * (count + 1),
        out_specs=[vmem()] * 5,
        compiler_params=params(12),
        cost_estimate=cost(2 * spread.size * width, 4 * spread.shape[0] * width),
        name="collect",
    )(spread, *parts)


def merge_kernel(own, right, left, ahead, behind, first, *rest):
    block = first.shape[0]
    width = ahead.shape[1]
    for c, last in enumerate((ahead, behind)):
        cols = pl.ds(c * width, width)
        total = own[:, cols] + right[:, cols].astype(f32) + left[:, cols].astype(f32)
        total = total + last[...].astype(f32)
        first[:, cols] = total[:block]
        for k, out in enumerate(rest):
            out[:, cols] = total[(k + 1) * block : (k + 2) * block].astype(bf16)


def merge(own, *others):
    size, width = own.shape
    block = (size // FAR, width)
    return pl.pallas_call(
        merge_kernel,
        out_shape=(jax.ShapeDtypeStruct(block, f32),) + (jax.ShapeDtypeStruct(block, bf16),) * (FAR - 1),
        in_specs=[vmem()] * 5,
        out_specs=[vmem()] * FAR,
        compiler_params=params(4),
        cost_estimate=cost(4 * size * width, 12 * size * width),
        name="merge",
    )(own, *others)


def half_swap(a):
    middle = a.shape[0] // 2
    return jnp.concatenate([a[middle:], a[:middle]], axis=0)


def route_kernel(first, one, two, three, rows, gain, router, ids, slots, hidden, payload):
    count, half = rows.shape
    total = first[...] + one[...].astype(f32) + two[...].astype(f32) + three[...].astype(f32)
    total = rows[...].astype(f32) + total
    hidden[...] = total
    square = jnp.sum(total * total, axis=1, keepdims=True)
    scale = lax.rsqrt((square + half_swap(square)) / D + norm_eps)
    normed = (total * scale * gain[...]).astype(bf16)
    payload[:, pl.ds(0, half)] = normed
    parts = [
        lax.dot_general(normed, router[:, pl.ds(c * half, half)], NT, preferred_element_type=f32)
        for c in range(HALVES)
    ]
    logits = jnp.where(iota(parts[0].shape, 0) < count // 2, parts[0], parts[1])
    logits = logits + half_swap(logits)
    logits = jnp.concatenate([logits] * (EXTRA // EXPERTS), axis=1)
    lane = iota(logits.shape, 1)
    place = jnp.zeros(logits.shape, jnp.int32)
    for k in range(TOP):
        place = jnp.where(lax.rem(lane, EXPERTS) == ids[:, k : k + 1], slots[:, k : k + 1] + 1, place)
    gates = jnp.where(place > 0, 1.0 / (1.0 + jnp.exp(-logits)), 0.0)
    share = route_scale * gates / jnp.sum(jnp.where(lane < EXPERTS, gates, 0.0), axis=1, keepdims=True)
    kind = lane // EXPERTS
    table = jnp.zeros(logits.shape, f32)
    for n in range(CAP):
        table = jnp.where((kind == n) & (place == n + 1), 1.0, table)
    rest = share
    for n in range(3):
        piece = rest.astype(bf16).astype(f32)
        table = jnp.where(kind == CAP + n, piece, table)
        rest = rest - piece
    payload[:, pl.ds(half, EXTRA)] = table.astype(bf16)


def route(added, rows, gain, router, ids, slots):
    count, half = rows.shape
    return pl.pallas_call(
        route_kernel,
        out_shape=(
            jax.ShapeDtypeStruct((count, half), f32),
            jax.ShapeDtypeStruct((count, half + EXTRA), bf16),
        ),
        in_specs=[vmem()] * 9,
        out_specs=[vmem()] * 2,
        compiler_params=params(4),
        cost_estimate=cost(4 * count * half * EXPERTS, 20 * count * half),
        name="route",
    )(*added, rows, gain, router, ids, slots)


def finish_kernel(hidden, first, one, two, three, out):
    seqs, steps, _ = out.shape
    half = hidden.shape[1]
    total = first[...] + one[...].astype(f32) + two[...].astype(f32) + three[...].astype(f32)
    total = (hidden[...] + total).astype(bf16)
    for c in range(HALVES):
        for b in range(seqs):
            at = (c * seqs + b) * steps
            out[b, :, pl.ds(c * half, half)] = total[at : at + steps]


def finish(hidden, added, shape):
    return pl.pallas_call(
        finish_kernel,
        out_shape=jax.ShapeDtypeStruct(shape, bf16),
        in_specs=[vmem()] * 5,
        out_specs=vmem(),
        compiler_params=params(4),
        cost_estimate=cost(5 * hidden.size, 14 * hidden.size),
        name="finish",
    )(hidden, *added)


def reduce_z(own, right, left, ahead, behind):
    right = shift_z(right, 1)
    left = shift_z(left, -1)
    ahead = shift_z(ahead, 2)
    behind = shift_z(behind, -2)
    first, *sent = merge(own, right, left, ahead, behind)
    others = [swap_far(rows, k + 1) for k, rows in enumerate(sent)]
    return first, *others


def layer(
    cache_kv,
    new_kv,
    queries,
    lengths,
    resid,
    value_up,
    out_proj,
    norm_gain,
    router,
    expert_ids,
    slots,
    w_gate,
    w_up,
    w_down,
):
    nx = lax.axis_size("x")
    seqs, steps = queries.shape[:2]
    tok = seqs * steps
    where = jnp.stack([lax.axis_index(a) for a in ("x", "zb", "j")]).astype(jnp.int32)
    where = jnp.concatenate([where, lengths.astype(jnp.int32)])

    tops, lows = pack(value_up.T, out_proj)
    top_left = swap_x(tops, 1)
    low_right = swap_x(lows, 3)
    low_left = swap_x(lows, 1)
    top_right = swap_x(tops, 3)

    outgoing = context_rows(where, nx, cache_kv, new_kv, queries)
    arrived = lax.all_to_all(
        outgoing.reshape(RING, nx * tok, LAT), ZAX, split_axis=0, concat_axis=0, tiled=True
    )
    top_far = swap_x(top_left, 3)
    low_far = swap_x(low_right, 1)
    near = [tops, lows, swap_core(tops), swap_core(lows)]
    for pair in ((top_left, low_left), (top_right, low_right)):
        near += [*pair, *map(swap_core, pair)]
    beyond = [top_far, low_far, swap_core(top_far), swap_core(low_far)]
    others = [swap_core(w) for w in (w_gate, w_up, w_down)]
    weights = stage((w_gate, others[0], w_up, others[1], w_down, others[2]))
    arrived = arrived.reshape(RING * nx * tok, LAT)
    most = attend_part(where, nx, arrived, near, tok, 0, None)
    added = reduce_z(*attend_part(where, nx, arrived, beyond, tok, nx - 1, most))

    half = D // HALVES
    rows = resid.reshape(tok, HALVES, half).swapaxes(0, 1).reshape(HALVES * tok, half)
    gain = jnp.repeat(norm_gain.astype(f32).reshape(HALVES, half), tok, axis=0)
    ids, places = [
        jnp.tile(a.reshape(tok, TOP).astype(jnp.int32), (HALVES, 1)) for a in (expert_ids, slots)
    ]
    hidden, payload = route(added, rows, gain, router.T, ids, places)

    ring = lax.all_gather(payload, ZAX, axis=0, tiled=True)
    *sent, spread = dispatch(where, nx, ring, tok)
    from_one, from_three, from_two = [swap_x(sent[i], COLUMNS[i]) for i in (1, 2, 3)]
    done = expert_part(where, (sent[0], from_one, from_three), weights)
    back_one, back_three = swap_x(done[1], 1), swap_x(done[2], 3)
    (far_done,) = expert_part(where, (from_two,), weights)
    back_two = swap_x(far_done, 2)
    added = reduce_z(*collect(spread, (done[0], back_one, back_three, back_two)))
    return finish(hidden, added, resid.shape)


def solution(mesh):
    chips = mesh.shape["ep"] // (RING * CORES)
    grid = mesh.devices.reshape(mesh.shape["rep"], chips, FAR, NEAR, CORES)
    fine = Mesh(grid, ("rep", "x", "zb", "j", "c"))
    ep = ("x", "zb", "j", "c")
    both = ("rep",) + ep
    return jax.shard_map(
        layer,
        mesh=fine,
        in_specs=(
            P(both, None, None),
            P(both, None, None),
            P(both, None, None, None),
            P(both),
            P(both, None, None),
            P(None, ep),
            P(ep, None),
            P(),
            P(),
            P(both, None, None),
            P(both, None, None),
            P(None, ep),
            P(None, ep),
            P(ep, None),
        ),
        out_specs=P(both, None, None),
        check_vma=False,
    )
```

```python
import functools
import math

import jax
import jax.numpy as jnp
from jax import lax
from jax.experimental import pallas as pl
from jax.experimental.pallas import tpu as pltpu
from jax.sharding import Mesh
from jax.sharding import PartitionSpec as P


D = 7168
LAT = 512
EXPERTS = 16
TOP = 8
CAP = 2
QK = 192

CORES = 2
NEAR = 4
FAR = 4
RING = NEAR * FAR
SLOTS = RING * CAP
LATE = FAR * CAP
EARLY = SLOTS - LATE
EXTRA = 128

route_scale = 2.827
norm_eps = 1e-06


ZAX = ("zb", "j")
f32, bf16 = jnp.float32, jnp.bfloat16
NT = (((1,), (1,)), ((), ()))


def swap_x(a, bits):
    return lax.ppermute(a, "x", [(i, i ^ bits) for i in range(lax.axis_size("x"))])


def shift_z(a, step):
    return lax.ppermute(a, ZAX, [(i, (i + step) % RING) for i in range(RING)])


def swap_far(a, bits):
    return lax.ppermute(a, "zb", [(i, i ^ bits) for i in range(FAR)])


def swap_core(a):
    return lax.ppermute(a, "c", [(i, i ^ 1) for i in range(CORES)])


def iota(shape, axis):
    return lax.broadcasted_iota(jnp.int32, shape, axis)


def one_hot(mask):
    return jnp.where(mask, 1.0, 0.0).astype(bf16)


COLUMNS = (0, 1, 3, 2)


def column(index, x):
    return x ^ jnp.where(index == 2, 3, jnp.where(index == 3, 2, index))


STEPS = (0, 1, RING - 1, 2, RING - 2)


def chip_at(place, where_ref):
    group, bits = place // FAR, lax.rem(place, FAR)
    step = 0
    for i, value in enumerate(STEPS):
        step = jnp.where(group == i, value, step)
    chip = lax.rem(NEAR * where_ref[1] + where_ref[2] + step, RING)
    return NEAR * ((chip // NEAR) ^ bits) + lax.rem(chip, NEAR)


def of_tile(rows, n, tiles):
    size = rows.shape[0] // len(STEPS)
    if n < tiles // 2:
        return rows[: 4 * size]
    return jnp.concatenate([rows[: 3 * size], rows[4 * size :]], axis=0)


def smem():
    return pl.BlockSpec(memory_space=pltpu.SMEM)


def vmem():
    return pl.BlockSpec(memory_space=pltpu.VMEM)


def hbm():
    return pl.BlockSpec(memory_space=pltpu.HBM)


def held_in_hbm(a):
    return pltpu.with_memory_space_constraint(a, pltpu.HBM)


def held_in_vmem(a):
    return pltpu.with_memory_space_constraint(a, pltpu.VMEM)


def params(mib):
    return pltpu.CompilerParams(vmem_limit_bytes=mib << 20)


def cost(flops, nbytes):
    return pl.CostEstimate(flops=flops, bytes_accessed=nbytes, transcendentals=0)


def context_kernel(nx, where_ref, keys, queries, new, out, held):
    seq = pl.program_id(0)
    seqs = pl.num_programs(0)
    steps, heads = queries.shape[1], queries.shape[2]
    count = steps * heads
    scale = 1.0 / math.sqrt(QK)
    query = queries[0].reshape(count, queries.shape[3])
    score = jnp.dot(query, keys[0], preferred_element_type=f32) * scale
    score = jnp.where(iota(score.shape, 1) < where_ref[3 + seq], score, -jnp.inf)
    wide = query.astype(f32)
    step_of = iota((count, 1), 0) // heads
    latest = []
    peak = jnp.max(score, axis=1, keepdims=True)
    for t in range(steps):
        key = new[0, t : t + 1, :].astype(f32)
        got = jnp.sum(wide * key, axis=1, keepdims=True) * scale
        got = jnp.where(step_of >= t, got, -jnp.inf)
        latest.append(got)
        peak = jnp.maximum(peak, got)
    probs = jnp.exp(score - peak)
    total = jnp.sum(probs, axis=1, keepdims=True)
    latest = [jnp.exp(got - peak) for got in latest]
    for got in latest:
        total = total + got
    share = 1.0 / total
    probs = (probs * share).astype(bf16)
    context = lax.dot_general(probs, keys[0, :LAT, :], NT, preferred_element_type=f32)
    for t, got in enumerate(latest):
        part = (got * share).astype(bf16).astype(f32)
        context = context + part * new[0, t : t + 1, :LAT].astype(f32)
    held[pl.ds(pl.multiple_of(seq * count, count), count), :] = context.astype(bf16)

    @pl.when(seq == seqs - 1)
    def _():
        rows = held.shape[0]
        tok = rows // heads
        shape = (rows, rows)
        to, source = iota(shape, 0), iota(shape, 1)
        hop = lax.rem(to // tok, nx)
        head = column(hop, where_ref[0]) * RING + to // (tok * nx)
        take = (lax.rem(to, tok) == source // heads) & (head == lax.rem(source, heads))
        out[...] = jnp.dot(one_hot(take), held[...], preferred_element_type=f32).astype(bf16)


def context_rows(where, nx, cache_kv, new_kv, queries):
    seqs, length, width = cache_kv.shape
    steps, heads = queries.shape[1:3]
    rows = seqs * steps * heads
    keys = jnp.swapaxes(cache_kv, 1, 2)
    return pl.pallas_call(
        functools.partial(context_kernel, nx),
        grid=(seqs,),
        out_shape=jax.ShapeDtypeStruct((rows, LAT), bf16),
        in_specs=[
            smem(),
            pl.BlockSpec((1, width, length), lambda b: (b, 0, 0)),
            pl.BlockSpec((1, steps, heads, width), lambda b: (b, 0, 0, 0)),
            pl.BlockSpec((1, steps, width), lambda b: (b, 0, 0)),
        ],
        out_specs=pl.BlockSpec((rows, LAT), lambda b: (0, 0)),
        scratch_shapes=[pltpu.VMEM((rows, LAT), bf16)],
        compiler_params=params(24),
        cost_estimate=cost(2 * rows * length * (width + LAT), 2 * cache_kv.size),
        name="context_rows",
    )(where, held_in_hbm(keys), held_in_hbm(queries), held_in_hbm(new_kv))


def pack_kernel(up, rows, tops, lows, sem):
    half, at = tops.shape[0], up.shape[1]
    copies = []
    for i, out in enumerate((tops, lows)):
        part = pl.ds(i * half, half)
        copies.append(pltpu.make_async_copy(rows.at[part], out.at[:, pl.ds(at, rows.shape[1])], sem.at[i, 0]))
        copies.append(pltpu.make_async_copy(up.at[part], out.at[:, pl.ds(0, at)], sem.at[i, 1]))
    for copy in copies:
        copy.start()
    for copy in copies:
        copy.wait()


def pack(up, rows):
    shape = (rows.shape[0] // 2, up.shape[1] + rows.shape[1])
    return pl.pallas_call(
        pack_kernel,
        out_shape=(jax.ShapeDtypeStruct(shape, bf16),) * 2,
        in_specs=[hbm()] * 2,
        out_specs=[vmem()] * 2,
        scratch_shapes=[pltpu.SemaphoreType.DMA((2, 2))],
        compiler_params=params(12),
        cost_estimate=cost(1, 4 * rows.size),
        name="pack",
    )(held_in_hbm(up), held_in_hbm(rows))


def join_kernel(count, *refs):
    at = 0
    for ref in refs[:count]:
        refs[count][pl.ds(at, ref.shape[0])] = ref[...]
        at += ref.shape[0]


def join(*arrays):
    rows, width = sum(a.shape[0] for a in arrays), arrays[0].shape[1]
    return pl.pallas_call(
        functools.partial(join_kernel, len(arrays)),
        out_shape=jax.ShapeDtypeStruct((rows, width), bf16),
        in_specs=[vmem()] * len(arrays),
        out_specs=vmem(),
        compiler_params=params(4),
        cost_estimate=cost(rows * width, 4 * rows * width),
        name="join",
    )(*arrays)


HALVES = 2
TILE = 256


def put_rows(got, outs, n):
    own, right, left, ahead, behind = outs
    size, width = own.shape[0], ahead.shape[1]
    cols = pl.ds(n * TILE, TILE)
    own[:, cols] = got[:size]
    right[:, cols] = got[size : 2 * size].astype(bf16)
    left[:, cols] = got[2 * size : 3 * size].astype(bf16)
    last, at = (ahead, n * TILE) if n * TILE < width else (behind, n * TILE - width)
    last[:, pl.ds(at, TILE)] = got[3 * size :].astype(bf16)


def row_shapes(size, width):
    return (
        jax.ShapeDtypeStruct((size, width), f32),
        jax.ShapeDtypeStruct((size, width), bf16),
        jax.ShapeDtypeStruct((size, width), bf16),
        jax.ShapeDtypeStruct((size, width // 2), bf16),
        jax.ShapeDtypeStruct((size, width // 2), bf16),
    )


def tiles_of(parts, at, n):
    half = (parts[0].shape[1] - at) // HALVES
    got = [p[:, pl.ds(at + c * half + n * TILE, TILE)] for c in range(HALVES) for p in parts]
    return jnp.concatenate(got, axis=0)


def attend_kernel(tok, nx, count, hops, last, where_ref, arrived, *refs):
    pieces, outs = refs[:count], refs[count:]
    if last:
        before, outs = outs[0], outs[1:]
    up = jnp.concatenate([piece[:, pl.ds(0, LAT)] for piece in pieces], axis=0)
    values = lax.dot_general(arrived[...], up, NT, preferred_element_type=f32)
    hop = lax.rem(iota(values.shape, 0) // tok, nx)
    part = iota(values.shape, 1) // (values.shape[1] // len(hops))
    wanted = sum(jnp.where(part == i, value, 0) for i, value in enumerate(hops))
    values = jnp.where(hop == wanted, values, 0.0).astype(bf16)
    shape = (len(STEPS) * FAR * HALVES * tok, arrived.shape[0])
    row, source = iota(shape, 0), iota(shape, 1)
    chip = chip_at(row // (HALVES * tok), where_ref)
    take = (source // (tok * nx) == chip) & (lax.rem(source, tok) == lax.rem(row, tok))
    half = lax.rem(row // tok, HALVES)
    taken = [
        jnp.dot(one_hot(take & (half == c)), values, preferred_element_type=f32).astype(bf16)
        for c in range(HALVES)
    ]
    values = jnp.concatenate(taken, axis=1)
    tiles = outs[0].shape[1] // TILE
    for n in range(tiles):
        got = jnp.dot(of_tile(values, n, tiles), tiles_of(pieces, LAT, n), preferred_element_type=f32)
        cols = pl.ds(n * TILE, TILE)
        if last:
            put_rows(before[:, cols] + got, outs, n)
        else:
            outs[0][:, cols] = got


def attend_part(where, nx, arrived, pieces, hops, tok, before):
    depth = sum(p.shape[0] for p in pieces)
    width = (pieces[0].shape[1] - LAT) // HALVES
    count = len(pieces)
    last = before is not None
    part = jax.ShapeDtypeStruct((RING * HALVES * tok, width), f32)
    return pl.pallas_call(
        functools.partial(attend_kernel, tok, nx, count, hops, last),
        out_shape=row_shapes(FAR * HALVES * tok, width) if last else part,
        in_specs=[smem(), vmem()] + [vmem()] * count + [vmem()] * last,
        out_specs=[vmem()] * 5 if last else vmem(),
        compiler_params=params(6),
        cost_estimate=cost(8 * RING * tok * depth * width * HALVES, 4 * depth * width),
        name="attend_part",
    )(where, arrived, *pieces, *([before] if last else []))


SEND_TILE = 512


def slot_rows(tok, nx, where_ref, table):
    count = table.shape[0]
    shape = (nx * CAP, EXTRA)
    row, place = iota(shape, 0), iota(shape, 1)
    expert = FAR * column(row // CAP, where_ref[0]) + where_ref[1]
    hot = one_hot(place == lax.rem(row, CAP) * EXPERTS + expert)
    got = lax.dot_general(hot, table, NT, preferred_element_type=f32)
    shape = (count // (HALVES * tok) * CAP, count)
    slot, token = iota(shape, 0), iota(shape, 1)
    same = slot // CAP == token // (HALVES * tok)
    half = lax.rem(token // tok, HALVES)
    parts = []
    for c in range(HALVES):
        for r in range(nx):
            sel = jnp.where(lax.rem(slot, CAP) == 0, got[CAP * r : CAP * r + 1], got[CAP * r + 1 : CAP * r + 2])
            parts.append(jnp.where(same & (half == c), sel, 0.0))
    return jnp.concatenate(parts, axis=0).astype(bf16)


def dispatch_kernel(tok, nx, inputs, where_ref, *refs):
    tokens, outs = refs[:inputs], refs[inputs:]
    width = tokens[0].shape[1]
    half = width - EXTRA

    def columns(at, size):
        return jnp.concatenate([ref[:, pl.ds(at, size)] for ref in tokens], axis=0)

    table = columns(half, EXTRA)
    both = slot_rows(tok, nx, where_ref, table)
    rows = both.shape[0] // HALVES
    slots = rows // nx
    for n in range(half // SEND_TILE):
        got = jnp.dot(both, columns(n * SEND_TILE, SEND_TILE), preferred_element_type=f32).astype(bf16)
        for c in range(HALVES):
            for r in range(nx):
                at = c * rows + r * slots
                outs[r][:, pl.ds(c * half + n * SEND_TILE, SEND_TILE)] = got[at : at + slots]
    got = jnp.dot(both[:rows], table, preferred_element_type=f32).astype(bf16)
    for r in range(nx):
        outs[r][:, pl.ds(HALVES * half, EXTRA)] = got[r * slots : (r + 1) * slots]


def dispatch(where, nx, tokens, tok):
    count, width = sum(a.shape[0] for a in tokens), tokens[0].shape[1]
    full = HALVES * (width - EXTRA) + EXTRA
    slots = count // (HALVES * tok) * CAP
    return pl.pallas_call(
        functools.partial(dispatch_kernel, tok, nx, len(tokens)),
        out_shape=(jax.ShapeDtypeStruct((slots, full), bf16),) * nx,
        in_specs=[smem()] + [vmem()] * len(tokens),
        out_specs=[vmem()] * nx,
        compiler_params=params(12),
        cost_estimate=cost(2 * nx * slots * count * full, 4 * count * width),
        name="dispatch",
    )(where, *tokens)


def plan_kernel(tok, nx, inputs, group, turn, where_ref, *refs):
    tokens, out = refs[:inputs], refs[inputs]
    width = tokens[0].shape[1]
    table = jnp.concatenate([ref[:, pl.ds(width - EXTRA, EXTRA)] for ref in tokens], axis=0)
    both = slot_rows(tok, nx, where_ref, table)
    shape = (out.shape[0], table.shape[0])
    row, token = iota(shape, 0), iota(shape, 1)
    unit = HALVES * tok
    wanted = chip_at(group * FAR + row // unit, where_ref)
    source = token // unit
    chip = NEAR * lax.rem(source, FAR) + lax.rem(where_ref[2] + turn + source // FAR, NEAR)
    take = (chip == wanted) & (lax.rem(token, unit) == lax.rem(row, unit))
    out[...] = lax.dot_general(one_hot(take), both, NT, preferred_element_type=f32).astype(bf16)


def plan(where, nx, tokens, tok, group, groups, turn):
    count = sum(a.shape[0] for a in tokens)
    unit = HALVES * tok
    shape = (groups * FAR * unit, HALVES * nx * (count // unit * CAP))
    return pl.pallas_call(
        functools.partial(plan_kernel, tok, nx, len(tokens), group, turn),
        out_shape=jax.ShapeDtypeStruct(shape, bf16),
        in_specs=[smem()] + [vmem()] * len(tokens),
        out_specs=vmem(),
        compiler_params=params(4),
        cost_estimate=cost(2 * shape[0] * shape[1] * count, 2 * shape[0] * shape[1]),
        name="plan",
    )(where, *tokens)


CHUNKS = 14


def pair_kernel(first, second, out, sem):
    rows = first.shape[0]
    copies = [
        pltpu.make_async_copy(ref, out.at[pl.ds(i * rows, rows)], sem.at[i])
        for i, ref in enumerate((first, second))
    ]
    for copy in copies:
        copy.start()
    for copy in copies:
        copy.wait()


def pair(first, second):
    rows, width = first.shape
    return pl.pallas_call(
        pair_kernel,
        out_shape=jax.ShapeDtypeStruct((2 * rows, width), bf16),
        in_specs=[hbm()] * 2,
        out_specs=vmem(),
        scratch_shapes=[pltpu.SemaphoreType.DMA((2,))],
        compiler_params=params(4),
        cost_estimate=cost(1, 8 * rows * width),
        name="pair",
    )(held_in_hbm(first), held_in_hbm(second))


def stage_kernel(gate, up, others, down_a, down_b, wide, deep, sem):
    rows, part = gate.shape
    parts = gate, others.at[pl.ds(0, rows)], up, others.at[pl.ds(rows, rows)]
    copies = [
        pltpu.make_async_copy(ref, wide.at[:, pl.ds(i * part, part)], sem.at[i])
        for i, ref in enumerate(parts)
    ]
    copies += [
        pltpu.make_async_copy(ref, deep.at[pl.ds(i * part, part)], sem.at[4 + i])
        for i, ref in enumerate((down_a, down_b))
    ]
    for copy in copies:
        copy.start()
    for copy in copies:
        copy.wait()


def stage(weights):
    dim, part = weights[0].shape
    return pl.pallas_call(
        stage_kernel,
        out_shape=(
            jax.ShapeDtypeStruct((dim, 4 * part), bf16),
            jax.ShapeDtypeStruct((2 * part, dim), bf16),
        ),
        in_specs=[hbm()] * 5,
        out_specs=[vmem()] * 2,
        scratch_shapes=[pltpu.SemaphoreType.DMA((6,))],
        compiler_params=params(4),
        cost_estimate=cost(4 * 1000 * dim * part, 12 * dim * part),
        name="stage",
    )(*[held_in_hbm(w) for w in weights])


def expert_kernel(groups, where_ref, *refs):
    tokens, refs = refs[: 2 * groups], refs[2 * groups :]
    (wide, deep), (early, late) = refs[:2], (refs[2 : groups + 2], refs[groups + 2 : -1])
    held = refs[-1]
    dim = wide.shape[0]
    part = wide.shape[1] // 2
    chunk = dim // CHUNKS
    chunks = CHUNKS
    for g in range(groups):
        held[pl.ds(g * SLOTS, EARLY)] = tokens[2 * g][...]
        held[pl.ds(g * SLOTS + EARLY, LATE)] = tokens[2 * g + 1][...]

    total = jnp.dot(held[:, pl.ds(0, dim)], wide[...], preferred_element_type=f32)
    gate, upward = total[:, :part], total[:, part:]
    act = (gate / (1.0 + jnp.exp(-gate)) * upward).astype(bf16)
    shape = (EXTRA, EXTRA)
    expert = FAR * where_ref[0] + where_ref[1]
    from_share = iota(shape, 0) - CAP * EXPERTS
    hot = (from_share >= 0) & (from_share < 3 * EXPERTS) & (lax.rem(from_share + EXTRA, EXPERTS) == expert)
    share = jnp.dot(held[:, pl.ds(dim, EXTRA)], one_hot(hot), preferred_element_type=f32)[:, :1]

    @pl.loop(0, 2)
    def _(i):
        for k in range(chunks // 2):
            cols = pl.ds(pl.multiple_of((i * (chunks // 2) + k) * chunk, chunk), chunk)
            got = jnp.dot(act, deep[:, cols], preferred_element_type=f32) * share
            for g in range(groups):
                rows = got[g * SLOTS : (g + 1) * SLOTS].astype(bf16)
                early[g][:, cols] = rows[:EARLY]
                late[g][:, cols] = rows[EARLY:]


def expert_part(where, tokens, weights):
    wide, deep = weights
    dim = wide.shape[0]
    groups = len(tokens) // 2
    rows = groups * SLOTS
    return pl.pallas_call(
        functools.partial(expert_kernel, groups),
        out_shape=(jax.ShapeDtypeStruct((EARLY, dim), bf16),) * groups
        + (jax.ShapeDtypeStruct((LATE, dim), bf16),) * groups,
        in_specs=[smem()] + [vmem()] * (2 * groups + 2),
        out_specs=[vmem()] * (2 * groups),
        scratch_shapes=[pltpu.VMEM((rows, dim + EXTRA), bf16)],
        compiler_params=params(8),
        cost_estimate=cost(6 * rows * wide.size, 2 * rows * dim),
        name="expert_part",
    )(where, *tokens, held_in_vmem(wide), held_in_vmem(deep))


def collect_kernel(count, spread, *refs):
    parts, (right, left, ahead, behind) = refs[:count], refs[count:]
    size = right.shape[0]
    tiles = right.shape[1] // TILE
    for n in range(tiles):
        cols = pl.ds(n * TILE, TILE)
        rows = spread[...]
        first = n < tiles // 2
        rows = rows[: 3 * size] if first else jnp.concatenate([rows[: 2 * size], rows[3 * size :]], axis=0)
        got = jnp.dot(rows, tiles_of(parts, 0, n), preferred_element_type=f32).astype(bf16)
        right[:, cols] = got[:size]
        left[:, cols] = got[size : 2 * size]
        last, at = (ahead, n * TILE) if first else (behind, (n - tiles // 2) * TILE)
        last[:, pl.ds(at, TILE)] = got[2 * size :]


def collect(spread, parts):
    width = parts[0].shape[1] // HALVES
    count = len(parts)
    return pl.pallas_call(
        functools.partial(collect_kernel, count),
        out_shape=row_shapes(spread.shape[0] // (len(STEPS) - 1), width)[1:],
        in_specs=[vmem()] * (count + 1),
        out_specs=[vmem()] * 4,
        compiler_params=params(12),
        cost_estimate=cost(2 * spread.size * width, 4 * spread.shape[0] * width),
        name="collect",
    )(spread, *parts)


def merge_kernel(count, *refs):
    mine, (right, left, ahead, behind, first), rest = refs[:count], refs[count : count + 5], refs[count + 5 :]
    block = first.shape[0]
    tiles = first.shape[1] // TILE
    for n in range(tiles):
        cols = pl.ds(n * TILE, TILE)
        if count == 1:
            total = mine[0][:, cols]
        else:
            total = jnp.dot(mine[0][...], tiles_of(mine[1:], 0, n), preferred_element_type=f32)
        last, at = (ahead, n * TILE) if n < tiles // 2 else (behind, (n - tiles // 2) * TILE)
        total = total + right[:, cols].astype(f32) + left[:, cols].astype(f32)
        total = total + last[:, pl.ds(at, TILE)].astype(f32)
        first[:, cols] = total[:block]
        for k, out in enumerate(rest):
            out[:, cols] = total[(k + 1) * block : (k + 2) * block].astype(bf16)


def merge(mine, others):
    size, width = others[0].shape
    block = (size // FAR, width)
    return pl.pallas_call(
        functools.partial(merge_kernel, len(mine)),
        out_shape=(jax.ShapeDtypeStruct(block, f32),) + (jax.ShapeDtypeStruct(block, bf16),) * (FAR - 1),
        in_specs=[vmem()] * (len(mine) + 4),
        out_specs=[vmem()] * FAR,
        compiler_params=params(4),
        cost_estimate=cost(4 * size * width, 12 * size * width),
        name="merge",
    )(*mine, *others)


def half_swap(a):
    middle = a.shape[0] // 2
    return jnp.concatenate([a[middle:], a[:middle]], axis=0)


def route_kernel(first, one, two, three, rows, gain, router, ids, slots, hidden, payload):
    count, half = rows.shape
    total = first[...] + one[...].astype(f32) + two[...].astype(f32) + three[...].astype(f32)
    total = rows[...].astype(f32) + total
    hidden[...] = total
    square = jnp.sum(total * total, axis=1, keepdims=True)
    scale = lax.rsqrt((square + half_swap(square)) / D + norm_eps)
    normed = (total * scale * gain[...]).astype(bf16)
    payload[:, pl.ds(0, half)] = normed
    parts = [
        lax.dot_general(normed, router[:, pl.ds(c * half, half)], NT, preferred_element_type=f32)
        for c in range(HALVES)
    ]
    logits = jnp.where(iota(parts[0].shape, 0) < count // 2, parts[0], parts[1])
    logits = logits + half_swap(logits)
    logits = jnp.concatenate([logits] * (EXTRA // EXPERTS), axis=1)
    lane = iota(logits.shape, 1)
    place = jnp.zeros(logits.shape, jnp.int32)
    for k in range(TOP):
        place = jnp.where(lax.rem(lane, EXPERTS) == ids[:, k : k + 1], slots[:, k : k + 1] + 1, place)
    gates = jnp.where(place > 0, 1.0 / (1.0 + jnp.exp(-logits)), 0.0)
    share = route_scale * gates / jnp.sum(jnp.where(lane < EXPERTS, gates, 0.0), axis=1, keepdims=True)
    kind = lane // EXPERTS
    table = jnp.zeros(logits.shape, f32)
    for n in range(CAP):
        table = jnp.where((kind == n) & (place == n + 1), 1.0, table)
    rest = share
    for n in range(3):
        piece = rest.astype(bf16).astype(f32)
        table = jnp.where(kind == CAP + n, piece, table)
        rest = rest - piece
    payload[:, pl.ds(half, EXTRA)] = table.astype(bf16)


def route(added, rows, gain, router, ids, slots):
    count, half = rows.shape
    return pl.pallas_call(
        route_kernel,
        out_shape=(
            jax.ShapeDtypeStruct((count, half), f32),
            jax.ShapeDtypeStruct((count, half + EXTRA), bf16),
        ),
        in_specs=[vmem()] * 9,
        out_specs=[vmem()] * 2,
        compiler_params=params(4),
        cost_estimate=cost(4 * count * half * EXPERTS, 20 * count * half),
        name="route",
    )(*added, rows, gain, router, ids, slots)


def finish_kernel(hidden, first, one, two, three, out):
    seqs, steps, _ = out.shape
    half = hidden.shape[1]
    total = first[...] + one[...].astype(f32) + two[...].astype(f32) + three[...].astype(f32)
    total = (hidden[...] + total).astype(bf16)
    for c in range(HALVES):
        for b in range(seqs):
            at = (c * seqs + b) * steps
            out[b, :, pl.ds(c * half, half)] = total[at : at + steps]


def finish(hidden, added, shape):
    return pl.pallas_call(
        finish_kernel,
        out_shape=jax.ShapeDtypeStruct(shape, bf16),
        in_specs=[vmem()] * 5,
        out_specs=vmem(),
        compiler_params=params(4),
        cost_estimate=cost(5 * hidden.size, 14 * hidden.size),
        name="finish",
    )(hidden, *added)


def reduce_z(mine, right, left, ahead, behind):
    others = shift_z(right, 1), shift_z(left, -1), shift_z(ahead, 2), shift_z(behind, -2)
    first, *sent = merge(mine, others)
    others = [swap_far(rows, k + 1) for k, rows in enumerate(sent)]
    return first, *others


def layer(
    cache_kv,
    new_kv,
    queries,
    lengths,
    resid,
    value_up,
    out_proj,
    norm_gain,
    router,
    expert_ids,
    slots,
    w_gate,
    w_up,
    w_down,
):
    nx = lax.axis_size("x")
    seqs, steps = queries.shape[:2]
    tok = seqs * steps
    where = jnp.stack([lax.axis_index(a) for a in ("x", "zb", "j")]).astype(jnp.int32)
    where = jnp.concatenate([where, lengths.astype(jnp.int32)])

    tops, lows = pack(value_up.T, out_proj)
    top_left = swap_x(tops, 1)
    low_right = swap_x(lows, 3)
    low_left = swap_x(lows, 1)
    top_right = swap_x(tops, 3)

    outgoing = context_rows(where, nx, cache_kv, new_kv, queries)
    arrived = lax.all_to_all(
        outgoing.reshape(RING, nx * tok, LAT), ZAX, split_axis=0, concat_axis=0, tiled=True
    )
    top_far = swap_x(top_left, 3)
    low_far = swap_x(low_right, 1)
    mine = join(tops, lows)
    near = join(top_left, low_left, top_right, low_right)
    pieces = [mine, swap_core(mine)]
    pieces += [near, swap_core(near)]
    beyond = [top_far, low_far, swap_core(top_far), swap_core(low_far)]
    both = pair(w_gate, w_up)
    others = swap_core(both), swap_core(w_down)
    weights = stage((w_gate, w_up, others[0], w_down, others[1]))
    arrived = arrived.reshape(RING * nx * tok, LAT)
    most = attend_part(where, nx, arrived, pieces, (0, 0, 1, 2, 1, 2), tok, None)
    own, *rows = attend_part(where, nx, arrived, beyond, (3,) * 4, tok, most)
    added = reduce_z((own,), *rows)

    half = D // HALVES
    rows = resid.reshape(tok, HALVES, half).swapaxes(0, 1).reshape(HALVES * tok, half)
    gain = jnp.repeat(norm_gain.astype(f32).reshape(HALVES, half), tok, axis=0)
    ids, places = [
        jnp.tile(a.reshape(tok, TOP).astype(jnp.int32), (HALVES, 1)) for a in (expert_ids, slots)
    ]
    hidden, payload = route(added, rows, gain, router.T, ids, places)

    ring = lax.all_gather(payload, "zb", axis=0, tiled=True)
    middle = ring.shape[0] // 2
    above, below = shift_z(ring, -1), shift_z(ring, 1)
    beyond = shift_z(ring[:middle], -2), shift_z(ring[middle:], 2)
    near = (above, *beyond, below)
    sent = dispatch(where, nx, (ring,), tok)
    late_in = [swap_x(sent[i], COLUMNS[i]) for i in range(1, nx)]
    late_in = [sent[0], *late_in]
    sent = dispatch(where, nx, near, tok)
    early_in = [swap_x(sent[i], COLUMNS[i]) for i in range(1, nx)]
    early_in = [sent[0], *early_in]
    late = plan(where, nx, (ring,), tok, 0, 1, 0)
    early = plan(where, nx, near, tok, 1, len(STEPS) - 1, 1)
    got = [pair for pairs in zip(early_in, late_in) for pair in pairs]
    first = expert_part(where, got[2:6], weights)
    second = expert_part(where, got[:2] + got[6:], weights)
    done = [[second[2 * n], *first[2 * n : 2 * n + 2], second[2 * n + 1]] for n in range(2)]
    first = [done[0][0]] + [swap_x(done[0][i], COLUMNS[i]) for i in range(1, nx)]
    second = [done[1][0]] + [swap_x(done[1][i], COLUMNS[i]) for i in range(1, nx)]
    added = reduce_z((late, *second), *collect(early, first))
    return finish(hidden, added, resid.shape)


def solution(mesh):
    chips = mesh.shape["ep"] // (RING * CORES)
    grid = mesh.devices.reshape(mesh.shape["rep"], chips, FAR, NEAR, CORES)
    fine = Mesh(grid, ("rep", "x", "zb", "j", "c"))
    ep = ("x", "zb", "j", "c")
    both = ("rep",) + ep
    return jax.shard_map(
        layer,
        mesh=fine,
        in_specs=(
            P(both, None, None),
            P(both, None, None),
            P(both, None, None, None),
            P(both),
            P(both, None, None),
            P(None, ep),
            P(ep, None),
            P(),
            P(),
            P(both, None, None),
            P(both, None, None),
            P(None, ep),
            P(None, ep),
            P(ep, None),
        ),
        out_specs=P(both, None, None),
        check_vma=False,
    )
```

```python
import functools
import math

import jax
import jax.numpy as jnp
from jax import lax
from jax.experimental import pallas as pl
from jax.experimental.pallas import tpu as pltpu
from jax.sharding import Mesh
from jax.sharding import PartitionSpec as P


D = 7168
LAT = 512
VH = 128
EXPERTS = 16
TOP = 8
CAP = 2
QK = 192

CORES = 2
NEAR = 4
FAR = 4
RING = NEAR * FAR
SLOTS = RING * CAP
TURNS = (1, NEAR - 1, 2, 0)
PARTS = (2 * FAR * CAP, FAR * CAP, FAR * CAP)
EXTRA = 128

route_scale = 2.827
norm_eps = 1e-06


ZAX = ("zb", "j")
f32, bf16 = jnp.float32, jnp.bfloat16
NT = (((1,), (1,)), ((), ()))


def swap_x(a, bits):
    return lax.ppermute(a, "x", [(i, i ^ bits) for i in range(lax.axis_size("x"))])


def shift_z(a, step):
    return lax.ppermute(a, ZAX, [(i, (i + step) % RING) for i in range(RING)])


def swap_far(a, bits):
    return lax.ppermute(a, "zb", [(i, i ^ bits) for i in range(FAR)])


def swap_core(a):
    return lax.ppermute(a, "c", [(i, i ^ 1) for i in range(CORES)])


def iota(shape, axis):
    return lax.broadcasted_iota(jnp.int32, shape, axis)


def one_hot(mask):
    return jnp.where(mask, 1.0, 0.0).astype(bf16)


COLUMNS = (0, 1, 3, 2)


def column(index, x):
    return x ^ jnp.where(index == 2, 3, jnp.where(index == 3, 2, index))


STEPS = (0, 1, RING - 1, 2, RING - 2)


def chip_at(place, where_ref):
    group, bits = place // FAR, lax.rem(place, FAR)
    step = 0
    for i, value in enumerate(STEPS):
        step = jnp.where(group == i, value, step)
    chip = lax.rem(NEAR * where_ref[1] + where_ref[2] + step, RING)
    return NEAR * ((chip // NEAR) ^ bits) + lax.rem(chip, NEAR)


def of_tile(rows, n, tiles):
    size = rows.shape[0] // len(STEPS)
    if n < tiles // 2:
        return rows[: 4 * size]
    return jnp.concatenate([rows[: 3 * size], rows[4 * size :]], axis=0)


def smem():
    return pl.BlockSpec(memory_space=pltpu.SMEM)


def vmem():
    return pl.BlockSpec(memory_space=pltpu.VMEM)


def hbm():
    return pl.BlockSpec(memory_space=pltpu.HBM)


def held_in_hbm(a):
    return pltpu.with_memory_space_constraint(a, pltpu.HBM)


def held_in_vmem(a):
    return pltpu.with_memory_space_constraint(a, pltpu.VMEM)


def params(mib):
    return pltpu.CompilerParams(vmem_limit_bytes=mib << 20)


def cost(flops, nbytes):
    return pl.CostEstimate(flops=flops, bytes_accessed=nbytes, transcendentals=0)


def context_kernel(nx, where_ref, keys, queries, new, out, held):
    seq = pl.program_id(0)
    seqs = pl.num_programs(0)
    steps, heads = queries.shape[1], queries.shape[2]
    count = steps * heads
    scale = 1.0 / math.sqrt(QK)
    query = queries[0].reshape(count, queries.shape[3])
    score = jnp.dot(query, keys[0], preferred_element_type=f32) * scale
    score = jnp.where(iota(score.shape, 1) < where_ref[3 + seq], score, -jnp.inf)
    wide = query.astype(f32)
    step_of = iota((count, 1), 0) // heads
    latest = []
    peak = jnp.max(score, axis=1, keepdims=True)
    for t in range(steps):
        key = new[0, t : t + 1, :].astype(f32)
        got = jnp.sum(wide * key, axis=1, keepdims=True) * scale
        got = jnp.where(step_of >= t, got, -jnp.inf)
        latest.append(got)
        peak = jnp.maximum(peak, got)
    probs = jnp.exp(score - peak)
    total = jnp.sum(probs, axis=1, keepdims=True)
    latest = [jnp.exp(got - peak) for got in latest]
    for got in latest:
        total = total + got
    share = 1.0 / total
    probs = (probs * share).astype(bf16)
    context = lax.dot_general(probs, keys[0, :LAT, :], NT, preferred_element_type=f32)
    for t, got in enumerate(latest):
        part = (got * share).astype(bf16).astype(f32)
        context = context + part * new[0, t : t + 1, :LAT].astype(f32)
    held[pl.ds(pl.multiple_of(seq * count, count), count), :] = context.astype(bf16)

    @pl.when(seq == seqs - 1)
    def _():
        rows = held.shape[0]
        tok = rows // heads
        shape = (rows, rows)
        to, source = iota(shape, 0), iota(shape, 1)
        hop = lax.rem(to // tok, nx)
        head = column(hop, where_ref[0]) * RING + to // (tok * nx)
        take = (lax.rem(to, tok) == source // heads) & (head == lax.rem(source, heads))
        out[...] = jnp.dot(one_hot(take), held[...], preferred_element_type=f32).astype(bf16)


def context_rows(where, nx, cache_kv, new_kv, queries):
    seqs, length, width = cache_kv.shape
    steps, heads = queries.shape[1:3]
    rows = seqs * steps * heads
    keys = jnp.swapaxes(cache_kv, 1, 2)
    return pl.pallas_call(
        functools.partial(context_kernel, nx),
        grid=(seqs,),
        out_shape=jax.ShapeDtypeStruct((rows, LAT), bf16),
        in_specs=[
            smem(),
            pl.BlockSpec((1, width, length), lambda b: (b, 0, 0)),
            pl.BlockSpec((1, steps, heads, width), lambda b: (b, 0, 0, 0)),
            pl.BlockSpec((1, steps, width), lambda b: (b, 0, 0)),
        ],
        out_specs=pl.BlockSpec((rows, LAT), lambda b: (0, 0)),
        scratch_shapes=[pltpu.VMEM((rows, LAT), bf16)],
        compiler_params=params(24),
        cost_estimate=cost(2 * rows * length * (width + LAT), 2 * cache_kv.size),
        name="context_rows",
    )(where, held_in_hbm(keys), held_in_hbm(queries), held_in_hbm(new_kv))


def pack_kernel(up, rows, tops, lows, sem):
    half, at = tops.shape[0], up.shape[1]
    copies = []
    for i, out in enumerate((tops, lows)):
        part = pl.ds(i * half, half)
        copies.append(pltpu.make_async_copy(rows.at[part], out.at[:, pl.ds(at, rows.shape[1])], sem.at[i, 0]))
        copies.append(pltpu.make_async_copy(up.at[part], out.at[:, pl.ds(0, at)], sem.at[i, 1]))
    for copy in copies:
        copy.start()
    for copy in copies:
        copy.wait()


def pack(up, rows):
    shape = (rows.shape[0] // 2, up.shape[1] + rows.shape[1])
    return pl.pallas_call(
        pack_kernel,
        out_shape=(jax.ShapeDtypeStruct(shape, bf16),) * 2,
        in_specs=[hbm()] * 2,
        out_specs=[vmem()] * 2,
        scratch_shapes=[pltpu.SemaphoreType.DMA((2, 2))],
        compiler_params=params(12),
        cost_estimate=cost(1, 4 * rows.size),
        name="pack",
    )(held_in_hbm(up), held_in_hbm(rows))


HALVES = 2
TILE = 256


def put_rows(got, outs, n):
    own, right, left, ahead, behind = outs
    size, width = own.shape[0], ahead.shape[1]
    cols = pl.ds(n * TILE, TILE)
    own[:, cols] = got[:size]
    right[:, cols] = got[size : 2 * size].astype(bf16)
    left[:, cols] = got[2 * size : 3 * size].astype(bf16)
    last, at = (ahead, n * TILE) if n * TILE < width else (behind, n * TILE - width)
    last[:, pl.ds(at, TILE)] = got[3 * size :].astype(bf16)


def row_shapes(size, width):
    return (
        jax.ShapeDtypeStruct((size, width), f32),
        jax.ShapeDtypeStruct((size, width), bf16),
        jax.ShapeDtypeStruct((size, width), bf16),
        jax.ShapeDtypeStruct((size, width // 2), bf16),
        jax.ShapeDtypeStruct((size, width // 2), bf16),
    )


def tiles_of(parts, at, n):
    half = (parts[0].shape[1] - at) // HALVES
    got = [p[:, pl.ds(at + c * half + n * TILE, TILE)] for c in range(HALVES) for p in parts]
    return jnp.concatenate(got, axis=0)


def attend_kernel(tok, nx, count, first, last, where_ref, arrived, *refs):
    pieces, outs = refs[:count], refs[count:]
    if last:
        before, outs = outs[0], outs[1:]
    up = jnp.concatenate([piece[:, pl.ds(0, LAT)] for piece in pieces], axis=0)
    values = lax.dot_general(arrived[...], up, NT, preferred_element_type=f32)
    hop = lax.rem(iota(values.shape, 0) // tok, nx)
    values = jnp.where(hop == first + iota(values.shape, 1) // VH, values, 0.0).astype(bf16)
    shape = (len(STEPS) * FAR * HALVES * tok, arrived.shape[0])
    row, source = iota(shape, 0), iota(shape, 1)
    chip = chip_at(row // (HALVES * tok), where_ref)
    take = (source // (tok * nx) == chip) & (lax.rem(source, tok) == lax.rem(row, tok))
    half = lax.rem(row // tok, HALVES)
    taken = [
        jnp.dot(one_hot(take & (half == c)), values, preferred_element_type=f32).astype(bf16)
        for c in range(HALVES)
    ]
    values = jnp.concatenate(taken, axis=1)
    tiles = outs[0].shape[1] // TILE
    for n in range(tiles):
        got = jnp.dot(of_tile(values, n, tiles), tiles_of(pieces, LAT, n), preferred_element_type=f32)
        cols = pl.ds(n * TILE, TILE)
        if last:
            put_rows(before[:, cols] + got, outs, n)
        else:
            outs[0][:, cols] = got


def attend_part(where, nx, arrived, pieces, tok, first, before):
    depth = sum(p.shape[0] for p in pieces)
    width = (pieces[0].shape[1] - LAT) // HALVES
    count = len(pieces)
    last = before is not None
    part = jax.ShapeDtypeStruct((RING * HALVES * tok, width), f32)
    return pl.pallas_call(
        functools.partial(attend_kernel, tok, nx, count, first, last),
        out_shape=row_shapes(FAR * HALVES * tok, width) if last else part,
        in_specs=[smem(), vmem()] + [vmem()] * count + [vmem()] * last,
        out_specs=[vmem()] * 5 if last else vmem(),
        compiler_params=params(6),
        cost_estimate=cost(8 * RING * tok * depth * width * HALVES, 4 * depth * width),
        name="attend_part",
    )(where, arrived, *pieces, *([before] if last else []))


SEND_TILE = 512


def slot_rows(tok, nx, where_ref, table):
    count = table.shape[0]
    shape = (nx * CAP, EXTRA)
    row, place = iota(shape, 0), iota(shape, 1)
    expert = FAR * column(row // CAP, where_ref[0]) + where_ref[1]
    hot = one_hot(place == lax.rem(row, CAP) * EXPERTS + expert)
    got = lax.dot_general(hot, table, NT, preferred_element_type=f32)
    shape = (SLOTS, count)
    slot, token = iota(shape, 0), iota(shape, 1)
    source = slot // CAP
    turn = sum(jnp.where(source // FAR == i, value, 0) for i, value in enumerate(TURNS))
    chip = NEAR * lax.rem(source, FAR) + lax.rem(where_ref[2] + turn, NEAR)
    same = chip == token // (HALVES * tok)
    half = lax.rem(token // tok, HALVES)
    rows = []
    for r in range(nx):
        sel = jnp.where(lax.rem(slot, CAP) == 0, got[CAP * r : CAP * r + 1], got[CAP * r + 1 : CAP * r + 2])
        rows.append(jnp.where(same, sel, 0.0))
    return [[jnp.where(half == c, sel, 0.0) for sel in rows] for c in range(HALVES)]


def dispatch_kernel(tok, nx, where_ref, tokens, *outs):
    half = tokens.shape[1] - EXTRA
    table = tokens[:, pl.ds(half, EXTRA)]
    both = jnp.concatenate(sum(slot_rows(tok, nx, where_ref, table), []), axis=0).astype(bf16)
    rows = nx * SLOTS
    for n in range(half // SEND_TILE):
        got = jnp.dot(both, tokens[:, pl.ds(n * SEND_TILE, SEND_TILE)], preferred_element_type=f32).astype(bf16)
        for c in range(HALVES):
            for r in range(nx):
                at = c * rows + r * SLOTS
                outs[r][:, pl.ds(c * half + n * SEND_TILE, SEND_TILE)] = got[at : at + SLOTS]
    got = jnp.dot(both[:rows], table, preferred_element_type=f32).astype(bf16)
    for r in range(nx):
        outs[r][:, pl.ds(HALVES * half, EXTRA)] = got[r * SLOTS : (r + 1) * SLOTS]


def dispatch(where, nx, tokens, tok):
    count, width = tokens.shape
    full = HALVES * (width - EXTRA) + EXTRA
    return pl.pallas_call(
        functools.partial(dispatch_kernel, tok, nx),
        out_shape=(jax.ShapeDtypeStruct((SLOTS, full), bf16),) * nx,
        in_specs=[smem(), vmem()],
        out_specs=[vmem()] * nx,
        compiler_params=params(12),
        cost_estimate=cost(2 * nx * SLOTS * count * full, 4 * count * width),
        name="dispatch",
    )(where, tokens)


def plan_kernel(tok, nx, where_ref, tokens, *outs):
    count, width = tokens.shape
    halves = slot_rows(tok, nx, where_ref, tokens[:, pl.ds(width - EXTRA, EXTRA)])
    unit = HALVES * tok
    at = 0
    for out, group, size in zip(outs, (1, 3, 0), PARTS):
        shape = (out.shape[0], count)
        row, token = iota(shape, 0), iota(shape, 1)
        take = token // unit == chip_at(group * FAR + row // unit, where_ref)
        take = take & (lax.rem(token, unit) == lax.rem(row, unit))
        sel = jnp.concatenate([sel[at : at + size] for rows in halves for sel in rows], axis=0).astype(bf16)
        out[...] = lax.dot_general(one_hot(take), sel, NT, preferred_element_type=f32).astype(bf16)
        at += size


def plan(where, nx, tokens, tok):
    count, _ = tokens.shape
    near = count // NEAR
    shapes = [(rows * near, HALVES * nx * size) for rows, size in zip((2, 2, 1), PARTS)]
    return pl.pallas_call(
        functools.partial(plan_kernel, tok, nx),
        out_shape=[jax.ShapeDtypeStruct(shape, bf16) for shape in shapes],
        in_specs=[smem(), vmem()],
        out_specs=[vmem()] * len(PARTS),
        compiler_params=params(6),
        cost_estimate=cost(2 * count * SLOTS * count, 4 * count * SLOTS),
        name="plan",
    )(where, tokens)


CHUNKS = 7


def stage_kernel(gate_a, gate_b, up_a, up_b, down_a, down_b, wide, deep, sem):
    part = gate_a.shape[1]
    copies = [
        pltpu.make_async_copy(ref, wide.at[:, pl.ds(i * part, part)], sem.at[i])
        for i, ref in enumerate((gate_a, gate_b, up_a, up_b))
    ]
    copies += [
        pltpu.make_async_copy(ref, deep.at[pl.ds(i * part, part)], sem.at[4 + i])
        for i, ref in enumerate((down_a, down_b))
    ]
    for copy in copies:
        copy.start()
    for copy in copies:
        copy.wait()


def stage(weights):
    dim, part = weights[0].shape
    return pl.pallas_call(
        stage_kernel,
        out_shape=(
            jax.ShapeDtypeStruct((dim, 4 * part), bf16),
            jax.ShapeDtypeStruct((2 * part, dim), bf16),
        ),
        in_specs=[hbm()] * 6,
        out_specs=[vmem()] * 2,
        scratch_shapes=[pltpu.SemaphoreType.DMA((6,))],
        compiler_params=params(4),
        cost_estimate=cost(4 * 1000 * dim * part, 12 * dim * part),
        name="stage",
    )(*[held_in_hbm(w) for w in weights])


def expert_kernel(groups, where_ref, *refs):
    tokens = refs[:groups]
    wide, deep = refs[groups : groups + 2]
    outs = refs[groups + 2 : groups + 2 + len(PARTS) * groups]
    held = refs[-1] if groups > 1 else tokens[0]
    dim = wide.shape[0]
    part = wide.shape[1] // 2
    chunk = dim // CHUNKS
    if groups > 1:
        for g, ref in enumerate(tokens):
            held[pl.ds(g * SLOTS, SLOTS)] = ref[...]
    total = jnp.dot(held[:, pl.ds(0, dim)], wide[...], preferred_element_type=f32)
    gate, upward = total[:, :part], total[:, part:]
    act = (gate / (1.0 + jnp.exp(-gate)) * upward).astype(bf16)
    shape = (EXTRA, EXTRA)
    expert = FAR * where_ref[0] + where_ref[1]
    from_share = iota(shape, 0) - CAP * EXPERTS
    hot = (from_share >= 0) & (from_share < 3 * EXPERTS) & (lax.rem(from_share + EXTRA, EXPERTS) == expert)
    share = jnp.dot(held[:, pl.ds(dim, EXTRA)], one_hot(hot), preferred_element_type=f32)[:, :1]
    for k in range(CHUNKS):
        cols = pl.ds(k * chunk, chunk)
        got = jnp.dot(act, deep[:, cols], preferred_element_type=f32) * share
        for g in range(groups):
            at = g * SLOTS
            for n, size in enumerate(PARTS):
                outs[n * groups + g][:, cols] = got[at : at + size].astype(bf16)
                at += size


def expert_part(where, tokens, weights):
    wide, deep = weights
    dim = wide.shape[0]
    groups = len(tokens)
    rows = groups * SLOTS
    held = [pltpu.VMEM((rows, dim + EXTRA), bf16)] if groups > 1 else []
    return pl.pallas_call(
        functools.partial(expert_kernel, groups),
        out_shape=[jax.ShapeDtypeStruct((size, dim), bf16) for size in PARTS for _ in range(groups)],
        in_specs=[smem()] + [vmem()] * (groups + 2),
        out_specs=[vmem()] * (len(PARTS) * groups),
        scratch_shapes=held,
        compiler_params=params(8),
        cost_estimate=cost(6 * rows * wide.size, 2 * rows * dim),
        name="expert_part",
    )(where, *tokens, held_in_vmem(wide), held_in_vmem(deep))


def collect_kernel(count, spread, *refs):
    parts, outs = refs[:count], refs[count:]
    half = spread.shape[0] // len(outs)
    width = outs[0].shape[1]
    whole = parts[0].shape[1] // HALVES == width
    for n in range(parts[0].shape[1] // HALVES // TILE):
        place, at = n * TILE // width, n * TILE % width
        rows = spread[...] if whole else spread[pl.ds(place * half, half), :]
        got = jnp.dot(rows, tiles_of(parts, 0, n), preferred_element_type=f32).astype(bf16)
        for i, out in enumerate(outs if whole else (outs[place],)):
            out[:, pl.ds(at, TILE)] = got[i * half : (i + 1) * half]


def collect(spread, parts, width):
    rows, count = spread.shape[0] // 2, len(parts)
    return pl.pallas_call(
        functools.partial(collect_kernel, count),
        out_shape=(jax.ShapeDtypeStruct((rows, width), bf16),) * 2,
        in_specs=[vmem()] * (count + 1),
        out_specs=[vmem()] * 2,
        compiler_params=params(12),
        cost_estimate=cost(2 * spread.size * width, 4 * spread.shape[0] * width),
        name="collect",
    )(spread, *parts)


def merge_kernel(count, *refs):
    mine, (right, left, ahead, behind, first), rest = refs[:count], refs[count : count + 5], refs[count + 5 :]
    block = first.shape[0]
    tiles = first.shape[1] // TILE
    for n in range(tiles):
        cols = pl.ds(n * TILE, TILE)
        if count == 1:
            total = mine[0][:, cols]
        else:
            total = jnp.dot(mine[0][...], tiles_of(mine[1:], 0, n), preferred_element_type=f32)
        last, at = (ahead, n * TILE) if n < tiles // 2 else (behind, (n - tiles // 2) * TILE)
        total = total + right[:, cols].astype(f32) + left[:, cols].astype(f32)
        total = total + last[:, pl.ds(at, TILE)].astype(f32)
        first[:, cols] = total[:block]
        for k, out in enumerate(rest):
            out[:, cols] = total[(k + 1) * block : (k + 2) * block].astype(bf16)


def merge(mine, others):
    size, width = others[0].shape
    block = (size // FAR, width)
    return pl.pallas_call(
        functools.partial(merge_kernel, len(mine)),
        out_shape=(jax.ShapeDtypeStruct(block, f32),) + (jax.ShapeDtypeStruct(block, bf16),) * (FAR - 1),
        in_specs=[vmem()] * (len(mine) + 4),
        out_specs=[vmem()] * FAR,
        compiler_params=params(4),
        cost_estimate=cost(4 * size * width, 12 * size * width),
        name="merge",
    )(*mine, *others)


def half_swap(a):
    middle = a.shape[0] // 2
    return jnp.concatenate([a[middle:], a[:middle]], axis=0)


def route_kernel(first, one, two, three, rows, gain, router, ids, slots, hidden, payload):
    count, half = rows.shape
    total = first[...] + one[...].astype(f32) + two[...].astype(f32) + three[...].astype(f32)
    total = rows[...].astype(f32) + total
    hidden[...] = total
    square = jnp.sum(total * total, axis=1, keepdims=True)
    scale = lax.rsqrt((square + half_swap(square)) / D + norm_eps)
    normed = (total * scale * gain[...]).astype(bf16)
    payload[:, pl.ds(0, half)] = normed
    parts = [
        lax.dot_general(normed, router[:, pl.ds(c * half, half)], NT, preferred_element_type=f32)
        for c in range(HALVES)
    ]
    logits = jnp.where(iota(parts[0].shape, 0) < count // 2, parts[0], parts[1])
    logits = logits + half_swap(logits)
    logits = jnp.concatenate([logits] * (EXTRA // EXPERTS), axis=1)
    lane = iota(logits.shape, 1)
    place = jnp.zeros(logits.shape, jnp.int32)
    for k in range(TOP):
        place = jnp.where(lax.rem(lane, EXPERTS) == ids[:, k : k + 1], slots[:, k : k + 1] + 1, place)
    gates = jnp.where(place > 0, 1.0 / (1.0 + jnp.exp(-logits)), 0.0)
    share = route_scale * gates / jnp.sum(jnp.where(lane < EXPERTS, gates, 0.0), axis=1, keepdims=True)
    kind = lane // EXPERTS
    table = jnp.zeros(logits.shape, f32)
    for n in range(CAP):
        table = jnp.where((kind == n) & (place == n + 1), 1.0, table)
    rest = share
    for n in range(3):
        piece = rest.astype(bf16).astype(f32)
        table = jnp.where(kind == CAP + n, piece, table)
        rest = rest - piece
    payload[:, pl.ds(half, EXTRA)] = table.astype(bf16)


def route(added, rows, gain, router, ids, slots):
    count, half = rows.shape
    return pl.pallas_call(
        route_kernel,
        out_shape=(
            jax.ShapeDtypeStruct((count, half), f32),
            jax.ShapeDtypeStruct((count, half + EXTRA), bf16),
        ),
        in_specs=[vmem()] * 9,
        out_specs=[vmem()] * 2,
        compiler_params=params(4),
        cost_estimate=cost(4 * count * half * EXPERTS, 20 * count * half),
        name="route",
    )(*added, rows, gain, router, ids, slots)


def finish_kernel(hidden, first, one, two, three, out):
    seqs, steps, _ = out.shape
    half = hidden.shape[1]
    total = first[...] + one[...].astype(f32) + two[...].astype(f32) + three[...].astype(f32)
    total = (hidden[...] + total).astype(bf16)
    for c in range(HALVES):
        for b in range(seqs):
            at = (c * seqs + b) * steps
            out[b, :, pl.ds(c * half, half)] = total[at : at + steps]


def finish(hidden, added, shape):
    return pl.pallas_call(
        finish_kernel,
        out_shape=jax.ShapeDtypeStruct(shape, bf16),
        in_specs=[vmem()] * 5,
        out_specs=vmem(),
        compiler_params=params(4),
        cost_estimate=cost(5 * hidden.size, 14 * hidden.size),
        name="finish",
    )(hidden, *added)


def one_on(right, left):
    return shift_z(right, 1), shift_z(left, -1)


def two_on(ahead, behind):
    return shift_z(ahead, 2), shift_z(behind, -2)


def far_on(mine, others):
    first, *sent = merge(mine, others)
    others = [swap_far(rows, k + 1) for k, rows in enumerate(sent)]
    return first, *others


def layer(
    cache_kv,
    new_kv,
    queries,
    lengths,
    resid,
    value_up,
    out_proj,
    norm_gain,
    router,
    expert_ids,
    slots,
    w_gate,
    w_up,
    w_down,
):
    nx = lax.axis_size("x")
    seqs, steps = queries.shape[:2]
    tok = seqs * steps
    where = jnp.stack([lax.axis_index(a) for a in ("x", "zb", "j")]).astype(jnp.int32)
    where = jnp.concatenate([where, lengths.astype(jnp.int32)])

    tops, lows = pack(value_up.T, out_proj)
    top_left = swap_x(tops, 1)
    low_right = swap_x(lows, 3)
    low_left = swap_x(lows, 1)
    top_right = swap_x(tops, 3)

    outgoing = context_rows(where, nx, cache_kv, new_kv, queries)
    arrived = lax.all_to_all(
        outgoing.reshape(RING, nx * tok, LAT), ZAX, split_axis=0, concat_axis=0, tiled=True
    )
    top_far = swap_x(top_left, 3)
    low_far = swap_x(low_right, 1)
    near = [tops, lows, swap_core(tops), swap_core(lows)]
    for pair in ((top_left, low_left), (top_right, low_right)):
        near += [*pair, *map(swap_core, pair)]
    beyond = [top_far, low_far, swap_core(top_far), swap_core(low_far)]
    others = [swap_core(w) for w in (w_gate, w_up, w_down)]
    weights = stage((w_gate, others[0], w_up, others[1], w_down, others[2]))
    arrived = arrived.reshape(RING * nx * tok, LAT)
    most = attend_part(where, nx, arrived, near, tok, 0, None)
    own, *rows = attend_part(where, nx, arrived, beyond, tok, nx - 1, most)
    added = far_on((own,), one_on(*rows[:2]) + two_on(*rows[2:]))

    half = D // HALVES
    rows = resid.reshape(tok, HALVES, half).swapaxes(0, 1).reshape(HALVES * tok, half)
    gain = jnp.repeat(norm_gain.astype(f32).reshape(HALVES, half), tok, axis=0)
    ids, places = [
        jnp.tile(a.reshape(tok, TOP).astype(jnp.int32), (HALVES, 1)) for a in (expert_ids, slots)
    ]
    hidden, payload = route(added, rows, gain, router.T, ids, places)

    ring = lax.all_gather(payload, ZAX, axis=0, tiled=True)
    sent = dispatch(where, nx, ring, tok)
    got = [swap_x(sent[i], COLUMNS[i]) for i in range(1, nx)]
    spreads = plan(where, nx, ring, tok)
    done = expert_part(where, (sent[0], *got[: nx - 2]), weights)
    last = expert_part(where, got[nx - 2 :], weights)
    backs = []
    for n in range(len(PARTS)):
        rows = [*done[n * (nx - 1) : (n + 1) * (nx - 1)], last[n]]
        backs.append(rows[:1] + [swap_x(rows[i], COLUMNS[i]) for i in range(1, nx)])
    near = one_on(*collect(spreads[0], backs[0], half))
    two = collect(spreads[1], backs[1], half // 2)
    near += two_on(*two)
    added = far_on((spreads[2], *backs[2]), near)
    return finish(hidden, added, resid.shape)


def solution(mesh):
    chips = mesh.shape["ep"] // (RING * CORES)
    grid = mesh.devices.reshape(mesh.shape["rep"], chips, FAR, NEAR, CORES)
    fine = Mesh(grid, ("rep", "x", "zb", "j", "c"))
    ep = ("x", "zb", "j", "c")
    both = ("rep",) + ep
    return jax.shard_map(
        layer,
        mesh=fine,
        in_specs=(
            P(both, None, None),
            P(both, None, None),
            P(both, None, None, None),
            P(both),
            P(both, None, None),
            P(None, ep),
            P(ep, None),
            P(),
            P(),
            P(both, None, None),
            P(both, None, None),
            P(None, ep),
            P(None, ep),
            P(ep, None),
        ),
        out_specs=P(both, None, None),
        check_vma=False,
    )
```

```python
import functools
import math

import jax
import jax.numpy as jnp
from jax import lax
from jax.experimental import pallas as pl
from jax.experimental.pallas import tpu as pltpu
from jax.sharding import Mesh
from jax.sharding import PartitionSpec as P


D = 7168
LAT = 512
EXPERTS = 16
TOP = 8
CAP = 2
QK = 192

CORES = 2
NEAR = 4
FAR = 4
RING = NEAR * FAR
SLOTS = RING * CAP
LATE = FAR * CAP
EARLY = SLOTS - LATE
EXTRA = 128

route_scale = 2.827
norm_eps = 1e-06


ZAX = ("zb", "j")
f32, bf16 = jnp.float32, jnp.bfloat16
NT = (((1,), (1,)), ((), ()))


def swap_x(a, bits):
    return lax.ppermute(a, "x", [(i, i ^ bits) for i in range(lax.axis_size("x"))])


def shift_z(a, step):
    return lax.ppermute(a, ZAX, [(i, (i + step) % RING) for i in range(RING)])


def swap_far(a, bits):
    return lax.ppermute(a, "zb", [(i, i ^ bits) for i in range(FAR)])


def swap_core(a):
    return lax.ppermute(a, "c", [(i, i ^ 1) for i in range(CORES)])


def iota(shape, axis):
    return lax.broadcasted_iota(jnp.int32, shape, axis)


def one_hot(mask):
    return jnp.where(mask, 1.0, 0.0).astype(bf16)


COLUMNS = (0, 1, 3, 2)


def column(index, x):
    return x ^ jnp.where(index == 2, 3, jnp.where(index == 3, 2, index))


STEPS = (0, 1, RING - 1, 2, RING - 2)


def chip_at(place, where_ref):
    group, bits = place // FAR, lax.rem(place, FAR)
    step = 0
    for i, value in enumerate(STEPS):
        step = jnp.where(group == i, value, step)
    chip = lax.rem(NEAR * where_ref[1] + where_ref[2] + step, RING)
    return NEAR * ((chip // NEAR) ^ bits) + lax.rem(chip, NEAR)


def of_tile(rows, n, tiles):
    size = rows.shape[0] // len(STEPS)
    if n < tiles // 2:
        return rows[: 4 * size]
    return jnp.concatenate([rows[: 3 * size], rows[4 * size :]], axis=0)


def smem():
    return pl.BlockSpec(memory_space=pltpu.SMEM)


def vmem():
    return pl.BlockSpec(memory_space=pltpu.VMEM)


def hbm():
    return pl.BlockSpec(memory_space=pltpu.HBM)


def held_in_hbm(a):
    return pltpu.with_memory_space_constraint(a, pltpu.HBM)


def held_in_vmem(a):
    return pltpu.with_memory_space_constraint(a, pltpu.VMEM)


def params(mib):
    return pltpu.CompilerParams(vmem_limit_bytes=mib << 20)


def cost(flops, nbytes):
    return pl.CostEstimate(flops=flops, bytes_accessed=nbytes, transcendentals=0)


def context_kernel(nx, where_ref, keys, queries, new, out, held):
    seq = pl.program_id(0)
    seqs = pl.num_programs(0)
    steps, heads = queries.shape[1], queries.shape[2]
    count = steps * heads
    scale = 1.0 / math.sqrt(QK)
    query = queries[0].reshape(count, queries.shape[3])
    score = jnp.dot(query, keys[0], preferred_element_type=f32) * scale
    score = jnp.where(iota(score.shape, 1) < where_ref[3 + seq], score, -jnp.inf)
    wide = query.astype(f32)
    step_of = iota((count, 1), 0) // heads
    latest = []
    peak = jnp.max(score, axis=1, keepdims=True)
    for t in range(steps):
        key = new[0, t : t + 1, :].astype(f32)
        got = jnp.sum(wide * key, axis=1, keepdims=True) * scale
        got = jnp.where(step_of >= t, got, -jnp.inf)
        latest.append(got)
        peak = jnp.maximum(peak, got)
    probs = jnp.exp(score - peak)
    total = jnp.sum(probs, axis=1, keepdims=True)
    latest = [jnp.exp(got - peak) for got in latest]
    for got in latest:
        total = total + got
    share = 1.0 / total
    probs = (probs * share).astype(bf16)
    context = lax.dot_general(probs, keys[0, :LAT, :], NT, preferred_element_type=f32)
    for t, got in enumerate(latest):
        part = (got * share).astype(bf16).astype(f32)
        context = context + part * new[0, t : t + 1, :LAT].astype(f32)
    held[pl.ds(pl.multiple_of(seq * count, count), count), :] = context.astype(bf16)

    @pl.when(seq == seqs - 1)
    def _():
        rows = held.shape[0]
        tok = rows // heads
        shape = (rows, rows)
        to, source = iota(shape, 0), iota(shape, 1)
        hop = lax.rem(to // tok, nx)
        head = column(hop, where_ref[0]) * RING + to // (tok * nx)
        take = (lax.rem(to, tok) == source // heads) & (head == lax.rem(source, heads))
        out[...] = jnp.dot(one_hot(take), held[...], preferred_element_type=f32).astype(bf16)


def context_rows(where, nx, cache_kv, new_kv, queries):
    seqs, length, width = cache_kv.shape
    steps, heads = queries.shape[1:3]
    rows = seqs * steps * heads
    keys = jnp.swapaxes(cache_kv, 1, 2)
    return pl.pallas_call(
        functools.partial(context_kernel, nx),
        grid=(seqs,),
        out_shape=jax.ShapeDtypeStruct((rows, LAT), bf16),
        in_specs=[
            smem(),
            pl.BlockSpec((1, width, length), lambda b: (b, 0, 0)),
            pl.BlockSpec((1, steps, heads, width), lambda b: (b, 0, 0, 0)),
            pl.BlockSpec((1, steps, width), lambda b: (b, 0, 0)),
        ],
        out_specs=pl.BlockSpec((rows, LAT), lambda b: (0, 0)),
        scratch_shapes=[pltpu.VMEM((rows, LAT), bf16)],
        compiler_params=params(24),
        cost_estimate=cost(2 * rows * length * (width + LAT), 2 * cache_kv.size),
        name="context_rows",
    )(where, held_in_hbm(keys), held_in_hbm(queries), held_in_hbm(new_kv))


def pack_kernel(up, rows, tops, lows, sem):
    half, at = tops.shape[0], up.shape[1]
    copies = []
    for i, out in enumerate((tops, lows)):
        part = pl.ds(i * half, half)
        copies.append(pltpu.make_async_copy(rows.at[part], out.at[:, pl.ds(at, rows.shape[1])], sem.at[i, 0]))
        copies.append(pltpu.make_async_copy(up.at[part], out.at[:, pl.ds(0, at)], sem.at[i, 1]))
    for copy in copies:
        copy.start()
    for copy in copies:
        copy.wait()


def pack(up, rows):
    shape = (rows.shape[0] // 2, up.shape[1] + rows.shape[1])
    return pl.pallas_call(
        pack_kernel,
        out_shape=(jax.ShapeDtypeStruct(shape, bf16),) * 2,
        in_specs=[hbm()] * 2,
        out_specs=[vmem()] * 2,
        scratch_shapes=[pltpu.SemaphoreType.DMA((2, 2))],
        compiler_params=params(12),
        cost_estimate=cost(1, 4 * rows.size),
        name="pack",
    )(held_in_hbm(up), held_in_hbm(rows))


def join_kernel(count, *refs):
    at = 0
    for ref in refs[:count]:
        refs[count][pl.ds(at, ref.shape[0])] = ref[...]
        at += ref.shape[0]


def join(*arrays):
    rows, width = sum(a.shape[0] for a in arrays), arrays[0].shape[1]
    return pl.pallas_call(
        functools.partial(join_kernel, len(arrays)),
        out_shape=jax.ShapeDtypeStruct((rows, width), bf16),
        in_specs=[vmem()] * len(arrays),
        out_specs=vmem(),
        compiler_params=params(4),
        cost_estimate=cost(rows * width, 4 * rows * width),
        name="join",
    )(*arrays)


HALVES = 2
TILE = 256


def put_rows(got, outs, n):
    own, right, left, ahead, behind = outs
    size, width = own.shape[0], ahead.shape[1]
    cols = pl.ds(n * TILE, TILE)
    own[:, cols] = got[:size]
    right[:, cols] = got[size : 2 * size].astype(bf16)
    left[:, cols] = got[2 * size : 3 * size].astype(bf16)
    last, at = (ahead, n * TILE) if n * TILE < width else (behind, n * TILE - width)
    last[:, pl.ds(at, TILE)] = got[3 * size :].astype(bf16)


def row_shapes(size, width):
    return (
        jax.ShapeDtypeStruct((size, width), f32),
        jax.ShapeDtypeStruct((size, width), bf16),
        jax.ShapeDtypeStruct((size, width), bf16),
        jax.ShapeDtypeStruct((size, width // 2), bf16),
        jax.ShapeDtypeStruct((size, width // 2), bf16),
    )


def tiles_of(parts, at, n):
    half = (parts[0].shape[1] - at) // HALVES
    got = [p[:, pl.ds(at + c * half + n * TILE, TILE)] for c in range(HALVES) for p in parts]
    return jnp.concatenate(got, axis=0)


def attend_kernel(tok, nx, count, hops, last, where_ref, arrived, *refs):
    pieces, outs = refs[:count], refs[count:]
    if last:
        before, outs = outs[0], outs[1:]
    up = jnp.concatenate([piece[:, pl.ds(0, LAT)] for piece in pieces], axis=0)
    values = lax.dot_general(arrived[...], up, NT, preferred_element_type=f32)
    hop = lax.rem(iota(values.shape, 0) // tok, nx)
    part = iota(values.shape, 1) // (values.shape[1] // len(hops))
    wanted = sum(jnp.where(part == i, value, 0) for i, value in enumerate(hops))
    values = jnp.where(hop == wanted, values, 0.0).astype(bf16)
    shape = (len(STEPS) * FAR * HALVES * tok, arrived.shape[0])
    row, source = iota(shape, 0), iota(shape, 1)
    chip = chip_at(row // (HALVES * tok), where_ref)
    take = (source // (tok * nx) == chip) & (lax.rem(source, tok) == lax.rem(row, tok))
    half = lax.rem(row // tok, HALVES)
    taken = [
        jnp.dot(one_hot(take & (half == c)), values, preferred_element_type=f32).astype(bf16)
        for c in range(HALVES)
    ]
    values = jnp.concatenate(taken, axis=1)
    tiles = outs[0].shape[1] // TILE
    for n in range(tiles):
        got = jnp.dot(of_tile(values, n, tiles), tiles_of(pieces, LAT, n), preferred_element_type=f32)
        cols = pl.ds(n * TILE, TILE)
        if last:
            put_rows(before[:, cols] + got, outs, n)
        else:
            outs[0][:, cols] = got


def attend_part(where, nx, arrived, pieces, hops, tok, before):
    depth = sum(p.shape[0] for p in pieces)
    width = (pieces[0].shape[1] - LAT) // HALVES
    count = len(pieces)
    last = before is not None
    part = jax.ShapeDtypeStruct((RING * HALVES * tok, width), f32)
    return pl.pallas_call(
        functools.partial(attend_kernel, tok, nx, count, hops, last),
        out_shape=row_shapes(FAR * HALVES * tok, width) if last else part,
        in_specs=[smem(), vmem()] + [vmem()] * count + [vmem()] * last,
        out_specs=[vmem()] * 5 if last else vmem(),
        compiler_params=params(6),
        cost_estimate=cost(8 * RING * tok * depth * width * HALVES, 4 * depth * width),
        name="attend_part",
    )(where, arrived, *pieces, *([before] if last else []))


def ring_kernel(where_ref, *refs):
    parts, (whole, lower, upper) = refs[:FAR], refs[FAR:]
    rows, middle = parts[0].shape[0], lower.shape[0]
    for bits, part in enumerate(parts):
        whole[pl.ds(pl.multiple_of((where_ref[1] ^ bits) * rows, rows), rows)] = part[...]
    lower[...] = whole[pl.ds(0, middle)]
    upper[...] = whole[pl.ds(middle, middle)]


def ring_of(where, parts):
    rows, width = parts[0].shape
    shapes = [(FAR * rows, width), (FAR * rows // 2, width), (FAR * rows // 2, width)]
    return pl.pallas_call(
        ring_kernel,
        out_shape=[jax.ShapeDtypeStruct(shape, bf16) for shape in shapes],
        in_specs=[smem()] + [vmem()] * FAR,
        out_specs=[vmem()] * 3,
        compiler_params=params(4),
        cost_estimate=cost(rows * width, 12 * rows * width),
        name="ring",
    )(where, *parts)


SEND_TILE = 512


def slot_rows(tok, nx, where_ref, table):
    count = table.shape[0]
    shape = (nx * CAP, EXTRA)
    row, place = iota(shape, 0), iota(shape, 1)
    expert = FAR * column(row // CAP, where_ref[0]) + where_ref[1]
    hot = one_hot(place == lax.rem(row, CAP) * EXPERTS + expert)
    got = lax.dot_general(hot, table, NT, preferred_element_type=f32)
    shape = (count // (HALVES * tok) * CAP, count)
    slot, token = iota(shape, 0), iota(shape, 1)
    same = slot // CAP == token // (HALVES * tok)
    half = lax.rem(token // tok, HALVES)
    parts = []
    for c in range(HALVES):
        for r in range(nx):
            sel = jnp.where(lax.rem(slot, CAP) == 0, got[CAP * r : CAP * r + 1], got[CAP * r + 1 : CAP * r + 2])
            parts.append(jnp.where(same & (half == c), sel, 0.0))
    return jnp.concatenate(parts, axis=0).astype(bf16)


def dispatch_kernel(tok, nx, inputs, where_ref, *refs):
    tokens, outs = refs[:inputs], refs[inputs:]
    width = tokens[0].shape[1]
    half = width - EXTRA

    def columns(at, size):
        return jnp.concatenate([ref[:, pl.ds(at, size)] for ref in tokens], axis=0)

    table = columns(half, EXTRA)
    both = slot_rows(tok, nx, where_ref, table)
    rows = both.shape[0] // HALVES
    slots = rows // nx
    for n in range(half // SEND_TILE):
        got = jnp.dot(both, columns(n * SEND_TILE, SEND_TILE), preferred_element_type=f32).astype(bf16)
        for c in range(HALVES):
            for r in range(nx):
                at = c * rows + r * slots
                outs[r][:, pl.ds(c * half + n * SEND_TILE, SEND_TILE)] = got[at : at + slots]
    got = jnp.dot(both[:rows], table, preferred_element_type=f32).astype(bf16)
    for r in range(nx):
        outs[r][:, pl.ds(HALVES * half, EXTRA)] = got[r * slots : (r + 1) * slots]


def dispatch(where, nx, tokens, tok):
    count, width = sum(a.shape[0] for a in tokens), tokens[0].shape[1]
    full = HALVES * (width - EXTRA) + EXTRA
    slots = count // (HALVES * tok) * CAP
    return pl.pallas_call(
        functools.partial(dispatch_kernel, tok, nx, len(tokens)),
        out_shape=(jax.ShapeDtypeStruct((slots, full), bf16),) * nx,
        in_specs=[smem()] + [vmem()] * len(tokens),
        out_specs=[vmem()] * nx,
        compiler_params=params(12),
        cost_estimate=cost(2 * nx * slots * count * full, 4 * count * width),
        name="dispatch",
    )(where, *tokens)


def plan_kernel(tok, nx, inputs, group, turn, where_ref, *refs):
    tokens, out = refs[:inputs], refs[inputs]
    width = tokens[0].shape[1]
    table = jnp.concatenate([ref[:, pl.ds(width - EXTRA, EXTRA)] for ref in tokens], axis=0)
    both = slot_rows(tok, nx, where_ref, table)
    shape = (out.shape[0], table.shape[0])
    row, token = iota(shape, 0), iota(shape, 1)
    unit = HALVES * tok
    wanted = chip_at(group * FAR + row // unit, where_ref)
    source = token // unit
    chip = NEAR * lax.rem(source, FAR) + lax.rem(where_ref[2] + turn + source // FAR, NEAR)
    take = (chip == wanted) & (lax.rem(token, unit) == lax.rem(row, unit))
    out[...] = lax.dot_general(one_hot(take), both, NT, preferred_element_type=f32).astype(bf16)


def plan(where, nx, tokens, tok, group, groups, turn):
    count = sum(a.shape[0] for a in tokens)
    unit = HALVES * tok
    shape = (groups * FAR * unit, HALVES * nx * (count // unit * CAP))
    return pl.pallas_call(
        functools.partial(plan_kernel, tok, nx, len(tokens), group, turn),
        out_shape=jax.ShapeDtypeStruct(shape, bf16),
        in_specs=[smem()] + [vmem()] * len(tokens),
        out_specs=vmem(),
        compiler_params=params(4),
        cost_estimate=cost(2 * shape[0] * shape[1] * count, 2 * shape[0] * shape[1]),
        name="plan",
    )(where, *tokens)


CHUNKS = 7


def pair_kernel(first, second, out, sem):
    rows = first.shape[0]
    copies = [
        pltpu.make_async_copy(ref, out.at[pl.ds(i * rows, rows)], sem.at[i])
        for i, ref in enumerate((first, second))
    ]
    for copy in copies:
        copy.start()
    for copy in copies:
        copy.wait()


def pair(first, second):
    rows, width = first.shape
    return pl.pallas_call(
        pair_kernel,
        out_shape=jax.ShapeDtypeStruct((2 * rows, width), bf16),
        in_specs=[hbm()] * 2,
        out_specs=vmem(),
        scratch_shapes=[pltpu.SemaphoreType.DMA((2,))],
        compiler_params=params(4),
        cost_estimate=cost(1, 8 * rows * width),
        name="pair",
    )(held_in_hbm(first), held_in_hbm(second))


def stage_kernel(gate, up, others, down_a, down_b, wide, deep, sem):
    rows, part = gate.shape
    parts = gate, others.at[pl.ds(0, rows)], up, others.at[pl.ds(rows, rows)]
    copies = [
        pltpu.make_async_copy(ref, wide.at[:, pl.ds(i * part, part)], sem.at[i])
        for i, ref in enumerate(parts)
    ]
    copies += [
        pltpu.make_async_copy(ref, deep.at[pl.ds(i * part, part)], sem.at[4 + i])
        for i, ref in enumerate((down_a, down_b))
    ]
    for copy in copies:
        copy.start()
    for copy in copies:
        copy.wait()


def stage(weights):
    dim, part = weights[0].shape
    return pl.pallas_call(
        stage_kernel,
        out_shape=(
            jax.ShapeDtypeStruct((dim, 4 * part), bf16),
            jax.ShapeDtypeStruct((2 * part, dim), bf16),
        ),
        in_specs=[hbm()] * 5,
        out_specs=[vmem()] * 2,
        scratch_shapes=[pltpu.SemaphoreType.DMA((6,))],
        compiler_params=params(4),
        cost_estimate=cost(4 * 1000 * dim * part, 12 * dim * part),
        name="stage",
    )(*[held_in_hbm(w) for w in weights])


def expert_kernel(groups, where_ref, *refs):
    tokens = refs[:groups]
    wide, deep = refs[groups : groups + 2]
    early, late = refs[groups + 2 : 2 * groups + 2], refs[2 * groups + 2 : 3 * groups + 2]
    held = refs[3 * groups + 2] if groups > 1 else tokens[0]
    dim = wide.shape[0]
    part = wide.shape[1] // 2
    chunk = dim // CHUNKS
    if groups > 1:
        for g, ref in enumerate(tokens):
            held[pl.ds(g * SLOTS, SLOTS)] = ref[...]
    total = jnp.dot(held[:, pl.ds(0, dim)], wide[...], preferred_element_type=f32)
    gate, upward = total[:, :part], total[:, part:]
    act = (gate / (1.0 + jnp.exp(-gate)) * upward).astype(bf16)
    shape = (EXTRA, EXTRA)
    expert = FAR * where_ref[0] + where_ref[1]
    from_share = iota(shape, 0) - CAP * EXPERTS
    hot = (from_share >= 0) & (from_share < 3 * EXPERTS) & (lax.rem(from_share + EXTRA, EXPERTS) == expert)
    share = jnp.dot(held[:, pl.ds(dim, EXTRA)], one_hot(hot), preferred_element_type=f32)[:, :1]
    for k in range(CHUNKS):
        cols = pl.ds(k * chunk, chunk)
        got = jnp.dot(act, deep[:, cols], preferred_element_type=f32) * share
        for g in range(groups):
            rows = got[g * SLOTS : (g + 1) * SLOTS].astype(bf16)
            early[g][:, cols] = rows[:EARLY]
            late[g][:, cols] = rows[EARLY:]


def expert_part(where, tokens, weights):
    wide, deep = weights
    dim = wide.shape[0]
    groups = len(tokens)
    rows = groups * SLOTS
    held = [pltpu.VMEM((rows, dim + EXTRA), bf16)] if groups > 1 else []
    return pl.pallas_call(
        functools.partial(expert_kernel, groups),
        out_shape=(jax.ShapeDtypeStruct((EARLY, dim), bf16),) * groups
        + (jax.ShapeDtypeStruct((LATE, dim), bf16),) * groups,
        in_specs=[smem()] + [vmem()] * (groups + 2),
        out_specs=[vmem()] * (2 * groups),
        scratch_shapes=held,
        compiler_params=params(8),
        cost_estimate=cost(6 * rows * wide.size, 2 * rows * dim),
        name="expert_part",
    )(where, *tokens, held_in_vmem(wide), held_in_vmem(deep))


def collect_kernel(count, spread, *refs):
    parts, (right, left, ahead, behind) = refs[:count], refs[count:]
    size = right.shape[0]
    tiles = right.shape[1] // TILE
    for n in range(tiles):
        cols = pl.ds(n * TILE, TILE)
        rows = spread[...]
        first = n < tiles // 2
        rows = rows[: 3 * size] if first else jnp.concatenate([rows[: 2 * size], rows[3 * size :]], axis=0)
        got = jnp.dot(rows, tiles_of(parts, 0, n), preferred_element_type=f32).astype(bf16)
        right[:, cols] = got[:size]
        left[:, cols] = got[size : 2 * size]
        last, at = (ahead, n * TILE) if first else (behind, (n - tiles // 2) * TILE)
        last[:, pl.ds(at, TILE)] = got[2 * size :]


def collect(spread, parts):
    width = parts[0].shape[1] // HALVES
    count = len(parts)
    return pl.pallas_call(
        functools.partial(collect_kernel, count),
        out_shape=row_shapes(spread.shape[0] // (len(STEPS) - 1), width)[1:],
        in_specs=[vmem()] * (count + 1),
        out_specs=[vmem()] * 4,
        compiler_params=params(12),
        cost_estimate=cost(2 * spread.size * width, 4 * spread.shape[0] * width),
        name="collect",
    )(spread, *parts)


def merge_kernel(count, *refs):
    mine, (right, left, ahead, behind, first), rest = refs[:count], refs[count : count + 5], refs[count + 5 :]
    block = first.shape[0]
    tiles = first.shape[1] // TILE
    for n in range(tiles):
        cols = pl.ds(n * TILE, TILE)
        if count == 1:
            total = mine[0][:, cols]
        else:
            total = jnp.dot(mine[0][...], tiles_of(mine[1:], 0, n), preferred_element_type=f32)
        last, at = (ahead, n * TILE) if n < tiles // 2 else (behind, (n - tiles // 2) * TILE)
        total = total + right[:, cols].astype(f32) + left[:, cols].astype(f32)
        total = total + last[:, pl.ds(at, TILE)].astype(f32)
        first[:, cols] = total[:block]
        for k, out in enumerate(rest):
            out[:, cols] = total[(k + 1) * block : (k + 2) * block].astype(bf16)


def merge(mine, others):
    size, width = others[0].shape
    block = (size // FAR, width)
    return pl.pallas_call(
        functools.partial(merge_kernel, len(mine)),
        out_shape=(jax.ShapeDtypeStruct(block, f32),) + (jax.ShapeDtypeStruct(block, bf16),) * (FAR - 1),
        in_specs=[vmem()] * (len(mine) + 4),
        out_specs=[vmem()] * FAR,
        compiler_params=params(4),
        cost_estimate=cost(4 * size * width, 12 * size * width),
        name="merge",
    )(*mine, *others)


def half_swap(a):
    middle = a.shape[0] // 2
    return jnp.concatenate([a[middle:], a[:middle]], axis=0)


def route_kernel(first, one, two, three, rows, gain, router, ids, slots, hidden, payload):
    count, half = rows.shape
    total = first[...] + one[...].astype(f32) + two[...].astype(f32) + three[...].astype(f32)
    total = rows[...].astype(f32) + total
    hidden[...] = total
    square = jnp.sum(total * total, axis=1, keepdims=True)
    scale = lax.rsqrt((square + half_swap(square)) / D + norm_eps)
    normed = (total * scale * gain[...]).astype(bf16)
    payload[:, pl.ds(0, half)] = normed
    parts = [
        lax.dot_general(normed, router[:, pl.ds(c * half, half)], NT, preferred_element_type=f32)
        for c in range(HALVES)
    ]
    logits = jnp.where(iota(parts[0].shape, 0) < count // 2, parts[0], parts[1])
    logits = logits + half_swap(logits)
    logits = jnp.concatenate([logits] * (EXTRA // EXPERTS), axis=1)
    lane = iota(logits.shape, 1)
    place = jnp.zeros(logits.shape, jnp.int32)
    for k in range(TOP):
        place = jnp.where(lax.rem(lane, EXPERTS) == ids[:, k : k + 1], slots[:, k : k + 1] + 1, place)
    gates = jnp.where(place > 0, 1.0 / (1.0 + jnp.exp(-logits)), 0.0)
    share = route_scale * gates / jnp.sum(jnp.where(lane < EXPERTS, gates, 0.0), axis=1, keepdims=True)
    kind = lane // EXPERTS
    table = jnp.zeros(logits.shape, f32)
    for n in range(CAP):
        table = jnp.where((kind == n) & (place == n + 1), 1.0, table)
    rest = share
    for n in range(3):
        piece = rest.astype(bf16).astype(f32)
        table = jnp.where(kind == CAP + n, piece, table)
        rest = rest - piece
    payload[:, pl.ds(half, EXTRA)] = table.astype(bf16)


def route(added, rows, gain, router, ids, slots):
    count, half = rows.shape
    return pl.pallas_call(
        route_kernel,
        out_shape=(
            jax.ShapeDtypeStruct((count, half), f32),
            jax.ShapeDtypeStruct((count, half + EXTRA), bf16),
        ),
        in_specs=[vmem()] * 9,
        out_specs=[vmem()] * 2,
        compiler_params=params(4),
        cost_estimate=cost(4 * count * half * EXPERTS, 20 * count * half),
        name="route",
    )(*added, rows, gain, router, ids, slots)


def finish_kernel(hidden, first, one, two, three, out):
    seqs, steps, _ = out.shape
    half = hidden.shape[1]
    total = first[...] + one[...].astype(f32) + two[...].astype(f32) + three[...].astype(f32)
    total = (hidden[...] + total).astype(bf16)
    for c in range(HALVES):
        for b in range(seqs):
            at = (c * seqs + b) * steps
            out[b, :, pl.ds(c * half, half)] = total[at : at + steps]


def finish(hidden, added, shape):
    return pl.pallas_call(
        finish_kernel,
        out_shape=jax.ShapeDtypeStruct(shape, bf16),
        in_specs=[vmem()] * 5,
        out_specs=vmem(),
        compiler_params=params(4),
        cost_estimate=cost(5 * hidden.size, 14 * hidden.size),
        name="finish",
    )(hidden, *added)


def reduce_z(mine, right, left, ahead, behind):
    others = shift_z(right, 1), shift_z(left, -1), shift_z(ahead, 2), shift_z(behind, -2)
    first, *sent = merge(mine, others)
    others = [swap_far(rows, k + 1) for k, rows in enumerate(sent)]
    return first, *others


def layer(
    cache_kv,
    new_kv,
    queries,
    lengths,
    resid,
    value_up,
    out_proj,
    norm_gain,
    router,
    expert_ids,
    slots,
    w_gate,
    w_up,
    w_down,
):
    nx = lax.axis_size("x")
    seqs, steps = queries.shape[:2]
    tok = seqs * steps
    where = jnp.stack([lax.axis_index(a) for a in ("x", "zb", "j")]).astype(jnp.int32)
    where = jnp.concatenate([where, lengths.astype(jnp.int32)])

    tops, lows = pack(value_up.T, out_proj)
    top_left = swap_x(tops, 1)
    low_right = swap_x(lows, 3)
    low_left = swap_x(lows, 1)
    top_right = swap_x(tops, 3)

    outgoing = context_rows(where, nx, cache_kv, new_kv, queries)
    arrived = lax.all_to_all(
        outgoing.reshape(RING, nx * tok, LAT), ZAX, split_axis=0, concat_axis=0, tiled=True
    )
    top_far = swap_x(top_left, 3)
    low_far = swap_x(low_right, 1)
    mine = join(tops, lows)
    near = join(top_left, low_left, top_right, low_right)
    pieces = [mine, swap_core(mine)]
    pieces += [near, swap_core(near)]
    beyond = [top_far, low_far, swap_core(top_far), swap_core(low_far)]
    both = pair(w_gate, w_up)
    others = swap_core(both), swap_core(w_down)
    weights = stage((w_gate, w_up, others[0], w_down, others[1]))
    arrived = arrived.reshape(RING * nx * tok, LAT)
    most = attend_part(where, nx, arrived, pieces, (0, 0, 1, 2, 1, 2), tok, None)
    own, *rows = attend_part(where, nx, arrived, beyond, (3,) * 4, tok, most)
    added = reduce_z((own,), *rows)

    half = D // HALVES
    rows = resid.reshape(tok, HALVES, half).swapaxes(0, 1).reshape(HALVES * tok, half)
    gain = jnp.repeat(norm_gain.astype(f32).reshape(HALVES, half), tok, axis=0)
    ids, places = [
        jnp.tile(a.reshape(tok, TOP).astype(jnp.int32), (HALVES, 1)) for a in (expert_ids, slots)
    ]
    hidden, payload = route(added, rows, gain, router.T, ids, places)

    ring, lower, upper = ring_of(where, [payload] + [swap_far(payload, k) for k in range(1, FAR)])
    near = shift_z(ring, -1), shift_z(lower, -2), shift_z(upper, 2), shift_z(ring, 1)
    sent = dispatch(where, nx, (*near, ring), tok)
    got = [swap_x(sent[i], COLUMNS[i]) for i in range(1, nx)]
    late = plan(where, nx, (ring,), tok, 0, 1, 0)
    early = plan(where, nx, near, tok, 1, len(STEPS) - 1, 1)
    done = expert_part(where, (sent[0], *got[: nx - 2]), weights)
    done = [list(done[: nx - 1]), list(done[nx - 1 :])]
    for rows, last in zip(done, expert_part(where, got[nx - 2 :], weights)):
        rows.append(last)
    first = [done[0][0]] + [swap_x(done[0][i], COLUMNS[i]) for i in range(1, nx)]
    second = [done[1][0]] + [swap_x(done[1][i], COLUMNS[i]) for i in range(1, nx)]
    added = reduce_z((late, *second), *collect(early, first))
    return finish(hidden, added, resid.shape)


def solution(mesh):
    chips = mesh.shape["ep"] // (RING * CORES)
    grid = mesh.devices.reshape(mesh.shape["rep"], chips, FAR, NEAR, CORES)
    fine = Mesh(grid, ("rep", "x", "zb", "j", "c"))
    ep = ("x", "zb", "j", "c")
    both = ("rep",) + ep
    return jax.shard_map(
        layer,
        mesh=fine,
        in_specs=(
            P(both, None, None),
            P(both, None, None),
            P(both, None, None, None),
            P(both),
            P(both, None, None),
            P(None, ep),
            P(ep, None),
            P(),
            P(),
            P(both, None, None),
            P(both, None, None),
            P(None, ep),
            P(None, ep),
            P(ep, None),
        ),
        out_specs=P(both, None, None),
        check_vma=False,
    )
```

```python
import functools
import math

import jax
import jax.numpy as jnp
from jax import lax
from jax.experimental import pallas as pl
from jax.experimental.pallas import tpu as pltpu
from jax.sharding import Mesh
from jax.sharding import PartitionSpec as P


D = 7168
LAT = 512
VH = 128
EXPERTS = 16
TOP = 8
CAP = 2
QK = 192

CORES = 2
NEAR = 4
FAR = 4
RING = NEAR * FAR
SLOTS = RING * CAP
LATE = FAR * CAP
EARLY = SLOTS - LATE
EXTRA = 128

route_scale = 2.827
norm_eps = 1e-06


ZAX = ("zb", "j")
f32, bf16 = jnp.float32, jnp.bfloat16
NT = (((1,), (1,)), ((), ()))


def swap_x(a, bits):
    return lax.ppermute(a, "x", [(i, i ^ bits) for i in range(lax.axis_size("x"))])


def shift_z(a, step):
    return lax.ppermute(a, ZAX, [(i, (i + step) % RING) for i in range(RING)])


def swap_far(a, bits):
    return lax.ppermute(a, "zb", [(i, i ^ bits) for i in range(FAR)])


def swap_core(a):
    return lax.ppermute(a, "c", [(i, i ^ 1) for i in range(CORES)])


def iota(shape, axis):
    return lax.broadcasted_iota(jnp.int32, shape, axis)


def one_hot(mask):
    return jnp.where(mask, 1.0, 0.0).astype(bf16)


COLUMNS = (0, 1, 3, 2)


def column(index, x):
    return x ^ jnp.where(index == 2, 3, jnp.where(index == 3, 2, index))


STEPS = (0, 1, RING - 1, 2, RING - 2)


def chip_at(place, where_ref):
    group, bits = place // FAR, lax.rem(place, FAR)
    step = 0
    for i, value in enumerate(STEPS):
        step = jnp.where(group == i, value, step)
    chip = lax.rem(NEAR * where_ref[1] + where_ref[2] + step, RING)
    return NEAR * ((chip // NEAR) ^ bits) + lax.rem(chip, NEAR)


def of_tile(rows, n, tiles):
    size = rows.shape[0] // len(STEPS)
    if n < tiles // 2:
        return rows[: 4 * size]
    return jnp.concatenate([rows[: 3 * size], rows[4 * size :]], axis=0)


def smem():
    return pl.BlockSpec(memory_space=pltpu.SMEM)


def vmem():
    return pl.BlockSpec(memory_space=pltpu.VMEM)


def hbm():
    return pl.BlockSpec(memory_space=pltpu.HBM)


def held_in_hbm(a):
    return pltpu.with_memory_space_constraint(a, pltpu.HBM)


def held_in_vmem(a):
    return pltpu.with_memory_space_constraint(a, pltpu.VMEM)


def params(mib):
    return pltpu.CompilerParams(vmem_limit_bytes=mib << 20)


def cost(flops, nbytes):
    return pl.CostEstimate(flops=flops, bytes_accessed=nbytes, transcendentals=0)


def context_kernel(nx, turn, where_ref, *refs):
    keys, queries, new, out, buffer, held, sem = refs[-7:]
    seqs, steps, heads = queries.shape[:3]
    count = steps * heads
    scale = 1.0 / math.sqrt(QK)

    def copy(seq):
        return pltpu.make_async_copy(keys.at[seq], buffer.at[seq], sem.at[seq])

    @pl.when(where_ref[3 + seqs] == turn)
    def _():
        for seq in range(seqs):
            copy(seq).start()

        @pl.loop(0, seqs)
        def _(seq):
            query = queries[seq].reshape(count, queries.shape[3])
            copy(seq).wait()
            score = jnp.dot(query, buffer[seq], preferred_element_type=f32) * scale
            score = jnp.where(iota(score.shape, 1) < where_ref[3 + seq], score, -jnp.inf)
            wide = query.astype(f32)
            step_of = iota((count, 1), 0) // heads
            latest = []
            peak = jnp.max(score, axis=1, keepdims=True)
            for t in range(steps):
                key = new[seq, t : t + 1, :].astype(f32)
                got = jnp.sum(wide * key, axis=1, keepdims=True) * scale
                got = jnp.where(step_of >= t, got, -jnp.inf)
                latest.append(got)
                peak = jnp.maximum(peak, got)
            probs = jnp.exp(score - peak)
            total = jnp.sum(probs, axis=1, keepdims=True)
            latest = [jnp.exp(got - peak) for got in latest]
            for got in latest:
                total = total + got
            share = 1.0 / total
            probs = (probs * share).astype(bf16)
            context = lax.dot_general(probs, buffer[seq, :LAT, :], NT, preferred_element_type=f32)
            for t, got in enumerate(latest):
                part = (got * share).astype(bf16).astype(f32)
                context = context + part * new[seq, t : t + 1, :LAT].astype(f32)
            held[pl.ds(pl.multiple_of(seq * count, count), count), :] = context.astype(bf16)

        rows = held.shape[0]
        tok = rows // heads
        shape = (rows, rows)
        to, source = iota(shape, 0), iota(shape, 1)
        hop = lax.rem(to // tok, nx)
        head = column(hop, where_ref[0]) * RING + to // (tok * nx)
        take = (lax.rem(to, tok) == source // heads) & (head == lax.rem(source, heads))
        out[...] = jnp.dot(one_hot(take), held[...], preferred_element_type=f32).astype(bf16)

    for before in refs[:-7]:

        @pl.when(where_ref[3 + seqs] != turn)
        def _():
            out[...] = before[...]


def context_rows(where, nx, cache_kv, new_kv, queries, turn, before):
    seqs, length, width = cache_kv.shape
    steps, heads = queries.shape[1:3]
    rows = seqs * steps * heads
    keys = jnp.swapaxes(cache_kv, 1, 2)
    kept = [] if before is None else [before]
    return pl.pallas_call(
        functools.partial(context_kernel, nx, turn),
        out_shape=jax.ShapeDtypeStruct((rows, LAT), bf16),
        in_specs=[smem()] + [vmem()] * len(kept) + [hbm(), vmem(), vmem()],
        out_specs=vmem(),
        scratch_shapes=[
            pltpu.VMEM((seqs, width, length), bf16),
            pltpu.VMEM((rows, LAT), bf16),
            pltpu.SemaphoreType.DMA((seqs,)),
        ],
        compiler_params=params(24),
        cost_estimate=cost(2 * rows * length * (width + LAT), 2 * cache_kv.size),
        name="context_rows",
    )(where, *kept, held_in_hbm(keys), queries, new_kv)


def pack_kernel(up, rows, tops, lows, sem):
    half, at = tops.shape[0], up.shape[1]
    copies = []
    for i, out in enumerate((tops, lows)):
        part = pl.ds(i * half, half)
        copies.append(pltpu.make_async_copy(rows.at[part], out.at[:, pl.ds(at, rows.shape[1])], sem.at[i, 0]))
        copies.append(pltpu.make_async_copy(up.at[part], out.at[:, pl.ds(0, at)], sem.at[i, 1]))
    for copy in copies:
        copy.start()
    for copy in copies:
        copy.wait()


def pack(up, rows):
    shape = (rows.shape[0] // 2, up.shape[1] + rows.shape[1])
    return pl.pallas_call(
        pack_kernel,
        out_shape=(jax.ShapeDtypeStruct(shape, bf16),) * 2,
        in_specs=[hbm()] * 2,
        out_specs=[vmem()] * 2,
        scratch_shapes=[pltpu.SemaphoreType.DMA((2, 2))],
        compiler_params=params(12),
        cost_estimate=cost(1, 4 * rows.size),
        name="pack",
    )(held_in_hbm(up), held_in_hbm(rows))


HALVES = 2
TILE = 256


def put_rows(got, outs, n):
    own, right, left, ahead, behind = outs
    size, width = own.shape[0], ahead.shape[1]
    cols = pl.ds(n * TILE, TILE)
    own[:, cols] = got[:size]
    right[:, cols] = got[size : 2 * size].astype(bf16)
    left[:, cols] = got[2 * size : 3 * size].astype(bf16)
    last, at = (ahead, n * TILE) if n * TILE < width else (behind, n * TILE - width)
    last[:, pl.ds(at, TILE)] = got[3 * size :].astype(bf16)


def row_shapes(size, width):
    return (
        jax.ShapeDtypeStruct((size, width), f32),
        jax.ShapeDtypeStruct((size, width), bf16),
        jax.ShapeDtypeStruct((size, width), bf16),
        jax.ShapeDtypeStruct((size, width // 2), bf16),
        jax.ShapeDtypeStruct((size, width // 2), bf16),
    )


def tiles_of(parts, at, n):
    half = (parts[0].shape[1] - at) // HALVES
    got = [p[:, pl.ds(at + c * half + n * TILE, TILE)] for c in range(HALVES) for p in parts]
    return jnp.concatenate(got, axis=0)


def attend_kernel(tok, nx, count, first, last, where_ref, arrived, *refs):
    pieces, outs = refs[:count], refs[count:]
    if last:
        before, outs = outs[0], outs[1:]
    up = jnp.concatenate([piece[:, pl.ds(0, LAT)] for piece in pieces], axis=0)
    values = lax.dot_general(arrived[...], up, NT, preferred_element_type=f32)
    hop = lax.rem(iota(values.shape, 0) // tok, nx)
    values = jnp.where(hop == first + iota(values.shape, 1) // VH, values, 0.0).astype(bf16)
    shape = (len(STEPS) * FAR * HALVES * tok, arrived.shape[0])
    row, source = iota(shape, 0), iota(shape, 1)
    chip = chip_at(row // (HALVES * tok), where_ref)
    take = (source // (tok * nx) == chip) & (lax.rem(source, tok) == lax.rem(row, tok))
    half = lax.rem(row // tok, HALVES)
    taken = [
        jnp.dot(one_hot(take & (half == c)), values, preferred_element_type=f32).astype(bf16)
        for c in range(HALVES)
    ]
    values = jnp.concatenate(taken, axis=1)
    tiles = outs[0].shape[1] // TILE
    for n in range(tiles):
        got = jnp.dot(of_tile(values, n, tiles), tiles_of(pieces, LAT, n), preferred_element_type=f32)
        cols = pl.ds(n * TILE, TILE)
        if last:
            put_rows(before[:, cols] + got, outs, n)
        else:
            outs[0][:, cols] = got


def attend_part(where, nx, arrived, pieces, tok, first, before):
    depth = sum(p.shape[0] for p in pieces)
    width = (pieces[0].shape[1] - LAT) // HALVES
    count = len(pieces)
    last = before is not None
    part = jax.ShapeDtypeStruct((RING * HALVES * tok, width), f32)
    return pl.pallas_call(
        functools.partial(attend_kernel, tok, nx, count, first, last),
        out_shape=row_shapes(FAR * HALVES * tok, width) if last else part,
        in_specs=[smem(), vmem()] + [vmem()] * count + [vmem()] * last,
        out_specs=[vmem()] * 5 if last else vmem(),
        compiler_params=params(6),
        cost_estimate=cost(8 * RING * tok * depth * width * HALVES, 4 * depth * width),
        name="attend_part",
    )(where, arrived, *pieces, *([before] if last else []))


SEND_TILE = 512


def dispatch_kernel(tok, nx, where_ref, tokens, *refs):
    outs, (early, late) = refs[:nx], refs[nx:]
    count, width = tokens.shape
    half = width - EXTRA
    table = tokens[:, pl.ds(half, EXTRA)]
    shape = (nx * CAP, EXTRA)
    row, place = iota(shape, 0), iota(shape, 1)
    expert = FAR * column(row // CAP, where_ref[0]) + where_ref[1]
    hot = one_hot(place == lax.rem(row, CAP) * EXPERTS + expert)
    got = lax.dot_general(hot, table, NT, preferred_element_type=f32)
    shape = (SLOTS, count)
    slot, token = iota(shape, 0), iota(shape, 1)
    source = slot // CAP
    chip = NEAR * lax.rem(source, FAR) + lax.rem(where_ref[2] + source // FAR + 1, NEAR)
    parts = []
    for r in range(nx):
        sel = jnp.where(lax.rem(slot, CAP) == 0, got[CAP * r : CAP * r + 1], got[CAP * r + 1 : CAP * r + 2])
        parts.append(jnp.where(chip == token // (HALVES * tok), sel, 0.0))
    of_half = lax.rem(token // tok, HALVES)
    halves = [[jnp.where(of_half == c, sel, 0.0) for sel in parts] for c in range(HALVES)]
    both = jnp.concatenate(sum(halves, []), axis=0).astype(bf16)
    rows = nx * SLOTS
    for n in range(half // SEND_TILE):
        got = jnp.dot(both, tokens[:, pl.ds(n * SEND_TILE, SEND_TILE)], preferred_element_type=f32).astype(bf16)
        for c in range(HALVES):
            for r in range(nx):
                at = c * rows + r * SLOTS
                outs[r][:, pl.ds(c * half + n * SEND_TILE, SEND_TILE)] = got[at : at + SLOTS]
    got = jnp.dot(both[:rows], table, preferred_element_type=f32).astype(bf16)
    for r in range(nx):
        outs[r][:, pl.ds(HALVES * half, EXTRA)] = got[r * SLOTS : (r + 1) * SLOTS]
    for out, group, at, end in ((early, 1, 0, EARLY), (late, 0, EARLY, SLOTS)):
        shape = (out.shape[0], count)
        row, token = iota(shape, 0), iota(shape, 1)
        chip = chip_at(group * FAR + row // (HALVES * tok), where_ref)
        take = (token // (HALVES * tok) == chip) & (lax.rem(token, HALVES * tok) == lax.rem(row, HALVES * tok))
        sel = jnp.concatenate([sel[at:end] for sels in halves for sel in sels], axis=0).astype(bf16)
        out[...] = lax.dot_general(one_hot(take), sel, NT, preferred_element_type=f32).astype(bf16)


def dispatch(where, nx, tokens, tok):
    count, width = tokens.shape
    full = HALVES * (width - EXTRA) + EXTRA
    near = count // NEAR
    return pl.pallas_call(
        functools.partial(dispatch_kernel, tok, nx),
        out_shape=(jax.ShapeDtypeStruct((SLOTS, full), bf16),) * nx
        + (
            jax.ShapeDtypeStruct(((len(STEPS) - 1) * near, HALVES * nx * EARLY), bf16),
            jax.ShapeDtypeStruct((near, HALVES * nx * LATE), bf16),
        ),
        in_specs=[smem(), vmem()],
        out_specs=[vmem()] * (nx + 2),
        compiler_params=params(12),
        cost_estimate=cost(2 * nx * SLOTS * count * full, 4 * count * width),
        name="dispatch",
    )(where, tokens)


CHUNKS = 7


def stage_kernel(gate_a, gate_b, up_a, up_b, down_a, down_b, wide, deep, sem):
    part = gate_a.shape[1]
    copies = [
        pltpu.make_async_copy(ref, wide.at[:, pl.ds(i * part, part)], sem.at[i])
        for i, ref in enumerate((gate_a, gate_b, up_a, up_b))
    ]
    copies += [
        pltpu.make_async_copy(ref, deep.at[pl.ds(i * part, part)], sem.at[4 + i])
        for i, ref in enumerate((down_a, down_b))
    ]
    for copy in copies:
        copy.start()
    for copy in copies:
        copy.wait()


def stage(weights):
    dim, part = weights[0].shape
    return pl.pallas_call(
        stage_kernel,
        out_shape=(
            jax.ShapeDtypeStruct((dim, 4 * part), bf16),
            jax.ShapeDtypeStruct((2 * part, dim), bf16),
        ),
        in_specs=[hbm()] * 6,
        out_specs=[vmem()] * 2,
        scratch_shapes=[pltpu.SemaphoreType.DMA((6,))],
        compiler_params=params(4),
        cost_estimate=cost(4 * 1000 * dim * part, 12 * dim * part),
        name="stage",
    )(*[held_in_hbm(w) for w in weights])


def expert_kernel(groups, where_ref, *refs):
    tokens = refs[:groups]
    wide, deep = refs[groups : groups + 2]
    early, late = refs[groups + 2 : 2 * groups + 2], refs[2 * groups + 2 : 3 * groups + 2]
    held = refs[3 * groups + 2] if groups > 1 else tokens[0]
    dim = wide.shape[0]
    part = wide.shape[1] // 2
    chunk = dim // CHUNKS
    if groups > 1:
        for g, ref in enumerate(tokens):
            held[pl.ds(g * SLOTS, SLOTS)] = ref[...]
    total = jnp.dot(held[:, pl.ds(0, dim)], wide[...], preferred_element_type=f32)
    gate, upward = total[:, :part], total[:, part:]
    act = (gate / (1.0 + jnp.exp(-gate)) * upward).astype(bf16)
    shape = (EXTRA, EXTRA)
    expert = FAR * where_ref[0] + where_ref[1]
    from_share = iota(shape, 0) - CAP * EXPERTS
    hot = (from_share >= 0) & (from_share < 3 * EXPERTS) & (lax.rem(from_share + EXTRA, EXPERTS) == expert)
    share = jnp.dot(held[:, pl.ds(dim, EXTRA)], one_hot(hot), preferred_element_type=f32)[:, :1]
    for k in range(CHUNKS):
        cols = pl.ds(k * chunk, chunk)
        got = jnp.dot(act, deep[:, cols], preferred_element_type=f32) * share
        for g in range(groups):
            rows = got[g * SLOTS : (g + 1) * SLOTS].astype(bf16)
            early[g][:, cols] = rows[:EARLY]
            late[g][:, cols] = rows[EARLY:]


def expert_part(where, tokens, weights):
    wide, deep = weights
    dim = wide.shape[0]
    groups = len(tokens)
    rows = groups * SLOTS
    held = [pltpu.VMEM((rows, dim + EXTRA), bf16)] if groups > 1 else []
    return pl.pallas_call(
        functools.partial(expert_kernel, groups),
        out_shape=(jax.ShapeDtypeStruct((EARLY, dim), bf16),) * groups
        + (jax.ShapeDtypeStruct((LATE, dim), bf16),) * groups,
        in_specs=[smem()] + [vmem()] * (groups + 2),
        out_specs=[vmem()] * (2 * groups),
        scratch_shapes=held,
        compiler_params=params(8),
        cost_estimate=cost(6 * rows * wide.size, 2 * rows * dim),
        name="expert_part",
    )(where, *tokens, held_in_vmem(wide), held_in_vmem(deep))


def collect_kernel(count, spread, *refs):
    parts, (right, left, ahead, behind) = refs[:count], refs[count:]
    size = right.shape[0]
    tiles = right.shape[1] // TILE
    for n in range(tiles):
        cols = pl.ds(n * TILE, TILE)
        rows = spread[...]
        first = n < tiles // 2
        rows = rows[: 3 * size] if first else jnp.concatenate([rows[: 2 * size], rows[3 * size :]], axis=0)
        got = jnp.dot(rows, tiles_of(parts, 0, n), preferred_element_type=f32).astype(bf16)
        right[:, cols] = got[:size]
        left[:, cols] = got[size : 2 * size]
        last, at = (ahead, n * TILE) if first else (behind, (n - tiles // 2) * TILE)
        last[:, pl.ds(at, TILE)] = got[2 * size :]


def collect(spread, parts):
    width = parts[0].shape[1] // HALVES
    count = len(parts)
    return pl.pallas_call(
        functools.partial(collect_kernel, count),
        out_shape=row_shapes(spread.shape[0] // (len(STEPS) - 1), width)[1:],
        in_specs=[vmem()] * (count + 1),
        out_specs=[vmem()] * 4,
        compiler_params=params(12),
        cost_estimate=cost(2 * spread.size * width, 4 * spread.shape[0] * width),
        name="collect",
    )(spread, *parts)


def merge_kernel(count, *refs):
    mine, (right, left, ahead, behind, first), rest = refs[:count], refs[count : count + 5], refs[count + 5 :]
    block = first.shape[0]
    tiles = first.shape[1] // TILE
    for n in range(tiles):
        cols = pl.ds(n * TILE, TILE)
        if count == 1:
            total = mine[0][:, cols]
        else:
            total = jnp.dot(mine[0][...], tiles_of(mine[1:], 0, n), preferred_element_type=f32)
        last, at = (ahead, n * TILE) if n < tiles // 2 else (behind, (n - tiles // 2) * TILE)
        total = total + right[:, cols].astype(f32) + left[:, cols].astype(f32)
        total = total + last[:, pl.ds(at, TILE)].astype(f32)
        first[:, cols] = total[:block]
        for k, out in enumerate(rest):
            out[:, cols] = total[(k + 1) * block : (k + 2) * block].astype(bf16)


def merge(mine, others):
    size, width = others[0].shape
    block = (size // FAR, width)
    return pl.pallas_call(
        functools.partial(merge_kernel, len(mine)),
        out_shape=(jax.ShapeDtypeStruct(block, f32),) + (jax.ShapeDtypeStruct(block, bf16),) * (FAR - 1),
        in_specs=[vmem()] * (len(mine) + 4),
        out_specs=[vmem()] * FAR,
        compiler_params=params(4),
        cost_estimate=cost(4 * size * width, 12 * size * width),
        name="merge",
    )(*mine, *others)


def half_swap(a):
    middle = a.shape[0] // 2
    return jnp.concatenate([a[middle:], a[:middle]], axis=0)


def route_kernel(first, one, two, three, rows, gain, router, ids, slots, hidden, payload):
    count, half = rows.shape
    total = first[...] + one[...].astype(f32) + two[...].astype(f32) + three[...].astype(f32)
    total = rows[...].astype(f32) + total
    hidden[...] = total
    square = jnp.sum(total * total, axis=1, keepdims=True)
    scale = lax.rsqrt((square + half_swap(square)) / D + norm_eps)
    normed = (total * scale * gain[...]).astype(bf16)
    payload[:, pl.ds(0, half)] = normed
    parts = [
        lax.dot_general(normed, router[:, pl.ds(c * half, half)], NT, preferred_element_type=f32)
        for c in range(HALVES)
    ]
    logits = jnp.where(iota(parts[0].shape, 0) < count // 2, parts[0], parts[1])
    logits = logits + half_swap(logits)
    logits = jnp.concatenate([logits] * (EXTRA // EXPERTS), axis=1)
    lane = iota(logits.shape, 1)
    place = jnp.zeros(logits.shape, jnp.int32)
    for k in range(TOP):
        place = jnp.where(lax.rem(lane, EXPERTS) == ids[:, k : k + 1], slots[:, k : k + 1] + 1, place)
    gates = jnp.where(place > 0, 1.0 / (1.0 + jnp.exp(-logits)), 0.0)
    share = route_scale * gates / jnp.sum(jnp.where(lane < EXPERTS, gates, 0.0), axis=1, keepdims=True)
    kind = lane // EXPERTS
    table = jnp.zeros(logits.shape, f32)
    for n in range(CAP):
        table = jnp.where((kind == n) & (place == n + 1), 1.0, table)
    rest = share
    for n in range(3):
        piece = rest.astype(bf16).astype(f32)
        table = jnp.where(kind == CAP + n, piece, table)
        rest = rest - piece
    payload[:, pl.ds(half, EXTRA)] = table.astype(bf16)


def route(added, rows, gain, router, ids, slots):
    count, half = rows.shape
    return pl.pallas_call(
        route_kernel,
        out_shape=(
            jax.ShapeDtypeStruct((count, half), f32),
            jax.ShapeDtypeStruct((count, half + EXTRA), bf16),
        ),
        in_specs=[vmem()] * 9,
        out_specs=[vmem()] * 2,
        compiler_params=params(4),
        cost_estimate=cost(4 * count * half * EXPERTS, 20 * count * half),
        name="route",
    )(*added, rows, gain, router, ids, slots)


def finish_kernel(hidden, first, one, two, three, out):
    seqs, steps, _ = out.shape
    half = hidden.shape[1]
    total = first[...] + one[...].astype(f32) + two[...].astype(f32) + three[...].astype(f32)
    total = (hidden[...] + total).astype(bf16)
    for c in range(HALVES):
        for b in range(seqs):
            at = (c * seqs + b) * steps
            out[b, :, pl.ds(c * half, half)] = total[at : at + steps]


def finish(hidden, added, shape):
    return pl.pallas_call(
        finish_kernel,
        out_shape=jax.ShapeDtypeStruct(shape, bf16),
        in_specs=[vmem()] * 5,
        out_specs=vmem(),
        compiler_params=params(4),
        cost_estimate=cost(5 * hidden.size, 14 * hidden.size),
        name="finish",
    )(hidden, *added)


def reduce_z(mine, right, left, ahead, behind):
    others = shift_z(right, 1), shift_z(left, -1), shift_z(ahead, 2), shift_z(behind, -2)
    first, *sent = merge(mine, others)
    others = [swap_far(rows, k + 1) for k, rows in enumerate(sent)]
    return first, *others


def layer(
    cache_kv,
    new_kv,
    queries,
    lengths,
    resid,
    value_up,
    out_proj,
    norm_gain,
    router,
    expert_ids,
    slots,
    w_gate,
    w_up,
    w_down,
):
    nx = lax.axis_size("x")
    seqs, steps = queries.shape[:2]
    tok = seqs * steps
    where = jnp.stack([lax.axis_index(a) for a in ("x", "zb", "j")]).astype(jnp.int32)
    core = lax.axis_index("c").astype(jnp.int32)
    where = jnp.concatenate([where, lengths.astype(jnp.int32), core.reshape(1)])

    tops, lows = pack(value_up.T, out_proj)
    attend = functools.partial(context_rows, where, nx, cache_kv, new_kv, queries)
    outgoing = attend(0, None)
    top_left = swap_x(tops, 1)
    low_right = swap_x(lows, 3)
    low_left = swap_x(lows, 1)
    top_right = swap_x(tops, 3)
    outgoing = attend(1, outgoing)
    arrived = lax.all_to_all(
        outgoing.reshape(RING, nx * tok, LAT), ZAX, split_axis=0, concat_axis=0, tiled=True
    )
    top_far = swap_x(top_left, 3)
    low_far = swap_x(low_right, 1)
    near = [tops, lows, swap_core(tops), swap_core(lows)]
    for pair in ((top_left, low_left), (top_right, low_right)):
        near += [*pair, *map(swap_core, pair)]
    beyond = [top_far, low_far, swap_core(top_far), swap_core(low_far)]
    others = [swap_core(w) for w in (w_gate, w_up, w_down)]
    weights = stage((w_gate, others[0], w_up, others[1], w_down, others[2]))
    arrived = arrived.reshape(RING * nx * tok, LAT)
    most = attend_part(where, nx, arrived, near, tok, 0, None)
    own, *rows = attend_part(where, nx, arrived, beyond, tok, nx - 1, most)
    added = reduce_z((own,), *rows)

    half = D // HALVES
    rows = resid.reshape(tok, HALVES, half).swapaxes(0, 1).reshape(HALVES * tok, half)
    gain = jnp.repeat(norm_gain.astype(f32).reshape(HALVES, half), tok, axis=0)
    ids, places = [
        jnp.tile(a.reshape(tok, TOP).astype(jnp.int32), (HALVES, 1)) for a in (expert_ids, slots)
    ]
    hidden, payload = route(added, rows, gain, router.T, ids, places)

    ring = lax.all_gather(payload, ZAX, axis=0, tiled=True)
    *sent, early, late = dispatch(where, nx, ring, tok)
    got = [swap_x(sent[i], COLUMNS[i]) for i in range(1, nx)]
    done = expert_part(where, (sent[0], *got[: nx - 2]), weights)
    done = [list(done[: nx - 1]), list(done[nx - 1 :])]
    for rows, last in zip(done, expert_part(where, got[nx - 2 :], weights)):
        rows.append(last)
    first = [done[0][0]] + [swap_x(done[0][i], COLUMNS[i]) for i in range(1, nx)]
    second = [done[1][0]] + [swap_x(done[1][i], COLUMNS[i]) for i in range(1, nx)]
    added = reduce_z((late, *second), *collect(early, first))
    return finish(hidden, added, resid.shape)


def solution(mesh):
    chips = mesh.shape["ep"] // (RING * CORES)
    grid = mesh.devices.reshape(mesh.shape["rep"], chips, FAR, NEAR, CORES)
    fine = Mesh(grid, ("rep", "x", "zb", "j", "c"))
    ep = ("x", "zb", "j", "c")
    both = ("rep",) + ep
    return jax.shard_map(
        layer,
        mesh=fine,
        in_specs=(
            P(both, None, None),
            P(both, None, None),
            P(both, None, None, None),
            P(both),
            P(both, None, None),
            P(None, ep),
            P(ep, None),
            P(),
            P(),
            P(both, None, None),
            P(both, None, None),
            P(None, ep),
            P(None, ep),
            P(ep, None),
        ),
        out_specs=P(both, None, None),
        check_vma=False,
    )
```

```python
import functools
import math

import jax
import jax.numpy as jnp
from jax import lax
from jax.experimental import pallas as pl
from jax.experimental.pallas import tpu as pltpu
from jax.sharding import Mesh
from jax.sharding import PartitionSpec as P


D = 7168
LAT = 512
VH = 128
EXPERTS = 16
TOP = 8
CAP = 2
QK = 192

CORES = 2
NEAR = 4
FAR = 4
RING = NEAR * FAR
SLOTS = RING * CAP
LATE = FAR * CAP
EARLY = SLOTS - LATE
EXTRA = 128

route_scale = 2.827
norm_eps = 1e-06

PAIR = 2
HALVES = 2
TILE = 256


ZAX = ("zb", "j")
f32, bf16 = jnp.float32, jnp.bfloat16
NT = (((1,), (1,)), ((), ()))


def swap_x(a, bits):
    return lax.ppermute(a, "x", [(i, i ^ bits) for i in range(lax.axis_size("x"))])


def shift_z(a, step):
    return lax.ppermute(a, ZAX, [(i, (i + step) % RING) for i in range(RING)])


def swap_far(a, bits):
    return lax.ppermute(a, "zb", [(i, i ^ bits) for i in range(FAR)])


def swap_core(a):
    return lax.ppermute(a, "c", [(i, i ^ 1) for i in range(CORES)])


def iota(shape, axis):
    return lax.broadcasted_iota(jnp.int32, shape, axis)


def one_hot(mask):
    return jnp.where(mask, 1.0, 0.0).astype(bf16)


COLUMNS = (0, 1, 3, 2)


def column(index, x):
    return x ^ jnp.where(index == 2, 3, jnp.where(index == 3, 2, index))


STEPS = (0, 1, RING - 1, 2, RING - 2)


def chip_at(place, where_ref):
    group, bits = place // FAR, lax.rem(place, FAR)
    step = 0
    for i, value in enumerate(STEPS):
        step = jnp.where(group == i, value, step)
    chip = lax.rem(NEAR * where_ref[1] + where_ref[2] + step, RING)
    return NEAR * ((chip // NEAR) ^ bits) + lax.rem(chip, NEAR)


def of_tile(rows, n, tiles):
    size = rows.shape[0] // len(STEPS)
    if n < tiles // 2:
        return rows[: 4 * size]
    return jnp.concatenate([rows[: 3 * size], rows[4 * size :]], axis=0)


def smem():
    return pl.BlockSpec(memory_space=pltpu.SMEM)


def vmem():
    return pl.BlockSpec(memory_space=pltpu.VMEM)


def hbm():
    return pl.BlockSpec(memory_space=pltpu.HBM)


def held_in_hbm(a):
    return pltpu.with_memory_space_constraint(a, pltpu.HBM)


def held_in_vmem(a):
    return pltpu.with_memory_space_constraint(a, pltpu.VMEM)


def params(mib):
    return pltpu.CompilerParams(vmem_limit_bytes=mib << 20)


def cost(flops, nbytes):
    return pl.CostEstimate(flops=flops, bytes_accessed=nbytes, transcendentals=0)


def context_kernel(nx, where_ref, keys, queries, new, out, held):
    seq = pl.program_id(0)
    seqs = pl.num_programs(0)
    steps, heads = queries.shape[1], queries.shape[2]
    count = steps * heads
    scale = 1.0 / math.sqrt(QK)
    query = queries[0].reshape(count, queries.shape[3])
    score = jnp.dot(query, keys[0], preferred_element_type=f32) * scale
    score = jnp.where(iota(score.shape, 1) < where_ref[3 + seq], score, -jnp.inf)
    wide = query.astype(f32)
    step_of = iota((count, 1), 0) // heads
    latest = []
    peak = jnp.max(score, axis=1, keepdims=True)
    for t in range(steps):
        key = new[0, t : t + 1, :].astype(f32)
        got = jnp.sum(wide * key, axis=1, keepdims=True) * scale
        got = jnp.where(step_of >= t, got, -jnp.inf)
        latest.append(got)
        peak = jnp.maximum(peak, got)
    probs = jnp.exp(score - peak)
    total = jnp.sum(probs, axis=1, keepdims=True)
    latest = [jnp.exp(got - peak) for got in latest]
    for got in latest:
        total = total + got
    share = 1.0 / total
    probs = (probs * share).astype(bf16)
    context = lax.dot_general(probs, keys[0, :LAT, :], NT, preferred_element_type=f32)
    for t, got in enumerate(latest):
        part = (got * share).astype(bf16).astype(f32)
        context = context + part * new[0, t : t + 1, :LAT].astype(f32)
    held[pl.ds(pl.multiple_of(seq * count, count), count), :] = context.astype(bf16)

    @pl.when(seq == seqs - 1)
    def _():
        rows = held.shape[0]
        tok = rows // heads
        shape = (rows, rows)
        to, source = iota(shape, 0), iota(shape, 1)
        hop = lax.rem(to // tok, nx)
        head = column(hop, where_ref[0]) * RING + to // (tok * nx)
        take = (lax.rem(to, tok) == source // heads) & (head == lax.rem(source, heads))
        out[...] = jnp.dot(one_hot(take), held[...], preferred_element_type=f32).astype(bf16)


def context_rows(where, nx, cache_kv, new_kv, queries):
    seqs, length, width = cache_kv.shape
    steps, heads = queries.shape[1:3]
    rows = seqs * steps * heads
    keys = jnp.swapaxes(cache_kv, 1, 2)
    return pl.pallas_call(
        functools.partial(context_kernel, nx),
        grid=(seqs,),
        out_shape=jax.ShapeDtypeStruct((rows, LAT), bf16),
        in_specs=[
            smem(),
            pl.BlockSpec((1, width, length), lambda b: (b, 0, 0)),
            pl.BlockSpec((1, steps, heads, width), lambda b: (b, 0, 0, 0)),
            pl.BlockSpec((1, steps, width), lambda b: (b, 0, 0)),
        ],
        out_specs=pl.BlockSpec((rows, LAT), lambda b: (0, 0)),
        scratch_shapes=[pltpu.VMEM((rows, LAT), bf16)],
        compiler_params=params(24),
        cost_estimate=cost(2 * rows * length * (width + LAT), 2 * cache_kv.size),
        name="context_rows",
    )(where, held_in_hbm(keys), held_in_hbm(queries), held_in_hbm(new_kv))


def pack_kernel(where_ref, up, rows, tops, lows, give, sem):
    half, at = tops.shape[0], up.shape[1]
    width = tops.shape[1] - at
    mine = lax.rem(where_ref[0], PAIR)
    copies = []
    for i, (out, side, first) in enumerate(((tops, mine, 0), (lows, mine, half), (give, 1 - mine, 0))):
        part = pl.ds(first, out.shape[0])
        cols = pl.ds(pl.multiple_of(side * width, TILE), width)
        copies.append(pltpu.make_async_copy(rows.at[part, cols], out.at[:, pl.ds(at, width)], sem.at[i, 0]))
        copies.append(pltpu.make_async_copy(up.at[part], out.at[:, pl.ds(0, at)], sem.at[i, 1]))
    for copy in copies:
        copy.start()
    for copy in copies:
        copy.wait()


def pack(where, up, rows):
    count, width = rows.shape[0], up.shape[1] + rows.shape[1] // PAIR
    return pl.pallas_call(
        pack_kernel,
        out_shape=(jax.ShapeDtypeStruct((count // 2, width), bf16),) * 2
        + (jax.ShapeDtypeStruct((count, width), bf16),),
        in_specs=[smem()] + [hbm()] * 2,
        out_specs=[vmem()] * 3,
        scratch_shapes=[pltpu.SemaphoreType.DMA((3, 2))],
        compiler_params=params(12),
        cost_estimate=cost(1, 4 * rows.size),
        name="pack",
    )(where, held_in_hbm(up), held_in_hbm(rows))


def put_rows(got, outs, n):
    own, right, left, ahead, behind = outs
    size, width = own.shape[0], ahead.shape[1]
    cols = pl.ds(n * TILE, TILE)
    own[:, cols] = got[:size]
    right[:, cols] = got[size : 2 * size].astype(bf16)
    left[:, cols] = got[2 * size : 3 * size].astype(bf16)
    last, at = (ahead, n * TILE) if n * TILE < width else (behind, n * TILE - width)
    last[:, pl.ds(at, TILE)] = got[3 * size :].astype(bf16)


def row_shapes(size, width):
    return (
        jax.ShapeDtypeStruct((size, width), f32),
        jax.ShapeDtypeStruct((size, width), bf16),
        jax.ShapeDtypeStruct((size, width), bf16),
        jax.ShapeDtypeStruct((size, width // 2), bf16),
        jax.ShapeDtypeStruct((size, width // 2), bf16),
    )


def tiles_of(parts, at, n):
    half = (parts[0].shape[1] - at) // HALVES
    got = [p[:, pl.ds(at + c * half + n * TILE, TILE)] for c in range(HALVES) for p in parts]
    return jnp.concatenate(got, axis=0)


def values_kernel(tok, nx, arrived, *refs):
    pieces, out = refs[:-1], refs[-1]
    up = jnp.concatenate([piece[:, pl.ds(0, LAT)] for piece in pieces], axis=0)
    values = lax.dot_general(arrived[...], up, NT, preferred_element_type=f32)
    hop = lax.rem(iota(values.shape, 0) // tok, nx)
    values = jnp.where(hop == iota(values.shape, 1) // VH, values, 0.0).astype(bf16)
    shape = (out.shape[0], arrived.shape[0])
    row, source = iota(shape, 0), iota(shape, 1)
    take = (source // (tok * nx) == row // tok) & (lax.rem(source, tok) == lax.rem(row, tok))
    out[...] = jnp.dot(one_hot(take), values, preferred_element_type=f32).astype(bf16)


def values_of(nx, arrived, pieces, tok):
    shape = (arrived.shape[0] // nx, nx * VH)
    return pl.pallas_call(
        functools.partial(values_kernel, tok, nx),
        out_shape=jax.ShapeDtypeStruct(shape, bf16),
        in_specs=[vmem()] * (1 + len(pieces)),
        out_specs=vmem(),
        compiler_params=params(6),
        cost_estimate=cost(2 * arrived.size * nx * VH, 2 * arrived.size),
        name="values",
    )(arrived, *pieces)


def attend_kernel(tok, where_ref, own, other, *refs):
    pieces, outs = refs[:-5], refs[-5:]
    count, depth = own.shape
    blocks = [other[:, pl.ds((i ^ 1) * VH, VH)] for i in range(depth // VH)]
    values = jnp.concatenate([own[...], jnp.concatenate(blocks, axis=1)], axis=0)
    shape = (len(STEPS) * FAR * PAIR * tok, PAIR * count)
    row, source = iota(shape, 0), iota(shape, 1)
    chip = chip_at(row // (PAIR * tok), where_ref)
    take = (source // count == lax.rem(row // tok, PAIR)) & (lax.rem(source, tok) == lax.rem(row, tok))
    take = take & (lax.rem(source, count) // tok == chip)
    values = jnp.dot(one_hot(take), values, preferred_element_type=f32).astype(bf16)
    tiles = outs[0].shape[1] // TILE
    for n in range(tiles):
        rows = jnp.concatenate([p[:, pl.ds(LAT + n * TILE, TILE)] for p in pieces], axis=0)
        put_rows(jnp.dot(of_tile(values, n, tiles), rows, preferred_element_type=f32), outs, n)


def attend(where, own, other, pieces, tok):
    depth = own.shape[1]
    width = pieces[0].shape[1] - LAT
    return pl.pallas_call(
        functools.partial(attend_kernel, tok),
        out_shape=row_shapes(FAR * PAIR * tok, width),
        in_specs=[smem()] + [vmem()] * (2 + len(pieces)),
        out_specs=[vmem()] * 5,
        compiler_params=params(6),
        cost_estimate=cost(4 * RING * tok * depth * width * PAIR, 2 * depth * width),
        name="attend",
    )(where, own, other, *pieces)


SEND_TILE = 512


def dispatch_kernel(tok, nx, where_ref, tokens, *refs):
    outs, (early, late) = refs[:nx], refs[nx:]
    count, width = tokens.shape
    half = width - EXTRA
    table = tokens[:, pl.ds(half, EXTRA)]
    shape = (nx * CAP, EXTRA)
    row, place = iota(shape, 0), iota(shape, 1)
    expert = FAR * column(row // CAP, where_ref[0]) + where_ref[1]
    hot = one_hot(place == lax.rem(row, CAP) * EXPERTS + expert)
    got = lax.dot_general(hot, table, NT, preferred_element_type=f32)
    shape = (SLOTS, count)
    slot, token = iota(shape, 0), iota(shape, 1)
    source = slot // CAP
    chip = NEAR * lax.rem(source, FAR) + lax.rem(where_ref[2] + source // FAR + 1, NEAR)
    parts = []
    for r in range(nx):
        sel = jnp.where(lax.rem(slot, CAP) == 0, got[CAP * r : CAP * r + 1], got[CAP * r + 1 : CAP * r + 2])
        parts.append(jnp.where(chip == token // (HALVES * tok), sel, 0.0))
    of_half = lax.rem(token // tok, HALVES)
    halves = [[jnp.where(of_half == c, sel, 0.0) for sel in parts] for c in range(HALVES)]
    both = jnp.concatenate(sum(halves, []), axis=0).astype(bf16)
    rows = nx * SLOTS
    for n in range(half // SEND_TILE):
        got = jnp.dot(both, tokens[:, pl.ds(n * SEND_TILE, SEND_TILE)], preferred_element_type=f32).astype(bf16)
        for c in range(HALVES):
            for r in range(nx):
                at = c * rows + r * SLOTS
                outs[r][:, pl.ds(c * half + n * SEND_TILE, SEND_TILE)] = got[at : at + SLOTS]
    got = jnp.dot(both[:rows], table, preferred_element_type=f32).astype(bf16)
    for r in range(nx):
        outs[r][:, pl.ds(HALVES * half, EXTRA)] = got[r * SLOTS : (r + 1) * SLOTS]
    for out, group, at, end in ((early, 1, 0, EARLY), (late, 0, EARLY, SLOTS)):
        shape = (out.shape[0], count)
        row, token = iota(shape, 0), iota(shape, 1)
        chip = chip_at(group * FAR + row // (HALVES * tok), where_ref)
        take = (token // (HALVES * tok) == chip) & (lax.rem(token, HALVES * tok) == lax.rem(row, HALVES * tok))
        sel = jnp.concatenate([sel[at:end] for sels in halves for sel in sels], axis=0).astype(bf16)
        out[...] = lax.dot_general(one_hot(take), sel, NT, preferred_element_type=f32).astype(bf16)


def dispatch(where, nx, tokens, tok):
    count, width = tokens.shape
    full = HALVES * (width - EXTRA) + EXTRA
    near = count // NEAR
    return pl.pallas_call(
        functools.partial(dispatch_kernel, tok, nx),
        out_shape=(jax.ShapeDtypeStruct((SLOTS, full), bf16),) * nx
        + (
            jax.ShapeDtypeStruct(((len(STEPS) - 1) * near, HALVES * nx * EARLY), bf16),
            jax.ShapeDtypeStruct((near, HALVES * nx * LATE), bf16),
        ),
        in_specs=[smem(), vmem()],
        out_specs=[vmem()] * (nx + 2),
        compiler_params=params(12),
        cost_estimate=cost(2 * nx * SLOTS * count * full, 4 * count * width),
        name="dispatch",
    )(where, tokens)


CHUNKS = 7


def stage_kernel(gate_a, gate_b, up_a, up_b, down_a, down_b, wide, deep, sem):
    part = gate_a.shape[1]
    copies = [
        pltpu.make_async_copy(ref, wide.at[:, pl.ds(i * part, part)], sem.at[i])
        for i, ref in enumerate((gate_a, gate_b, up_a, up_b))
    ]
    copies += [
        pltpu.make_async_copy(ref, deep.at[pl.ds(i * part, part)], sem.at[4 + i])
        for i, ref in enumerate((down_a, down_b))
    ]
    for copy in copies:
        copy.start()
    for copy in copies:
        copy.wait()


def stage(weights):
    dim, part = weights[0].shape
    return pl.pallas_call(
        stage_kernel,
        out_shape=(
            jax.ShapeDtypeStruct((dim, 4 * part), bf16),
            jax.ShapeDtypeStruct((2 * part, dim), bf16),
        ),
        in_specs=[hbm()] * 6,
        out_specs=[vmem()] * 2,
        scratch_shapes=[pltpu.SemaphoreType.DMA((6,))],
        compiler_params=params(4),
        cost_estimate=cost(4 * 1000 * dim * part, 12 * dim * part),
        name="stage",
    )(*[held_in_hbm(w) for w in weights])


def expert_kernel(groups, where_ref, *refs):
    tokens = refs[:groups]
    wide, deep = refs[groups : groups + 2]
    early, late = refs[groups + 2 : 2 * groups + 2], refs[2 * groups + 2 : 3 * groups + 2]
    held = refs[3 * groups + 2] if groups > 1 else tokens[0]
    dim = wide.shape[0]
    part = wide.shape[1] // 2
    chunk = dim // CHUNKS
    if groups > 1:
        for g, ref in enumerate(tokens):
            held[pl.ds(g * SLOTS, SLOTS)] = ref[...]
    total = jnp.dot(held[:, pl.ds(0, dim)], wide[...], preferred_element_type=f32)
    gate, upward = total[:, :part], total[:, part:]
    act = (gate / (1.0 + jnp.exp(-gate)) * upward).astype(bf16)
    shape = (EXTRA, EXTRA)
    expert = FAR * where_ref[0] + where_ref[1]
    from_share = iota(shape, 0) - CAP * EXPERTS
    hot = (from_share >= 0) & (from_share < 3 * EXPERTS) & (lax.rem(from_share + EXTRA, EXPERTS) == expert)
    share = jnp.dot(held[:, pl.ds(dim, EXTRA)], one_hot(hot), preferred_element_type=f32)[:, :1]
    for k in range(CHUNKS):
        cols = pl.ds(k * chunk, chunk)
        got = jnp.dot(act, deep[:, cols], preferred_element_type=f32) * share
        for g in range(groups):
            rows = got[g * SLOTS : (g + 1) * SLOTS].astype(bf16)
            early[g][:, cols] = rows[:EARLY]
            late[g][:, cols] = rows[EARLY:]


def expert_part(where, tokens, weights):
    wide, deep = weights
    dim = wide.shape[0]
    groups = len(tokens)
    rows = groups * SLOTS
    held = [pltpu.VMEM((rows, dim + EXTRA), bf16)] if groups > 1 else []
    return pl.pallas_call(
        functools.partial(expert_kernel, groups),
        out_shape=(jax.ShapeDtypeStruct((EARLY, dim), bf16),) * groups
        + (jax.ShapeDtypeStruct((LATE, dim), bf16),) * groups,
        in_specs=[smem()] + [vmem()] * (groups + 2),
        out_specs=[vmem()] * (2 * groups),
        scratch_shapes=held,
        compiler_params=params(8),
        cost_estimate=cost(6 * rows * wide.size, 2 * rows * dim),
        name="expert_part",
    )(where, *tokens, held_in_vmem(wide), held_in_vmem(deep))


def collect_kernel(count, spread, *refs):
    parts, (right, left, ahead, behind) = refs[:count], refs[count:]
    size = right.shape[0]
    tiles = right.shape[1] // TILE
    for n in range(tiles):
        cols = pl.ds(n * TILE, TILE)
        rows = spread[...]
        first = n < tiles // 2
        rows = rows[: 3 * size] if first else jnp.concatenate([rows[: 2 * size], rows[3 * size :]], axis=0)
        got = jnp.dot(rows, tiles_of(parts, 0, n), preferred_element_type=f32).astype(bf16)
        right[:, cols] = got[:size]
        left[:, cols] = got[size : 2 * size]
        last, at = (ahead, n * TILE) if first else (behind, (n - tiles // 2) * TILE)
        last[:, pl.ds(at, TILE)] = got[2 * size :]


def collect(spread, parts):
    width = parts[0].shape[1] // HALVES
    count = len(parts)
    return pl.pallas_call(
        functools.partial(collect_kernel, count),
        out_shape=row_shapes(spread.shape[0] // (len(STEPS) - 1), width)[1:],
        in_specs=[vmem()] * (count + 1),
        out_specs=[vmem()] * 4,
        compiler_params=params(12),
        cost_estimate=cost(2 * spread.size * width, 4 * spread.shape[0] * width),
        name="collect",
    )(spread, *parts)


def merge_kernel(count, *refs):
    mine, (right, left, ahead, behind, first), rest = refs[:count], refs[count : count + 5], refs[count + 5 :]
    block = first.shape[0]
    tiles = first.shape[1] // TILE
    for n in range(tiles):
        cols = pl.ds(n * TILE, TILE)
        if count == 1:
            total = mine[0][:, cols]
        else:
            total = jnp.dot(mine[0][...], tiles_of(mine[1:], 0, n), preferred_element_type=f32)
        last, at = (ahead, n * TILE) if n < tiles // 2 else (behind, (n - tiles // 2) * TILE)
        total = total + right[:, cols].astype(f32) + left[:, cols].astype(f32)
        total = total + last[:, pl.ds(at, TILE)].astype(f32)
        first[:, cols] = total[:block]
        for k, out in enumerate(rest):
            out[:, cols] = total[(k + 1) * block : (k + 2) * block].astype(bf16)


def merge(mine, others):
    size, width = others[0].shape
    block = (size // FAR, width)
    return pl.pallas_call(
        functools.partial(merge_kernel, len(mine)),
        out_shape=(jax.ShapeDtypeStruct(block, f32),) + (jax.ShapeDtypeStruct(block, bf16),) * (FAR - 1),
        in_specs=[vmem()] * (len(mine) + 4),
        out_specs=[vmem()] * FAR,
        compiler_params=params(4),
        cost_estimate=cost(4 * size * width, 12 * size * width),
        name="merge",
    )(*mine, *others)


def half_swap(a):
    middle = a.shape[0] // 2
    return jnp.concatenate([a[middle:], a[:middle]], axis=0)


def settle_kernel(first, one, two, three, mine, give):
    total = first[...] + one[...].astype(f32) + two[...].astype(f32) + three[...].astype(f32)
    mine[...] = total[: mine.shape[0]]
    give[...] = total[mine.shape[0] :].astype(bf16)


def settle(added):
    count, width = added[0].shape
    shape = (count // PAIR, width)
    return pl.pallas_call(
        settle_kernel,
        out_shape=(jax.ShapeDtypeStruct(shape, f32), jax.ShapeDtypeStruct(shape, bf16)),
        in_specs=[vmem()] * 4,
        out_specs=[vmem()] * 2,
        compiler_params=params(4),
        cost_estimate=cost(4 * count * width, 14 * count * width),
        name="settle",
    )(*added)


def route_kernel(where_ref, mine, got, rows, gain, router, ids, slots, hidden, payload):
    count, half = rows.shape
    here = iota((count, 1), 0) // (count // HALVES) == lax.rem(where_ref[0], PAIR)
    both = [jnp.concatenate([part[...].astype(f32)] * HALVES, axis=0) for part in (mine, got)]
    total = rows[...].astype(f32) + jnp.where(here, *both)
    hidden[...] = total
    square = jnp.sum(total * total, axis=1, keepdims=True)
    scale = lax.rsqrt((square + half_swap(square)) / D + norm_eps)
    normed = (total * scale * gain[...]).astype(bf16)
    payload[:, pl.ds(0, half)] = normed
    parts = [
        lax.dot_general(normed, router[:, pl.ds(c * half, half)], NT, preferred_element_type=f32)
        for c in range(HALVES)
    ]
    logits = jnp.where(iota(parts[0].shape, 0) < count // 2, parts[0], parts[1])
    logits = logits + half_swap(logits)
    logits = jnp.concatenate([logits] * (EXTRA // EXPERTS), axis=1)
    lane = iota(logits.shape, 1)
    place = jnp.zeros(logits.shape, jnp.int32)
    for k in range(TOP):
        place = jnp.where(lax.rem(lane, EXPERTS) == ids[:, k : k + 1], slots[:, k : k + 1] + 1, place)
    gates = jnp.where(place > 0, 1.0 / (1.0 + jnp.exp(-logits)), 0.0)
    share = route_scale * gates / jnp.sum(jnp.where(lane < EXPERTS, gates, 0.0), axis=1, keepdims=True)
    kind = lane // EXPERTS
    table = jnp.zeros(logits.shape, f32)
    for n in range(CAP):
        table = jnp.where((kind == n) & (place == n + 1), 1.0, table)
    rest = share
    for n in range(3):
        piece = rest.astype(bf16).astype(f32)
        table = jnp.where(kind == CAP + n, piece, table)
        rest = rest - piece
    payload[:, pl.ds(half, EXTRA)] = table.astype(bf16)


def route(where, mine, got, rows, gain, router, ids, slots):
    count, half = rows.shape
    return pl.pallas_call(
        route_kernel,
        out_shape=(
            jax.ShapeDtypeStruct((count, half), f32),
            jax.ShapeDtypeStruct((count, half + EXTRA), bf16),
        ),
        in_specs=[smem()] + [vmem()] * 7,
        out_specs=[vmem()] * 2,
        compiler_params=params(4),
        cost_estimate=cost(4 * count * half * EXPERTS, 20 * count * half),
        name="route",
    )(where, mine, got, rows, gain, router, ids, slots)


def finish_kernel(hidden, first, one, two, three, out):
    seqs, steps, _ = out.shape
    half = hidden.shape[1]
    total = first[...] + one[...].astype(f32) + two[...].astype(f32) + three[...].astype(f32)
    total = (hidden[...] + total).astype(bf16)
    for c in range(HALVES):
        for b in range(seqs):
            at = (c * seqs + b) * steps
            out[b, :, pl.ds(c * half, half)] = total[at : at + steps]


def finish(hidden, added, shape):
    return pl.pallas_call(
        finish_kernel,
        out_shape=jax.ShapeDtypeStruct(shape, bf16),
        in_specs=[vmem()] * 5,
        out_specs=vmem(),
        compiler_params=params(4),
        cost_estimate=cost(5 * hidden.size, 14 * hidden.size),
        name="finish",
    )(hidden, *added)


def reduce_z(mine, right, left, ahead, behind):
    others = shift_z(right, 1), shift_z(left, -1), shift_z(ahead, 2), shift_z(behind, -2)
    first, *sent = merge(mine, others)
    others = [swap_far(rows, k + 1) for k, rows in enumerate(sent)]
    return first, *others


def layer(
    cache_kv,
    new_kv,
    queries,
    lengths,
    resid,
    value_up,
    out_proj,
    norm_gain,
    router,
    expert_ids,
    slots,
    w_gate,
    w_up,
    w_down,
):
    nx = lax.axis_size("x")
    seqs, steps = queries.shape[:2]
    tok = seqs * steps
    where = jnp.stack([lax.axis_index(a) for a in ("x", "zb", "j")]).astype(jnp.int32)
    where = jnp.concatenate([where, lengths.astype(jnp.int32)])

    tops, lows, give = pack(where, value_up.T, out_proj)
    left, right = swap_x(give, 1), swap_x(give, 3)
    outgoing = context_rows(where, nx, cache_kv, new_kv, queries)
    arrived = lax.all_to_all(
        outgoing.reshape(RING, nx * tok, LAT), ZAX, split_axis=0, concat_axis=0, tiled=True
    )
    top_half, low_half = swap_x(tops, 1), swap_x(lows, 3)
    top_far, low_far = swap_x(top_half, 3), swap_x(low_half, 1)
    pieces = [tops, lows, swap_core(tops), swap_core(lows)]
    for rows in (left, right):
        pieces += [rows, swap_core(rows)]
    pieces += [top_far, low_far, swap_core(top_far), swap_core(low_far)]
    others = [swap_core(w) for w in (w_gate, w_up, w_down)]
    weights = stage((w_gate, others[0], w_up, others[1], w_down, others[2]))
    values = values_of(nx, arrived.reshape(RING * nx * tok, LAT), pieces, tok)
    own, *rows = attend(where, values, swap_x(values, 1), pieces, tok)
    mine, give = settle(reduce_z((own,), *rows))
    other = swap_x(give, 1)

    half = D // HALVES
    rows = resid.reshape(tok, HALVES, half).swapaxes(0, 1).reshape(HALVES * tok, half)
    gain = jnp.repeat(norm_gain.astype(f32).reshape(HALVES, half), tok, axis=0)
    ids, places = [
        jnp.tile(a.reshape(tok, TOP).astype(jnp.int32), (HALVES, 1)) for a in (expert_ids, slots)
    ]
    hidden, payload = route(where, mine, other, rows, gain, router.T, ids, places)

    ring = lax.all_gather(payload, ZAX, axis=0, tiled=True)
    *sent, early, late = dispatch(where, nx, ring, tok)
    got = [swap_x(sent[i], COLUMNS[i]) for i in range(1, nx)]
    done = expert_part(where, (sent[0], *got[: nx - 2]), weights)
    done = [list(done[: nx - 1]), list(done[nx - 1 :])]
    for rows, last in zip(done, expert_part(where, got[nx - 2 :], weights)):
        rows.append(last)
    first = [done[0][0]] + [swap_x(done[0][i], COLUMNS[i]) for i in range(1, nx)]
    second = [done[1][0]] + [swap_x(done[1][i], COLUMNS[i]) for i in range(1, nx)]
    added = reduce_z((late, *second), *collect(early, first))
    return finish(hidden, added, resid.shape)


def solution(mesh):
    chips = mesh.shape["ep"] // (RING * CORES)
    grid = mesh.devices.reshape(mesh.shape["rep"], chips, FAR, NEAR, CORES)
    fine = Mesh(grid, ("rep", "x", "zb", "j", "c"))
    ep = ("x", "zb", "j", "c")
    both = ("rep",) + ep
    return jax.shard_map(
        layer,
        mesh=fine,
        in_specs=(
            P(both, None, None),
            P(both, None, None),
            P(both, None, None, None),
            P(both),
            P(both, None, None),
            P(None, ep),
            P(ep, None),
            P(),
            P(),
            P(both, None, None),
            P(both, None, None),
            P(None, ep),
            P(None, ep),
            P(ep, None),
        ),
        out_specs=P(both, None, None),
        check_vma=False,
    )
```

```python
import functools
import math

import jax
import jax.numpy as jnp
from jax import lax
from jax.experimental import pallas as pl
from jax.experimental.pallas import tpu as pltpu
from jax.sharding import Mesh
from jax.sharding import PartitionSpec as P


D = 7168
LAT = 512
EXPERTS = 16
TOP = 8
CAP = 2
QK = 192

CORES = 2
NEAR = 4
FAR = 4
RING = NEAR * FAR
SLOTS = RING * CAP
LATE = FAR * CAP
EARLY = SLOTS - LATE
EXTRA = 128

route_scale = 2.827
norm_eps = 1e-06


ZAX = ("zb", "j")
f32, bf16 = jnp.float32, jnp.bfloat16
NT = (((1,), (1,)), ((), ()))


def swap_x(a, bits):
    return lax.ppermute(a, "x", [(i, i ^ bits) for i in range(lax.axis_size("x"))])


def swap_x_by_group(a, even, odd):
    nx = lax.axis_size("x")
    bits = [odd if g % 2 and paired() else even for g in range(lax.axis_size("rep"))]
    return lax.ppermute(a, ("rep", "x"), [(g * nx + i, g * nx + (i ^ b)) for g, b in enumerate(bits) for i in range(nx)])


def paired():
    return lax.axis_size("rep") % 2 == 0


def swap_group(a):
    return lax.ppermute(a, "rep", [(i, i ^ 1) for i in range(lax.axis_size("rep"))])


def shift_z(a, step):
    return lax.ppermute(a, ZAX, [(i, (i + step) % RING) for i in range(RING)])


def swap_far(a, bits):
    return lax.ppermute(a, "zb", [(i, i ^ bits) for i in range(FAR)])


def swap_core(a):
    return lax.ppermute(a, "c", [(i, i ^ 1) for i in range(CORES)])


def iota(shape, axis):
    return lax.broadcasted_iota(jnp.int32, shape, axis)


def one_hot(mask):
    return jnp.where(mask, 1.0, 0.0).astype(bf16)


COLUMNS = (0, 1, 3, 2)


def column(index, x):
    return x ^ jnp.where(index == 2, 3, jnp.where(index == 3, 2, index))


STEPS = (0, 1, RING - 1, 2, RING - 2)


def chip_at(place, where_ref):
    group, bits = place // FAR, lax.rem(place, FAR)
    step = 0
    for i, value in enumerate(STEPS):
        step = jnp.where(group == i, value, step)
    chip = lax.rem(NEAR * where_ref[1] + where_ref[2] + step, RING)
    return NEAR * ((chip // NEAR) ^ bits) + lax.rem(chip, NEAR)


def of_tile(rows, n, tiles):
    size = rows.shape[0] // len(STEPS)
    if n < tiles // 2:
        return rows[: 4 * size]
    return jnp.concatenate([rows[: 3 * size], rows[4 * size :]], axis=0)


def smem():
    return pl.BlockSpec(memory_space=pltpu.SMEM)


def vmem():
    return pl.BlockSpec(memory_space=pltpu.VMEM)


def hbm():
    return pl.BlockSpec(memory_space=pltpu.HBM)


def held_in_hbm(a):
    return pltpu.with_memory_space_constraint(a, pltpu.HBM)


def held_in_vmem(a):
    return pltpu.with_memory_space_constraint(a, pltpu.VMEM)


def params(mib):
    return pltpu.CompilerParams(vmem_limit_bytes=mib << 20)


def cost(flops, nbytes):
    return pl.CostEstimate(flops=flops, bytes_accessed=nbytes, transcendentals=0)


def context_kernel(nx, where_ref, keys, queries, new, out, held):
    seq = pl.program_id(0)
    seqs = pl.num_programs(0)
    steps, heads = queries.shape[1], queries.shape[2]
    count = steps * heads
    scale = 1.0 / math.sqrt(QK)
    query = queries[0].reshape(count, queries.shape[3])
    score = jnp.dot(query, keys[0], preferred_element_type=f32) * scale
    score = jnp.where(iota(score.shape, 1) < where_ref[3 + seq], score, -jnp.inf)
    wide = query.astype(f32)
    step_of = iota((count, 1), 0) // heads
    latest = []
    peak = jnp.max(score, axis=1, keepdims=True)
    for t in range(steps):
        key = new[0, t : t + 1, :].astype(f32)
        got = jnp.sum(wide * key, axis=1, keepdims=True) * scale
        got = jnp.where(step_of >= t, got, -jnp.inf)
        latest.append(got)
        peak = jnp.maximum(peak, got)
    probs = jnp.exp(score - peak)
    total = jnp.sum(probs, axis=1, keepdims=True)
    latest = [jnp.exp(got - peak) for got in latest]
    for got in latest:
        total = total + got
    share = 1.0 / total
    probs = (probs * share).astype(bf16)
    context = lax.dot_general(probs, keys[0, :LAT, :], NT, preferred_element_type=f32)
    for t, got in enumerate(latest):
        part = (got * share).astype(bf16).astype(f32)
        context = context + part * new[0, t : t + 1, :LAT].astype(f32)
    held[pl.ds(pl.multiple_of(seq * count, count), count), :] = context.astype(bf16)

    @pl.when(seq == seqs - 1)
    def _():
        rows = held.shape[0]
        tok = rows // heads
        shape = (rows, rows)
        to, source = iota(shape, 0), iota(shape, 1)
        hop = lax.rem(to // tok, nx)
        head = column(hop, where_ref[0]) * RING + to // (tok * nx)
        take = (lax.rem(to, tok) == source // heads) & (head == lax.rem(source, heads))
        out[...] = jnp.dot(one_hot(take), held[...], preferred_element_type=f32).astype(bf16)


def context_rows(where, nx, cache_kv, new_kv, queries):
    seqs, length, width = cache_kv.shape
    steps, heads = queries.shape[1:3]
    rows = seqs * steps * heads
    keys = jnp.swapaxes(cache_kv, 1, 2)
    return pl.pallas_call(
        functools.partial(context_kernel, nx),
        grid=(seqs,),
        out_shape=jax.ShapeDtypeStruct((rows, LAT), bf16),
        in_specs=[
            smem(),
            pl.BlockSpec((1, width, length), lambda b: (b, 0, 0)),
            pl.BlockSpec((1, steps, heads, width), lambda b: (b, 0, 0, 0)),
            pl.BlockSpec((1, steps, width), lambda b: (b, 0, 0)),
        ],
        out_specs=pl.BlockSpec((rows, LAT), lambda b: (0, 0)),
        scratch_shapes=[pltpu.VMEM((rows, LAT), bf16)],
        compiler_params=params(24),
        cost_estimate=cost(2 * rows * length * (width + LAT), 2 * cache_kv.size),
        name="context_rows",
    )(where, held_in_hbm(keys), held_in_hbm(queries), held_in_hbm(new_kv))


def pack_kernel(up, rows, tops, lows, sem):
    half, at = tops.shape[0], up.shape[1]
    copies = []
    for i, out in enumerate((tops, lows)):
        part = pl.ds(i * half, half)
        copies.append(pltpu.make_async_copy(rows.at[part], out.at[:, pl.ds(at, rows.shape[1])], sem.at[i, 0]))
        copies.append(pltpu.make_async_copy(up.at[part], out.at[:, pl.ds(0, at)], sem.at[i, 1]))
    for copy in copies:
        copy.start()
    for copy in copies:
        copy.wait()


def pack(up, rows):
    shape = (rows.shape[0] // 2, up.shape[1] + rows.shape[1])
    return pl.pallas_call(
        pack_kernel,
        out_shape=(jax.ShapeDtypeStruct(shape, bf16),) * 2,
        in_specs=[hbm()] * 2,
        out_specs=[vmem()] * 2,
        scratch_shapes=[pltpu.SemaphoreType.DMA((2, 2))],
        compiler_params=params(12),
        cost_estimate=cost(1, 4 * rows.size),
        name="pack",
    )(held_in_hbm(up), held_in_hbm(rows))


HALVES = 2
TILE = 256


def put_rows(got, outs, n):
    own, right, left, ahead, behind = outs
    size, width = own.shape[0], ahead.shape[1]
    cols = pl.ds(n * TILE, TILE)
    own[:, cols] = got[:size]
    right[:, cols] = got[size : 2 * size].astype(bf16)
    left[:, cols] = got[2 * size : 3 * size].astype(bf16)
    last, at = (ahead, n * TILE) if n * TILE < width else (behind, n * TILE - width)
    last[:, pl.ds(at, TILE)] = got[3 * size :].astype(bf16)


def row_shapes(size, width):
    return (
        jax.ShapeDtypeStruct((size, width), f32),
        jax.ShapeDtypeStruct((size, width), bf16),
        jax.ShapeDtypeStruct((size, width), bf16),
        jax.ShapeDtypeStruct((size, width // 2), bf16),
        jax.ShapeDtypeStruct((size, width // 2), bf16),
    )


def tiles_of(parts, at, n):
    half = (parts[0].shape[1] - at) // HALVES
    got = [p[:, pl.ds(at + c * half + n * TILE, TILE)] for c in range(HALVES) for p in parts]
    return jnp.concatenate(got, axis=0)


def attend_kernel(tok, nx, count, hops, last, where_ref, arrived, *refs):
    pieces, outs = refs[:count], refs[count:]
    if last:
        before, outs = outs[0], outs[1:]
    up = jnp.concatenate([piece[:, pl.ds(0, LAT)] for piece in pieces], axis=0)
    values = lax.dot_general(arrived[...], up, NT, preferred_element_type=f32)
    hop = lax.rem(iota(values.shape, 0) // tok, nx)
    odd = where_ref[where_ref.shape[0] - 1]
    part = iota(values.shape, 1) // (up.shape[0] // len(hops))
    wanted = 0
    for i, (at, step) in enumerate(hops):
        wanted = jnp.where(part == i, at + step * odd, wanted)
    values = jnp.where(hop == wanted, values, 0.0).astype(bf16)
    shape = (len(STEPS) * FAR * HALVES * tok, arrived.shape[0])
    row, source = iota(shape, 0), iota(shape, 1)
    chip = chip_at(row // (HALVES * tok), where_ref)
    take = (source // (tok * nx) == chip) & (lax.rem(source, tok) == lax.rem(row, tok))
    half = lax.rem(row // tok, HALVES)
    taken = [
        jnp.dot(one_hot(take & (half == c)), values, preferred_element_type=f32).astype(bf16)
        for c in range(HALVES)
    ]
    values = jnp.concatenate(taken, axis=1)
    tiles = outs[0].shape[1] // TILE
    for n in range(tiles):
        got = jnp.dot(of_tile(values, n, tiles), tiles_of(pieces, LAT, n), preferred_element_type=f32)
        cols = pl.ds(n * TILE, TILE)
        if last:
            put_rows(before[:, cols] + got, outs, n)
        else:
            outs[0][:, cols] = got


def attend_part(where, nx, arrived, pieces, tok, hops, before):
    depth = sum(p.shape[0] for p in pieces)
    width = (pieces[0].shape[1] - LAT) // HALVES
    count = len(pieces)
    last = before is not None
    part = jax.ShapeDtypeStruct((RING * HALVES * tok, width), f32)
    return pl.pallas_call(
        functools.partial(attend_kernel, tok, nx, count, hops, last),
        out_shape=row_shapes(FAR * HALVES * tok, width) if last else part,
        in_specs=[smem(), vmem()] + [vmem()] * count + [vmem()] * last,
        out_specs=[vmem()] * 5 if last else vmem(),
        compiler_params=params(6),
        cost_estimate=cost(8 * RING * tok * depth * width * HALVES, 4 * depth * width),
        name="attend_part",
    )(where, arrived, *pieces, *([before] if last else []))


SEND_TILE = 512


def dispatch_kernel(tok, nx, where_ref, tokens, *refs):
    outs, (early, late) = refs[:nx], refs[nx:]
    count, width = tokens.shape
    half = width - EXTRA
    table = tokens[:, pl.ds(half, EXTRA)]
    shape = (nx * CAP, EXTRA)
    row, place = iota(shape, 0), iota(shape, 1)
    expert = FAR * column(row // CAP, where_ref[0]) + where_ref[1]
    hot = one_hot(place == lax.rem(row, CAP) * EXPERTS + expert)
    got = lax.dot_general(hot, table, NT, preferred_element_type=f32)
    shape = (SLOTS, count)
    slot, token = iota(shape, 0), iota(shape, 1)
    source = slot // CAP
    chip = NEAR * lax.rem(source, FAR) + lax.rem(where_ref[2] + source // FAR + 1, NEAR)
    parts = []
    for r in range(nx):
        sel = jnp.where(lax.rem(slot, CAP) == 0, got[CAP * r : CAP * r + 1], got[CAP * r + 1 : CAP * r + 2])
        parts.append(jnp.where(chip == token // (HALVES * tok), sel, 0.0))
    of_half = lax.rem(token // tok, HALVES)
    halves = [[jnp.where(of_half == c, sel, 0.0) for sel in parts] for c in range(HALVES)]
    both = jnp.concatenate(sum(halves, []), axis=0).astype(bf16)
    rows = nx * SLOTS
    for n in range(half // SEND_TILE):
        got = jnp.dot(both, tokens[:, pl.ds(n * SEND_TILE, SEND_TILE)], preferred_element_type=f32).astype(bf16)
        for c in range(HALVES):
            for r in range(nx):
                at = c * rows + r * SLOTS
                outs[r][:, pl.ds(c * half + n * SEND_TILE, SEND_TILE)] = got[at : at + SLOTS]
    got = jnp.dot(both[:rows], table, preferred_element_type=f32).astype(bf16)
    for r in range(nx):
        outs[r][:, pl.ds(HALVES * half, EXTRA)] = got[r * SLOTS : (r + 1) * SLOTS]
    for out, group, at, end in ((early, 1, 0, EARLY), (late, 0, EARLY, SLOTS)):
        shape = (out.shape[0], count)
        row, token = iota(shape, 0), iota(shape, 1)
        chip = chip_at(group * FAR + row // (HALVES * tok), where_ref)
        take = (token // (HALVES * tok) == chip) & (lax.rem(token, HALVES * tok) == lax.rem(row, HALVES * tok))
        sel = jnp.concatenate([sel[at:end] for sels in halves for sel in sels], axis=0).astype(bf16)
        out[...] = lax.dot_general(one_hot(take), sel, NT, preferred_element_type=f32).astype(bf16)


def dispatch(where, nx, tokens, tok):
    count, width = tokens.shape
    full = HALVES * (width - EXTRA) + EXTRA
    near = count // NEAR
    return pl.pallas_call(
        functools.partial(dispatch_kernel, tok, nx),
        out_shape=(jax.ShapeDtypeStruct((SLOTS, full), bf16),) * nx
        + (
            jax.ShapeDtypeStruct(((len(STEPS) - 1) * near, HALVES * nx * EARLY), bf16),
            jax.ShapeDtypeStruct((near, HALVES * nx * LATE), bf16),
        ),
        in_specs=[smem(), vmem()],
        out_specs=[vmem()] * (nx + 2),
        compiler_params=params(12),
        cost_estimate=cost(2 * nx * SLOTS * count * full, 4 * count * width),
        name="dispatch",
    )(where, tokens)


CHUNKS = 7


def stage_kernel(gate_a, gate_b, up_a, up_b, down_a, down_b, wide, deep, sem):
    part = gate_a.shape[1]
    copies = [
        pltpu.make_async_copy(ref, wide.at[:, pl.ds(i * part, part)], sem.at[i])
        for i, ref in enumerate((gate_a, gate_b, up_a, up_b))
    ]
    copies += [
        pltpu.make_async_copy(ref, deep.at[pl.ds(i * part, part)], sem.at[4 + i])
        for i, ref in enumerate((down_a, down_b))
    ]
    for copy in copies:
        copy.start()
    for copy in copies:
        copy.wait()


def stage(weights):
    dim, part = weights[0].shape
    return pl.pallas_call(
        stage_kernel,
        out_shape=(
            jax.ShapeDtypeStruct((dim, 4 * part), bf16),
            jax.ShapeDtypeStruct((2 * part, dim), bf16),
        ),
        in_specs=[hbm()] * 6,
        out_specs=[vmem()] * 2,
        scratch_shapes=[pltpu.SemaphoreType.DMA((6,))],
        compiler_params=params(4),
        cost_estimate=cost(4 * 1000 * dim * part, 12 * dim * part),
        name="stage",
    )(*[held_in_hbm(w) for w in weights])


def expert_kernel(groups, where_ref, *refs):
    tokens = refs[:groups]
    wide, deep = refs[groups : groups + 2]
    early, late = refs[groups + 2 : 2 * groups + 2], refs[2 * groups + 2 : 3 * groups + 2]
    held = refs[3 * groups + 2] if groups > 1 else tokens[0]
    dim = wide.shape[0]
    part = wide.shape[1] // 2
    chunk = dim // CHUNKS
    if groups > 1:
        for g, ref in enumerate(tokens):
            held[pl.ds(g * SLOTS, SLOTS)] = ref[...]
    total = jnp.dot(held[:, pl.ds(0, dim)], wide[...], preferred_element_type=f32)
    gate, upward = total[:, :part], total[:, part:]
    act = (gate / (1.0 + jnp.exp(-gate)) * upward).astype(bf16)
    shape = (EXTRA, EXTRA)
    expert = FAR * where_ref[0] + where_ref[1]
    from_share = iota(shape, 0) - CAP * EXPERTS
    hot = (from_share >= 0) & (from_share < 3 * EXPERTS) & (lax.rem(from_share + EXTRA, EXPERTS) == expert)
    share = jnp.dot(held[:, pl.ds(dim, EXTRA)], one_hot(hot), preferred_element_type=f32)[:, :1]
    for k in range(CHUNKS):
        cols = pl.ds(k * chunk, chunk)
        got = jnp.dot(act, deep[:, cols], preferred_element_type=f32) * share
        for g in range(groups):
            rows = got[g * SLOTS : (g + 1) * SLOTS].astype(bf16)
            early[g][:, cols] = rows[:EARLY]
            late[g][:, cols] = rows[EARLY:]


def expert_part(where, tokens, weights):
    wide, deep = weights
    dim = wide.shape[0]
    groups = len(tokens)
    rows = groups * SLOTS
    held = [pltpu.VMEM((rows, dim + EXTRA), bf16)] if groups > 1 else []
    return pl.pallas_call(
        functools.partial(expert_kernel, groups),
        out_shape=(jax.ShapeDtypeStruct((EARLY, dim), bf16),) * groups
        + (jax.ShapeDtypeStruct((LATE, dim), bf16),) * groups,
        in_specs=[smem()] + [vmem()] * (groups + 2),
        out_specs=[vmem()] * (2 * groups),
        scratch_shapes=held,
        compiler_params=params(8),
        cost_estimate=cost(6 * rows * wide.size, 2 * rows * dim),
        name="expert_part",
    )(where, *tokens, held_in_vmem(wide), held_in_vmem(deep))


def collect_kernel(count, spread, *refs):
    parts, (right, left, ahead, behind) = refs[:count], refs[count:]
    size = right.shape[0]
    tiles = right.shape[1] // TILE
    for n in range(tiles):
        cols = pl.ds(n * TILE, TILE)
        rows = spread[...]
        first = n < tiles // 2
        rows = rows[: 3 * size] if first else jnp.concatenate([rows[: 2 * size], rows[3 * size :]], axis=0)
        got = jnp.dot(rows, tiles_of(parts, 0, n), preferred_element_type=f32).astype(bf16)
        right[:, cols] = got[:size]
        left[:, cols] = got[size : 2 * size]
        last, at = (ahead, n * TILE) if first else (behind, (n - tiles // 2) * TILE)
        last[:, pl.ds(at, TILE)] = got[2 * size :]


def collect(spread, parts):
    width = parts[0].shape[1] // HALVES
    count = len(parts)
    return pl.pallas_call(
        functools.partial(collect_kernel, count),
        out_shape=row_shapes(spread.shape[0] // (len(STEPS) - 1), width)[1:],
        in_specs=[vmem()] * (count + 1),
        out_specs=[vmem()] * 4,
        compiler_params=params(12),
        cost_estimate=cost(2 * spread.size * width, 4 * spread.shape[0] * width),
        name="collect",
    )(spread, *parts)


def merge_kernel(count, *refs):
    mine, (right, left, ahead, behind, first), rest = refs[:count], refs[count : count + 5], refs[count + 5 :]
    block = first.shape[0]
    tiles = first.shape[1] // TILE
    for n in range(tiles):
        cols = pl.ds(n * TILE, TILE)
        if count == 1:
            total = mine[0][:, cols]
        else:
            total = jnp.dot(mine[0][...], tiles_of(mine[1:], 0, n), preferred_element_type=f32)
        last, at = (ahead, n * TILE) if n < tiles // 2 else (behind, (n - tiles // 2) * TILE)
        total = total + right[:, cols].astype(f32) + left[:, cols].astype(f32)
        total = total + last[:, pl.ds(at, TILE)].astype(f32)
        first[:, cols] = total[:block]
        for k, out in enumerate(rest):
            out[:, cols] = total[(k + 1) * block : (k + 2) * block].astype(bf16)


def merge(mine, others):
    size, width = others[0].shape
    block = (size // FAR, width)
    return pl.pallas_call(
        functools.partial(merge_kernel, len(mine)),
        out_shape=(jax.ShapeDtypeStruct(block, f32),) + (jax.ShapeDtypeStruct(block, bf16),) * (FAR - 1),
        in_specs=[vmem()] * (len(mine) + 4),
        out_specs=[vmem()] * FAR,
        compiler_params=params(4),
        cost_estimate=cost(4 * size * width, 12 * size * width),
        name="merge",
    )(*mine, *others)


def half_swap(a):
    middle = a.shape[0] // 2
    return jnp.concatenate([a[middle:], a[:middle]], axis=0)


def route_kernel(first, one, two, three, rows, gain, router, ids, slots, hidden, payload):
    count, half = rows.shape
    total = first[...] + one[...].astype(f32) + two[...].astype(f32) + three[...].astype(f32)
    total = rows[...].astype(f32) + total
    hidden[...] = total
    square = jnp.sum(total * total, axis=1, keepdims=True)
    scale = lax.rsqrt((square + half_swap(square)) / D + norm_eps)
    normed = (total * scale * gain[...]).astype(bf16)
    payload[:, pl.ds(0, half)] = normed
    parts = [
        lax.dot_general(normed, router[:, pl.ds(c * half, half)], NT, preferred_element_type=f32)
        for c in range(HALVES)
    ]
    logits = jnp.where(iota(parts[0].shape, 0) < count // 2, parts[0], parts[1])
    logits = logits + half_swap(logits)
    logits = jnp.concatenate([logits] * (EXTRA // EXPERTS), axis=1)
    lane = iota(logits.shape, 1)
    place = jnp.zeros(logits.shape, jnp.int32)
    for k in range(TOP):
        place = jnp.where(lax.rem(lane, EXPERTS) == ids[:, k : k + 1], slots[:, k : k + 1] + 1, place)
    gates = jnp.where(place > 0, 1.0 / (1.0 + jnp.exp(-logits)), 0.0)
    share = route_scale * gates / jnp.sum(jnp.where(lane < EXPERTS, gates, 0.0), axis=1, keepdims=True)
    kind = lane // EXPERTS
    table = jnp.zeros(logits.shape, f32)
    for n in range(CAP):
        table = jnp.where((kind == n) & (place == n + 1), 1.0, table)
    rest = share
    for n in range(3):
        piece = rest.astype(bf16).astype(f32)
        table = jnp.where(kind == CAP + n, piece, table)
        rest = rest - piece
    payload[:, pl.ds(half, EXTRA)] = table.astype(bf16)


def route(added, rows, gain, router, ids, slots):
    count, half = rows.shape
    return pl.pallas_call(
        route_kernel,
        out_shape=(
            jax.ShapeDtypeStruct((count, half), f32),
            jax.ShapeDtypeStruct((count, half + EXTRA), bf16),
        ),
        in_specs=[vmem()] * 9,
        out_specs=[vmem()] * 2,
        compiler_params=params(4),
        cost_estimate=cost(4 * count * half * EXPERTS, 20 * count * half),
        name="route",
    )(*added, rows, gain, router, ids, slots)


def finish_kernel(hidden, first, one, two, three, out):
    seqs, steps, _ = out.shape
    half = hidden.shape[1]
    total = first[...] + one[...].astype(f32) + two[...].astype(f32) + three[...].astype(f32)
    total = (hidden[...] + total).astype(bf16)
    for c in range(HALVES):
        for b in range(seqs):
            at = (c * seqs + b) * steps
            out[b, :, pl.ds(c * half, half)] = total[at : at + steps]


def finish(hidden, added, shape):
    return pl.pallas_call(
        finish_kernel,
        out_shape=jax.ShapeDtypeStruct(shape, bf16),
        in_specs=[vmem()] * 5,
        out_specs=vmem(),
        compiler_params=params(4),
        cost_estimate=cost(5 * hidden.size, 14 * hidden.size),
        name="finish",
    )(hidden, *added)


def reduce_z(mine, right, left, ahead, behind):
    others = shift_z(right, 1), shift_z(left, -1), shift_z(ahead, 2), shift_z(behind, -2)
    first, *sent = merge(mine, others)
    others = [swap_far(rows, k + 1) for k, rows in enumerate(sent)]
    return first, *others


def layer(
    cache_kv,
    new_kv,
    queries,
    lengths,
    resid,
    value_up,
    out_proj,
    norm_gain,
    router,
    expert_ids,
    slots,
    w_gate,
    w_up,
    w_down,
):
    nx = lax.axis_size("x")
    seqs, steps = queries.shape[:2]
    tok = seqs * steps
    where = jnp.stack([lax.axis_index(a) for a in ("x", "zb", "j")]).astype(jnp.int32)
    odd = lax.rem(lax.axis_index("rep"), 2) if paired() else jnp.int32(0)
    where = jnp.concatenate([where, lengths.astype(jnp.int32), odd.astype(jnp.int32).reshape(1)])

    tops, lows = pack(value_up.T, out_proj)
    top_near, low_near = swap_x_by_group(tops, 1, 3), swap_x_by_group(lows, 3, 1)
    outgoing = context_rows(where, nx, cache_kv, new_kv, queries)
    arrived = lax.all_to_all(
        outgoing.reshape(RING, nx * tok, LAT), ZAX, split_axis=0, concat_axis=0, tiled=True
    )
    if paired():
        top_other, low_other = swap_group(top_near), swap_group(low_near)
    else:
        top_other, low_other = swap_x(tops, 3), swap_x(lows, 1)
    top_far, low_far = swap_x_by_group(top_near, 3, 1), swap_x_by_group(low_near, 1, 3)
    near = [top_near, swap_core(top_near), low_near, swap_core(low_near)]
    near += [top_far, low_far, swap_core(top_far), swap_core(low_far)]
    near += [tops, lows, swap_core(tops), swap_core(lows)]
    beyond = [top_other, swap_core(top_other), low_other, swap_core(low_other)]
    others = [swap_core(w) for w in (w_gate, w_up, w_down)]
    weights = stage((w_gate, others[0], w_up, others[1], w_down, others[2]))
    arrived = arrived.reshape(RING * nx * tok, LAT)
    most = attend_part(where, nx, arrived, near, tok, ((1, 1), (2, -1), (3, 0), (3, 0), (0, 0), (0, 0)), None)
    own, *rows = attend_part(where, nx, arrived, beyond, tok, ((2, -1), (1, 1)), most)
    added = reduce_z((own,), *rows)

    half = D // HALVES
    rows = resid.reshape(tok, HALVES, half).swapaxes(0, 1).reshape(HALVES * tok, half)
    gain = jnp.repeat(norm_gain.astype(f32).reshape(HALVES, half), tok, axis=0)
    ids, places = [
        jnp.tile(a.reshape(tok, TOP).astype(jnp.int32), (HALVES, 1)) for a in (expert_ids, slots)
    ]
    hidden, payload = route(added, rows, gain, router.T, ids, places)

    ring = lax.all_gather(payload, ZAX, axis=0, tiled=True)
    *sent, early, late = dispatch(where, nx, ring, tok)
    got = [swap_x(sent[i], COLUMNS[i]) for i in range(1, nx)]
    done = expert_part(where, (sent[0], *got[: nx - 2]), weights)
    done = [list(done[: nx - 1]), list(done[nx - 1 :])]
    for rows, last in zip(done, expert_part(where, got[nx - 2 :], weights)):
        rows.append(last)
    first = [done[0][0]] + [swap_x(done[0][i], COLUMNS[i]) for i in range(1, nx)]
    second = [done[1][0]] + [swap_x(done[1][i], COLUMNS[i]) for i in range(1, nx)]
    added = reduce_z((late, *second), *collect(early, first))
    return finish(hidden, added, resid.shape)


def solution(mesh):
    chips = mesh.shape["ep"] // (RING * CORES)
    grid = mesh.devices.reshape(mesh.shape["rep"], chips, FAR, NEAR, CORES)
    fine = Mesh(grid, ("rep", "x", "zb", "j", "c"))
    ep = ("x", "zb", "j", "c")
    both = ("rep",) + ep
    return jax.shard_map(
        layer,
        mesh=fine,
        in_specs=(
            P(both, None, None),
            P(both, None, None),
            P(both, None, None, None),
            P(both),
            P(both, None, None),
            P(None, ep),
            P(ep, None),
            P(),
            P(),
            P(both, None, None),
            P(both, None, None),
            P(None, ep),
            P(None, ep),
            P(ep, None),
        ),
        out_specs=P(both, None, None),
        check_vma=False,
    )
```

```python
import functools
import math

import jax
import jax.numpy as jnp
from jax import lax
from jax.experimental import pallas as pl
from jax.experimental.pallas import tpu as pltpu
from jax.sharding import Mesh
from jax.sharding import PartitionSpec as P


D = 7168
LAT = 512
VH = 128
EXPERTS = 16
TOP = 8
CAP = 2
QK = 192

CORES = 2
NEAR = 4
FAR = 4
RING = NEAR * FAR
SLOTS = RING * CAP
LATE = FAR * CAP
EARLY = SLOTS - LATE
EXTRA = 128

route_scale = 2.827
norm_eps = 1e-06


ZAX = ("zb", "j")
f32, bf16 = jnp.float32, jnp.bfloat16
NT = (((1,), (1,)), ((), ()))


def swap_x(a, bits):
    return lax.ppermute(a, "x", [(i, i ^ bits) for i in range(lax.axis_size("x"))])


def shift_z(a, step):
    return lax.ppermute(a, ZAX, [(i, (i + step) % RING) for i in range(RING)])


def swap_far(a, bits):
    return lax.ppermute(a, "zb", [(i, i ^ bits) for i in range(FAR)])


def swap_core(a):
    return lax.ppermute(a, "c", [(i, i ^ 1) for i in range(CORES)])


def iota(shape, axis):
    return lax.broadcasted_iota(jnp.int32, shape, axis)


def one_hot(mask):
    return jnp.where(mask, 1.0, 0.0).astype(bf16)


COLUMNS = (0, 1, 3, 2)


def column(index, x):
    return x ^ jnp.where(index == 2, 3, jnp.where(index == 3, 2, index))


STEPS = (0, 1, RING - 1, 2, RING - 2)


def chip_at(place, where_ref):
    group, bits = place // FAR, lax.rem(place, FAR)
    step = 0
    for i, value in enumerate(STEPS):
        step = jnp.where(group == i, value, step)
    chip = lax.rem(NEAR * where_ref[1] + where_ref[2] + step, RING)
    return NEAR * ((chip // NEAR) ^ bits) + lax.rem(chip, NEAR)


def of_tile(rows, n, tiles):
    size = rows.shape[0] // len(STEPS)
    if n < tiles // 2:
        return rows[: 4 * size]
    return jnp.concatenate([rows[: 3 * size], rows[4 * size :]], axis=0)


def smem():
    return pl.BlockSpec(memory_space=pltpu.SMEM)


def vmem():
    return pl.BlockSpec(memory_space=pltpu.VMEM)


def hbm():
    return pl.BlockSpec(memory_space=pltpu.HBM)


def held_in_hbm(a):
    return pltpu.with_memory_space_constraint(a, pltpu.HBM)


def held_in_vmem(a):
    return pltpu.with_memory_space_constraint(a, pltpu.VMEM)


def params(mib):
    return pltpu.CompilerParams(vmem_limit_bytes=mib << 20)


def cost(flops, nbytes):
    return pl.CostEstimate(flops=flops, bytes_accessed=nbytes, transcendentals=0)


def context_kernel(nx, where_ref, keys, queries, new, out, held):
    seq = pl.program_id(0)
    seqs = pl.num_programs(0)
    steps, heads = queries.shape[1], queries.shape[2]
    count = steps * heads
    scale = 1.0 / math.sqrt(QK)
    query = queries[0].reshape(count, queries.shape[3])
    score = jnp.dot(query, keys[0], preferred_element_type=f32) * scale
    score = jnp.where(iota(score.shape, 1) < where_ref[3 + seq], score, -jnp.inf)
    wide = query.astype(f32)
    step_of = iota((count, 1), 0) // heads
    latest = []
    peak = jnp.max(score, axis=1, keepdims=True)
    for t in range(steps):
        key = new[0, t : t + 1, :].astype(f32)
        got = jnp.sum(wide * key, axis=1, keepdims=True) * scale
        got = jnp.where(step_of >= t, got, -jnp.inf)
        latest.append(got)
        peak = jnp.maximum(peak, got)
    probs = jnp.exp(score - peak)
    total = jnp.sum(probs, axis=1, keepdims=True)
    latest = [jnp.exp(got - peak) for got in latest]
    for got in latest:
        total = total + got
    share = 1.0 / total
    probs = (probs * share).astype(bf16)
    context = lax.dot_general(probs, keys[0, :LAT, :], NT, preferred_element_type=f32)
    for t, got in enumerate(latest):
        part = (got * share).astype(bf16).astype(f32)
        context = context + part * new[0, t : t + 1, :LAT].astype(f32)
    held[pl.ds(pl.multiple_of(seq * count, count), count), :] = context.astype(bf16)

    @pl.when(seq == seqs - 1)
    def _():
        rows = held.shape[0]
        tok = rows // heads
        shape = (rows, rows)
        to, source = iota(shape, 0), iota(shape, 1)
        hop = lax.rem(to // tok, nx)
        head = column(hop, where_ref[0]) * RING + to // (tok * nx)
        take = (lax.rem(to, tok) == source // heads) & (head == lax.rem(source, heads))
        out[...] = jnp.dot(one_hot(take), held[...], preferred_element_type=f32).astype(bf16)


def context_rows(where, nx, cache_kv, new_kv, queries):
    seqs, length, width = cache_kv.shape
    steps, heads = queries.shape[1:3]
    rows = seqs * steps * heads
    keys = jnp.swapaxes(cache_kv, 1, 2)
    return pl.pallas_call(
        functools.partial(context_kernel, nx),
        grid=(seqs,),
        out_shape=jax.ShapeDtypeStruct((rows, LAT), bf16),
        in_specs=[
            smem(),
            pl.BlockSpec((1, width, length), lambda b: (b, 0, 0)),
            pl.BlockSpec((1, steps, heads, width), lambda b: (b, 0, 0, 0)),
            pl.BlockSpec((1, steps, width), lambda b: (b, 0, 0)),
        ],
        out_specs=pl.BlockSpec((rows, LAT), lambda b: (0, 0)),
        scratch_shapes=[pltpu.VMEM((rows, LAT), bf16)],
        compiler_params=params(24),
        cost_estimate=cost(2 * rows * length * (width + LAT), 2 * cache_kv.size),
        name="context_rows",
    )(where, held_in_hbm(keys), held_in_hbm(queries), held_in_hbm(new_kv))


def pack_kernel(up, rows, tops, lows, sem):
    half, at = tops.shape[0], up.shape[1]
    copies = []
    for i, out in enumerate((tops, lows)):
        part = pl.ds(i * half, half)
        copies.append(pltpu.make_async_copy(rows.at[part], out.at[:, pl.ds(at, rows.shape[1])], sem.at[i, 0]))
        copies.append(pltpu.make_async_copy(up.at[part], out.at[:, pl.ds(0, at)], sem.at[i, 1]))
    for copy in copies:
        copy.start()
    for copy in copies:
        copy.wait()


def pack(up, rows):
    shape = (rows.shape[0] // 2, up.shape[1] + rows.shape[1])
    return pl.pallas_call(
        pack_kernel,
        out_shape=(jax.ShapeDtypeStruct(shape, bf16),) * 2,
        in_specs=[hbm()] * 2,
        out_specs=[vmem()] * 2,
        scratch_shapes=[pltpu.SemaphoreType.DMA((2, 2))],
        compiler_params=params(12),
        cost_estimate=cost(1, 4 * rows.size),
        name="pack",
    )(held_in_hbm(up), held_in_hbm(rows))


HALVES = 2
TILE = 256


def put_rows(got, outs, n):
    own, right, left, ahead, behind = outs
    size, width = own.shape[0], ahead.shape[1]
    cols = pl.ds(n * TILE, TILE)
    own[:, cols] = got[:size]
    right[:, cols] = got[size : 2 * size].astype(bf16)
    left[:, cols] = got[2 * size : 3 * size].astype(bf16)
    last, at = (ahead, n * TILE) if n * TILE < width else (behind, n * TILE - width)
    last[:, pl.ds(at, TILE)] = got[3 * size :].astype(bf16)


def row_shapes(size, width):
    return (
        jax.ShapeDtypeStruct((size, width), f32),
        jax.ShapeDtypeStruct((size, width), bf16),
        jax.ShapeDtypeStruct((size, width), bf16),
        jax.ShapeDtypeStruct((size, width // 2), bf16),
        jax.ShapeDtypeStruct((size, width // 2), bf16),
    )


def tiles_of(parts, at, n):
    half = (parts[0].shape[1] - at) // HALVES
    got = [p[:, pl.ds(at + c * half + n * TILE, TILE)] for c in range(HALVES) for p in parts]
    return jnp.concatenate(got, axis=0)


def attend_kernel(tok, nx, count, first, last, where_ref, arrived, *refs):
    pieces, outs = refs[:count], refs[count:]
    if last:
        before, outs = outs[0], outs[1:]
    up = jnp.concatenate([piece[:, pl.ds(0, LAT)] for piece in pieces], axis=0)
    values = lax.dot_general(arrived[...], up, NT, preferred_element_type=f32)
    hop = lax.rem(iota(values.shape, 0) // tok, nx)
    values = jnp.where(hop == first + iota(values.shape, 1) // VH, values, 0.0).astype(bf16)
    shape = (len(STEPS) * FAR * HALVES * tok, arrived.shape[0])
    row, source = iota(shape, 0), iota(shape, 1)
    chip = chip_at(row // (HALVES * tok), where_ref)
    take = (source // (tok * nx) == chip) & (lax.rem(source, tok) == lax.rem(row, tok))
    half = lax.rem(row // tok, HALVES)
    taken = [
        jnp.dot(one_hot(take & (half == c)), values, preferred_element_type=f32).astype(bf16)
        for c in range(HALVES)
    ]
    values = jnp.concatenate(taken, axis=1)
    tiles = outs[0].shape[1] // TILE
    for n in range(tiles):
        got = jnp.dot(of_tile(values, n, tiles), tiles_of(pieces, LAT, n), preferred_element_type=f32)
        cols = pl.ds(n * TILE, TILE)
        if last:
            put_rows(before[:, cols] + got, outs, n)
        else:
            outs[0][:, cols] = got


def attend_part(where, nx, arrived, pieces, tok, first, before):
    depth = sum(p.shape[0] for p in pieces)
    width = (pieces[0].shape[1] - LAT) // HALVES
    count = len(pieces)
    last = before is not None
    part = jax.ShapeDtypeStruct((RING * HALVES * tok, width), f32)
    return pl.pallas_call(
        functools.partial(attend_kernel, tok, nx, count, first, last),
        out_shape=row_shapes(FAR * HALVES * tok, width) if last else part,
        in_specs=[smem(), vmem()] + [vmem()] * count + [vmem()] * last,
        out_specs=[vmem()] * 5 if last else vmem(),
        compiler_params=params(6),
        cost_estimate=cost(8 * RING * tok * depth * width * HALVES, 4 * depth * width),
        name="attend_part",
    )(where, arrived, *pieces, *([before] if last else []))


SEND_TILE = 512


def dispatch_kernel(tok, nx, where_ref, tokens, *refs):
    outs, (early, late) = refs[:nx], refs[nx:]
    count, width = tokens.shape
    half = width - EXTRA
    table = tokens[:, pl.ds(half, EXTRA)]
    shape = (nx * CAP, EXTRA)
    row, place = iota(shape, 0), iota(shape, 1)
    expert = FAR * column(row // CAP, where_ref[0]) + where_ref[1]
    hot = one_hot(place == lax.rem(row, CAP) * EXPERTS + expert)
    got = lax.dot_general(hot, table, NT, preferred_element_type=f32)
    shape = (SLOTS, count)
    slot, token = iota(shape, 0), iota(shape, 1)
    source = slot // CAP
    chip = NEAR * lax.rem(source, FAR) + lax.rem(where_ref[2] + source // FAR + 1, NEAR)
    parts = []
    for r in range(nx):
        sel = jnp.where(lax.rem(slot, CAP) == 0, got[CAP * r : CAP * r + 1], got[CAP * r + 1 : CAP * r + 2])
        parts.append(jnp.where(chip == token // (HALVES * tok), sel, 0.0))
    of_half = lax.rem(token // tok, HALVES)
    halves = [[jnp.where(of_half == c, sel, 0.0) for sel in parts] for c in range(HALVES)]
    both = jnp.concatenate(sum(halves, []), axis=0).astype(bf16)
    rows = nx * SLOTS
    for n in range(half // SEND_TILE):
        got = jnp.dot(both, tokens[:, pl.ds(n * SEND_TILE, SEND_TILE)], preferred_element_type=f32).astype(bf16)
        for c in range(HALVES):
            for r in range(nx):
                at = c * rows + r * SLOTS
                outs[r][:, pl.ds(c * half + n * SEND_TILE, SEND_TILE)] = got[at : at + SLOTS]
    got = jnp.dot(both[:rows], table, preferred_element_type=f32).astype(bf16)
    for r in range(nx):
        outs[r][:, pl.ds(HALVES * half, EXTRA)] = got[r * SLOTS : (r + 1) * SLOTS]
    for out, group, at, end in ((early, 1, 0, EARLY), (late, 0, EARLY, SLOTS)):
        shape = (out.shape[0], count)
        row, token = iota(shape, 0), iota(shape, 1)
        chip = chip_at(group * FAR + row // (HALVES * tok), where_ref)
        take = (token // (HALVES * tok) == chip) & (lax.rem(token, HALVES * tok) == lax.rem(row, HALVES * tok))
        sel = jnp.concatenate([sel[at:end] for sels in halves for sel in sels], axis=0).astype(bf16)
        out[...] = lax.dot_general(one_hot(take), sel, NT, preferred_element_type=f32).astype(bf16)


def dispatch(where, nx, tokens, tok):
    count, width = tokens.shape
    full = HALVES * (width - EXTRA) + EXTRA
    near = count // NEAR
    return pl.pallas_call(
        functools.partial(dispatch_kernel, tok, nx),
        out_shape=(jax.ShapeDtypeStruct((SLOTS, full), bf16),) * nx
        + (
            jax.ShapeDtypeStruct(((len(STEPS) - 1) * near, HALVES * nx * EARLY), bf16),
            jax.ShapeDtypeStruct((near, HALVES * nx * LATE), bf16),
        ),
        in_specs=[smem(), vmem()],
        out_specs=[vmem()] * (nx + 2),
        compiler_params=params(12),
        cost_estimate=cost(2 * nx * SLOTS * count * full, 4 * count * width),
        name="dispatch",
    )(where, tokens)


CHUNKS = 7


def stage_kernel(gate_a, gate_b, up_a, up_b, down_a, down_b, wide, deep, sem):
    part = gate_a.shape[1]
    copies = [
        pltpu.make_async_copy(ref, wide.at[:, pl.ds(i * part, part)], sem.at[i])
        for i, ref in enumerate((gate_a, gate_b, up_a, up_b))
    ]
    copies += [
        pltpu.make_async_copy(ref, deep.at[pl.ds(i * part, part)], sem.at[4 + i])
        for i, ref in enumerate((down_a, down_b))
    ]
    for copy in copies:
        copy.start()
    for copy in copies:
        copy.wait()


def stage(weights):
    dim, part = weights[0].shape
    return pl.pallas_call(
        stage_kernel,
        out_shape=(
            jax.ShapeDtypeStruct((dim, 4 * part), bf16),
            jax.ShapeDtypeStruct((2 * part, dim), bf16),
        ),
        in_specs=[hbm()] * 6,
        out_specs=[vmem()] * 2,
        scratch_shapes=[pltpu.SemaphoreType.DMA((6,))],
        compiler_params=params(4),
        cost_estimate=cost(4 * 1000 * dim * part, 12 * dim * part),
        name="stage",
    )(*[held_in_hbm(w) for w in weights])


def expert_kernel(groups, where_ref, *refs):
    tokens = refs[:groups]
    wide, deep = refs[groups : groups + 2]
    early, late = refs[groups + 2 : 2 * groups + 2], refs[2 * groups + 2 : 3 * groups + 2]
    held = refs[3 * groups + 2] if groups > 1 else tokens[0]
    dim = wide.shape[0]
    part = wide.shape[1] // 2
    chunk = dim // CHUNKS
    if groups > 1:
        for g, ref in enumerate(tokens):
            held[pl.ds(g * SLOTS, SLOTS)] = ref[...]
    total = jnp.dot(held[:, pl.ds(0, dim)], wide[...], preferred_element_type=f32)
    gate, upward = total[:, :part], total[:, part:]
    act = (gate / (1.0 + jnp.exp(-gate)) * upward).astype(bf16)
    shape = (EXTRA, EXTRA)
    expert = FAR * where_ref[0] + where_ref[1]
    from_share = iota(shape, 0) - CAP * EXPERTS
    hot = (from_share >= 0) & (from_share < 3 * EXPERTS) & (lax.rem(from_share + EXTRA, EXPERTS) == expert)
    share = jnp.dot(held[:, pl.ds(dim, EXTRA)], one_hot(hot), preferred_element_type=f32)[:, :1]
    for k in range(CHUNKS):
        cols = pl.ds(k * chunk, chunk)
        got = jnp.dot(act, deep[:, cols], preferred_element_type=f32) * share
        for g in range(groups):
            rows = got[g * SLOTS : (g + 1) * SLOTS].astype(bf16)
            early[g][:, cols] = rows[:EARLY]
            late[g][:, cols] = rows[EARLY:]


def expert_part(where, tokens, weights):
    wide, deep = weights
    dim = wide.shape[0]
    groups = len(tokens)
    rows = groups * SLOTS
    held = [pltpu.VMEM((rows, dim + EXTRA), bf16)] if groups > 1 else []
    return pl.pallas_call(
        functools.partial(expert_kernel, groups),
        out_shape=(jax.ShapeDtypeStruct((EARLY, dim), bf16),) * groups
        + (jax.ShapeDtypeStruct((LATE, dim), bf16),) * groups,
        in_specs=[smem()] + [vmem()] * (groups + 2),
        out_specs=[vmem()] * (2 * groups),
        scratch_shapes=held,
        compiler_params=params(8),
        cost_estimate=cost(6 * rows * wide.size, 2 * rows * dim),
        name="expert_part",
    )(where, *tokens, held_in_vmem(wide), held_in_vmem(deep))


def collect_kernel(count, spread, *refs):
    parts, (right, left, ahead, behind) = refs[:count], refs[count:]
    size = right.shape[0]
    tiles = right.shape[1] // TILE
    for n in range(tiles):
        cols = pl.ds(n * TILE, TILE)
        rows = spread[...]
        first = n < tiles // 2
        rows = rows[: 3 * size] if first else jnp.concatenate([rows[: 2 * size], rows[3 * size :]], axis=0)
        got = jnp.dot(rows, tiles_of(parts, 0, n), preferred_element_type=f32).astype(bf16)
        right[:, cols] = got[:size]
        left[:, cols] = got[size : 2 * size]
        last, at = (ahead, n * TILE) if first else (behind, (n - tiles // 2) * TILE)
        last[:, pl.ds(at, TILE)] = got[2 * size :]


def collect(spread, parts):
    width = parts[0].shape[1] // HALVES
    count = len(parts)
    return pl.pallas_call(
        functools.partial(collect_kernel, count),
        out_shape=row_shapes(spread.shape[0] // (len(STEPS) - 1), width)[1:],
        in_specs=[vmem()] * (count + 1),
        out_specs=[vmem()] * 4,
        compiler_params=params(12),
        cost_estimate=cost(2 * spread.size * width, 4 * spread.shape[0] * width),
        name="collect",
    )(spread, *parts)


def merge_kernel(count, *refs):
    mine, (right, left, ahead, behind, first), rest = refs[:count], refs[count : count + 5], refs[count + 5 :]
    block = first.shape[0]
    tiles = first.shape[1] // TILE
    for n in range(tiles):
        cols = pl.ds(n * TILE, TILE)
        if count == 1:
            total = mine[0][:, cols]
        else:
            total = jnp.dot(mine[0][...], tiles_of(mine[1:], 0, n), preferred_element_type=f32)
        last, at = (ahead, n * TILE) if n < tiles // 2 else (behind, (n - tiles // 2) * TILE)
        total = total + right[:, cols].astype(f32) + left[:, cols].astype(f32)
        total = total + last[:, pl.ds(at, TILE)].astype(f32)
        first[:, cols] = total[:block]
        for k, out in enumerate(rest):
            out[:, cols] = total[(k + 1) * block : (k + 2) * block].astype(bf16)


def merge(mine, others):
    size, width = others[0].shape
    block = (size // FAR, width)
    return pl.pallas_call(
        functools.partial(merge_kernel, len(mine)),
        out_shape=(jax.ShapeDtypeStruct(block, f32),) + (jax.ShapeDtypeStruct(block, bf16),) * (FAR - 1),
        in_specs=[vmem()] * (len(mine) + 4),
        out_specs=[vmem()] * FAR,
        compiler_params=params(4),
        cost_estimate=cost(4 * size * width, 12 * size * width),
        name="merge",
    )(*mine, *others)


def half_swap(a):
    middle = a.shape[0] // 2
    return jnp.concatenate([a[middle:], a[:middle]], axis=0)


def route_kernel(first, one, two, three, rows, gain, router, ids, slots, hidden, payload):
    count, half = rows.shape
    total = first[...] + one[...].astype(f32) + two[...].astype(f32) + three[...].astype(f32)
    total = rows[...].astype(f32) + total
    hidden[...] = total
    square = jnp.sum(total * total, axis=1, keepdims=True)
    scale = lax.rsqrt((square + half_swap(square)) / D + norm_eps)
    normed = (total * scale * gain[...]).astype(bf16)
    payload[:, pl.ds(0, half)] = normed
    parts = [
        lax.dot_general(normed, router[:, pl.ds(c * half, half)], NT, preferred_element_type=f32)
        for c in range(HALVES)
    ]
    logits = jnp.where(iota(parts[0].shape, 0) < count // 2, parts[0], parts[1])
    logits = logits + half_swap(logits)
    logits = jnp.concatenate([logits] * (EXTRA // EXPERTS), axis=1)
    lane = iota(logits.shape, 1)
    place = jnp.zeros(logits.shape, jnp.int32)
    for k in range(TOP):
        place = jnp.where(lax.rem(lane, EXPERTS) == ids[:, k : k + 1], slots[:, k : k + 1] + 1, place)
    gates = jnp.where(place > 0, 1.0 / (1.0 + jnp.exp(-logits)), 0.0)
    share = route_scale * gates / jnp.sum(jnp.where(lane < EXPERTS, gates, 0.0), axis=1, keepdims=True)
    kind = lane // EXPERTS
    table = jnp.zeros(logits.shape, f32)
    for n in range(CAP):
        table = jnp.where((kind == n) & (place == n + 1), 1.0, table)
    rest = share
    for n in range(3):
        piece = rest.astype(bf16).astype(f32)
        table = jnp.where(kind == CAP + n, piece, table)
        rest = rest - piece
    payload[:, pl.ds(half, EXTRA)] = table.astype(bf16)


def route(added, rows, gain, router, ids, slots):
    count, half = rows.shape
    return pl.pallas_call(
        route_kernel,
        out_shape=(
            jax.ShapeDtypeStruct((count, half), f32),
            jax.ShapeDtypeStruct((count, half + EXTRA), bf16),
        ),
        in_specs=[vmem()] * 9,
        out_specs=[vmem()] * 2,
        compiler_params=params(4),
        cost_estimate=cost(4 * count * half * EXPERTS, 20 * count * half),
        name="route",
    )(*added, rows, gain, router, ids, slots)


def finish_kernel(hidden, first, one, two, three, out):
    seqs, steps, _ = out.shape
    half = hidden.shape[1]
    total = first[...] + one[...].astype(f32) + two[...].astype(f32) + three[...].astype(f32)
    total = (hidden[...] + total).astype(bf16)
    for c in range(HALVES):
        for b in range(seqs):
            at = (c * seqs + b) * steps
            out[b, :, pl.ds(c * half, half)] = total[at : at + steps]


def finish(hidden, added, shape):
    return pl.pallas_call(
        finish_kernel,
        out_shape=jax.ShapeDtypeStruct(shape, bf16),
        in_specs=[vmem()] * 5,
        out_specs=vmem(),
        compiler_params=params(4),
        cost_estimate=cost(5 * hidden.size, 14 * hidden.size),
        name="finish",
    )(hidden, *added)


def reduce_z(mine, right, left, ahead, behind):
    others = shift_z(right, 1), shift_z(left, -1), shift_z(ahead, 2), shift_z(behind, -2)
    first, *sent = merge(mine, others)
    others = [swap_far(rows, k + 1) for k, rows in enumerate(sent)]
    return first, *others


def layer(
    cache_kv,
    new_kv,
    queries,
    lengths,
    resid,
    value_up,
    out_proj,
    norm_gain,
    router,
    expert_ids,
    slots,
    w_gate,
    w_up,
    w_down,
):
    nx = lax.axis_size("x")
    seqs, steps = queries.shape[:2]
    tok = seqs * steps
    where = jnp.stack([lax.axis_index(a) for a in ("x", "zb", "j")]).astype(jnp.int32)
    where = jnp.concatenate([where, lengths.astype(jnp.int32)])

    tops, lows = pack(value_up.T, out_proj)
    top_left = swap_x(tops, 1)
    low_right = swap_x(lows, 3)
    low_left = swap_x(lows, 1)
    top_right = swap_x(tops, 3)

    outgoing = context_rows(where, nx, cache_kv, new_kv, queries)
    arrived = lax.all_to_all(
        outgoing.reshape(RING, nx * tok, LAT), ZAX, split_axis=0, concat_axis=0, tiled=True
    )
    top_far = swap_x(top_left, 3)
    low_far = swap_x(low_right, 1)
    near = [tops, lows, swap_core(tops), swap_core(lows)]
    for pair in ((top_left, low_left), (top_right, low_right)):
        near += [*pair, *map(swap_core, pair)]
    beyond = [top_far, low_far, swap_core(top_far), swap_core(low_far)]
    others = [swap_core(w) for w in (w_gate, w_up, w_down)]
    weights = stage((w_gate, others[0], w_up, others[1], w_down, others[2]))
    arrived = arrived.reshape(RING * nx * tok, LAT)
    most = attend_part(where, nx, arrived, near, tok, 0, None)
    own, *rows = attend_part(where, nx, arrived, beyond, tok, nx - 1, most)
    added = reduce_z((own,), *rows)

    half = D // HALVES
    rows = resid.reshape(tok, HALVES, half).swapaxes(0, 1).reshape(HALVES * tok, half)
    gain = jnp.repeat(norm_gain.astype(f32).reshape(HALVES, half), tok, axis=0)
    ids, places = [
        jnp.tile(a.reshape(tok, TOP).astype(jnp.int32), (HALVES, 1)) for a in (expert_ids, slots)
    ]
    hidden, payload = route(added, rows, gain, router.T, ids, places)

    ring = lax.all_gather(payload, ZAX, axis=0, tiled=True)
    *sent, early, late = dispatch(where, nx, ring, tok)
    got = [swap_x(sent[i], COLUMNS[i]) for i in range(1, nx)]
    done = expert_part(where, (sent[0], *got[: nx - 2]), weights)
    done = [list(done[: nx - 1]), list(done[nx - 1 :])]
    for rows, last in zip(done, expert_part(where, got[nx - 2 :], weights)):
        rows.append(last)
    first = [done[0][0]] + [swap_x(done[0][i], COLUMNS[i]) for i in range(1, nx)]
    second = [done[1][0]] + [swap_x(done[1][i], COLUMNS[i]) for i in range(1, nx)]
    added = reduce_z((late, *second), *collect(early, first))
    return finish(hidden, added, resid.shape)


def solution(mesh):
    chips = mesh.shape["ep"] // (RING * CORES)
    grid = mesh.devices.reshape(mesh.shape["rep"], chips, FAR, NEAR, CORES)
    fine = Mesh(grid, ("rep", "x", "zb", "j", "c"))
    ep = ("x", "zb", "j", "c")
    both = ("rep",) + ep
    return jax.shard_map(
        layer,
        mesh=fine,
        in_specs=(
            P(both, None, None),
            P(both, None, None),
            P(both, None, None, None),
            P(both),
            P(both, None, None),
            P(None, ep),
            P(ep, None),
            P(),
            P(),
            P(both, None, None),
            P(both, None, None),
            P(None, ep),
            P(None, ep),
            P(ep, None),
        ),
        out_specs=P(both, None, None),
        check_vma=False,
    )
```

```python
import functools
import math

import jax
import jax.numpy as jnp
from jax import lax
from jax.experimental import pallas as pl
from jax.experimental.pallas import tpu as pltpu
from jax.sharding import Mesh
from jax.sharding import PartitionSpec as P


D = 7168
LAT = 512
VH = 128
EXPERTS = 16
TOP = 8
CAP = 2
QK = 192

CORES = 2
NEAR = 4
FAR = 4
RING = NEAR * FAR
SLOTS = RING * CAP
LATE = FAR * CAP
EARLY = SLOTS - LATE
EXTRA = 128

route_scale = 2.827
norm_eps = 1e-06


ZAX = ("zb", "j")
f32, bf16 = jnp.float32, jnp.bfloat16
NT = (((1,), (1,)), ((), ()))


def swap_x(a, bits):
    return lax.ppermute(a, "x", [(i, i ^ bits) for i in range(lax.axis_size("x"))])


def shift_z(a, step):
    return lax.ppermute(a, ZAX, [(i, (i + step) % RING) for i in range(RING)])


def swap_far(a, bits):
    return lax.ppermute(a, "zb", [(i, i ^ bits) for i in range(FAR)])


def swap_core(a):
    return lax.ppermute(a, "c", [(i, i ^ 1) for i in range(CORES)])


def iota(shape, axis):
    return lax.broadcasted_iota(jnp.int32, shape, axis)


def one_hot(mask):
    return jnp.where(mask, 1.0, 0.0).astype(bf16)


def column(index, x):
    return x ^ jnp.where(index == 2, 3, jnp.where(index == 3, 2, index))


EXPERT_COLUMNS = (0, 2, 1, 3)


def expert_column(index, x):
    return x ^ jnp.where(index == 1, 2, jnp.where(index == 2, 1, index))


STEPS = (0, 1, RING - 1, 2, RING - 2)


def chip_at(place, where_ref):
    group, bits = place // FAR, lax.rem(place, FAR)
    step = 0
    for i, value in enumerate(STEPS):
        step = jnp.where(group == i, value, step)
    chip = lax.rem(NEAR * where_ref[1] + where_ref[2] + step, RING)
    return NEAR * ((chip // NEAR) ^ bits) + lax.rem(chip, NEAR)


def of_tile(rows, n, tiles):
    size = rows.shape[0] // len(STEPS)
    if n < tiles // 2:
        return rows[: 4 * size]
    return jnp.concatenate([rows[: 3 * size], rows[4 * size :]], axis=0)


def smem():
    return pl.BlockSpec(memory_space=pltpu.SMEM)


def vmem():
    return pl.BlockSpec(memory_space=pltpu.VMEM)


def hbm():
    return pl.BlockSpec(memory_space=pltpu.HBM)


def held_in_hbm(a):
    return pltpu.with_memory_space_constraint(a, pltpu.HBM)


def held_in_vmem(a):
    return pltpu.with_memory_space_constraint(a, pltpu.VMEM)


def params(mib):
    return pltpu.CompilerParams(vmem_limit_bytes=mib << 20)


def cost(flops, nbytes):
    return pl.CostEstimate(flops=flops, bytes_accessed=nbytes, transcendentals=0)


def context_kernel(nx, where_ref, keys, queries, new, out, held):
    seq = pl.program_id(0)
    seqs = pl.num_programs(0)
    steps, heads = queries.shape[1], queries.shape[2]
    count = steps * heads
    scale = 1.0 / math.sqrt(QK)
    query = queries[0].reshape(count, queries.shape[3])
    score = jnp.dot(query, keys[0], preferred_element_type=f32) * scale
    score = jnp.where(iota(score.shape, 1) < where_ref[3 + seq], score, -jnp.inf)
    wide = query.astype(f32)
    step_of = iota((count, 1), 0) // heads
    latest = []
    peak = jnp.max(score, axis=1, keepdims=True)
    for t in range(steps):
        key = new[0, t : t + 1, :].astype(f32)
        got = jnp.sum(wide * key, axis=1, keepdims=True) * scale
        got = jnp.where(step_of >= t, got, -jnp.inf)
        latest.append(got)
        peak = jnp.maximum(peak, got)
    probs = jnp.exp(score - peak)
    total = jnp.sum(probs, axis=1, keepdims=True)
    latest = [jnp.exp(got - peak) for got in latest]
    for got in latest:
        total = total + got
    share = 1.0 / total
    probs = (probs * share).astype(bf16)
    context = lax.dot_general(probs, keys[0, :LAT, :], NT, preferred_element_type=f32)
    for t, got in enumerate(latest):
        part = (got * share).astype(bf16).astype(f32)
        context = context + part * new[0, t : t + 1, :LAT].astype(f32)
    held[pl.ds(pl.multiple_of(seq * count, count), count), :] = context.astype(bf16)

    @pl.when(seq == seqs - 1)
    def _():
        rows = held.shape[0]
        tok = rows // heads
        shape = (rows, rows)
        to, source = iota(shape, 0), iota(shape, 1)
        hop = lax.rem(to // tok, nx)
        head = column(hop, where_ref[0]) * RING + to // (tok * nx)
        take = (lax.rem(to, tok) == source // heads) & (head == lax.rem(source, heads))
        out[...] = jnp.dot(one_hot(take), held[...], preferred_element_type=f32).astype(bf16)


def context_rows(where, nx, cache_kv, new_kv, queries):
    seqs, length, width = cache_kv.shape
    steps, heads = queries.shape[1:3]
    rows = seqs * steps * heads
    keys = jnp.swapaxes(cache_kv, 1, 2)
    return pl.pallas_call(
        functools.partial(context_kernel, nx),
        grid=(seqs,),
        out_shape=jax.ShapeDtypeStruct((rows, LAT), bf16),
        in_specs=[
            smem(),
            pl.BlockSpec((1, width, length), lambda b: (b, 0, 0)),
            pl.BlockSpec((1, steps, heads, width), lambda b: (b, 0, 0, 0)),
            pl.BlockSpec((1, steps, width), lambda b: (b, 0, 0)),
        ],
        out_specs=pl.BlockSpec((rows, LAT), lambda b: (0, 0)),
        scratch_shapes=[pltpu.VMEM((rows, LAT), bf16)],
        compiler_params=params(24),
        cost_estimate=cost(2 * rows * length * (width + LAT), 2 * cache_kv.size),
        name="context_rows",
    )(where, held_in_hbm(keys), held_in_hbm(queries), held_in_hbm(new_kv))


def pack_kernel(first, up, rows, out, sem):
    part, at = pl.ds(first, out.shape[0]), up.shape[1]
    copies = [
        pltpu.make_async_copy(rows.at[part], out.at[:, pl.ds(at, rows.shape[1])], sem.at[0]),
        pltpu.make_async_copy(up.at[part], out.at[:, pl.ds(0, at)], sem.at[1]),
    ]
    for copy in copies:
        copy.start()
    for copy in copies:
        copy.wait()


def pack(up, rows, first, count):
    return pl.pallas_call(
        functools.partial(pack_kernel, first),
        out_shape=jax.ShapeDtypeStruct((count, up.shape[1] + rows.shape[1]), bf16),
        in_specs=[hbm()] * 2,
        out_specs=vmem(),
        scratch_shapes=[pltpu.SemaphoreType.DMA((2,))],
        compiler_params=params(12),
        cost_estimate=cost(1, 4 * count * rows.shape[1]),
        name="pack",
    )(held_in_hbm(up), held_in_hbm(rows))


HALVES = 2
TILE = 256


def put_rows(got, outs, n):
    own, right, left, ahead, behind = outs
    size, width = own.shape[0], ahead.shape[1]
    cols = pl.ds(n * TILE, TILE)
    own[:, cols] = got[:size]
    right[:, cols] = got[size : 2 * size].astype(bf16)
    left[:, cols] = got[2 * size : 3 * size].astype(bf16)
    last, at = (ahead, n * TILE) if n * TILE < width else (behind, n * TILE - width)
    last[:, pl.ds(at, TILE)] = got[3 * size :].astype(bf16)


def row_shapes(size, width):
    return (
        jax.ShapeDtypeStruct((size, width), f32),
        jax.ShapeDtypeStruct((size, width), bf16),
        jax.ShapeDtypeStruct((size, width), bf16),
        jax.ShapeDtypeStruct((size, width // 2), bf16),
        jax.ShapeDtypeStruct((size, width // 2), bf16),
    )


def tiles_of(parts, at, n):
    half = (parts[0].shape[1] - at) // HALVES
    got = [p[:, pl.ds(at + c * half + n * TILE, TILE)] for c in range(HALVES) for p in parts]
    return jnp.concatenate(got, axis=0)


def attend_kernel(tok, nx, count, first, last, where_ref, arrived, *refs):
    pieces, outs = refs[:count], refs[count:]
    if last:
        before, outs = outs[0], outs[1:]
    up = jnp.concatenate([piece[:, pl.ds(0, LAT)] for piece in pieces], axis=0)
    values = lax.dot_general(arrived[...], up, NT, preferred_element_type=f32)
    hop = lax.rem(iota(values.shape, 0) // tok, nx)
    values = jnp.where(hop == first + iota(values.shape, 1) // VH, values, 0.0).astype(bf16)
    shape = (len(STEPS) * FAR * HALVES * tok, arrived.shape[0])
    row, source = iota(shape, 0), iota(shape, 1)
    chip = chip_at(row // (HALVES * tok), where_ref)
    take = (source // (tok * nx) == chip) & (lax.rem(source, tok) == lax.rem(row, tok))
    half = lax.rem(row // tok, HALVES)
    taken = [
        jnp.dot(one_hot(take & (half == c)), values, preferred_element_type=f32).astype(bf16)
        for c in range(HALVES)
    ]
    values = jnp.concatenate(taken, axis=1)
    tiles = outs[0].shape[1] // TILE
    for n in range(tiles):
        got = jnp.dot(of_tile(values, n, tiles), tiles_of(pieces, LAT, n), preferred_element_type=f32)
        cols = pl.ds(n * TILE, TILE)
        if last:
            put_rows(before[:, cols] + got, outs, n)
        else:
            outs[0][:, cols] = got


def attend_part(where, nx, arrived, pieces, tok, first, before):
    depth = sum(p.shape[0] for p in pieces)
    width = (pieces[0].shape[1] - LAT) // HALVES
    count = len(pieces)
    last = before is not None
    part = jax.ShapeDtypeStruct((RING * HALVES * tok, width), f32)
    return pl.pallas_call(
        functools.partial(attend_kernel, tok, nx, count, first, last),
        out_shape=row_shapes(FAR * HALVES * tok, width) if last else part,
        in_specs=[smem(), vmem()] + [vmem()] * count + [vmem()] * last,
        out_specs=[vmem()] * 5 if last else vmem(),
        compiler_params=params(6),
        cost_estimate=cost(8 * RING * tok * depth * width * HALVES, 4 * depth * width),
        name="attend_part",
    )(where, arrived, *pieces, *([before] if last else []))


SEND_TILE = 512


def slot_rows(tok, nx, where_ref, table):
    count = table.shape[0]
    shape = (nx * CAP, EXTRA)
    row, place = iota(shape, 0), iota(shape, 1)
    expert = FAR * expert_column(row // CAP, where_ref[0]) + where_ref[1]
    hot = one_hot(place == lax.rem(row, CAP) * EXPERTS + expert)
    got = lax.dot_general(hot, table, NT, preferred_element_type=f32)
    shape = (SLOTS, count)
    slot, token = iota(shape, 0), iota(shape, 1)
    source = slot // CAP
    chip = NEAR * lax.rem(source, FAR) + lax.rem(where_ref[2] + source // FAR + 1, NEAR)
    same = chip == token // (HALVES * tok)
    half = lax.rem(token // tok, HALVES)
    rows = []
    for r in range(nx):
        sel = jnp.where(lax.rem(slot, CAP) == 0, got[CAP * r : CAP * r + 1], got[CAP * r + 1 : CAP * r + 2])
        rows.append(jnp.where(same, sel, 0.0))
    return [[jnp.where(half == c, sel, 0.0) for sel in rows] for c in range(HALVES)]


def dispatch_kernel(tok, nx, where_ref, tokens, *outs):
    half = tokens.shape[1] - EXTRA
    table = tokens[:, pl.ds(half, EXTRA)]
    both = jnp.concatenate(sum(slot_rows(tok, nx, where_ref, table), []), axis=0).astype(bf16)
    rows = nx * SLOTS
    for n in range(half // SEND_TILE):
        got = jnp.dot(both, tokens[:, pl.ds(n * SEND_TILE, SEND_TILE)], preferred_element_type=f32).astype(bf16)
        for c in range(HALVES):
            for r in range(nx):
                at = c * rows + r * SLOTS
                outs[r][:, pl.ds(c * half + n * SEND_TILE, SEND_TILE)] = got[at : at + SLOTS]
    got = jnp.dot(both[:rows], table, preferred_element_type=f32).astype(bf16)
    for r in range(nx):
        outs[r][:, pl.ds(HALVES * half, EXTRA)] = got[r * SLOTS : (r + 1) * SLOTS]


def dispatch(where, nx, tokens, tok):
    count, width = tokens.shape
    full = HALVES * (width - EXTRA) + EXTRA
    return pl.pallas_call(
        functools.partial(dispatch_kernel, tok, nx),
        out_shape=(jax.ShapeDtypeStruct((SLOTS, full), bf16),) * nx,
        in_specs=[smem(), vmem()],
        out_specs=[vmem()] * nx,
        compiler_params=params(12),
        cost_estimate=cost(2 * nx * SLOTS * count * full, 4 * count * width),
        name="dispatch",
    )(where, tokens)


def plan_kernel(tok, nx, where_ref, tokens, early, late):
    count, width = tokens.shape
    halves = slot_rows(tok, nx, where_ref, tokens[:, pl.ds(width - EXTRA, EXTRA)])
    unit = HALVES * tok
    for out, group, at, end in ((early, 1, 0, EARLY), (late, 0, EARLY, SLOTS)):
        shape = (out.shape[0], count)
        row, token = iota(shape, 0), iota(shape, 1)
        take = token // unit == chip_at(group * FAR + row // unit, where_ref)
        take = take & (lax.rem(token, unit) == lax.rem(row, unit))
        sel = jnp.concatenate([sel[at:end] for rows in halves for sel in rows], axis=0).astype(bf16)
        out[...] = lax.dot_general(one_hot(take), sel, NT, preferred_element_type=f32).astype(bf16)


def plan(where, nx, tokens, tok):
    count = tokens.shape[0]
    near = count // NEAR
    return pl.pallas_call(
        functools.partial(plan_kernel, tok, nx),
        out_shape=(
            jax.ShapeDtypeStruct(((len(STEPS) - 1) * near, HALVES * nx * EARLY), bf16),
            jax.ShapeDtypeStruct((near, HALVES * nx * LATE), bf16),
        ),
        in_specs=[smem(), vmem()],
        out_specs=[vmem()] * 2,
        compiler_params=params(6),
        cost_estimate=cost(2 * count * SLOTS * count, 4 * count * SLOTS),
        name="plan",
    )(where, tokens)


CHUNKS = 7


def stage_kernel(gate_a, gate_b, up_a, up_b, down_a, down_b, wide, deep, sem):
    part = gate_a.shape[1]
    copies = [
        pltpu.make_async_copy(ref, wide.at[:, pl.ds(i * part, part)], sem.at[i])
        for i, ref in enumerate((gate_a, gate_b, up_a, up_b))
    ]
    copies += [
        pltpu.make_async_copy(ref, deep.at[pl.ds(i * part, part)], sem.at[4 + i])
        for i, ref in enumerate((down_a, down_b))
    ]
    for copy in copies:
        copy.start()
    for copy in copies:
        copy.wait()


def stage(weights):
    dim, part = weights[0].shape
    return pl.pallas_call(
        stage_kernel,
        out_shape=(
            jax.ShapeDtypeStruct((dim, 4 * part), bf16),
            jax.ShapeDtypeStruct((2 * part, dim), bf16),
        ),
        in_specs=[hbm()] * 6,
        out_specs=[vmem()] * 2,
        scratch_shapes=[pltpu.SemaphoreType.DMA((6,))],
        compiler_params=params(4),
        cost_estimate=cost(4 * 1000 * dim * part, 12 * dim * part),
        name="stage",
    )(*[held_in_hbm(w) for w in weights])


def expert_kernel(groups, where_ref, *refs):
    tokens = refs[:groups]
    wide, deep = refs[groups : groups + 2]
    early, late = refs[groups + 2 : 2 * groups + 2], refs[2 * groups + 2 : 3 * groups + 2]
    held = refs[3 * groups + 2] if groups > 1 else tokens[0]
    dim = wide.shape[0]
    part = wide.shape[1] // 2
    chunk = dim // CHUNKS
    if groups > 1:
        for g, ref in enumerate(tokens):
            held[pl.ds(g * SLOTS, SLOTS)] = ref[...]
    total = jnp.dot(held[:, pl.ds(0, dim)], wide[...], preferred_element_type=f32)
    gate, upward = total[:, :part], total[:, part:]
    act = (gate / (1.0 + jnp.exp(-gate)) * upward).astype(bf16)
    shape = (EXTRA, EXTRA)
    expert = FAR * where_ref[0] + where_ref[1]
    from_share = iota(shape, 0) - CAP * EXPERTS
    hot = (from_share >= 0) & (from_share < 3 * EXPERTS) & (lax.rem(from_share + EXTRA, EXPERTS) == expert)
    share = jnp.dot(held[:, pl.ds(dim, EXTRA)], one_hot(hot), preferred_element_type=f32)[:, :1]
    for k in range(CHUNKS):
        cols = pl.ds(k * chunk, chunk)
        got = jnp.dot(act, deep[:, cols], preferred_element_type=f32) * share
        for g in range(groups):
            rows = got[g * SLOTS : (g + 1) * SLOTS].astype(bf16)
            early[g][:, cols] = rows[:EARLY]
            late[g][:, cols] = rows[EARLY:]


def expert_part(where, tokens, weights):
    wide, deep = weights
    dim = wide.shape[0]
    groups = len(tokens)
    rows = groups * SLOTS
    held = [pltpu.VMEM((rows, dim + EXTRA), bf16)] if groups > 1 else []
    return pl.pallas_call(
        functools.partial(expert_kernel, groups),
        out_shape=(jax.ShapeDtypeStruct((EARLY, dim), bf16),) * groups
        + (jax.ShapeDtypeStruct((LATE, dim), bf16),) * groups,
        in_specs=[smem()] + [vmem()] * (groups + 2),
        out_specs=[vmem()] * (2 * groups),
        scratch_shapes=held,
        compiler_params=params(8),
        cost_estimate=cost(6 * rows * wide.size, 2 * rows * dim),
        name="expert_part",
    )(where, *tokens, held_in_vmem(wide), held_in_vmem(deep))


def collect_kernel(count, spread, *refs):
    parts, (right, left, ahead, behind) = refs[:count], refs[count:]
    size = right.shape[0]
    tiles = right.shape[1] // TILE
    for n in range(tiles):
        cols = pl.ds(n * TILE, TILE)
        rows = spread[...]
        first = n < tiles // 2
        rows = rows[: 3 * size] if first else jnp.concatenate([rows[: 2 * size], rows[3 * size :]], axis=0)
        got = jnp.dot(rows, tiles_of(parts, 0, n), preferred_element_type=f32).astype(bf16)
        right[:, cols] = got[:size]
        left[:, cols] = got[size : 2 * size]
        last, at = (ahead, n * TILE) if first else (behind, (n - tiles // 2) * TILE)
        last[:, pl.ds(at, TILE)] = got[2 * size :]


def collect(spread, parts):
    width = parts[0].shape[1] // HALVES
    count = len(parts)
    return pl.pallas_call(
        functools.partial(collect_kernel, count),
        out_shape=row_shapes(spread.shape[0] // (len(STEPS) - 1), width)[1:],
        in_specs=[vmem()] * (count + 1),
        out_specs=[vmem()] * 4,
        compiler_params=params(12),
        cost_estimate=cost(2 * spread.size * width, 4 * spread.shape[0] * width),
        name="collect",
    )(spread, *parts)


def merge_kernel(count, *refs):
    mine, (right, left, ahead, behind, first), rest = refs[:count], refs[count : count + 5], refs[count + 5 :]
    block = first.shape[0]
    tiles = first.shape[1] // TILE
    for n in range(tiles):
        cols = pl.ds(n * TILE, TILE)
        if count == 1:
            total = mine[0][:, cols]
        else:
            total = jnp.dot(mine[0][...], tiles_of(mine[1:], 0, n), preferred_element_type=f32)
        last, at = (ahead, n * TILE) if n < tiles // 2 else (behind, (n - tiles // 2) * TILE)
        total = total + right[:, cols].astype(f32) + left[:, cols].astype(f32)
        total = total + last[:, pl.ds(at, TILE)].astype(f32)
        first[:, cols] = total[:block]
        for k, out in enumerate(rest):
            out[:, cols] = total[(k + 1) * block : (k + 2) * block].astype(bf16)


def merge(mine, others):
    size, width = others[0].shape
    block = (size // FAR, width)
    return pl.pallas_call(
        functools.partial(merge_kernel, len(mine)),
        out_shape=(jax.ShapeDtypeStruct(block, f32),) + (jax.ShapeDtypeStruct(block, bf16),) * (FAR - 1),
        in_specs=[vmem()] * (len(mine) + 4),
        out_specs=[vmem()] * FAR,
        compiler_params=params(4),
        cost_estimate=cost(4 * size * width, 12 * size * width),
        name="merge",
    )(*mine, *others)


def half_swap(a):
    middle = a.shape[0] // 2
    return jnp.concatenate([a[middle:], a[:middle]], axis=0)


def route_kernel(first, one, two, three, rows, gain, router, ids, slots, hidden, payload):
    count, half = rows.shape
    total = first[...] + one[...].astype(f32) + two[...].astype(f32) + three[...].astype(f32)
    total = rows[...].astype(f32) + total
    hidden[...] = total
    square = jnp.sum(total * total, axis=1, keepdims=True)
    scale = lax.rsqrt((square + half_swap(square)) / D + norm_eps)
    normed = (total * scale * gain[...]).astype(bf16)
    payload[:, pl.ds(0, half)] = normed
    parts = [
        lax.dot_general(normed, router[:, pl.ds(c * half, half)], NT, preferred_element_type=f32)
        for c in range(HALVES)
    ]
    logits = jnp.where(iota(parts[0].shape, 0) < count // 2, parts[0], parts[1])
    logits = logits + half_swap(logits)
    logits = jnp.concatenate([logits] * (EXTRA // EXPERTS), axis=1)
    lane = iota(logits.shape, 1)
    place = jnp.zeros(logits.shape, jnp.int32)
    for k in range(TOP):
        place = jnp.where(lax.rem(lane, EXPERTS) == ids[:, k : k + 1], slots[:, k : k + 1] + 1, place)
    gates = jnp.where(place > 0, 1.0 / (1.0 + jnp.exp(-logits)), 0.0)
    share = route_scale * gates / jnp.sum(jnp.where(lane < EXPERTS, gates, 0.0), axis=1, keepdims=True)
    kind = lane // EXPERTS
    table = jnp.zeros(logits.shape, f32)
    for n in range(CAP):
        table = jnp.where((kind == n) & (place == n + 1), 1.0, table)
    rest = share
    for n in range(3):
        piece = rest.astype(bf16).astype(f32)
        table = jnp.where(kind == CAP + n, piece, table)
        rest = rest - piece
    payload[:, pl.ds(half, EXTRA)] = table.astype(bf16)


def route(added, rows, gain, router, ids, slots):
    count, half = rows.shape
    return pl.pallas_call(
        route_kernel,
        out_shape=(
            jax.ShapeDtypeStruct((count, half), f32),
            jax.ShapeDtypeStruct((count, half + EXTRA), bf16),
        ),
        in_specs=[vmem()] * 9,
        out_specs=[vmem()] * 2,
        compiler_params=params(4),
        cost_estimate=cost(4 * count * half * EXPERTS, 20 * count * half),
        name="route",
    )(*added, rows, gain, router, ids, slots)


def finish_kernel(hidden, first, one, two, three, out):
    seqs, steps, _ = out.shape
    half = hidden.shape[1]
    total = first[...] + one[...].astype(f32) + two[...].astype(f32) + three[...].astype(f32)
    total = (hidden[...] + total).astype(bf16)
    for c in range(HALVES):
        for b in range(seqs):
            at = (c * seqs + b) * steps
            out[b, :, pl.ds(c * half, half)] = total[at : at + steps]


def finish(hidden, added, shape):
    return pl.pallas_call(
        finish_kernel,
        out_shape=jax.ShapeDtypeStruct(shape, bf16),
        in_specs=[vmem()] * 5,
        out_specs=vmem(),
        compiler_params=params(4),
        cost_estimate=cost(5 * hidden.size, 14 * hidden.size),
        name="finish",
    )(hidden, *added)


def reduce_z(mine, right, left, ahead, behind):
    others = shift_z(right, 1), shift_z(left, -1), shift_z(ahead, 2), shift_z(behind, -2)
    first, *sent = merge(mine, others)
    others = [swap_far(rows, k + 1) for k, rows in enumerate(sent)]
    return first, *others


def layer(
    cache_kv,
    new_kv,
    queries,
    lengths,
    resid,
    value_up,
    out_proj,
    norm_gain,
    router,
    expert_ids,
    slots,
    w_gate,
    w_up,
    w_down,
):
    nx = lax.axis_size("x")
    seqs, steps = queries.shape[:2]
    tok = seqs * steps
    where = jnp.stack([lax.axis_index(a) for a in ("x", "zb", "j")]).astype(jnp.int32)
    where = jnp.concatenate([where, lengths.astype(jnp.int32)])

    half = out_proj.shape[0] // 2
    tops = pack(value_up.T, out_proj, 0, half)
    top_left = swap_x(tops, 1)
    lows = pack(value_up.T, out_proj, half, half)
    low_right = swap_x(lows, 3)
    low_left = swap_x(lows, 1)
    top_right = swap_x(tops, 3)

    outgoing = context_rows(where, nx, cache_kv, new_kv, queries)
    arrived = lax.all_to_all(
        outgoing.reshape(RING, nx * tok, LAT), ZAX, split_axis=0, concat_axis=0, tiled=True
    )
    top_far = swap_x(top_left, 3)
    low_far = swap_x(low_right, 1)
    near = [tops, lows, swap_core(tops), swap_core(lows)]
    for pair in ((top_left, low_left), (top_right, low_right)):
        near += [*pair, *map(swap_core, pair)]
    beyond = [top_far, low_far, swap_core(top_far), swap_core(low_far)]
    others = [swap_core(w) for w in (w_gate, w_up, w_down)]
    weights = stage((w_gate, others[0], w_up, others[1], w_down, others[2]))
    arrived = arrived.reshape(RING * nx * tok, LAT)
    most = attend_part(where, nx, arrived, near, tok, 0, None)
    own, *rows = attend_part(where, nx, arrived, beyond, tok, nx - 1, most)
    added = reduce_z((own,), *rows)

    half = D // HALVES
    rows = resid.reshape(tok, HALVES, half).swapaxes(0, 1).reshape(HALVES * tok, half)
    gain = jnp.repeat(norm_gain.astype(f32).reshape(HALVES, half), tok, axis=0)
    ids, places = [
        jnp.tile(a.reshape(tok, TOP).astype(jnp.int32), (HALVES, 1)) for a in (expert_ids, slots)
    ]
    hidden, payload = route(added, rows, gain, router.T, ids, places)

    ring = lax.all_gather(payload, ZAX, axis=0, tiled=True)
    sent = dispatch(where, nx, ring, tok)
    far = swap_x(sent[1], EXPERT_COLUMNS[1])
    near = [swap_x(sent[i], EXPERT_COLUMNS[i]) for i in range(2, nx)]
    early, late = plan(where, nx, ring, tok)
    done = [[], []]
    for groups in ((sent[0], far), tuple(near)):
        rows = expert_part(where, groups, weights)
        done[0] += rows[: len(groups)]
        done[1] += rows[len(groups) :]
    first = [done[0][0], swap_x(done[0][1], EXPERT_COLUMNS[1])]
    first += [swap_x(done[0][i], EXPERT_COLUMNS[i]) for i in range(2, nx)]
    second = [done[1][0]] + [swap_x(done[1][i], EXPERT_COLUMNS[i]) for i in range(1, nx)]
    added = reduce_z((late, *second), *collect(early, first))
    return finish(hidden, added, resid.shape)


def solution(mesh):
    chips = mesh.shape["ep"] // (RING * CORES)
    grid = mesh.devices.reshape(mesh.shape["rep"], chips, FAR, NEAR, CORES)
    fine = Mesh(grid, ("rep", "x", "zb", "j", "c"))
    ep = ("x", "zb", "j", "c")
    both = ("rep",) + ep
    return jax.shard_map(
        layer,
        mesh=fine,
        in_specs=(
            P(both, None, None),
            P(both, None, None),
            P(both, None, None, None),
            P(both),
            P(both, None, None),
            P(None, ep),
            P(ep, None),
            P(),
            P(),
            P(both, None, None),
            P(both, None, None),
            P(None, ep),
            P(None, ep),
            P(ep, None),
        ),
        out_specs=P(both, None, None),
        check_vma=False,
    )
```

```python
import functools
import math

import jax
import jax.numpy as jnp
from jax import lax
from jax.experimental import pallas as pl
from jax.experimental.pallas import tpu as pltpu
from jax.sharding import Mesh
from jax.sharding import PartitionSpec as P


D = 7168
LAT = 512
VH = 128
EXPERTS = 16
TOP = 8
CAP = 2
QK = 192

CORES = 2
NEAR = 4
FAR = 4
RING = NEAR * FAR
SLOTS = RING * CAP
LATE = FAR * CAP
EARLY = SLOTS - LATE
EXTRA = 128

route_scale = 2.827
norm_eps = 1e-06


ZAX = ("zb", "j")
f32, bf16 = jnp.float32, jnp.bfloat16
NT = (((1,), (1,)), ((), ()))


def swap_x(a, bits):
    return lax.ppermute(a, "x", [(i, i ^ bits) for i in range(lax.axis_size("x"))])


def shift_z(a, step):
    return lax.ppermute(a, ZAX, [(i, (i + step) % RING) for i in range(RING)])


def swap_far(a, bits):
    return lax.ppermute(a, "zb", [(i, i ^ bits) for i in range(FAR)])


def swap_core(a):
    return lax.ppermute(a, "c", [(i, i ^ 1) for i in range(CORES)])


def iota(shape, axis):
    return lax.broadcasted_iota(jnp.int32, shape, axis)


def one_hot(mask):
    return jnp.where(mask, 1.0, 0.0).astype(bf16)


def column(index, x):
    return x ^ jnp.where(index == 2, 3, jnp.where(index == 3, 2, index))


EXPERT_COLUMNS = (0, 2, 1, 3)


def expert_column(index, x):
    return x ^ jnp.where(index == 1, 2, jnp.where(index == 2, 1, index))


STEPS = (0, 1, RING - 1, 2, RING - 2)


def chip_at(place, where_ref):
    group, bits = place // FAR, lax.rem(place, FAR)
    step = 0
    for i, value in enumerate(STEPS):
        step = jnp.where(group == i, value, step)
    chip = lax.rem(NEAR * where_ref[1] + where_ref[2] + step, RING)
    return NEAR * ((chip // NEAR) ^ bits) + lax.rem(chip, NEAR)


def of_tile(rows, n, tiles):
    size = rows.shape[0] // len(STEPS)
    if n < tiles // 2:
        return rows[: 4 * size]
    return jnp.concatenate([rows[: 3 * size], rows[4 * size :]], axis=0)


def smem():
    return pl.BlockSpec(memory_space=pltpu.SMEM)


def vmem():
    return pl.BlockSpec(memory_space=pltpu.VMEM)


def hbm():
    return pl.BlockSpec(memory_space=pltpu.HBM)


def held_in_hbm(a):
    return pltpu.with_memory_space_constraint(a, pltpu.HBM)


def held_in_vmem(a):
    return pltpu.with_memory_space_constraint(a, pltpu.VMEM)


def params(mib):
    return pltpu.CompilerParams(vmem_limit_bytes=mib << 20)


def cost(flops, nbytes):
    return pl.CostEstimate(flops=flops, bytes_accessed=nbytes, transcendentals=0)


def context_kernel(nx, where_ref, keys, queries, new, out, held):
    seq = pl.program_id(0)
    seqs = pl.num_programs(0)
    steps, heads = queries.shape[1], queries.shape[2]
    count = steps * heads
    scale = 1.0 / math.sqrt(QK)
    query = queries[0].reshape(count, queries.shape[3])
    score = jnp.dot(query, keys[0], preferred_element_type=f32) * scale
    score = jnp.where(iota(score.shape, 1) < where_ref[3 + seq], score, -jnp.inf)
    wide = query.astype(f32)
    step_of = iota((count, 1), 0) // heads
    latest = []
    peak = jnp.max(score, axis=1, keepdims=True)
    for t in range(steps):
        key = new[0, t : t + 1, :].astype(f32)
        got = jnp.sum(wide * key, axis=1, keepdims=True) * scale
        got = jnp.where(step_of >= t, got, -jnp.inf)
        latest.append(got)
        peak = jnp.maximum(peak, got)
    probs = jnp.exp(score - peak)
    total = jnp.sum(probs, axis=1, keepdims=True)
    latest = [jnp.exp(got - peak) for got in latest]
    for got in latest:
        total = total + got
    share = 1.0 / total
    probs = (probs * share).astype(bf16)
    context = lax.dot_general(probs, keys[0, :LAT, :], NT, preferred_element_type=f32)
    for t, got in enumerate(latest):
        part = (got * share).astype(bf16).astype(f32)
        context = context + part * new[0, t : t + 1, :LAT].astype(f32)
    held[pl.ds(pl.multiple_of(seq * count, count), count), :] = context.astype(bf16)

    @pl.when(seq == seqs - 1)
    def _():
        rows = held.shape[0]
        tok = rows // heads
        shape = (rows, rows)
        to, source = iota(shape, 0), iota(shape, 1)
        hop = lax.rem(to // tok, nx)
        head = column(hop, where_ref[0]) * RING + to // (tok * nx)
        take = (lax.rem(to, tok) == source // heads) & (head == lax.rem(source, heads))
        out[...] = jnp.dot(one_hot(take), held[...], preferred_element_type=f32).astype(bf16)


def context_rows(where, nx, cache_kv, new_kv, queries):
    seqs, length, width = cache_kv.shape
    steps, heads = queries.shape[1:3]
    rows = seqs * steps * heads
    keys = jnp.swapaxes(cache_kv, 1, 2)
    return pl.pallas_call(
        functools.partial(context_kernel, nx),
        grid=(seqs,),
        out_shape=jax.ShapeDtypeStruct((rows, LAT), bf16),
        in_specs=[
            smem(),
            pl.BlockSpec((1, width, length), lambda b: (b, 0, 0)),
            pl.BlockSpec((1, steps, heads, width), lambda b: (b, 0, 0, 0)),
            pl.BlockSpec((1, steps, width), lambda b: (b, 0, 0)),
        ],
        out_specs=pl.BlockSpec((rows, LAT), lambda b: (0, 0)),
        scratch_shapes=[pltpu.VMEM((rows, LAT), bf16)],
        compiler_params=params(24),
        cost_estimate=cost(2 * rows * length * (width + LAT), 2 * cache_kv.size),
        name="context_rows",
    )(where, held_in_hbm(keys), held_in_hbm(queries), held_in_hbm(new_kv))


def pack_kernel(up, rows, tops, lows, sem):
    half, at = tops.shape[0], up.shape[1]
    copies = []
    for i, out in enumerate((tops, lows)):
        part = pl.ds(i * half, half)
        copies.append(pltpu.make_async_copy(rows.at[part], out.at[:, pl.ds(at, rows.shape[1])], sem.at[i, 0]))
        copies.append(pltpu.make_async_copy(up.at[part], out.at[:, pl.ds(0, at)], sem.at[i, 1]))
    for copy in copies:
        copy.start()
    for copy in copies:
        copy.wait()


def pack(up, rows):
    shape = (rows.shape[0] // 2, up.shape[1] + rows.shape[1])
    return pl.pallas_call(
        pack_kernel,
        out_shape=(jax.ShapeDtypeStruct(shape, bf16),) * 2,
        in_specs=[hbm()] * 2,
        out_specs=[vmem()] * 2,
        scratch_shapes=[pltpu.SemaphoreType.DMA((2, 2))],
        compiler_params=params(12),
        cost_estimate=cost(1, 4 * rows.size),
        name="pack",
    )(held_in_hbm(up), held_in_hbm(rows))


HALVES = 2
TILE = 256


def put_rows(got, outs, n):
    own, right, left, ahead, behind = outs
    size, width = own.shape[0], ahead.shape[1]
    cols = pl.ds(n * TILE, TILE)
    own[:, cols] = got[:size]
    right[:, cols] = got[size : 2 * size].astype(bf16)
    left[:, cols] = got[2 * size : 3 * size].astype(bf16)
    last, at = (ahead, n * TILE) if n * TILE < width else (behind, n * TILE - width)
    last[:, pl.ds(at, TILE)] = got[3 * size :].astype(bf16)


def row_shapes(size, width):
    return (
        jax.ShapeDtypeStruct((size, width), f32),
        jax.ShapeDtypeStruct((size, width), bf16),
        jax.ShapeDtypeStruct((size, width), bf16),
        jax.ShapeDtypeStruct((size, width // 2), bf16),
        jax.ShapeDtypeStruct((size, width // 2), bf16),
    )


def tiles_of(parts, at, n):
    half = (parts[0].shape[1] - at) // HALVES
    got = [p[:, pl.ds(at + c * half + n * TILE, TILE)] for c in range(HALVES) for p in parts]
    return jnp.concatenate(got, axis=0)


def attend_kernel(tok, nx, count, first, last, where_ref, arrived, *refs):
    pieces, outs = refs[:count], refs[count:]
    if last:
        before, outs = outs[0], outs[1:]
    up = jnp.concatenate([piece[:, pl.ds(0, LAT)] for piece in pieces], axis=0)
    values = lax.dot_general(arrived[...], up, NT, preferred_element_type=f32)
    hop = lax.rem(iota(values.shape, 0) // tok, nx)
    values = jnp.where(hop == first + iota(values.shape, 1) // VH, values, 0.0).astype(bf16)
    shape = (len(STEPS) * FAR * HALVES * tok, arrived.shape[0])
    row, source = iota(shape, 0), iota(shape, 1)
    chip = chip_at(row // (HALVES * tok), where_ref)
    take = (source // (tok * nx) == chip) & (lax.rem(source, tok) == lax.rem(row, tok))
    half = lax.rem(row // tok, HALVES)
    taken = [
        jnp.dot(one_hot(take & (half == c)), values, preferred_element_type=f32).astype(bf16)
        for c in range(HALVES)
    ]
    values = jnp.concatenate(taken, axis=1)
    tiles = outs[0].shape[1] // TILE
    for n in range(tiles):
        got = jnp.dot(of_tile(values, n, tiles), tiles_of(pieces, LAT, n), preferred_element_type=f32)
        cols = pl.ds(n * TILE, TILE)
        if last:
            put_rows(before[:, cols] + got, outs, n)
        else:
            outs[0][:, cols] = got


def attend_part(where, nx, arrived, pieces, tok, first, before):
    depth = sum(p.shape[0] for p in pieces)
    width = (pieces[0].shape[1] - LAT) // HALVES
    count = len(pieces)
    last = before is not None
    part = jax.ShapeDtypeStruct((RING * HALVES * tok, width), f32)
    return pl.pallas_call(
        functools.partial(attend_kernel, tok, nx, count, first, last),
        out_shape=row_shapes(FAR * HALVES * tok, width) if last else part,
        in_specs=[smem(), vmem()] + [vmem()] * count + [vmem()] * last,
        out_specs=[vmem()] * 5 if last else vmem(),
        compiler_params=params(6),
        cost_estimate=cost(8 * RING * tok * depth * width * HALVES, 4 * depth * width),
        name="attend_part",
    )(where, arrived, *pieces, *([before] if last else []))


SEND_TILE = 512


def dispatch_kernel(tok, nx, where_ref, tokens, *refs):
    outs, (early, late) = refs[:nx], refs[nx:]
    count, width = tokens.shape
    half = width - EXTRA
    table = tokens[:, pl.ds(half, EXTRA)]
    shape = (nx * CAP, EXTRA)
    row, place = iota(shape, 0), iota(shape, 1)
    expert = FAR * expert_column(row // CAP, where_ref[0]) + where_ref[1]
    hot = one_hot(place == lax.rem(row, CAP) * EXPERTS + expert)
    got = lax.dot_general(hot, table, NT, preferred_element_type=f32)
    shape = (SLOTS, count)
    slot, token = iota(shape, 0), iota(shape, 1)
    source = slot // CAP
    chip = NEAR * lax.rem(source, FAR) + lax.rem(where_ref[2] + source // FAR + 1, NEAR)
    parts = []
    for r in range(nx):
        sel = jnp.where(lax.rem(slot, CAP) == 0, got[CAP * r : CAP * r + 1], got[CAP * r + 1 : CAP * r + 2])
        parts.append(jnp.where(chip == token // (HALVES * tok), sel, 0.0))
    of_half = lax.rem(token // tok, HALVES)
    halves = [[jnp.where(of_half == c, sel, 0.0) for sel in parts] for c in range(HALVES)]
    both = jnp.concatenate(sum(halves, []), axis=0).astype(bf16)
    rows = nx * SLOTS
    for n in range(half // SEND_TILE):
        got = jnp.dot(both, tokens[:, pl.ds(n * SEND_TILE, SEND_TILE)], preferred_element_type=f32).astype(bf16)
        for c in range(HALVES):
            for r in range(nx):
                at = c * rows + r * SLOTS
                outs[r][:, pl.ds(c * half + n * SEND_TILE, SEND_TILE)] = got[at : at + SLOTS]
    got = jnp.dot(both[:rows], table, preferred_element_type=f32).astype(bf16)
    for r in range(nx):
        outs[r][:, pl.ds(HALVES * half, EXTRA)] = got[r * SLOTS : (r + 1) * SLOTS]
    for out, group, at, end in ((early, 1, 0, EARLY), (late, 0, EARLY, SLOTS)):
        shape = (out.shape[0], count)
        row, token = iota(shape, 0), iota(shape, 1)
        chip = chip_at(group * FAR + row // (HALVES * tok), where_ref)
        take = (token // (HALVES * tok) == chip) & (lax.rem(token, HALVES * tok) == lax.rem(row, HALVES * tok))
        sel = jnp.concatenate([sel[at:end] for sels in halves for sel in sels], axis=0).astype(bf16)
        out[...] = lax.dot_general(one_hot(take), sel, NT, preferred_element_type=f32).astype(bf16)


def dispatch(where, nx, tokens, tok):
    count, width = tokens.shape
    full = HALVES * (width - EXTRA) + EXTRA
    near = count // NEAR
    return pl.pallas_call(
        functools.partial(dispatch_kernel, tok, nx),
        out_shape=(jax.ShapeDtypeStruct((SLOTS, full), bf16),) * nx
        + (
            jax.ShapeDtypeStruct(((len(STEPS) - 1) * near, HALVES * nx * EARLY), bf16),
            jax.ShapeDtypeStruct((near, HALVES * nx * LATE), bf16),
        ),
        in_specs=[smem(), vmem()],
        out_specs=[vmem()] * (nx + 2),
        compiler_params=params(12),
        cost_estimate=cost(2 * nx * SLOTS * count * full, 4 * count * width),
        name="dispatch",
    )(where, tokens)


CHUNKS = 7


def stage_kernel(gate_a, gate_b, up_a, up_b, down_a, down_b, wide, deep, sem):
    part = gate_a.shape[1]
    copies = [
        pltpu.make_async_copy(ref, wide.at[:, pl.ds(i * part, part)], sem.at[i])
        for i, ref in enumerate((gate_a, gate_b, up_a, up_b))
    ]
    copies += [
        pltpu.make_async_copy(ref, deep.at[pl.ds(i * part, part)], sem.at[4 + i])
        for i, ref in enumerate((down_a, down_b))
    ]
    for copy in copies:
        copy.start()
    for copy in copies:
        copy.wait()


def stage(weights):
    dim, part = weights[0].shape
    return pl.pallas_call(
        stage_kernel,
        out_shape=(
            jax.ShapeDtypeStruct((dim, 4 * part), bf16),
            jax.ShapeDtypeStruct((2 * part, dim), bf16),
        ),
        in_specs=[hbm()] * 6,
        out_specs=[vmem()] * 2,
        scratch_shapes=[pltpu.SemaphoreType.DMA((6,))],
        compiler_params=params(4),
        cost_estimate=cost(4 * 1000 * dim * part, 12 * dim * part),
        name="stage",
    )(*[held_in_hbm(w) for w in weights])


def expert_kernel(groups, where_ref, *refs):
    tokens = refs[:groups]
    wide, deep = refs[groups : groups + 2]
    early, late = refs[groups + 2 : 2 * groups + 2], refs[2 * groups + 2 : 3 * groups + 2]
    held = refs[3 * groups + 2] if groups > 1 else tokens[0]
    dim = wide.shape[0]
    part = wide.shape[1] // 2
    chunk = dim // CHUNKS
    if groups > 1:
        for g, ref in enumerate(tokens):
            held[pl.ds(g * SLOTS, SLOTS)] = ref[...]
    total = jnp.dot(held[:, pl.ds(0, dim)], wide[...], preferred_element_type=f32)
    gate, upward = total[:, :part], total[:, part:]
    act = (gate / (1.0 + jnp.exp(-gate)) * upward).astype(bf16)
    shape = (EXTRA, EXTRA)
    expert = FAR * where_ref[0] + where_ref[1]
    from_share = iota(shape, 0) - CAP * EXPERTS
    hot = (from_share >= 0) & (from_share < 3 * EXPERTS) & (lax.rem(from_share + EXTRA, EXPERTS) == expert)
    share = jnp.dot(held[:, pl.ds(dim, EXTRA)], one_hot(hot), preferred_element_type=f32)[:, :1]
    for k in range(CHUNKS):
        cols = pl.ds(k * chunk, chunk)
        got = jnp.dot(act, deep[:, cols], preferred_element_type=f32) * share
        for g in range(groups):
            rows = got[g * SLOTS : (g + 1) * SLOTS].astype(bf16)
            early[g][:, cols] = rows[:EARLY]
            late[g][:, cols] = rows[EARLY:]


def expert_part(where, tokens, weights):
    wide, deep = weights
    dim = wide.shape[0]
    groups = len(tokens)
    rows = groups * SLOTS
    held = [pltpu.VMEM((rows, dim + EXTRA), bf16)] if groups > 1 else []
    return pl.pallas_call(
        functools.partial(expert_kernel, groups),
        out_shape=(jax.ShapeDtypeStruct((EARLY, dim), bf16),) * groups
        + (jax.ShapeDtypeStruct((LATE, dim), bf16),) * groups,
        in_specs=[smem()] + [vmem()] * (groups + 2),
        out_specs=[vmem()] * (2 * groups),
        scratch_shapes=held,
        compiler_params=params(8),
        cost_estimate=cost(6 * rows * wide.size, 2 * rows * dim),
        name="expert_part",
    )(where, *tokens, held_in_vmem(wide), held_in_vmem(deep))


def collect_kernel(count, spread, *refs):
    parts, (right, left, ahead, behind) = refs[:count], refs[count:]
    size = right.shape[0]
    tiles = right.shape[1] // TILE
    for n in range(tiles):
        cols = pl.ds(n * TILE, TILE)
        rows = spread[...]
        first = n < tiles // 2
        rows = rows[: 3 * size] if first else jnp.concatenate([rows[: 2 * size], rows[3 * size :]], axis=0)
        got = jnp.dot(rows, tiles_of(parts, 0, n), preferred_element_type=f32).astype(bf16)
        right[:, cols] = got[:size]
        left[:, cols] = got[size : 2 * size]
        last, at = (ahead, n * TILE) if first else (behind, (n - tiles // 2) * TILE)
        last[:, pl.ds(at, TILE)] = got[2 * size :]


def collect(spread, parts):
    width = parts[0].shape[1] // HALVES
    count = len(parts)
    return pl.pallas_call(
        functools.partial(collect_kernel, count),
        out_shape=row_shapes(spread.shape[0] // (len(STEPS) - 1), width)[1:],
        in_specs=[vmem()] * (count + 1),
        out_specs=[vmem()] * 4,
        compiler_params=params(12),
        cost_estimate=cost(2 * spread.size * width, 4 * spread.shape[0] * width),
        name="collect",
    )(spread, *parts)


def merge_kernel(count, *refs):
    mine, (right, left, ahead, behind), outs = refs[:count], refs[count : count + 4], refs[count + 4 :]
    first, one, upper, lower, three = outs
    block = first.shape[0]
    tiles = first.shape[1] // TILE
    for n in range(tiles):
        cols = pl.ds(n * TILE, TILE)
        if count == 1:
            total = mine[0][:, cols]
        else:
            total = jnp.dot(mine[0][...], tiles_of(mine[1:], 0, n), preferred_element_type=f32)
        last, at = (ahead, n * TILE) if n < tiles // 2 else (behind, (n - tiles // 2) * TILE)
        total = total + right[:, cols].astype(f32) + left[:, cols].astype(f32)
        total = total + last[:, pl.ds(at, TILE)].astype(f32)
        first[:, cols] = total[:block]
        one[:, cols] = total[block : 2 * block]
        three[:, cols] = total[3 * block :]
        last, at = (upper, n * TILE) if n < tiles // 2 else (lower, (n - tiles // 2) * TILE)
        last[:, pl.ds(at, TILE)] = total[2 * block : 3 * block].astype(bf16)


def merge(mine, others):
    size, width = others[0].shape
    block = jax.ShapeDtypeStruct((size // FAR, width), f32)
    part = jax.ShapeDtypeStruct((size // FAR, width // 2), bf16)
    return pl.pallas_call(
        functools.partial(merge_kernel, len(mine)),
        out_shape=(block, block, part, part, block),
        in_specs=[vmem()] * (len(mine) + 4),
        out_specs=[vmem()] * 5,
        compiler_params=params(4),
        cost_estimate=cost(4 * size * width, 12 * size * width),
        name="merge",
    )(*mine, *others)


def relay_kernel(one, three, upper, lower, to_one, to_three):
    half = upper.shape[1]
    to_one[:, :half] = one[:, :half].astype(bf16)
    to_one[:, half:] = (one[:, half:] + lower[...].astype(f32)).astype(bf16)
    to_three[:, :half] = (three[:, :half] + upper[...].astype(f32)).astype(bf16)
    to_three[:, half:] = three[:, half:].astype(bf16)


def relay(one, three, upper, lower):
    return pl.pallas_call(
        relay_kernel,
        out_shape=(jax.ShapeDtypeStruct(one.shape, bf16),) * 2,
        in_specs=[vmem()] * 4,
        out_specs=[vmem()] * 2,
        compiler_params=params(4),
        cost_estimate=cost(one.size, 14 * one.size),
        name="relay",
    )(one, three, upper, lower)


def half_swap(a):
    middle = a.shape[0] // 2
    return jnp.concatenate([a[middle:], a[:middle]], axis=0)


def route_kernel(first, one, three, rows, gain, router, ids, slots, hidden, payload):
    count, half = rows.shape
    total = first[...] + one[...].astype(f32) + three[...].astype(f32)
    total = rows[...].astype(f32) + total
    hidden[...] = total
    square = jnp.sum(total * total, axis=1, keepdims=True)
    scale = lax.rsqrt((square + half_swap(square)) / D + norm_eps)
    normed = (total * scale * gain[...]).astype(bf16)
    payload[:, pl.ds(0, half)] = normed
    parts = [
        lax.dot_general(normed, router[:, pl.ds(c * half, half)], NT, preferred_element_type=f32)
        for c in range(HALVES)
    ]
    logits = jnp.where(iota(parts[0].shape, 0) < count // 2, parts[0], parts[1])
    logits = logits + half_swap(logits)
    logits = jnp.concatenate([logits] * (EXTRA // EXPERTS), axis=1)
    lane = iota(logits.shape, 1)
    place = jnp.zeros(logits.shape, jnp.int32)
    for k in range(TOP):
        place = jnp.where(lax.rem(lane, EXPERTS) == ids[:, k : k + 1], slots[:, k : k + 1] + 1, place)
    gates = jnp.where(place > 0, 1.0 / (1.0 + jnp.exp(-logits)), 0.0)
    share = route_scale * gates / jnp.sum(jnp.where(lane < EXPERTS, gates, 0.0), axis=1, keepdims=True)
    kind = lane // EXPERTS
    table = jnp.zeros(logits.shape, f32)
    for n in range(CAP):
        table = jnp.where((kind == n) & (place == n + 1), 1.0, table)
    rest = share
    for n in range(3):
        piece = rest.astype(bf16).astype(f32)
        table = jnp.where(kind == CAP + n, piece, table)
        rest = rest - piece
    payload[:, pl.ds(half, EXTRA)] = table.astype(bf16)


def route(added, rows, gain, router, ids, slots):
    count, half = rows.shape
    return pl.pallas_call(
        route_kernel,
        out_shape=(
            jax.ShapeDtypeStruct((count, half), f32),
            jax.ShapeDtypeStruct((count, half + EXTRA), bf16),
        ),
        in_specs=[vmem()] * 8,
        out_specs=[vmem()] * 2,
        compiler_params=params(4),
        cost_estimate=cost(4 * count * half * EXPERTS, 20 * count * half),
        name="route",
    )(*added, rows, gain, router, ids, slots)


def finish_kernel(hidden, first, one, three, out):
    seqs, steps, _ = out.shape
    half = hidden.shape[1]
    total = first[...] + one[...].astype(f32) + three[...].astype(f32)
    total = (hidden[...] + total).astype(bf16)
    for c in range(HALVES):
        for b in range(seqs):
            at = (c * seqs + b) * steps
            out[b, :, pl.ds(c * half, half)] = total[at : at + steps]


def finish(hidden, added, shape):
    return pl.pallas_call(
        finish_kernel,
        out_shape=jax.ShapeDtypeStruct(shape, bf16),
        in_specs=[vmem()] * 4,
        out_specs=vmem(),
        compiler_params=params(4),
        cost_estimate=cost(4 * hidden.size, 12 * hidden.size),
        name="finish",
    )(hidden, *added)


def reduce_z(mine, right, left, ahead, behind):
    others = shift_z(right, 1), shift_z(left, -1), shift_z(ahead, 2), shift_z(behind, -2)
    first, one, upper, lower, three = merge(mine, others)
    upper, lower = swap_far(upper, 1), swap_far(lower, 3)
    one, three = relay(one, three, upper, lower)
    others = swap_far(one, 1), swap_far(three, 3)
    return first, *others


def layer(
    cache_kv,
    new_kv,
    queries,
    lengths,
    resid,
    value_up,
    out_proj,
    norm_gain,
    router,
    expert_ids,
    slots,
    w_gate,
    w_up,
    w_down,
):
    nx = lax.axis_size("x")
    seqs, steps = queries.shape[:2]
    tok = seqs * steps
    where = jnp.stack([lax.axis_index(a) for a in ("x", "zb", "j")]).astype(jnp.int32)
    where = jnp.concatenate([where, lengths.astype(jnp.int32)])

    tops, lows = pack(value_up.T, out_proj)
    top_left = swap_x(tops, 1)
    low_right = swap_x(lows, 3)
    low_left = swap_x(lows, 1)
    top_right = swap_x(tops, 3)

    outgoing = context_rows(where, nx, cache_kv, new_kv, queries)
    arrived = lax.all_to_all(
        outgoing.reshape(RING, nx * tok, LAT), ZAX, split_axis=0, concat_axis=0, tiled=True
    )
    top_far = swap_x(top_left, 3)
    low_far = swap_x(low_right, 1)
    near = [tops, lows, swap_core(tops), swap_core(lows)]
    for pair in ((top_left, low_left), (top_right, low_right)):
        near += [*pair, *map(swap_core, pair)]
    beyond = [top_far, low_far, swap_core(top_far), swap_core(low_far)]
    others = [swap_core(w) for w in (w_gate, w_up, w_down)]
    weights = stage((w_gate, others[0], w_up, others[1], w_down, others[2]))
    arrived = arrived.reshape(RING * nx * tok, LAT)
    most = attend_part(where, nx, arrived, near, tok, 0, None)
    own, *rows = attend_part(where, nx, arrived, beyond, tok, nx - 1, most)
    added = reduce_z((own,), *rows)

    half = D // HALVES
    rows = resid.reshape(tok, HALVES, half).swapaxes(0, 1).reshape(HALVES * tok, half)
    gain = jnp.repeat(norm_gain.astype(f32).reshape(HALVES, half), tok, axis=0)
    ids, places = [
        jnp.tile(a.reshape(tok, TOP).astype(jnp.int32), (HALVES, 1)) for a in (expert_ids, slots)
    ]
    hidden, payload = route(added, rows, gain, router.T, ids, places)

    ring = lax.all_gather(payload, ZAX, axis=0, tiled=True)
    *sent, early, late = dispatch(where, nx, ring, tok)
    far = swap_x(sent[1], EXPERT_COLUMNS[1])
    near = [swap_x(sent[i], EXPERT_COLUMNS[i]) for i in range(2, nx)]
    done = [[], []]
    for groups in ((sent[0], far), tuple(near)):
        rows = expert_part(where, groups, weights)
        done[0] += rows[: len(groups)]
        done[1] += rows[len(groups) :]
    first = [done[0][0], swap_x(done[0][1], EXPERT_COLUMNS[1])]
    first += [swap_x(done[0][i], EXPERT_COLUMNS[i]) for i in range(2, nx)]
    second = [done[1][0]] + [swap_x(done[1][i], EXPERT_COLUMNS[i]) for i in range(1, nx)]
    added = reduce_z((late, *second), *collect(early, first))
    return finish(hidden, added, resid.shape)


def solution(mesh):
    chips = mesh.shape["ep"] // (RING * CORES)
    grid = mesh.devices.reshape(mesh.shape["rep"], chips, FAR, NEAR, CORES)
    fine = Mesh(grid, ("rep", "x", "zb", "j", "c"))
    ep = ("x", "zb", "j", "c")
    both = ("rep",) + ep
    return jax.shard_map(
        layer,
        mesh=fine,
        in_specs=(
            P(both, None, None),
            P(both, None, None),
            P(both, None, None, None),
            P(both),
            P(both, None, None),
            P(None, ep),
            P(ep, None),
            P(),
            P(),
            P(both, None, None),
            P(both, None, None),
            P(None, ep),
            P(None, ep),
            P(ep, None),
        ),
        out_specs=P(both, None, None),
        check_vma=False,
    )
```

```python
import functools
import math

import jax
import jax.numpy as jnp
from jax import lax
from jax.experimental import pallas as pl
from jax.experimental.pallas import tpu as pltpu
from jax.sharding import Mesh
from jax.sharding import PartitionSpec as P


D = 7168
LAT = 512
VH = 128
EXPERTS = 16
TOP = 8
CAP = 2
QK = 192

CORES = 2
NEAR = 4
FAR = 4
RING = NEAR * FAR
SLOTS = RING * CAP
LATE = FAR * CAP
EARLY = SLOTS - LATE
EXTRA = 128

route_scale = 2.827
norm_eps = 1e-06


ZAX = ("zb", "j")
f32, bf16 = jnp.float32, jnp.bfloat16
NT = (((1,), (1,)), ((), ()))


def swap_x(a, bits):
    return lax.ppermute(a, "x", [(i, i ^ bits) for i in range(lax.axis_size("x"))])


def shift_z(a, step):
    return lax.ppermute(a, ZAX, [(i, (i + step) % RING) for i in range(RING)])


def swap_far(a, bits):
    return lax.ppermute(a, "zb", [(i, i ^ bits) for i in range(FAR)])


def swap_core(a):
    return lax.ppermute(a, "c", [(i, i ^ 1) for i in range(CORES)])


def iota(shape, axis):
    return lax.broadcasted_iota(jnp.int32, shape, axis)


def one_hot(mask):
    return jnp.where(mask, 1.0, 0.0).astype(bf16)


def column(index, x):
    return x ^ jnp.where(index == 2, 3, jnp.where(index == 3, 2, index))


EXPERT_COLUMNS = (0, 2, 1, 3)


def expert_column(index, x):
    return x ^ jnp.where(index == 1, 2, jnp.where(index == 2, 1, index))


STEPS = (0, 1, RING - 1, 2, RING - 2)


def chip_at(place, where_ref):
    group, bits = place // FAR, lax.rem(place, FAR)
    step = 0
    for i, value in enumerate(STEPS):
        step = jnp.where(group == i, value, step)
    chip = lax.rem(NEAR * where_ref[1] + where_ref[2] + step, RING)
    return NEAR * ((chip // NEAR) ^ bits) + lax.rem(chip, NEAR)


def of_tile(rows, n, tiles):
    size = rows.shape[0] // len(STEPS)
    if n < tiles // 2:
        return rows[: 4 * size]
    return jnp.concatenate([rows[: 3 * size], rows[4 * size :]], axis=0)


def smem():
    return pl.BlockSpec(memory_space=pltpu.SMEM)


def vmem():
    return pl.BlockSpec(memory_space=pltpu.VMEM)


def hbm():
    return pl.BlockSpec(memory_space=pltpu.HBM)


def held_in_hbm(a):
    return pltpu.with_memory_space_constraint(a, pltpu.HBM)


def held_in_vmem(a):
    return pltpu.with_memory_space_constraint(a, pltpu.VMEM)


def params(mib):
    return pltpu.CompilerParams(vmem_limit_bytes=mib << 20)


def cost(flops, nbytes):
    return pl.CostEstimate(flops=flops, bytes_accessed=nbytes, transcendentals=0)


def context_kernel(nx, where_ref, keys, queries, new, out, held):
    seq = pl.program_id(0)
    seqs = pl.num_programs(0)
    steps, heads = queries.shape[1], queries.shape[2]
    count = steps * heads
    scale = 1.0 / math.sqrt(QK)
    query = queries[0].reshape(count, queries.shape[3])
    score = jnp.dot(query, keys[0], preferred_element_type=f32) * scale
    score = jnp.where(iota(score.shape, 1) < where_ref[3 + seq], score, -jnp.inf)
    wide = query.astype(f32)
    step_of = iota((count, 1), 0) // heads
    latest = []
    peak = jnp.max(score, axis=1, keepdims=True)
    for t in range(steps):
        key = new[0, t : t + 1, :].astype(f32)
        got = jnp.sum(wide * key, axis=1, keepdims=True) * scale
        got = jnp.where(step_of >= t, got, -jnp.inf)
        latest.append(got)
        peak = jnp.maximum(peak, got)
    probs = jnp.exp(score - peak)
    total = jnp.sum(probs, axis=1, keepdims=True)
    latest = [jnp.exp(got - peak) for got in latest]
    for got in latest:
        total = total + got
    share = 1.0 / total
    probs = (probs * share).astype(bf16)
    context = lax.dot_general(probs, keys[0, :LAT, :], NT, preferred_element_type=f32)
    for t, got in enumerate(latest):
        part = (got * share).astype(bf16).astype(f32)
        context = context + part * new[0, t : t + 1, :LAT].astype(f32)
    held[pl.ds(pl.multiple_of(seq * count, count), count), :] = context.astype(bf16)

    @pl.when(seq == seqs - 1)
    def _():
        rows = held.shape[0]
        tok = rows // heads
        shape = (rows, rows)
        to, source = iota(shape, 0), iota(shape, 1)
        hop = lax.rem(to // tok, nx)
        head = column(hop, where_ref[0]) * RING + to // (tok * nx)
        take = (lax.rem(to, tok) == source // heads) & (head == lax.rem(source, heads))
        out[...] = jnp.dot(one_hot(take), held[...], preferred_element_type=f32).astype(bf16)


def context_rows(where, nx, cache_kv, new_kv, queries):
    seqs, length, width = cache_kv.shape
    steps, heads = queries.shape[1:3]
    rows = seqs * steps * heads
    keys = jnp.swapaxes(cache_kv, 1, 2)
    return pl.pallas_call(
        functools.partial(context_kernel, nx),
        grid=(seqs,),
        out_shape=jax.ShapeDtypeStruct((rows, LAT), bf16),
        in_specs=[
            smem(),
            pl.BlockSpec((1, width, length), lambda b: (b, 0, 0)),
            pl.BlockSpec((1, steps, heads, width), lambda b: (b, 0, 0, 0)),
            pl.BlockSpec((1, steps, width), lambda b: (b, 0, 0)),
        ],
        out_specs=pl.BlockSpec((rows, LAT), lambda b: (0, 0)),
        scratch_shapes=[pltpu.VMEM((rows, LAT), bf16)],
        compiler_params=params(24),
        cost_estimate=cost(2 * rows * length * (width + LAT), 2 * cache_kv.size),
        name="context_rows",
    )(where, held_in_hbm(keys), held_in_hbm(queries), held_in_hbm(new_kv))


def pack_kernel(up, rows, tops, lows, sem):
    half, at = tops.shape[0], up.shape[1]
    copies = []
    for i, out in enumerate((tops, lows)):
        part = pl.ds(i * half, half)
        copies.append(pltpu.make_async_copy(rows.at[part], out.at[:, pl.ds(at, rows.shape[1])], sem.at[i, 0]))
        copies.append(pltpu.make_async_copy(up.at[part], out.at[:, pl.ds(0, at)], sem.at[i, 1]))
    for copy in copies:
        copy.start()
    for copy in copies:
        copy.wait()


def pack(up, rows):
    shape = (rows.shape[0] // 2, up.shape[1] + rows.shape[1])
    return pl.pallas_call(
        pack_kernel,
        out_shape=(jax.ShapeDtypeStruct(shape, bf16),) * 2,
        in_specs=[hbm()] * 2,
        out_specs=[vmem()] * 2,
        scratch_shapes=[pltpu.SemaphoreType.DMA((2, 2))],
        compiler_params=params(12),
        cost_estimate=cost(1, 4 * rows.size),
        name="pack",
    )(held_in_hbm(up), held_in_hbm(rows))


HALVES = 2
TILE = 256


def put_rows(got, outs, n):
    own, right, left, ahead, behind = outs
    size, width = own.shape[0], ahead.shape[1]
    cols = pl.ds(n * TILE, TILE)
    own[:, cols] = got[:size]
    right[:, cols] = got[size : 2 * size].astype(bf16)
    left[:, cols] = got[2 * size : 3 * size].astype(bf16)
    last, at = (ahead, n * TILE) if n * TILE < width else (behind, n * TILE - width)
    last[:, pl.ds(at, TILE)] = got[3 * size :].astype(bf16)


def row_shapes(size, width):
    return (
        jax.ShapeDtypeStruct((size, width), f32),
        jax.ShapeDtypeStruct((size, width), bf16),
        jax.ShapeDtypeStruct((size, width), bf16),
        jax.ShapeDtypeStruct((size, width // 2), bf16),
        jax.ShapeDtypeStruct((size, width // 2), bf16),
    )


def tiles_of(parts, at, n):
    half = (parts[0].shape[1] - at) // HALVES
    got = [p[:, pl.ds(at + c * half + n * TILE, TILE)] for c in range(HALVES) for p in parts]
    return jnp.concatenate(got, axis=0)


def attend_kernel(tok, nx, count, first, last, where_ref, arrived, *refs):
    pieces, outs = refs[:count], refs[count:]
    if last:
        before, outs = outs[0], outs[1:]
    up = jnp.concatenate([piece[:, pl.ds(0, LAT)] for piece in pieces], axis=0)
    values = lax.dot_general(arrived[...], up, NT, preferred_element_type=f32)
    hop = lax.rem(iota(values.shape, 0) // tok, nx)
    values = jnp.where(hop == first + iota(values.shape, 1) // VH, values, 0.0).astype(bf16)
    shape = (len(STEPS) * FAR * HALVES * tok, arrived.shape[0])
    row, source = iota(shape, 0), iota(shape, 1)
    chip = chip_at(row // (HALVES * tok), where_ref)
    take = (source // (tok * nx) == chip) & (lax.rem(source, tok) == lax.rem(row, tok))
    half = lax.rem(row // tok, HALVES)
    taken = [
        jnp.dot(one_hot(take & (half == c)), values, preferred_element_type=f32).astype(bf16)
        for c in range(HALVES)
    ]
    values = jnp.concatenate(taken, axis=1)
    tiles = outs[0].shape[1] // TILE
    for n in range(tiles):
        got = jnp.dot(of_tile(values, n, tiles), tiles_of(pieces, LAT, n), preferred_element_type=f32)
        cols = pl.ds(n * TILE, TILE)
        if last:
            put_rows(before[:, cols] + got, outs, n)
        else:
            outs[0][:, cols] = got


def attend_part(where, nx, arrived, pieces, tok, first, before):
    depth = sum(p.shape[0] for p in pieces)
    width = (pieces[0].shape[1] - LAT) // HALVES
    count = len(pieces)
    last = before is not None
    part = jax.ShapeDtypeStruct((RING * HALVES * tok, width), f32)
    return pl.pallas_call(
        functools.partial(attend_kernel, tok, nx, count, first, last),
        out_shape=row_shapes(FAR * HALVES * tok, width) if last else part,
        in_specs=[smem(), vmem()] + [vmem()] * count + [vmem()] * last,
        out_specs=[vmem()] * 5 if last else vmem(),
        compiler_params=params(6),
        cost_estimate=cost(8 * RING * tok * depth * width * HALVES, 4 * depth * width),
        name="attend_part",
    )(where, arrived, *pieces, *([before] if last else []))


SEND_TILE = 512


def dispatch_kernel(tok, nx, where_ref, tokens, *refs):
    outs, (early, late) = refs[:nx], refs[nx:]
    count, width = tokens.shape
    half = width - EXTRA
    table = tokens[:, pl.ds(half, EXTRA)]
    shape = (nx * CAP, EXTRA)
    row, place = iota(shape, 0), iota(shape, 1)
    expert = FAR * expert_column(row // CAP, where_ref[0]) + where_ref[1]
    hot = one_hot(place == lax.rem(row, CAP) * EXPERTS + expert)
    got = lax.dot_general(hot, table, NT, preferred_element_type=f32)
    shape = (SLOTS, count)
    slot, token = iota(shape, 0), iota(shape, 1)
    source = slot // CAP
    chip = NEAR * lax.rem(source, FAR) + lax.rem(where_ref[2] + source // FAR + 1, NEAR)
    parts = []
    for r in range(nx):
        sel = jnp.where(lax.rem(slot, CAP) == 0, got[CAP * r : CAP * r + 1], got[CAP * r + 1 : CAP * r + 2])
        parts.append(jnp.where(chip == token // (HALVES * tok), sel, 0.0))
    of_half = lax.rem(token // tok, HALVES)
    halves = [[jnp.where(of_half == c, sel, 0.0) for sel in parts] for c in range(HALVES)]
    both = jnp.concatenate(sum(halves, []), axis=0).astype(bf16)
    rows = nx * SLOTS
    for n in range(half // SEND_TILE):
        got = jnp.dot(both, tokens[:, pl.ds(n * SEND_TILE, SEND_TILE)], preferred_element_type=f32).astype(bf16)
        for c in range(HALVES):
            for r in range(nx):
                at = c * rows + r * SLOTS
                outs[r][:, pl.ds(c * half + n * SEND_TILE, SEND_TILE)] = got[at : at + SLOTS]
    got = jnp.dot(both[:rows], table, preferred_element_type=f32).astype(bf16)
    for r in range(nx):
        outs[r][:, pl.ds(HALVES * half, EXTRA)] = got[r * SLOTS : (r + 1) * SLOTS]
    for out, group, at, end in ((early, 1, 0, EARLY), (late, 0, EARLY, SLOTS)):
        shape = (out.shape[0], count)
        row, token = iota(shape, 0), iota(shape, 1)
        chip = chip_at(group * FAR + row // (HALVES * tok), where_ref)
        take = (token // (HALVES * tok) == chip) & (lax.rem(token, HALVES * tok) == lax.rem(row, HALVES * tok))
        sel = jnp.concatenate([sel[at:end] for sels in halves for sel in sels], axis=0).astype(bf16)
        out[...] = lax.dot_general(one_hot(take), sel, NT, preferred_element_type=f32).astype(bf16)


def dispatch(where, nx, tokens, tok):
    count, width = tokens.shape
    full = HALVES * (width - EXTRA) + EXTRA
    near = count // NEAR
    return pl.pallas_call(
        functools.partial(dispatch_kernel, tok, nx),
        out_shape=(jax.ShapeDtypeStruct((SLOTS, full), bf16),) * nx
        + (
            jax.ShapeDtypeStruct(((len(STEPS) - 1) * near, HALVES * nx * EARLY), bf16),
            jax.ShapeDtypeStruct((near, HALVES * nx * LATE), bf16),
        ),
        in_specs=[smem(), vmem()],
        out_specs=[vmem()] * (nx + 2),
        compiler_params=params(12),
        cost_estimate=cost(2 * nx * SLOTS * count * full, 4 * count * width),
        name="dispatch",
    )(where, tokens)


CHUNKS = 7


def stage_kernel(gate_a, gate_b, up_a, up_b, down_a, down_b, wide, deep, sem):
    part = gate_a.shape[1]
    copies = [
        pltpu.make_async_copy(ref, wide.at[:, pl.ds(i * part, part)], sem.at[i])
        for i, ref in enumerate((gate_a, gate_b, up_a, up_b))
    ]
    copies += [
        pltpu.make_async_copy(ref, deep.at[pl.ds(i * part, part)], sem.at[4 + i])
        for i, ref in enumerate((down_a, down_b))
    ]
    for copy in copies:
        copy.start()
    for copy in copies:
        copy.wait()


def stage(weights):
    dim, part = weights[0].shape
    return pl.pallas_call(
        stage_kernel,
        out_shape=(
            jax.ShapeDtypeStruct((dim, 4 * part), bf16),
            jax.ShapeDtypeStruct((2 * part, dim), bf16),
        ),
        in_specs=[hbm()] * 6,
        out_specs=[vmem()] * 2,
        scratch_shapes=[pltpu.SemaphoreType.DMA((6,))],
        compiler_params=params(4),
        cost_estimate=cost(4 * 1000 * dim * part, 12 * dim * part),
        name="stage",
    )(*[held_in_hbm(w) for w in weights])


def expert_kernel(groups, where_ref, *refs):
    tokens = refs[:groups]
    wide, deep = refs[groups : groups + 2]
    early, late = refs[groups + 2 : 2 * groups + 2], refs[2 * groups + 2 : 3 * groups + 2]
    held = refs[3 * groups + 2] if groups > 1 else tokens[0]
    dim = wide.shape[0]
    part = wide.shape[1] // 2
    chunk = dim // CHUNKS
    if groups > 1:
        for g, ref in enumerate(tokens):
            held[pl.ds(g * SLOTS, SLOTS)] = ref[...]
    total = jnp.dot(held[:, pl.ds(0, dim)], wide[...], preferred_element_type=f32)
    gate, upward = total[:, :part], total[:, part:]
    act = (gate / (1.0 + jnp.exp(-gate)) * upward).astype(bf16)
    shape = (EXTRA, EXTRA)
    expert = FAR * where_ref[0] + where_ref[1]
    from_share = iota(shape, 0) - CAP * EXPERTS
    hot = (from_share >= 0) & (from_share < 3 * EXPERTS) & (lax.rem(from_share + EXTRA, EXPERTS) == expert)
    share = jnp.dot(held[:, pl.ds(dim, EXTRA)], one_hot(hot), preferred_element_type=f32)[:, :1]
    for k in range(CHUNKS):
        cols = pl.ds(k * chunk, chunk)
        got = jnp.dot(act, deep[:, cols], preferred_element_type=f32) * share
        for g in range(groups):
            rows = got[g * SLOTS : (g + 1) * SLOTS].astype(bf16)
            early[g][:, cols] = rows[:EARLY]
            late[g][:, cols] = rows[EARLY:]


def expert_part(where, tokens, weights):
    wide, deep = weights
    dim = wide.shape[0]
    groups = len(tokens)
    rows = groups * SLOTS
    held = [pltpu.VMEM((rows, dim + EXTRA), bf16)] if groups > 1 else []
    return pl.pallas_call(
        functools.partial(expert_kernel, groups),
        out_shape=(jax.ShapeDtypeStruct((EARLY, dim), bf16),) * groups
        + (jax.ShapeDtypeStruct((LATE, dim), bf16),) * groups,
        in_specs=[smem()] + [vmem()] * (groups + 2),
        out_specs=[vmem()] * (2 * groups),
        scratch_shapes=held,
        compiler_params=params(8),
        cost_estimate=cost(6 * rows * wide.size, 2 * rows * dim),
        name="expert_part",
    )(where, *tokens, held_in_vmem(wide), held_in_vmem(deep))


def collect_kernel(count, spread, *refs):
    parts, (right, left, ahead, behind) = refs[:count], refs[count:]
    size = right.shape[0]
    tiles = right.shape[1] // TILE
    for n in range(tiles):
        cols = pl.ds(n * TILE, TILE)
        rows = spread[...]
        first = n < tiles // 2
        rows = rows[: 3 * size] if first else jnp.concatenate([rows[: 2 * size], rows[3 * size :]], axis=0)
        got = jnp.dot(rows, tiles_of(parts, 0, n), preferred_element_type=f32).astype(bf16)
        right[:, cols] = got[:size]
        left[:, cols] = got[size : 2 * size]
        last, at = (ahead, n * TILE) if first else (behind, (n - tiles // 2) * TILE)
        last[:, pl.ds(at, TILE)] = got[2 * size :]


def collect(spread, parts):
    width = parts[0].shape[1] // HALVES
    count = len(parts)
    return pl.pallas_call(
        functools.partial(collect_kernel, count),
        out_shape=row_shapes(spread.shape[0] // (len(STEPS) - 1), width)[1:],
        in_specs=[vmem()] * (count + 1),
        out_specs=[vmem()] * 4,
        compiler_params=params(12),
        cost_estimate=cost(2 * spread.size * width, 4 * spread.shape[0] * width),
        name="collect",
    )(spread, *parts)


def merge_kernel(count, *refs):
    mine, (right, left, ahead, behind, first), rest = refs[:count], refs[count : count + 5], refs[count + 5 :]
    block = first.shape[0]
    tiles = first.shape[1] // TILE
    for n in range(tiles):
        cols = pl.ds(n * TILE, TILE)
        if count == 1:
            total = mine[0][:, cols]
        else:
            total = jnp.dot(mine[0][...], tiles_of(mine[1:], 0, n), preferred_element_type=f32)
        last, at = (ahead, n * TILE) if n < tiles // 2 else (behind, (n - tiles // 2) * TILE)
        total = total + right[:, cols].astype(f32) + left[:, cols].astype(f32)
        total = total + last[:, pl.ds(at, TILE)].astype(f32)
        first[:, cols] = total[:block]
        for k, out in enumerate(rest):
            out[:, cols] = total[(k + 1) * block : (k + 2) * block].astype(bf16)


def merge(mine, others):
    size, width = others[0].shape
    block = (size // FAR, width)
    return pl.pallas_call(
        functools.partial(merge_kernel, len(mine)),
        out_shape=(jax.ShapeDtypeStruct(block, f32),) + (jax.ShapeDtypeStruct(block, bf16),) * (FAR - 1),
        in_specs=[vmem()] * (len(mine) + 4),
        out_specs=[vmem()] * FAR,
        compiler_params=params(4),
        cost_estimate=cost(4 * size * width, 12 * size * width),
        name="merge",
    )(*mine, *others)


def half_swap(a):
    middle = a.shape[0] // 2
    return jnp.concatenate([a[middle:], a[:middle]], axis=0)


def route_kernel(first, one, two, three, rows, gain, router, ids, slots, hidden, payload):
    count, half = rows.shape
    total = first[...] + one[...].astype(f32) + two[...].astype(f32) + three[...].astype(f32)
    total = rows[...].astype(f32) + total
    hidden[...] = total
    square = jnp.sum(total * total, axis=1, keepdims=True)
    scale = lax.rsqrt((square + half_swap(square)) / D + norm_eps)
    normed = (total * scale * gain[...]).astype(bf16)
    payload[:, pl.ds(0, half)] = normed
    parts = [
        lax.dot_general(normed, router[:, pl.ds(c * half, half)], NT, preferred_element_type=f32)
        for c in range(HALVES)
    ]
    logits = jnp.where(iota(parts[0].shape, 0) < count // 2, parts[0], parts[1])
    logits = logits + half_swap(logits)
    logits = jnp.concatenate([logits] * (EXTRA // EXPERTS), axis=1)
    lane = iota(logits.shape, 1)
    place = jnp.zeros(logits.shape, jnp.int32)
    for k in range(TOP):
        place = jnp.where(lax.rem(lane, EXPERTS) == ids[:, k : k + 1], slots[:, k : k + 1] + 1, place)
    gates = jnp.where(place > 0, 1.0 / (1.0 + jnp.exp(-logits)), 0.0)
    share = route_scale * gates / jnp.sum(jnp.where(lane < EXPERTS, gates, 0.0), axis=1, keepdims=True)
    kind = lane // EXPERTS
    table = jnp.zeros(logits.shape, f32)
    for n in range(CAP):
        table = jnp.where((kind == n) & (place == n + 1), 1.0, table)
    rest = share
    for n in range(3):
        piece = rest.astype(bf16).astype(f32)
        table = jnp.where(kind == CAP + n, piece, table)
        rest = rest - piece
    payload[:, pl.ds(half, EXTRA)] = table.astype(bf16)


def route(added, rows, gain, router, ids, slots):
    count, half = rows.shape
    return pl.pallas_call(
        route_kernel,
        out_shape=(
            jax.ShapeDtypeStruct((count, half), f32),
            jax.ShapeDtypeStruct((count, half + EXTRA), bf16),
        ),
        in_specs=[vmem()] * 9,
        out_specs=[vmem()] * 2,
        compiler_params=params(4),
        cost_estimate=cost(4 * count * half * EXPERTS, 20 * count * half),
        name="route",
    )(*added, rows, gain, router, ids, slots)


def finish_kernel(hidden, first, one, two, three, out):
    seqs, steps, _ = out.shape
    half = hidden.shape[1]
    total = first[...] + one[...].astype(f32) + two[...].astype(f32) + three[...].astype(f32)
    total = (hidden[...] + total).astype(bf16)
    for c in range(HALVES):
        for b in range(seqs):
            at = (c * seqs + b) * steps
            out[b, :, pl.ds(c * half, half)] = total[at : at + steps]


def finish(hidden, added, shape):
    return pl.pallas_call(
        finish_kernel,
        out_shape=jax.ShapeDtypeStruct(shape, bf16),
        in_specs=[vmem()] * 5,
        out_specs=vmem(),
        compiler_params=params(4),
        cost_estimate=cost(5 * hidden.size, 14 * hidden.size),
        name="finish",
    )(hidden, *added)


def reduce_z(mine, right, left, ahead, behind):
    others = shift_z(right, 1), shift_z(left, -1), shift_z(ahead, 2), shift_z(behind, -2)
    first, *sent = merge(mine, others)
    others = [swap_far(rows, k + 1) for k, rows in enumerate(sent)]
    return first, *others


def layer(
    cache_kv,
    new_kv,
    queries,
    lengths,
    resid,
    value_up,
    out_proj,
    norm_gain,
    router,
    expert_ids,
    slots,
    w_gate,
    w_up,
    w_down,
):
    nx = lax.axis_size("x")
    seqs, steps = queries.shape[:2]
    tok = seqs * steps
    where = jnp.stack([lax.axis_index(a) for a in ("x", "zb", "j")]).astype(jnp.int32)
    where = jnp.concatenate([where, lengths.astype(jnp.int32)])

    tops, lows = pack(value_up.T, out_proj)
    top_left = swap_x(tops, 1)
    low_right = swap_x(lows, 3)
    low_left = swap_x(lows, 1)
    top_right = swap_x(tops, 3)

    outgoing = context_rows(where, nx, cache_kv, new_kv, queries)
    arrived = lax.all_to_all(
        outgoing.reshape(RING, nx * tok, LAT), ZAX, split_axis=0, concat_axis=0, tiled=True
    )
    top_far = swap_x(top_left, 3)
    low_far = swap_x(low_right, 1)
    near = [tops, lows, swap_core(tops), swap_core(lows)]
    for pair in ((top_left, low_left), (top_right, low_right)):
        near += [*pair, *map(swap_core, pair)]
    beyond = [top_far, low_far, swap_core(top_far), swap_core(low_far)]
    others = [swap_core(w) for w in (w_gate, w_up, w_down)]
    weights = stage((w_gate, others[0], w_up, others[1], w_down, others[2]))
    arrived = arrived.reshape(RING * nx * tok, LAT)
    most = attend_part(where, nx, arrived, near, tok, 0, None)
    own, *rows = attend_part(where, nx, arrived, beyond, tok, nx - 1, most)
    added = reduce_z((own,), *rows)

    half = D // HALVES
    rows = resid.reshape(tok, HALVES, half).swapaxes(0, 1).reshape(HALVES * tok, half)
    gain = jnp.repeat(norm_gain.astype(f32).reshape(HALVES, half), tok, axis=0)
    ids, places = [
        jnp.tile(a.reshape(tok, TOP).astype(jnp.int32), (HALVES, 1)) for a in (expert_ids, slots)
    ]
    hidden, payload = route(added, rows, gain, router.T, ids, places)

    ring = lax.all_gather(payload, ZAX, axis=0, tiled=True)
    *sent, early, late = dispatch(where, nx, ring, tok)
    far = swap_x(sent[1], EXPERT_COLUMNS[1])
    near = [swap_x(sent[i], EXPERT_COLUMNS[i]) for i in range(2, nx)]
    done = [[], []]
    for groups in ((sent[0], far), tuple(near)):
        rows = expert_part(where, groups, weights)
        done[0] += rows[: len(groups)]
        done[1] += rows[len(groups) :]
    first = [done[0][0], swap_x(done[0][1], EXPERT_COLUMNS[1])]
    first += [swap_x(done[0][i], EXPERT_COLUMNS[i]) for i in range(2, nx)]
    second = [done[1][0]] + [swap_x(done[1][i], EXPERT_COLUMNS[i]) for i in range(1, nx)]
    added = reduce_z((late, *second), *collect(early, first))
    return finish(hidden, added, resid.shape)


def solution(mesh):
    chips = mesh.shape["ep"] // (RING * CORES)
    grid = mesh.devices.reshape(mesh.shape["rep"], chips, FAR, NEAR, CORES)
    fine = Mesh(grid, ("rep", "x", "zb", "j", "c"))
    ep = ("x", "zb", "j", "c")
    both = ("rep",) + ep
    return jax.shard_map(
        layer,
        mesh=fine,
        in_specs=(
            P(both, None, None),
            P(both, None, None),
            P(both, None, None, None),
            P(both),
            P(both, None, None),
            P(None, ep),
            P(ep, None),
            P(),
            P(),
            P(both, None, None),
            P(both, None, None),
            P(None, ep),
            P(None, ep),
            P(ep, None),
        ),
        out_specs=P(both, None, None),
        check_vma=False,
    )
```
